32 devices in a mesh: dp: 8 (over z, x), mp: 4 (over y, core).
Axes of the slice: x: 2, y: 2, z: 4, core: 2. Of those that a mesh axis runs over, the one named last changes fastest.
Arguments:
- tokens: bfloat16 [8, 196, 1280], P('dp'), may hold values from -6 to 6
- pad_mask: int32 [8, 196], P('dp'), may hold values from 0 to 1, as said below
- cotangent: bfloat16 [8, 196, 1280], P('dp'), may hold values from -6 to 6
- norm_gains: float32 [2, 1280], replicated, may hold values from 0.5 to 1.5
- norm_biases: float32 [2, 1280], replicated, may hold values from -2 to 2
- out_biases: float32 [2, 1280], replicated, may hold values from -2 to 2
- qkv_bias: float32 [3840], P('mp'), may hold values from -2 to 2
- up_bias: float32 [5120], P('mp'), may hold values from -2 to 2
- rel_pos: float32 [2, 27, 80], replicated, may hold values from -0.6 to 0.6
- attn_owner: int32 [4, 64], P('mp'), may hold values from 0 to 63, as said below
- mlp_owner: int32 [4, 128], P('mp'), may hold values from 0 to 127, as said below
- attn_master: float32 [4, 64, 25600], P('mp', 'dp')
- mlp_master: float32 [4, 128, 25600], P('mp', 'dp')
- attn_left: float32 [4, 64, 25600], P('mp', 'dp'), may hold values from -0.5 to 0.5
- attn_right: float32 [4, 64, 25600], P('mp', 'dp'), may hold values from -0.5 to 0.5
- mlp_left: float32 [4, 128, 25600], P('mp', 'dp'), may hold values from -0.5 to 0.5
- mlp_right: float32 [4, 128, 25600], P('mp', 'dp'), may hold values from -0.5 to 0.5
- attn_first: float32 [4, 64, 25600], P('mp', 'dp')
- attn_second: float32 [4, 64, 25600], P('mp', 'dp'), as said below
- mlp_first: float32 [4, 128, 25600], P('mp', 'dp')
- mlp_second: float32 [4, 128, 25600], P('mp', 'dp'), as said below
Outputs:
- block_output: bfloat16 [8, 196, 1280], P('dp')
- tokens_grad: float32 [8, 196, 1280], P('dp')
- gains_grad: float32 [2, 1280], replicated
- biases_grad: float32 [2, 1280], replicated
- out_biases_grad: float32 [2, 1280], replicated
- qkv_bias_grad: float32 [3840], P('mp')
- up_bias_grad: float32 [5120], P('mp')
- rel_pos_grad: float32 [2, 27, 80], replicated
- attn_grad: float32 [4, 64, 25600], P('mp', 'dp')
- mlp_grad: float32 [4, 128, 25600], P('mp', 'dp')
- attn_new: float32 [4, 64, 25600], P('mp', 'dp')
- mlp_new: float32 [4, 128, 25600], P('mp', 'dp')
- attn_copy: bfloat16 [4, 64, 25600], P('mp', 'dp')
- mlp_copy: bfloat16 [4, 128, 25600], P('mp', 'dp')
- attn_first_new: float32 [4, 64, 25600], P('mp', 'dp')
- attn_second_new: float32 [4, 64, 25600], P('mp', 'dp')
- mlp_first_new: float32 [4, 128, 25600], P('mp', 'dp')
- mlp_second_new: float32 [4, 128, 25600], P('mp', 'dp')
The draws below stay inside these ranges and needn't reach their ends.
Inputs may be any that keep to these rules, and one draw needn't show every extreme that they name: `pad_mask`: slot s holds window s mod (25) of image s // 25, windows row-major in a 5 x 5 grid of 14 x 14 tokens, tokens row-major; slots of images from 1 on are all 0; in each image the 1 entries form a 64 x 64 square at an offset of 0 to 6 rows and columns. `attn_owner`: each row is a permutation of 0 to 63. `mlp_owner`: each row is a permutation of 0 to 127. `attn_second`: every entry is positive. `mlp_second`: every entry is positive.
All inputs are finite; a program needn't handle non-finite values.
Results may differ from the reference program's by a relative error of at most 0.017.
Values may be sent and summed in bfloat16 or wider, within the bound.
A program may use at most 192 MiB of HBM per device.

```python
import math
import jax
import jax.numpy as jnp
from jax import lax

D = 1280
HEADS = 16
HD = 80
FF = 5120
WIN = 14
GRID = 5
IMG = 64
BLOCK = 160
WIN_DEV = 1
WIN_TOK = 196
REL = 27
SLOTS = 8
QKV_TILES = 48
ATT_TILES = 64
UP_TILES = 64
MLP_TILES = 128
AREA = 25600
N_DP = 8
N_MP = 4


def tile_order(key, count, salt):
    part_keys = jax.random.split(jax.random.fold_in(key, salt), N_MP)
    return jax.vmap(lambda part_key: jax.random.permutation(part_key, count))(part_keys).astype(jnp.int32)


def tile_noise(key, count, salt):
    shape = (N_MP, count, BLOCK * BLOCK)
    return jax.random.normal(jax.random.fold_in(key, salt), shape, jnp.float32)


def draw_attn_owner(key, part):
    return tile_order(key, ATT_TILES, 101)


def draw_mlp_owner(key, part):
    return tile_order(key, MLP_TILES, 103)


def draw_attn_master(key, part):
    stored = tile_order(key, ATT_TILES, 101)
    scales = jnp.where(stored < QKV_TILES, D ** (-0.5), 8.0 * D ** (-0.5)).astype(jnp.float32)
    return tile_noise(key, ATT_TILES, 202) * scales[:, :, None]


def draw_mlp_master(key, part):
    stored = tile_order(key, MLP_TILES, 103)
    scales = jnp.where(stored < UP_TILES, D ** (-0.5), 1.5 * FF ** (-0.5)).astype(jnp.float32)
    return tile_noise(key, MLP_TILES, 204) * scales[:, :, None]


def grad_level():
    return 0.5 * math.sqrt(WIN_DEV * N_DP * WIN * WIN)


def moment_first(key, count, salt):
    return tile_noise(key, count, salt) * (0.11 * grad_level())


def moment_second(key, count, salt):
    shape = (N_MP, count, BLOCK * BLOCK)
    spread = jax.random.uniform(jax.random.fold_in(key, salt), shape, jnp.float32, -1.2, 1.2)
    return jnp.exp(spread) * (0.053 * grad_level() ** 2)


def draw_attn_first(key, part):
    return moment_first(key, ATT_TILES, 401)


def draw_attn_second(key, part):
    return moment_second(key, ATT_TILES, 402)


def draw_mlp_first(key, part):
    return moment_first(key, MLP_TILES, 403)


def draw_mlp_second(key, part):
    return moment_second(key, MLP_TILES, 404)


def draw_pad_mask(key, part):
    slot_count = WIN_DEV * N_DP
    per_image = GRID * GRID
    image_count = max(1, slot_count // per_image)
    offsets = jax.random.randint(jax.random.fold_in(key, 301), (image_count, 2), 0, GRID * WIN - IMG + 1)
    slot_index = jnp.arange(slot_count, dtype=jnp.int32)
    image_index = slot_index // per_image
    window_index = slot_index % per_image
    token_index = jnp.arange(WIN * WIN, dtype=jnp.int32)
    grid_row = (window_index // GRID)[:, None] * WIN + (token_index // WIN)[None, :]
    grid_col = (window_index % GRID)[:, None] * WIN + (token_index % WIN)[None, :]
    image_clip = jnp.minimum(image_index, image_count - 1)
    offset_row = offsets[image_clip, 0][:, None]
    offset_col = offsets[image_clip, 1][:, None]
    inside = (grid_row >= offset_row) & (grid_row < offset_row + IMG) & (grid_col >= offset_col) & (grid_col < offset_col + IMG)
    inside = inside & (image_index < image_count)[:, None]
    return inside.astype(jnp.int32)


def levels(key, dims, pieces, least, largest):
    loudness = 1.0
    for axis_at, shards_of in pieces:
        heights = jax.random.uniform(jax.random.fold_in(jax.random.fold_in(key, 6), axis_at), (shards_of,), jnp.float32, least / len(pieces), largest / len(pieces))
        loudness = loudness * jnp.repeat(jnp.exp(heights), dims[axis_at] // shards_of).reshape((-1,) + (1,) * (len(dims) - 1 - axis_at))
    return loudness


def gaussian(key, shape, width, bound, cuts=(), kind=jnp.bfloat16):
    array = jax.random.normal(key, shape, jnp.float32) * width
    if len(cuts) > 0:
        array = levels(key, shape, cuts, -0.22, 0.18) * array
    return jnp.clip(array, min=-bound, max=bound).astype(kind)


def setup_inputs(seed: int = 0) -> dict:
    arg_keys = jax.random.split(jax.random.key(seed), 22)
    return {
        "tokens": gaussian(arg_keys[0], (SLOTS, WIN_TOK, D), 1.0, 6.0, ((0, 8),)),
        "pad_mask": draw_pad_mask(jax.random.fold_in(arg_keys[21], 71), 0),
        "cotangent": gaussian(arg_keys[2], (SLOTS, WIN_TOK, D), 1.0, 6.0, ((0, 8),)),
        "norm_gains": jnp.clip(1.0 + 0.1 * jax.random.normal(arg_keys[3], (2, D), jnp.float32), 0.5, 1.5),
        "norm_biases": gaussian(arg_keys[4], (2, D), 0.3, 2.0, (), jnp.float32),
        "out_biases": gaussian(arg_keys[5], (2, D), 0.3, 2.0, (), jnp.float32),
        "qkv_bias": gaussian(arg_keys[6], (3 * D,), 0.3, 2.0, ((0, 4),), jnp.float32),
        "up_bias": gaussian(arg_keys[7], (FF,), 0.3, 2.0, ((0, 4),), jnp.float32),
        "rel_pos": gaussian(arg_keys[8], (2, REL, HD), 0.1, 0.6, (), jnp.float32),
        "attn_owner": draw_attn_owner(jax.random.fold_in(arg_keys[21], 71), 0),
        "mlp_owner": draw_mlp_owner(jax.random.fold_in(arg_keys[21], 71), 0),
        "attn_master": draw_attn_master(jax.random.fold_in(arg_keys[21], 71), 0),
        "mlp_master": draw_mlp_master(jax.random.fold_in(arg_keys[21], 71), 0),
        "attn_left": gaussian(arg_keys[13], (N_MP, ATT_TILES, AREA), BLOCK ** -0.5, 0.5, ((0, 4), (1, 8)), jnp.float32),
        "attn_right": gaussian(arg_keys[14], (N_MP, ATT_TILES, AREA), BLOCK ** -0.5, 0.5, ((0, 4), (1, 8)), jnp.float32),
        "mlp_left": gaussian(arg_keys[15], (N_MP, MLP_TILES, AREA), BLOCK ** -0.5, 0.5, ((0, 4), (1, 8)), jnp.float32),
        "mlp_right": gaussian(arg_keys[16], (N_MP, MLP_TILES, AREA), BLOCK ** -0.5, 0.5, ((0, 4), (1, 8)), jnp.float32),
        "attn_first": draw_attn_first(jax.random.fold_in(arg_keys[21], 71), 0),
        "attn_second": draw_attn_second(jax.random.fold_in(arg_keys[21], 71), 0),
        "mlp_first": draw_mlp_first(jax.random.fold_in(arg_keys[21], 71), 0),
        "mlp_second": draw_mlp_second(jax.random.fold_in(arg_keys[21], 71), 0),
    }


highest = lax.Precision.HIGHEST
norm_eps = 1e-06
beta_one = 0.9
beta_two = 0.95
adam_eps = 1e-08
learn_rate = 0.02

@jax.custom_vjp
def low(v):
    return lax.optimization_barrier(v.astype(jnp.bfloat16)).astype(jnp.float32)

@jax.custom_vjp
def low_back(v):
    return v

def low_keep(v):
    return (low(v), None)

def low_pass(kept, grad):
    return (grad,)

def back_keep(v):
    return (v, None)

def back_low(kept, grad):
    return (low(grad),)
low.defvjp(low_keep, low_pass)
low_back.defvjp(back_keep, back_low)

def layer_norm(values, norm_gain, norm_shift):
    centre = values - lax.optimization_barrier(jnp.mean(values, axis=-1, keepdims=True))
    spread = lax.optimization_barrier(jnp.mean(centre * centre, axis=-1, keepdims=True))
    return centre * lax.rsqrt(spread + norm_eps) * norm_gain + norm_shift

def gelu_exact(values):
    return 0.5 * values * (1.0 + lax.erf(values * 0.5 ** 0.5))

def rel_onehot(win_side):
    positions = jnp.arange(win_side, dtype=jnp.int32)
    offset = positions[:, None] - positions[None, :] + (win_side - 1)
    entries = jnp.arange(2 * win_side - 1, dtype=jnp.int32)
    return (offset[:, :, None] == entries[None, None, :]).astype(jnp.float32)

def rel_table(rel_rows, win_side):
    return jnp.einsum('ijr,rc->ijc', rel_onehot(win_side), rel_rows, precision=highest)

def untile(tile_rows, row_count, col_count, tile_side):
    shaped = tile_rows.reshape(row_count // tile_side, col_count // tile_side, tile_side, tile_side)
    return shaped.transpose(0, 2, 1, 3).reshape(row_count, col_count)

def matrices(attn_tiles, mlp_tiles, attn_owner, mlp_owner):
    tile_side = math.isqrt(attn_tiles.shape[2])
    attn_order = jnp.argsort(attn_owner, axis=1).astype(jnp.int32)
    mlp_order = jnp.argsort(mlp_owner, axis=1).astype(jnp.int32)
    attn_sorted = jnp.take_along_axis(attn_tiles, attn_order[:, :, None], axis=1)
    mlp_sorted = jnp.take_along_axis(mlp_tiles, mlp_order[:, :, None], axis=1)
    head_cols = D // N_MP
    unit_cols = FF // N_MP
    w_qkv = jnp.concatenate([untile(attn_sorted[model_index, :QKV_TILES], D, 3 * head_cols, tile_side) for model_index in range(N_MP)], axis=1)
    w_proj = jnp.concatenate([untile(attn_sorted[model_index, QKV_TILES:], head_cols, D, tile_side) for model_index in range(N_MP)], axis=0)
    w_up = jnp.concatenate([untile(mlp_sorted[model_index, :UP_TILES], D, unit_cols, tile_side) for model_index in range(N_MP)], axis=1)
    w_down = jnp.concatenate([untile(mlp_sorted[model_index, UP_TILES:], unit_cols, D, tile_side) for model_index in range(N_MP)], axis=0)
    return (w_qkv, w_proj, w_up, w_down)

def window_block(weights, group_tokens, group_mask):
    norm_gains, norm_biases, out_biases, qkv_bias, up_bias, rel_pos, w_qkv, w_proj, w_up, w_down = weights
    windows = group_tokens.shape[0]
    row_count = windows * WIN_TOK
    flat_rows = group_tokens.reshape(row_count, D)
    live_rows = group_mask.reshape(row_count, 1).astype(jnp.float32)
    normed = low(layer_norm(flat_rows, norm_gains[0], norm_biases[0]) * live_rows)
    mixed_rows = low(low_back(jnp.dot(normed, w_qkv, precision=highest) + qkv_bias))
    head_parts = mixed_rows.reshape(windows, WIN_TOK, N_MP, 3, HEADS // N_MP, HD)
    queries = head_parts[:, :, :, 0].reshape(windows, WIN_TOK, HEADS, HD)
    key_rows = head_parts[:, :, :, 1].reshape(windows, WIN_TOK, HEADS, HD)
    value_rows = head_parts[:, :, :, 2].reshape(windows, WIN_TOK, HEADS, HD)
    query_grid = queries.reshape(windows, WIN, WIN, HEADS, HD)
    table_h = rel_table(rel_pos[0], WIN)
    table_w = rel_table(rel_pos[1], WIN)
    scores = jnp.einsum('wqhc,wkhc->whqk', queries, key_rows, precision=highest) * HD ** (-0.5)
    along_h = jnp.einsum('wabhc,akc->whabk', query_grid, table_h, precision=highest)
    along_w = jnp.einsum('wabhc,blc->whabl', query_grid, table_w, precision=highest)
    scores = scores + (along_h[..., :, None] + along_w[..., None, :]).reshape(windows, HEADS, WIN_TOK, WIN_TOK)
    scores = low_back(scores)
    probs = low(jax.nn.softmax(scores, axis=-1))
    attended = jnp.einsum('whqk,wkhc->wqhc', probs, value_rows, precision=highest)
    attended = low(low_back(attended.reshape(row_count, N_MP, D // N_MP)))
    partial_attn = low(jnp.einsum('nmc,mcd->nmd', attended, w_proj.reshape(N_MP, D // N_MP, D), precision=highest))
    branch = low_back(lax.optimization_barrier(jnp.sum(partial_attn, axis=1)))
    middle = flat_rows + branch + out_biases[0]
    second = low(layer_norm(middle, norm_gains[1], norm_biases[1]))
    hidden = low_back(jnp.dot(second, w_up, precision=highest) + up_bias)
    active = low(gelu_exact(hidden))
    partial_mlp = low(jnp.einsum('nmf,mfd->nmd', active.reshape(row_count, N_MP, FF // N_MP), w_down.reshape(N_MP, FF // N_MP, D), precision=highest))
    result = (middle + lax.optimization_barrier(jnp.sum(partial_mlp, axis=1)) + out_biases[1]) * live_rows
    return result.reshape(windows, WIN_TOK, D)

def forward(tokens_f, norm_gains, norm_biases, out_biases, qkv_bias, up_bias, rel_pos, attn_master, mlp_master, pad_mask, attn_owner, mlp_owner):
    w_qkv, w_proj, w_up, w_down = matrices(low(attn_master), low(mlp_master), attn_owner, mlp_owner)
    weights = (norm_gains, norm_biases, out_biases, qkv_bias, up_bias, rel_pos, w_qkv, w_proj, w_up, w_down)
    group_tokens = tokens_f.reshape(N_DP, WIN_DEV, WIN_TOK, D)
    group_masks = pad_mask.reshape(N_DP, WIN_DEV, WIN_TOK)
    one_group = jax.checkpoint(lambda window_pair: window_block(weights, window_pair[0], window_pair[1]))
    return lax.map(one_group, (group_tokens, group_masks)).reshape(tokens_f.shape)

def soap_step(grad_tiles, master, left_basis, right_basis, first_moment, second_moment):
    tile_side = math.isqrt(grad_tiles.shape[2])
    square = (grad_tiles.shape[0], grad_tiles.shape[1], tile_side, tile_side)
    left_square = left_basis.reshape(square)
    right_square = right_basis.reshape(square)
    half_turn = jnp.einsum('mtji,mtjk->mtik', left_square, grad_tiles.reshape(square), precision=highest)
    rotated = jnp.einsum('mtik,mtkl->mtil', half_turn, right_square, precision=highest).reshape(grad_tiles.shape)
    first_new = beta_one * first_moment + (1.0 - beta_one) * rotated
    second_new = beta_two * second_moment + (1.0 - beta_two) * rotated * rotated
    direction = (first_new / (jnp.sqrt(second_new) + adam_eps)).reshape(square)
    back_half = jnp.einsum('mtij,mtjk->mtik', left_square, direction, precision=highest)
    update = jnp.einsum('mtik,mtlk->mtil', back_half, right_square, precision=highest).reshape(grad_tiles.shape)
    master_new = master - learn_rate * update
    return (master_new, master_new.astype(jnp.bfloat16), first_new, second_new)

def reference(tokens, pad_mask, cotangent, norm_gains, norm_biases, out_biases, qkv_bias, up_bias, rel_pos, attn_owner, mlp_owner, attn_master, mlp_master, attn_left, attn_right, mlp_left, mlp_right, attn_first, attn_second, mlp_first, mlp_second):
    tokens_f = tokens.astype(jnp.float32)

    def wrapped(tokens_in, gains_in, biases_in, outb_in, qkvb_in, upb_in, relp_in, attn_in, mlp_in):
        return forward(tokens_in, gains_in, biases_in, outb_in, qkvb_in, upb_in, relp_in, attn_in, mlp_in, pad_mask, attn_owner, mlp_owner)
    block_out, pullback = jax.vjp(wrapped, tokens_f, norm_gains, norm_biases, out_biases, qkv_bias, up_bias, rel_pos, attn_master, mlp_master)
    tokens_grad, gains_grad, biases_grad, out_grad, qkv_grad, up_grad, rel_grad, attn_grad, mlp_grad = pullback(cotangent.astype(jnp.float32))
    attn_new, attn_copy, attn_first_new, attn_second_new = soap_step(attn_grad, attn_master, attn_left, attn_right, attn_first, attn_second)
    mlp_new, mlp_copy, mlp_first_new, mlp_second_new = soap_step(mlp_grad, mlp_master, mlp_left, mlp_right, mlp_first, mlp_second)
    return (block_out.astype(jnp.bfloat16), tokens_grad, gains_grad, biases_grad, out_grad, qkv_grad, up_grad, rel_grad, attn_grad, mlp_grad, attn_new, mlp_new, attn_copy, mlp_copy, attn_first_new, attn_second_new, mlp_first_new, mlp_second_new)
```

```python
import math

import jax
import jax.numpy as jnp
import numpy as np
from jax import lax
from jax.experimental import pallas as pl
from jax.experimental.pallas import tpu as pltpu
from jax.sharding import PartitionSpec as P

highest = lax.Precision.HIGHEST
norm_eps = 1e-06
beta_one = 0.9
beta_two = 0.95
adam_eps = 1e-08
learn_rate = 0.02


def untile(tile_rows, row_count, col_count, tile_side):
    shaped = tile_rows.reshape(row_count // tile_side, col_count // tile_side, tile_side, tile_side)
    return shaped.transpose(0, 2, 1, 3).reshape(row_count, col_count)


def retile(matrix, tile_side):
    row_count, col_count = matrix.shape
    shaped = matrix.reshape(row_count // tile_side, tile_side, col_count // tile_side, tile_side)
    return shaped.transpose(0, 2, 1, 3).reshape(-1, tile_side * tile_side)


def rel_onehot(win_side):
    positions = jnp.arange(win_side, dtype=jnp.int32)
    offset = positions[:, None] - positions[None, :] + (win_side - 1)
    entries = jnp.arange(2 * win_side - 1, dtype=jnp.int32)
    return (offset[:, :, None] == entries[None, None, :]).astype(jnp.float32)


def norm_forward(values, norm_gain, norm_shift):
    centre = values - jnp.mean(values, axis=-1, keepdims=True)
    inverse = lax.rsqrt(jnp.mean(centre * centre, axis=-1, keepdims=True) + norm_eps)
    unit_rows = centre * inverse
    return (unit_rows * norm_gain + norm_shift, unit_rows, inverse)


def norm_backward(grad_in, unit_rows, inverse, norm_gain):
    grad_unit = grad_in * norm_gain
    centred = grad_unit - jnp.mean(grad_unit, axis=-1, keepdims=True)
    return inverse * (centred - unit_rows * jnp.mean(grad_unit * unit_rows, axis=-1, keepdims=True))


def gelu_pair(values):
    normal_cdf = 0.5 * (1.0 + lax.erf(values * 0.5**0.5))
    density = jnp.exp(-0.5 * values * values) * (2.0 * math.pi) ** (-0.5)
    return (values * normal_cdf, normal_cdf + values * density)


def soap_step(grad_tiles, master, left_basis, right_basis, first_moment, second_moment):
    tile_side = math.isqrt(grad_tiles.shape[2])
    square = (grad_tiles.shape[0], grad_tiles.shape[1], tile_side, tile_side)
    left_square = left_basis.reshape(square)
    right_square = right_basis.reshape(square)
    half_turn = jnp.einsum(
        "mtji,mtjk->mtik", left_square, grad_tiles.reshape(square), precision=highest
    )
    rotated = jnp.einsum("mtik,mtkl->mtil", half_turn, right_square, precision=highest).reshape(
        grad_tiles.shape
    )
    first_new = beta_one * first_moment + (1.0 - beta_one) * rotated
    second_new = beta_two * second_moment + (1.0 - beta_two) * rotated * rotated
    direction = (first_new / (jnp.sqrt(second_new) + adam_eps)).reshape(square)
    back_half = jnp.einsum("mtij,mtjk->mtik", left_square, direction, precision=highest)
    update = jnp.einsum("mtik,mtlk->mtil", back_half, right_square, precision=highest).reshape(
        grad_tiles.shape
    )
    master_new = master - learn_rate * update
    return (master_new, master_new.astype(jnp.bfloat16), first_new, second_new)


def local(
    tokens,
    pad_mask,
    cotangent,
    norm_gains,
    norm_biases,
    out_biases,
    qkv_bias,
    up_bias,
    rel_pos,
    attn_owner,
    mlp_owner,
    attn_master,
    mlp_master,
    attn_left,
    attn_right,
    mlp_left,
    mlp_right,
    attn_first,
    attn_second,
    mlp_first,
    mlp_second,
):
    windows, win_tokens, model_width = tokens.shape
    row_count = windows * win_tokens
    qkv_cols = qkv_bias.shape[0]
    head_cols = qkv_cols // 3
    unit_cols = up_bias.shape[0]
    head_dim = rel_pos.shape[2]
    heads_here = head_cols // head_dim
    win_side = (rel_pos.shape[1] + 1) // 2
    tile_side = math.isqrt(attn_master.shape[2])
    qkv_count = model_width // tile_side * (qkv_cols // tile_side)
    up_count = model_width // tile_side * (unit_cols // tile_side)
    score_scale = head_dim ** (-0.5)
    attn_stored, mlp_stored = (
        lax.all_gather(attn_master.astype(jnp.bfloat16), "dp", axis=1, tiled=True),
        lax.all_gather(mlp_master.astype(jnp.bfloat16), "dp", axis=1, tiled=True),
    )
    attn_order = jnp.argsort(attn_owner[0])
    mlp_order = jnp.argsort(mlp_owner[0])
    attn_sorted = attn_stored[0][attn_order]
    mlp_sorted = mlp_stored[0][mlp_order]
    w_qkv = untile(attn_sorted[:qkv_count], model_width, qkv_cols, tile_side)
    w_proj = untile(attn_sorted[qkv_count:], head_cols, model_width, tile_side)
    w_up = untile(mlp_sorted[:up_count], model_width, unit_cols, tile_side)
    w_down = untile(mlp_sorted[up_count:], unit_cols, model_width, tile_side)
    onehot = rel_onehot(win_side)
    table_h = jnp.einsum("ijr,rc->ijc", onehot, rel_pos[0], precision=highest)
    table_w = jnp.einsum("ijr,rc->ijc", onehot, rel_pos[1], precision=highest)
    flat_rows = tokens.reshape(row_count, model_width).astype(jnp.float32)
    live_rows = pad_mask.reshape(row_count, 1).astype(jnp.float32)
    normed, unit_one, inverse_one = norm_forward(flat_rows, norm_gains[0], norm_biases[0])
    normed_low = (normed * live_rows).astype(jnp.bfloat16)
    mixed_rows = (jnp.dot(normed_low, w_qkv, preferred_element_type=jnp.float32) + qkv_bias).astype(
        jnp.bfloat16
    )
    head_parts = mixed_rows.reshape(windows, win_tokens, 3, heads_here, head_dim)
    queries = head_parts[:, :, 0]
    key_rows = head_parts[:, :, 1]
    value_rows = head_parts[:, :, 2]
    query_grid = queries.astype(jnp.float32).reshape(
        windows, win_side, win_side, heads_here, head_dim
    )

    def score_rows():
        direct = (
            jnp.einsum("wqhc,wkhc->whqk", queries, key_rows, preferred_element_type=jnp.float32)
            * score_scale
        )
        along_h = jnp.einsum("wabhc,akc->whabk", query_grid, table_h, precision=highest)
        along_w = jnp.einsum("wabhc,blc->whabl", query_grid, table_w, precision=highest)
        return direct + (along_h[..., :, None] + along_w[..., None, :]).reshape(
            windows, heads_here, win_tokens, win_tokens
        )

    scores = score_rows()
    row_top = jnp.max(scores, axis=-1, keepdims=True)
    exponent = jnp.exp(scores - row_top)
    row_total = jnp.sum(exponent, axis=-1, keepdims=True)
    log_total = row_top + jnp.log(row_total)
    probs_low = (exponent / row_total).astype(jnp.bfloat16)
    attended = jnp.einsum(
        "whqk,wkhc->wqhc", probs_low, value_rows, preferred_element_type=jnp.float32
    )
    attended_low = attended.reshape(row_count, head_cols).astype(jnp.bfloat16)
    branch = lax.psum(
        jnp.dot(attended_low, w_proj, preferred_element_type=jnp.float32).astype(jnp.bfloat16), "mp"
    ).astype(jnp.float32)
    middle = flat_rows + branch + out_biases[0]
    second, unit_two, inverse_two = norm_forward(middle, norm_gains[1], norm_biases[1])
    second_low = second.astype(jnp.bfloat16)
    hidden = jnp.dot(second_low, w_up, preferred_element_type=jnp.float32) + up_bias
    active, gelu_slope = gelu_pair(hidden)
    active_low = active.astype(jnp.bfloat16)
    down_sum = lax.psum(
        jnp.dot(active_low, w_down, preferred_element_type=jnp.float32).astype(jnp.bfloat16), "mp"
    ).astype(jnp.float32)
    block_output = (
        ((middle + down_sum + out_biases[1]) * live_rows)
        .astype(jnp.bfloat16)
        .reshape(windows, win_tokens, model_width)
    )
    grad_out = cotangent.reshape(row_count, model_width).astype(jnp.float32) * live_rows
    grad_out_low = grad_out.astype(jnp.bfloat16)
    down_bias_grad = jnp.sum(grad_out, axis=0)
    w_down_grad = jnp.einsum(
        "nf,nd->fd", active_low, grad_out_low, preferred_element_type=jnp.float32
    )
    grad_active = jnp.einsum("nd,fd->nf", grad_out_low, w_down, preferred_element_type=jnp.float32)
    grad_hidden = (grad_active * gelu_slope).astype(jnp.bfloat16)
    up_bias_grad = jnp.sum(grad_hidden.astype(jnp.float32), axis=0)
    w_up_grad = jnp.einsum("nd,nf->df", second_low, grad_hidden, preferred_element_type=jnp.float32)
    mlp_stack = jnp.concatenate(
        [retile(w_up_grad, tile_side), retile(w_down_grad, tile_side)], axis=0
    )[mlp_owner[0]][None]
    grad_second = lax.psum(
        jnp.einsum("nf,df->nd", grad_hidden, w_up, preferred_element_type=jnp.float32).astype(
            jnp.bfloat16
        ),
        "mp",
    ).astype(jnp.float32)
    gain_two_grad = jnp.sum(grad_second * unit_two, axis=0)
    shift_two_grad = jnp.sum(grad_second, axis=0)
    grad_middle = grad_out + norm_backward(grad_second, unit_two, inverse_two, norm_gains[1])
    proj_bias_grad = jnp.sum(grad_middle, axis=0)
    grad_branch = grad_middle.astype(jnp.bfloat16)
    w_proj_grad = jnp.einsum(
        "nc,nd->cd", attended_low, grad_branch, preferred_element_type=jnp.float32
    )
    grad_attended = jnp.einsum("nd,cd->nc", grad_branch, w_proj, preferred_element_type=jnp.float32)
    grad_attended = grad_attended.astype(jnp.bfloat16).reshape(
        windows, win_tokens, heads_here, head_dim
    )
    probs_full = jnp.exp(score_rows() - log_total)
    probs_again = probs_full.astype(jnp.bfloat16)
    grad_probs = jnp.einsum(
        "wqhc,wkhc->whqk", grad_attended, value_rows, preferred_element_type=jnp.float32
    )
    grad_values = jnp.einsum(
        "whqk,wqhc->wkhc", probs_again, grad_attended, preferred_element_type=jnp.float32
    )
    grad_scores = (
        probs_full * (grad_probs - jnp.sum(probs_full * grad_probs, axis=-1, keepdims=True))
    ).astype(jnp.bfloat16)
    grad_queries = (
        jnp.einsum("whqk,wkhc->wqhc", grad_scores, key_rows, preferred_element_type=jnp.float32)
        * score_scale
    )
    grad_keys = (
        jnp.einsum("whqk,wqhc->wkhc", grad_scores, queries, preferred_element_type=jnp.float32)
        * score_scale
    )
    grad_grid = grad_scores.astype(jnp.float32).reshape(
        windows, heads_here, win_side, win_side, win_side, win_side
    )
    grad_h = jnp.sum(grad_grid, axis=5)
    grad_w = jnp.sum(grad_grid, axis=4)
    grad_rel_q = jnp.einsum("whabk,akc->wabhc", grad_h, table_h, precision=highest) + jnp.einsum(
        "whabl,blc->wabhc", grad_w, table_w, precision=highest
    )
    grad_queries = grad_queries + grad_rel_q.reshape(windows, win_tokens, heads_here, head_dim)
    table_h_grad = jnp.einsum("whabk,wabhc->akc", grad_h, query_grid, precision=highest)
    table_w_grad = jnp.einsum("whabl,wabhc->blc", grad_w, query_grid, precision=highest)
    rel_part = jnp.stack(
        [
            jnp.einsum("ijr,ijc->rc", onehot, table_h_grad, precision=highest),
            jnp.einsum("ijr,ijc->rc", onehot, table_w_grad, precision=highest),
        ]
    )
    grad_mixed = (
        jnp.stack([grad_queries, grad_keys, grad_values], axis=2)
        .reshape(row_count, qkv_cols)
        .astype(jnp.bfloat16)
    )
    qkv_bias_grad = jnp.sum(grad_mixed.astype(jnp.float32), axis=0)
    w_qkv_grad = jnp.einsum("nd,nc->dc", normed_low, grad_mixed, preferred_element_type=jnp.float32)
    grad_normed, rel_sum = (
        lax.psum(
            jnp.einsum("nc,dc->nd", grad_mixed, w_qkv, preferred_element_type=jnp.float32).astype(
                jnp.bfloat16
            ),
            "mp",
        ).astype(jnp.float32),
        lax.psum(rel_part.astype(jnp.bfloat16), "mp").astype(jnp.float32),
    )
    grad_normed = grad_normed * live_rows
    gain_one_grad = jnp.sum(grad_normed * unit_one, axis=0)
    shift_one_grad = jnp.sum(grad_normed, axis=0)
    tokens_grad = (
        grad_middle + norm_backward(grad_normed, unit_one, inverse_one, norm_gains[0])
    ).reshape(windows, win_tokens, model_width)
    attn_stack = jnp.concatenate(
        [retile(w_qkv_grad, tile_side), retile(w_proj_grad, tile_side)], axis=0
    )[attn_owner[0]][None]
    attn_grad, mlp_grad = (
        lax.psum_scatter(attn_stack, "dp", scatter_dimension=1, tiled=True),
        lax.psum_scatter(mlp_stack, "dp", scatter_dimension=1, tiled=True),
    )
    gains_grad, biases_grad, out_biases_grad, rel_pos_grad, qkv_bias_total, up_bias_total = (
        lax.psum(
            (
                jnp.stack([gain_one_grad, gain_two_grad]),
                jnp.stack([shift_one_grad, shift_two_grad]),
                jnp.stack([proj_bias_grad, down_bias_grad]),
                rel_sum,
                qkv_bias_grad,
                up_bias_grad,
            ),
            "dp",
        )
    )
    attn_new, attn_copy, attn_first_new, attn_second_new = soap_step(
        attn_grad, attn_master, attn_left, attn_right, attn_first, attn_second
    )
    mlp_new, mlp_copy, mlp_first_new, mlp_second_new = soap_step(
        mlp_grad, mlp_master, mlp_left, mlp_right, mlp_first, mlp_second
    )
    return (
        block_output,
        tokens_grad,
        gains_grad,
        biases_grad,
        out_biases_grad,
        qkv_bias_total,
        up_bias_total,
        rel_pos_grad,
        attn_grad,
        mlp_grad,
        attn_new,
        mlp_new,
        attn_copy,
        mlp_copy,
        attn_first_new,
        attn_second_new,
        mlp_first_new,
        mlp_second_new,
    )


BF = jnp.bfloat16
F32 = jnp.float32
ROWS = 208
SIDE = 160


def dot(a, b):
    return jnp.dot(a, b, preferred_element_type=F32)


def dot_nt(a, b):
    return lax.dot_general(a, b, (((1,), (1,)), ((), ())), preferred_element_type=F32)


def dot_tn(a, b):
    return lax.dot_general(a, b, (((0,), (0,)), ((), ())), preferred_element_type=F32)


def lane_at(shape):
    return lax.broadcasted_iota(jnp.int32, shape, len(shape) - 1)


def low_parts(value):
    high = value.astype(BF)
    return high, (value - high.astype(F32)).astype(BF)


def flat_to_square(read, square, count):
    lane = lane_at((count, 128))

    def body(group, carry):
        base = pl.multiple_of(group * 640, 128)
        x = [read(base + 128 * k) for k in range(5)]
        r1 = pltpu.roll(x[1], 96, 1)
        r2 = pltpu.roll(x[2], 96, 1)
        h2 = pltpu.roll(x[2], 64, 1)
        h3 = pltpu.roll(x[3], 64, 1)
        r3 = pltpu.roll(x[3], 32, 1)
        r4 = pltpu.roll(x[4], 32, 1)
        pairs = (
            (x[0], x[1]),
            (jnp.where(lane < 96, r1, r2), r2),
            (jnp.where(lane < 64, h2, h3), h3),
            (jnp.where(lane < 32, r3, r4), r4),
        )
        for m, (wide, narrow) in enumerate(pairs):
            square[0, pl.ds(4 * group + m, count, stride=SIDE), :] = wide
            square[1, pl.ds(4 * group + m, count, stride=SIDE), :] = narrow
        return carry

    lax.fori_loop(0, 40, body, 0)


def square_to_flat(square, write, count):
    lane = lane_at((count, 128))

    def body(group, carry):
        base = pl.multiple_of(group * 640, 128)
        a = [square[0, pl.ds(4 * group + m, count, stride=SIDE), :] for m in range(4)]
        b = [square[1, pl.ds(4 * group + m, count, stride=SIDE), :] for m in range(4)]
        a1 = pltpu.roll(a[1], 32, 1)
        b1 = pltpu.roll(b[1], 32, 1)
        a2 = pltpu.roll(a[2], 64, 1)
        b2 = pltpu.roll(b[2], 64, 1)
        a3 = pltpu.roll(a[3], 96, 1)
        b3 = pltpu.roll(b[3], 96, 1)
        write(base, a[0])
        write(base + 128, jnp.where(lane < 32, b[0], a1))
        write(base + 256, jnp.where(lane < 32, a1, jnp.where(lane < 64, b1, a2)))
        write(base + 384, jnp.where(lane < 64, a2, jnp.where(lane < 96, b2, a3)))
        write(base + 512, jnp.where(lane < 96, a3, b3))
        return carry

    lax.fori_loop(0, 40, body, 0)


def pack_body(attn, mlp, wire_attn, wire_mlp, square):
    lane = lane_at((SIDE, 128))
    for source, first, target, slot in ((attn, 0, wire_attn, 0), (mlp, 0, wire_mlp, 0), (mlp, 8, wire_mlp, 2)):
        flat_to_square(lambda at, s=source, f=first: s[f : f + 8, pl.ds(at, 128)], square, 8)
        for half in range(2):
            spare = None
            for q in range(4):
                row = (4 * half + q) * SIDE
                target[5 * (slot + half) + q] = square[0, row : row + SIDE, :].astype(BF)
                piece = square[1, row : row + SIDE, :]
                if q == 0:
                    spare = piece
                else:
                    spare = jnp.where(lane < 32 * q, spare, pltpu.roll(piece, 32 * q, 1))
            target[5 * (slot + half) + 4] = spare.astype(BF)


def unpack_narrow(wire, narrow, groups):
    def body(g, carry):
        last = wire[5 * g + 4]
        for q in range(4):
            narrow[4 * g + q] = last[:, 32 * q : 32 * q + 32]
        return carry

    lax.fori_loop(0, groups, body, 0)


def unpack_sorted(wire, narrow, order, base, outs, rows, cols):
    def body(t, carry):
        row = t // cols
        col = t - row * cols
        stored = order[base + t]
        where_at = pl.multiple_of(row * SIDE, 32)
        outs[col, pl.ds(where_at, SIDE), 0:128] = wire[(stored // 4) * 5 + stored % 4]
        outs[col, pl.ds(where_at, SIDE), 128:160] = narrow[stored]
        return carry

    lax.fori_loop(0, rows * cols, body, 0)


def norm_parts(x):
    mean = jnp.mean(x, axis=-1, keepdims=True)
    centre = x - mean
    inverse = lax.rsqrt(jnp.mean(centre * centre, axis=-1, keepdims=True) + norm_eps)
    return centre * inverse, inverse


def norm_back(grad_in, unit, inverse, gain):
    w = grad_in * gain
    return inverse * (
        w - jnp.mean(w, axis=-1, keepdims=True) - unit * jnp.mean(w * unit, axis=-1, keepdims=True)
    )


def padded(ref, rows, kind=F32):
    value = ref[...].astype(kind)
    return jnp.concatenate([value, jnp.zeros((ROWS - rows, value.shape[1]), kind)], axis=0)


def attn_forward(mixed, rel_hi, rel_lo, pick, spread, probs, att, scale, tokens_here):
    lane = lane_at((ROWS, SIDE))
    key_ok = lane_at((ROWS, ROWS)) < tokens_here
    head = SIDE // 2
    for p in range(2):
        q, k, v = mixed[p], mixed[2 + p], mixed[4 + p]
        parts = []
        for h in range(2):
            mine = (lane >= head) if h else (lane < head)
            qm = jnp.where(mine, q, jnp.zeros_like(q))
            s = dot_nt(qm, k) * scale
            a_hi, a_lo = low_parts(dot_nt(qm, rel_hi[...]) + dot_nt(qm, rel_lo[...]))
            for c in range(7):
                mask = pick[:, 128 * c : 128 * c + 128]
                table = spread[128 * c : 128 * c + 128, :]
                s = s + dot(a_hi * mask, table) + dot(a_lo * mask, table)
            s = jnp.where(key_ok, s, -1e30)
            top = jnp.max(s, axis=-1, keepdims=True)
            e = jnp.exp(s - top)
            pr = e / jnp.sum(e, axis=-1, keepdims=True)
            probs[2 * p + h] = pr
            parts.append(dot(pr.astype(BF), v))
        att[p] = jnp.where(lane < head, parts[0], parts[1]).astype(BF)


def attn_backward(mixed, rel_hi, rel_lo, pick, spread, probs, gatt, gm, rel_out, scale):
    lane = lane_at((ROWS, SIDE))
    head = SIDE // 2
    for p in range(2):
        q, k, v = mixed[p], mixed[2 + p], mixed[4 + p]
        ga = gatt[p]
        dq, dk, dv, dr = [], [], [], []
        for h in range(2):
            mine = (lane >= head) if h else (lane < head)
            pr = probs[2 * p + h]
            gam = jnp.where(mine, ga, jnp.zeros_like(ga))
            gp = dot_nt(gam, v)
            dv.append(dot_tn(pr.astype(BF), ga))
            ds = (pr * (gp - jnp.sum(pr * gp, axis=-1, keepdims=True))).astype(BF)
            da = None
            for c in range(7):
                term = dot_nt(ds, spread[128 * c : 128 * c + 128, :]) * pick[:, 128 * c : 128 * c + 128].astype(F32)
                da = term if da is None else da + term
            da_hi, da_lo = low_parts(da)
            relq = dot(da_hi, rel_hi[...]) + dot(da_lo, rel_hi[...]) + dot(da_hi, rel_lo[...])
            dq.append(dot(ds, k) * scale + relq)
            dk.append(dot_tn(ds, q) * scale)
            dr.append(dot_tn(da_hi, q) + dot_tn(da_lo, q))
        gm[p] = jnp.where(lane < head, dq[0], dq[1]).astype(BF)
        gm[2 + p] = jnp.where(lane < head, dk[0], dk[1]).astype(BF)
        gm[4 + p] = jnp.where(lane < head, dv[0], dv[1]).astype(BF)
        rel = jnp.where(lane_at((128, SIDE)) < head, dr[0], dr[1])
        if p == 0:
            rel_out[...] = rel
        else:
            rel_out[...] += rel


def attn_fwd_body(order, tokens, live, gains, biases, qkv_bias, rel_hi, rel_lo, pick, spread, wire,
                  part, normed, mixed, probs, att, w_qkv, w_proj, narrow, block):
    t = tokens.shape[0]
    x = padded(tokens, t)
    unit, _ = norm_parts(x)
    normed[...] = ((unit * gains[0:1, :] + biases[0:1, :]) * live[...]).astype(BF)
    unpack_narrow(wire, narrow, wire.shape[0] // 5)
    unpack_sorted(wire, narrow, order, 0, w_qkv, 8, 6)
    unpack_sorted(wire, narrow, order, 48, w_proj, 2, 8)

    def mix(j, carry):
        mixed[j] = (dot(normed[...], w_qkv[j]) + qkv_bias[pl.ds(j, 1), :]).astype(BF)
        return carry

    lax.fori_loop(0, 6, mix, 0)
    attn_forward(mixed, rel_hi, rel_lo, pick, spread, probs, att, (SIDE // 2) ** -0.5, t)

    def project(n, carry):
        value = dot(att[0], w_proj[n, 0:SIDE, :]) + dot(att[1], w_proj[n, SIDE : 2 * SIDE, :])
        block[n] = value
        return carry

    lax.fori_loop(0, 8, project, 0)
    for n in range(8):
        part[:, SIDE * n : SIDE * n + SIDE] = block[n][0:t, :].astype(BF)


def mlp_body(order, tokens, live, cotangent, branch, gains, biases, out_biases, up_bias, wire,
             part_down, part_second, sec_blocks, act_blocks, gh, go, bias_sums, w_up, w_down, narrow, block, second):
    t = tokens.shape[0]
    x = padded(tokens, t)
    middle = x + padded(branch, t) + out_biases[0:1, :]
    unit, _ = norm_parts(middle)
    second[...] = (unit * gains[1:2, :] + biases[1:2, :]).astype(BF)
    grad_out = padded(cotangent, t) * live[...]
    for n in range(8):
        sec_blocks[n] = second[:, SIDE * n : SIDE * n + SIDE]
        go[n] = grad_out[:, SIDE * n : SIDE * n + SIDE].astype(BF)
    unpack_narrow(wire, narrow, wire.shape[0] // 5)
    unpack_sorted(wire, narrow, order, 0, w_up, 8, 8)
    unpack_sorted(wire, narrow, order, 64, w_down, 8, 8)

    def hidden_block(j, carry):
        row = pl.multiple_of(j * SIDE, 32)
        hid = dot(second[...], w_up[j]) + up_bias[pl.ds(j, 1), :]
        cdf = 0.5 * (1.0 + lax.erf(hid * 0.5**0.5))
        slope = cdf + hid * (jnp.exp(-0.5 * hid * hid) * (2.0 * math.pi) ** -0.5)
        act_blocks[j] = (hid * cdf).astype(BF)
        ga = dot_nt(go[0], w_down[0, pl.ds(row, SIDE), :])
        for n in range(1, 8):
            ga = ga + dot_nt(go[n], w_down[n, pl.ds(row, SIDE), :])
        low = (ga * slope).astype(BF)
        gh[j] = low
        bias_sums[pl.ds(j, 1), :] = jnp.sum(low.astype(F32), axis=0, keepdims=True)
        return carry

    lax.fori_loop(0, 8, hidden_block, 0)

    def second_back(i, carry):
        row = pl.multiple_of(i * SIDE, 32)
        value = dot_nt(gh[0], w_up[0, pl.ds(row, SIDE), :])
        for j in range(1, 8):
            value = value + dot_nt(gh[j], w_up[j, pl.ds(row, SIDE), :])
        block[i] = value
        return carry

    lax.fori_loop(0, 8, second_back, 0)
    for n in range(8):
        part_second[:, SIDE * n : SIDE * n + SIDE] = block[n][0:t, :].astype(BF)

    def down(n, carry):
        value = dot(act_blocks[0], w_down[n, 0:SIDE, :])
        for j in range(1, 8):
            value = value + dot(act_blocks[j], w_down[n, j * SIDE : (j + 1) * SIDE, :])
        block[n] = value
        return carry

    lax.fori_loop(0, 8, down, 0)
    for n in range(8):
        part_down[:, SIDE * n : SIDE * n + SIDE] = block[n][0:t, :].astype(BF)


def grad_tiles_body(left_at, right_at, count, read_left, read_right, wire):
    lane = lane_at((SIDE, 128))

    def body(g, carry):
        spare = None
        for q in range(4):
            s = 4 * g + q
            tile = dot_tn(read_left(left_at[s]), read_right(right_at[s]))
            wire[5 * g + q] = tile[:, 0:128].astype(BF)
            piece = jnp.concatenate([tile[:, 128:160], jnp.zeros((SIDE, 96), F32)], axis=1)
            spare = piece if q == 0 else jnp.where(lane < 32 * q, spare, pltpu.roll(piece, 32 * q, 1))
        wire[5 * g + 4] = spare.astype(BF)
        return carry

    lax.fori_loop(0, count // 4, body, 0)


def mid_back_body(order, tokens, live, cotangent, branch, down_sum, second_sum, gains, out_biases,
                  wire, mixed, probs, normed, att, rel_hi, rel_lo, pick, spread,
                  block_out, grad_middle_out, part_normed, rel_out, gm, gb, nb, sums, bias_sums,
                  w_qkv, w_proj, narrow, block, gatt):
    t = tokens.shape[0]
    x = padded(tokens, t)
    middle = x + padded(branch, t) + out_biases[0:1, :]
    result = (middle + padded(down_sum, t) + out_biases[1:2, :]) * live[...]
    block_out[...] = result[0:t, :].astype(BF)
    grad_out = padded(cotangent, t) * live[...]
    unit, inverse = norm_parts(middle)
    grad_second = padded(second_sum, t)
    sums[0:1, :] = jnp.sum(grad_second * unit, axis=0, keepdims=True)
    sums[1:2, :] = jnp.sum(grad_second, axis=0, keepdims=True)
    sums[2:3, :] = jnp.sum(grad_out, axis=0, keepdims=True)
    grad_middle = grad_out + norm_back(grad_second, unit, inverse, gains[1:2, :])
    sums[3:4, :] = jnp.sum(grad_middle, axis=0, keepdims=True)
    grad_middle_out[...] = grad_middle[0:t, :]
    for n in range(8):
        gb[n] = grad_middle[:, SIDE * n : SIDE * n + SIDE].astype(BF)
        nb[n] = normed[:, SIDE * n : SIDE * n + SIDE]
    unpack_narrow(wire, narrow, wire.shape[0] // 5)
    unpack_sorted(wire, narrow, order, 0, w_qkv, 8, 6)
    unpack_sorted(wire, narrow, order, 48, w_proj, 2, 8)
    for p in range(2):
        value = dot_nt(gb[0], w_proj[0, p * SIDE : (p + 1) * SIDE, :])
        for n in range(1, 8):
            value = value + dot_nt(gb[n], w_proj[n, p * SIDE : (p + 1) * SIDE, :])
        gatt[p] = value.astype(BF)
    attn_backward(mixed, rel_hi, rel_lo, pick, spread, probs, gatt, gm, rel_out, (SIDE // 2) ** -0.5)
    for j in range(6):
        bias_sums[j : j + 1, :] = jnp.sum(gm[j].astype(F32), axis=0, keepdims=True)

    def normed_back(i, carry):
        row = pl.multiple_of(i * SIDE, 32)
        value = dot_nt(gm[0], w_qkv[0, pl.ds(row, SIDE), :])
        for j in range(1, 6):
            value = value + dot_nt(gm[j], w_qkv[j, pl.ds(row, SIDE), :])
        block[i] = value
        return carry

    lax.fori_loop(0, 8, normed_back, 0)
    for n in range(8):
        part_normed[:, SIDE * n : SIDE * n + SIDE] = block[n][0:t, :].astype(BF)


def token_back_body(tokens, live, normed_sum, grad_middle, gains, tokens_grad, sums):
    x = tokens[...].astype(F32)
    unit, inverse = norm_parts(x)
    grad_normed = normed_sum[...].astype(F32) * live[...]
    sums[0:1, :] = jnp.sum(grad_normed * unit, axis=0, keepdims=True)
    sums[1:2, :] = jnp.sum(grad_normed, axis=0, keepdims=True)
    tokens_grad[...] = grad_middle[...] + norm_back(grad_normed, unit, inverse, gains[0:1, :])


def square_tile(square, t):
    row = pl.multiple_of(t * SIDE, 32)
    return jnp.concatenate([square[0, pl.ds(row, SIDE), :], square[1, pl.ds(row, SIDE), 0:32]], axis=1)


def put_tile(square, t, value):
    row = pl.multiple_of(t * SIDE, 32)
    square[0, pl.ds(row, SIDE), :] = value[:, 0:128]
    square[1, pl.ds(row, SIDE), 0:32] = value[:, 128:160]


def split_dot(kind, a, b):
    a_hi, a_lo = low_parts(a)
    b_hi, b_lo = low_parts(b)
    return kind(a_hi, b_hi) + (kind(a_hi, b_lo) + kind(a_lo, b_hi))


def soap_group(r0, grad_square, master, left, right, first, second,
               grad_out, new_out, copy_out, first_out, second_out, sq_left, sq_right, sq_work):
    rows = slice(r0, r0 + 8)

    def writer(ref):
        def write(at, value):
            ref[rows, pl.ds(at, 128)] = value
        return write

    flat_to_square(lambda at: left[rows, pl.ds(at, 128)], sq_left, 8)
    flat_to_square(lambda at: right[rows, pl.ds(at, 128)], sq_right, 8)
    square_to_flat(grad_square, writer(grad_out), 8)

    def rotate(t, carry):
        l, r = square_tile(sq_left, t), square_tile(sq_right, t)
        half = split_dot(dot_tn, l, square_tile(grad_square, t))
        put_tile(sq_work, t, split_dot(dot, half, r))
        return carry

    lax.fori_loop(0, 8, rotate, 0)

    def moments(at, rotated):
        cols = pl.ds(at, 128)
        f = beta_one * first[rows, cols] + (1.0 - beta_one) * rotated
        s = beta_two * second[rows, cols] + (1.0 - beta_two) * rotated * rotated
        first_out[rows, cols] = f
        second_out[rows, cols] = s
        new_out[rows, cols] = f / (jnp.sqrt(s) + adam_eps)

    square_to_flat(sq_work, moments, 8)
    flat_to_square(lambda at: new_out[rows, pl.ds(at, 128)], sq_work, 8)

    def turn_back(t, carry):
        l, r = square_tile(sq_left, t), square_tile(sq_right, t)
        half = split_dot(dot, l, square_tile(sq_work, t))
        put_tile(sq_work, t, split_dot(dot_nt, half, r))
        return carry

    lax.fori_loop(0, 8, turn_back, 0)

    def finish(at, update):
        cols = pl.ds(at, 128)
        value = master[rows, cols] - learn_rate * update
        new_out[rows, cols] = value
        copy_out[rows, cols] = value.astype(BF)

    square_to_flat(sq_work, finish, 8)


def soap_body(wire, master, left, right, first, second,
              grad_out, new_out, copy_out, first_out, second_out, sq_grad, sq_left, sq_right, sq_work):
    for r in range(master.shape[0] // 8):
        for half in range(2):
            last = wire[5 * (2 * r + half) + 4].astype(F32)
            for q in range(4):
                row = (4 * half + q) * SIDE
                sq_grad[0, row : row + SIDE, :] = wire[5 * (2 * r + half) + q].astype(F32)
                sq_grad[1, row : row + SIDE, :] = last if q == 0 else pltpu.roll(last, 128 - 32 * q, 1)
        soap_group(8 * r, sq_grad, master, left, right, first, second,
                   grad_out, new_out, copy_out, first_out, second_out, sq_left, sq_right, sq_work)


def build(mesh):
    placed = (
        P("dp", None, None),
        P("dp", None),
        P("dp", None, None),
        P(),
        P(),
        P(),
        P("mp"),
        P("mp"),
        P(),
        P("mp", None),
        P("mp", None),
        P("mp", "dp", None),
        P("mp", "dp", None),
        P("mp", "dp", None),
        P("mp", "dp", None),
        P("mp", "dp", None),
        P("mp", "dp", None),
        P("mp", "dp", None),
        P("mp", "dp", None),
        P("mp", "dp", None),
        P("mp", "dp", None),
    )
    return jax.shard_map(
        fast_local if dict(mesh.shape) == {"dp": 8, "mp": 4} else local,
        mesh=mesh,
        in_specs=placed,
        out_specs=(
            P("dp", None, None),
            P("dp", None, None),
            P(),
            P(),
            P(),
            P("mp"),
            P("mp"),
            P(),
            P("mp", "dp", None),
            P("mp", "dp", None),
            P("mp", "dp", None),
            P("mp", "dp", None),
            P("mp", "dp", None),
            P("mp", "dp", None),
            P("mp", "dp", None),
            P("mp", "dp", None),
            P("mp", "dp", None),
            P("mp", "dp", None),
        ),
        check_vma=False,
    )


VM = pl.BlockSpec(memory_space=pltpu.VMEM)
SM = pl.BlockSpec(memory_space=pltpu.SMEM)
LIMIT = 60 * 1024 * 1024


def call(body, tables, args, outs, scratch, name):
    return pl.pallas_call(
        body,
        out_shape=[jax.ShapeDtypeStruct(shape, kind) for shape, kind in outs],
        in_specs=[SM] * len(tables) + [VM] * len(args),
        out_specs=[VM] * len(outs),
        scratch_shapes=[pltpu.VMEM(shape, kind) for shape, kind in scratch],
        compiler_params=pltpu.CompilerParams(vmem_limit_bytes=LIMIT),
        name=name,
    )(*tables, *args)


def rel_constants(side):
    rows = np.arange(ROWS)
    lanes = np.arange(896)
    within, along = lanes % 64, lanes // 64
    high = np.where(rows < side * side, rows // side, -1)[:, None]
    wide = np.where(rows < side * side, rows % side, -1)[:, None]
    pick = np.where(within[None] < 32, high == along[None], wide == along[None])
    keys = np.arange(ROWS)
    key_h, key_w = keys // side, keys % side
    offset = np.where(within[:, None] < 32, along[:, None] - key_h[None], along[:, None] - key_w[None]) + side - 1
    spread = (offset == (within % 32)[:, None]) & (keys < side * side)[None]
    return jnp.asarray(pick, BF), jnp.asarray(spread, BF)


def inverse_order(owner):
    count = owner.shape[0]
    at = jnp.arange(count, dtype=jnp.int32)
    return jnp.sum(jnp.where(owner[:, None] == at[None, :], at[:, None], 0), axis=0)


def fast_local(
    tokens, pad_mask, cotangent, norm_gains, norm_biases, out_biases, qkv_bias, up_bias, rel_pos,
    attn_owner, mlp_owner, attn_master, mlp_master, attn_left, attn_right, mlp_left, mlp_right,
    attn_first, attn_second, mlp_first, mlp_second,
):
    t, width = tokens.shape[1:]
    tok, cot = tokens[0], cotangent[0]
    live = jnp.pad(pad_mask[0].astype(F32), (0, ROWS - t))[:, None]
    qb, ub = qkv_bias.reshape(6, SIDE), up_bias.reshape(8, SIDE)
    rel = jnp.pad(rel_pos, ((0, 0), (0, 32 - rel_pos.shape[1]), (0, 0))).reshape(64, SIDE // 2)
    rel_hi, rel_lo = low_parts(jnp.tile(rel, (2, 2)))
    pick, spread = rel_constants((rel_pos.shape[1] + 1) // 2)
    own_a, own_m = attn_owner[0], mlp_owner[0]
    ord_a, ord_m = inverse_order(own_a), inverse_order(own_m)
    xa = jnp.where(own_a < 48, own_a // 6, 8 + (own_a - 48) // 8)
    ya = jnp.where(own_a < 48, own_a % 6, 6 + (own_a - 48) % 8)
    xm, ym = own_m // 8, (own_m // 64) * 8 + own_m % 8

    wire_a, wire_m = call(
        pack_body, (), (attn_master[0], mlp_master[0]),
        [((10, SIDE, 128), BF), ((20, SIDE, 128), BF)], [((2, 8 * SIDE, 128), F32)], "pack")
    all_a = lax.all_gather(wire_a, "dp", axis=0, tiled=True)
    all_m = lax.all_gather(wire_m, "dp", axis=0, tiled=True)

    part, normed, mixed, probs, att = call(
        attn_fwd_body, (ord_a,),
        (tok, live, norm_gains, norm_biases, qb, rel_hi, rel_lo, pick, spread, all_a),
        [((t, width), BF), ((ROWS, width), BF), ((6, ROWS, SIDE), BF), ((4, ROWS, ROWS), F32), ((2, ROWS, SIDE), BF)],
        [((6, 8 * SIDE, SIDE), BF), ((8, 2 * SIDE, SIDE), BF), ((64, SIDE, 32), BF), ((8, ROWS, SIDE), F32)],
        "attn_fwd")
    branch = lax.psum(part, "mp")
    part_down, part_second, sec_blocks, act_blocks, gh, go, up_sums = call(
        mlp_body, (ord_m,),
        (tok, live, cot, branch, norm_gains, norm_biases, out_biases, ub, all_m),
        [((t, width), BF), ((t, width), BF)] + [((8, ROWS, SIDE), BF)] * 4 + [((8, SIDE), F32)],
        [((8, 8 * SIDE, SIDE), BF), ((8, 8 * SIDE, SIDE), BF), ((128, SIDE, 32), BF), ((8, ROWS, SIDE), F32), ((ROWS, width), BF)],
        "mlp")
    second_sum = lax.psum(part_second, "mp")
    down_sum = lax.psum(part_down, "mp")

    def mlp_tiles(left_at, right_at, sec, act, gh_ref, go_ref, wire, lefts, rights):
        lefts[0:8], lefts[8:16] = sec[...], act[...]
        rights[0:8], rights[8:16] = gh_ref[...], go_ref[...]
        grad_tiles_body(left_at, right_at, 128, lambda i: lefts[i], lambda i: rights[i], wire)

    stack_m, = call(
        mlp_tiles, (xm, ym), (sec_blocks, act_blocks, gh, go), [((160, SIDE, 128), BF)],
        [((16, ROWS, SIDE), BF)] * 2, "mlp_tiles")
    sum_m = lax.psum_scatter(stack_m, "dp", scatter_dimension=0, tiled=True)

    block_out, grad_middle, part_normed, rel_part, gm, gb, nb, sums_two, qkv_sums = call(
        mid_back_body, (ord_a,),
        (tok, live, cot, branch, down_sum, second_sum, norm_gains, out_biases, all_a, mixed, probs, normed, att,
         rel_hi, rel_lo, pick, spread),
        [((t, width), BF), ((t, width), F32), ((t, width), BF), ((128, SIDE), F32), ((6, ROWS, SIDE), BF),
         ((8, ROWS, SIDE), BF), ((8, ROWS, SIDE), BF), ((4, width), F32), ((6, SIDE), F32)],
        [((6, 8 * SIDE, SIDE), BF), ((8, 2 * SIDE, SIDE), BF), ((64, SIDE, 32), BF), ((8, ROWS, SIDE), F32),
         ((2, ROWS, SIDE), BF)],
        "mid_back")
    rel_half = SIDE // 2
    rel_fold = rel_part[:64] + rel_part[64:]
    rel_fold = (rel_fold[:, :rel_half] + rel_fold[:, rel_half:]).reshape(2, 32, rel_half)[:, : rel_pos.shape[1]]
    normed_sum = lax.psum(part_normed, "mp")
    rel_sum = lax.psum(rel_fold.astype(BF), "mp").astype(F32)

    def attn_tiles(left_at, right_at, nb_ref, att_ref, gm_ref, gb_ref, wire, lefts, rights):
        lefts[0:8], lefts[8:10] = nb_ref[...], att_ref[...]
        rights[0:6], rights[6:14] = gm_ref[...], gb_ref[...]
        grad_tiles_body(left_at, right_at, 64, lambda i: lefts[i], lambda i: rights[i], wire)

    stack_a, = call(
        attn_tiles, (xa, ya), (nb, att, gm, gb), [((80, SIDE, 128), BF)],
        [((10, ROWS, SIDE), BF), ((14, ROWS, SIDE), BF)], "attn_tiles")
    sum_a = lax.psum_scatter(stack_a, "dp", scatter_dimension=0, tiled=True)
    tokens_grad, sums_one = call(
        token_back_body, (), (tok, live[:t], normed_sum, grad_middle, norm_gains),
        [((t, width), F32), ((2, width), F32)], [], "token_back")
    gains_grad, biases_grad, outb_grad, rel_grad, qkv_grad, up_grad = lax.psum(
        (
            jnp.stack([sums_one[0], sums_two[0]]),
            jnp.stack([sums_one[1], sums_two[1]]),
            jnp.stack([sums_two[3], sums_two[2]]),
            rel_sum,
            qkv_sums.reshape(-1),
            up_sums.reshape(-1),
        ),
        "dp",
    )

    def soap(wire, master, left, right, first, second, name):
        shape = master.shape[1:]
        outs = call(
            soap_body, (), (wire, master[0], left[0], right[0], first[0], second[0]),
            [(shape, F32), (shape, F32), (shape, BF), (shape, F32), (shape, F32)],
            [((2, 8 * SIDE, 128), F32)] * 4, name)
        return [value[None] for value in outs]

    mg, mn, mc, mf, ms = soap(sum_m, mlp_master, mlp_left, mlp_right, mlp_first, mlp_second, "soap_mlp")
    ag, an, ac, af, as_ = soap(sum_a, attn_master, attn_left, attn_right, attn_first, attn_second, "soap_attn")
    return (block_out[None], tokens_grad[None], gains_grad, biases_grad, outb_grad, qkv_grad, up_grad, rel_grad,
            ag, mg, an, mn, ac, mc, af, as_, mf, ms)


def solution(mesh):
    return build(mesh)
```

```python
import math

import jax
import jax.numpy as jnp
import numpy as np
from jax import lax
from jax.experimental import pallas as pl
from jax.experimental.pallas import tpu as pltpu
from jax.sharding import PartitionSpec as P

highest = lax.Precision.HIGHEST
norm_eps = 1e-06
beta_one = 0.9
beta_two = 0.95
adam_eps = 1e-08
learn_rate = 0.02


def untile(tile_rows, row_count, col_count, tile_side):
    shaped = tile_rows.reshape(row_count // tile_side, col_count // tile_side, tile_side, tile_side)
    return shaped.transpose(0, 2, 1, 3).reshape(row_count, col_count)


def retile(matrix, tile_side):
    row_count, col_count = matrix.shape
    shaped = matrix.reshape(row_count // tile_side, tile_side, col_count // tile_side, tile_side)
    return shaped.transpose(0, 2, 1, 3).reshape(-1, tile_side * tile_side)


def rel_onehot(win_side):
    positions = jnp.arange(win_side, dtype=jnp.int32)
    offset = positions[:, None] - positions[None, :] + (win_side - 1)
    entries = jnp.arange(2 * win_side - 1, dtype=jnp.int32)
    return (offset[:, :, None] == entries[None, None, :]).astype(jnp.float32)


def norm_forward(values, norm_gain, norm_shift):
    centre = values - jnp.mean(values, axis=-1, keepdims=True)
    inverse = lax.rsqrt(jnp.mean(centre * centre, axis=-1, keepdims=True) + norm_eps)
    unit_rows = centre * inverse
    return (unit_rows * norm_gain + norm_shift, unit_rows, inverse)


def norm_backward(grad_in, unit_rows, inverse, norm_gain):
    grad_unit = grad_in * norm_gain
    centred = grad_unit - jnp.mean(grad_unit, axis=-1, keepdims=True)
    return inverse * (centred - unit_rows * jnp.mean(grad_unit * unit_rows, axis=-1, keepdims=True))


def gelu_pair(values):
    normal_cdf = 0.5 * (1.0 + lax.erf(values * 0.5**0.5))
    density = jnp.exp(-0.5 * values * values) * (2.0 * math.pi) ** (-0.5)
    return (values * normal_cdf, normal_cdf + values * density)


def soap_step(grad_tiles, master, left_basis, right_basis, first_moment, second_moment):
    tile_side = math.isqrt(grad_tiles.shape[2])
    square = (grad_tiles.shape[0], grad_tiles.shape[1], tile_side, tile_side)
    left_square = left_basis.reshape(square)
    right_square = right_basis.reshape(square)
    half_turn = jnp.einsum(
        "mtji,mtjk->mtik", left_square, grad_tiles.reshape(square), precision=highest
    )
    rotated = jnp.einsum("mtik,mtkl->mtil", half_turn, right_square, precision=highest).reshape(
        grad_tiles.shape
    )
    first_new = beta_one * first_moment + (1.0 - beta_one) * rotated
    second_new = beta_two * second_moment + (1.0 - beta_two) * rotated * rotated
    direction = (first_new / (jnp.sqrt(second_new) + adam_eps)).reshape(square)
    back_half = jnp.einsum("mtij,mtjk->mtik", left_square, direction, precision=highest)
    update = jnp.einsum("mtik,mtlk->mtil", back_half, right_square, precision=highest).reshape(
        grad_tiles.shape
    )
    master_new = master - learn_rate * update
    return (master_new, master_new.astype(jnp.bfloat16), first_new, second_new)


def local(
    tokens,
    pad_mask,
    cotangent,
    norm_gains,
    norm_biases,
    out_biases,
    qkv_bias,
    up_bias,
    rel_pos,
    attn_owner,
    mlp_owner,
    attn_master,
    mlp_master,
    attn_left,
    attn_right,
    mlp_left,
    mlp_right,
    attn_first,
    attn_second,
    mlp_first,
    mlp_second,
):
    windows, win_tokens, model_width = tokens.shape
    row_count = windows * win_tokens
    qkv_cols = qkv_bias.shape[0]
    head_cols = qkv_cols // 3
    unit_cols = up_bias.shape[0]
    head_dim = rel_pos.shape[2]
    heads_here = head_cols // head_dim
    win_side = (rel_pos.shape[1] + 1) // 2
    tile_side = math.isqrt(attn_master.shape[2])
    qkv_count = model_width // tile_side * (qkv_cols // tile_side)
    up_count = model_width // tile_side * (unit_cols // tile_side)
    score_scale = head_dim ** (-0.5)
    attn_stored, mlp_stored = (
        lax.all_gather(attn_master.astype(jnp.bfloat16), "dp", axis=1, tiled=True),
        lax.all_gather(mlp_master.astype(jnp.bfloat16), "dp", axis=1, tiled=True),
    )
    attn_order = jnp.argsort(attn_owner[0])
    mlp_order = jnp.argsort(mlp_owner[0])
    attn_sorted = attn_stored[0][attn_order]
    mlp_sorted = mlp_stored[0][mlp_order]
    w_qkv = untile(attn_sorted[:qkv_count], model_width, qkv_cols, tile_side)
    w_proj = untile(attn_sorted[qkv_count:], head_cols, model_width, tile_side)
    w_up = untile(mlp_sorted[:up_count], model_width, unit_cols, tile_side)
    w_down = untile(mlp_sorted[up_count:], unit_cols, model_width, tile_side)
    onehot = rel_onehot(win_side)
    table_h = jnp.einsum("ijr,rc->ijc", onehot, rel_pos[0], precision=highest)
    table_w = jnp.einsum("ijr,rc->ijc", onehot, rel_pos[1], precision=highest)
    flat_rows = tokens.reshape(row_count, model_width).astype(jnp.float32)
    live_rows = pad_mask.reshape(row_count, 1).astype(jnp.float32)
    normed, unit_one, inverse_one = norm_forward(flat_rows, norm_gains[0], norm_biases[0])
    normed_low = (normed * live_rows).astype(jnp.bfloat16)
    mixed_rows = (jnp.dot(normed_low, w_qkv, preferred_element_type=jnp.float32) + qkv_bias).astype(
        jnp.bfloat16
    )
    head_parts = mixed_rows.reshape(windows, win_tokens, 3, heads_here, head_dim)
    queries = head_parts[:, :, 0]
    key_rows = head_parts[:, :, 1]
    value_rows = head_parts[:, :, 2]
    query_grid = queries.astype(jnp.float32).reshape(
        windows, win_side, win_side, heads_here, head_dim
    )

    def score_rows():
        direct = (
            jnp.einsum("wqhc,wkhc->whqk", queries, key_rows, preferred_element_type=jnp.float32)
            * score_scale
        )
        along_h = jnp.einsum("wabhc,akc->whabk", query_grid, table_h, precision=highest)
        along_w = jnp.einsum("wabhc,blc->whabl", query_grid, table_w, precision=highest)
        return direct + (along_h[..., :, None] + along_w[..., None, :]).reshape(
            windows, heads_here, win_tokens, win_tokens
        )

    scores = score_rows()
    row_top = jnp.max(scores, axis=-1, keepdims=True)
    exponent = jnp.exp(scores - row_top)
    row_total = jnp.sum(exponent, axis=-1, keepdims=True)
    log_total = row_top + jnp.log(row_total)
    probs_low = (exponent / row_total).astype(jnp.bfloat16)
    attended = jnp.einsum(
        "whqk,wkhc->wqhc", probs_low, value_rows, preferred_element_type=jnp.float32
    )
    attended_low = attended.reshape(row_count, head_cols).astype(jnp.bfloat16)
    branch = lax.psum(
        jnp.dot(attended_low, w_proj, preferred_element_type=jnp.float32).astype(jnp.bfloat16), "mp"
    ).astype(jnp.float32)
    middle = flat_rows + branch + out_biases[0]
    second, unit_two, inverse_two = norm_forward(middle, norm_gains[1], norm_biases[1])
    second_low = second.astype(jnp.bfloat16)
    hidden = jnp.dot(second_low, w_up, preferred_element_type=jnp.float32) + up_bias
    active, gelu_slope = gelu_pair(hidden)
    active_low = active.astype(jnp.bfloat16)
    down_sum = lax.psum(
        jnp.dot(active_low, w_down, preferred_element_type=jnp.float32).astype(jnp.bfloat16), "mp"
    ).astype(jnp.float32)
    block_output = (
        ((middle + down_sum + out_biases[1]) * live_rows)
        .astype(jnp.bfloat16)
        .reshape(windows, win_tokens, model_width)
    )
    grad_out = cotangent.reshape(row_count, model_width).astype(jnp.float32) * live_rows
    grad_out_low = grad_out.astype(jnp.bfloat16)
    down_bias_grad = jnp.sum(grad_out, axis=0)
    w_down_grad = jnp.einsum(
        "nf,nd->fd", active_low, grad_out_low, preferred_element_type=jnp.float32
    )
    grad_active = jnp.einsum("nd,fd->nf", grad_out_low, w_down, preferred_element_type=jnp.float32)
    grad_hidden = (grad_active * gelu_slope).astype(jnp.bfloat16)
    up_bias_grad = jnp.sum(grad_hidden.astype(jnp.float32), axis=0)
    w_up_grad = jnp.einsum("nd,nf->df", second_low, grad_hidden, preferred_element_type=jnp.float32)
    mlp_stack = jnp.concatenate(
        [retile(w_up_grad, tile_side), retile(w_down_grad, tile_side)], axis=0
    )[mlp_owner[0]][None]
    grad_second = lax.psum(
        jnp.einsum("nf,df->nd", grad_hidden, w_up, preferred_element_type=jnp.float32).astype(
            jnp.bfloat16
        ),
        "mp",
    ).astype(jnp.float32)
    gain_two_grad = jnp.sum(grad_second * unit_two, axis=0)
    shift_two_grad = jnp.sum(grad_second, axis=0)
    grad_middle = grad_out + norm_backward(grad_second, unit_two, inverse_two, norm_gains[1])
    proj_bias_grad = jnp.sum(grad_middle, axis=0)
    grad_branch = grad_middle.astype(jnp.bfloat16)
    w_proj_grad = jnp.einsum(
        "nc,nd->cd", attended_low, grad_branch, preferred_element_type=jnp.float32
    )
    grad_attended = jnp.einsum("nd,cd->nc", grad_branch, w_proj, preferred_element_type=jnp.float32)
    grad_attended = grad_attended.astype(jnp.bfloat16).reshape(
        windows, win_tokens, heads_here, head_dim
    )
    probs_full = jnp.exp(score_rows() - log_total)
    probs_again = probs_full.astype(jnp.bfloat16)
    grad_probs = jnp.einsum(
        "wqhc,wkhc->whqk", grad_attended, value_rows, preferred_element_type=jnp.float32
    )
    grad_values = jnp.einsum(
        "whqk,wqhc->wkhc", probs_again, grad_attended, preferred_element_type=jnp.float32
    )
    grad_scores = (
        probs_full * (grad_probs - jnp.sum(probs_full * grad_probs, axis=-1, keepdims=True))
    ).astype(jnp.bfloat16)
    grad_queries = (
        jnp.einsum("whqk,wkhc->wqhc", grad_scores, key_rows, preferred_element_type=jnp.float32)
        * score_scale
    )
    grad_keys = (
        jnp.einsum("whqk,wqhc->wkhc", grad_scores, queries, preferred_element_type=jnp.float32)
        * score_scale
    )
    grad_grid = grad_scores.astype(jnp.float32).reshape(
        windows, heads_here, win_side, win_side, win_side, win_side
    )
    grad_h = jnp.sum(grad_grid, axis=5)
    grad_w = jnp.sum(grad_grid, axis=4)
    grad_rel_q = jnp.einsum("whabk,akc->wabhc", grad_h, table_h, precision=highest) + jnp.einsum(
        "whabl,blc->wabhc", grad_w, table_w, precision=highest
    )
    grad_queries = grad_queries + grad_rel_q.reshape(windows, win_tokens, heads_here, head_dim)
    table_h_grad = jnp.einsum("whabk,wabhc->akc", grad_h, query_grid, precision=highest)
    table_w_grad = jnp.einsum("whabl,wabhc->blc", grad_w, query_grid, precision=highest)
    rel_part = jnp.stack(
        [
            jnp.einsum("ijr,ijc->rc", onehot, table_h_grad, precision=highest),
            jnp.einsum("ijr,ijc->rc", onehot, table_w_grad, precision=highest),
        ]
    )
    grad_mixed = (
        jnp.stack([grad_queries, grad_keys, grad_values], axis=2)
        .reshape(row_count, qkv_cols)
        .astype(jnp.bfloat16)
    )
    qkv_bias_grad = jnp.sum(grad_mixed.astype(jnp.float32), axis=0)
    w_qkv_grad = jnp.einsum("nd,nc->dc", normed_low, grad_mixed, preferred_element_type=jnp.float32)
    grad_normed, rel_sum = (
        lax.psum(
            jnp.einsum("nc,dc->nd", grad_mixed, w_qkv, preferred_element_type=jnp.float32).astype(
                jnp.bfloat16
            ),
            "mp",
        ).astype(jnp.float32),
        lax.psum(rel_part.astype(jnp.bfloat16), "mp").astype(jnp.float32),
    )
    grad_normed = grad_normed * live_rows
    gain_one_grad = jnp.sum(grad_normed * unit_one, axis=0)
    shift_one_grad = jnp.sum(grad_normed, axis=0)
    tokens_grad = (
        grad_middle + norm_backward(grad_normed, unit_one, inverse_one, norm_gains[0])
    ).reshape(windows, win_tokens, model_width)
    attn_stack = jnp.concatenate(
        [retile(w_qkv_grad, tile_side), retile(w_proj_grad, tile_side)], axis=0
    )[attn_owner[0]][None]
    attn_grad, mlp_grad = (
        lax.psum_scatter(attn_stack, "dp", scatter_dimension=1, tiled=True),
        lax.psum_scatter(mlp_stack, "dp", scatter_dimension=1, tiled=True),
    )
    gains_grad, biases_grad, out_biases_grad, rel_pos_grad, qkv_bias_total, up_bias_total = (
        lax.psum(
            (
                jnp.stack([gain_one_grad, gain_two_grad]),
                jnp.stack([shift_one_grad, shift_two_grad]),
                jnp.stack([proj_bias_grad, down_bias_grad]),
                rel_sum,
                qkv_bias_grad,
                up_bias_grad,
            ),
            "dp",
        )
    )
    attn_new, attn_copy, attn_first_new, attn_second_new = soap_step(
        attn_grad, attn_master, attn_left, attn_right, attn_first, attn_second
    )
    mlp_new, mlp_copy, mlp_first_new, mlp_second_new = soap_step(
        mlp_grad, mlp_master, mlp_left, mlp_right, mlp_first, mlp_second
    )
    return (
        block_output,
        tokens_grad,
        gains_grad,
        biases_grad,
        out_biases_grad,
        qkv_bias_total,
        up_bias_total,
        rel_pos_grad,
        attn_grad,
        mlp_grad,
        attn_new,
        mlp_new,
        attn_copy,
        mlp_copy,
        attn_first_new,
        attn_second_new,
        mlp_first_new,
        mlp_second_new,
    )


BF = jnp.bfloat16
F32 = jnp.float32
ROWS = 208
SIDE = 160


def dot(a, b):
    return jnp.dot(a, b, preferred_element_type=F32)


def dot_nt(a, b):
    return lax.dot_general(a, b, (((1,), (1,)), ((), ())), preferred_element_type=F32)


def dot_tn(a, b):
    return lax.dot_general(a, b, (((0,), (0,)), ((), ())), preferred_element_type=F32)


def lane_at(shape):
    return lax.broadcasted_iota(jnp.int32, shape, len(shape) - 1)


def low_parts(value):
    high = value.astype(BF)
    return high, (value - high.astype(F32)).astype(BF)


def flat_to_square(read, square, count=8):
    lane = lane_at((8, 128))

    def rows_of(base):
        x = [read(base + 128 * k) for k in range(5)]
        r1 = pltpu.roll(x[1], 96, 1)
        r2 = pltpu.roll(x[2], 96, 1)
        h2 = pltpu.roll(x[2], 64, 1)
        h3 = pltpu.roll(x[3], 64, 1)
        r3 = pltpu.roll(x[3], 32, 1)
        r4 = pltpu.roll(x[4], 32, 1)
        return (
            (x[0], x[1]),
            (jnp.where(lane < 96, r1, r2), r2),
            (jnp.where(lane < 64, h2, h3), h3),
            (jnp.where(lane < 32, r3, r4), r4),
        )

    def body(group, carry):
        base = pl.multiple_of(group * 1280, 128)
        rows = rows_of(base) + rows_of(base + 640)
        for part in range(2):
            stacked = jnp.stack([row[part] for row in rows], axis=0)
            square[part, :, pl.ds(pl.multiple_of(8 * group, 8), 8), :] = jnp.swapaxes(stacked, 0, 1)
        return carry

    lax.fori_loop(0, 20, body, 0)


def square_to_flat(square, write, count=8):
    lane = lane_at((8, 128))

    def body(group, carry):
        at = pl.ds(pl.multiple_of(8 * group, 8), 8)
        wide = jnp.swapaxes(square[0, :, at, :], 0, 1)
        narrow = jnp.swapaxes(square[1, :, at, :], 0, 1)
        for half in range(2):
            base = pl.multiple_of(group * 1280, 128) + 640 * half
            a = [wide[4 * half + m] for m in range(4)]
            b = [narrow[4 * half + m] for m in range(4)]
            a1 = pltpu.roll(a[1], 32, 1)
            b1 = pltpu.roll(b[1], 32, 1)
            a2 = pltpu.roll(a[2], 64, 1)
            b2 = pltpu.roll(b[2], 64, 1)
            a3 = pltpu.roll(a[3], 96, 1)
            b3 = pltpu.roll(b[3], 96, 1)
            write(base, a[0])
            write(base + 128, jnp.where(lane < 32, b[0], a1))
            write(base + 256, jnp.where(lane < 32, a1, jnp.where(lane < 64, b1, a2)))
            write(base + 384, jnp.where(lane < 64, a2, jnp.where(lane < 96, b2, a3)))
            write(base + 512, jnp.where(lane < 96, a3, b3))
        return carry

    lax.fori_loop(0, 20, body, 0)


def pack_eight(source, first, wire, base, square):
    lane = lane_at((SIDE, 128))
    flat_to_square(lambda at: source[first : first + 8, pl.ds(at, 128)], square)
    for half in range(2):
        spare = None
        for q in range(4):
            wire[base + 5 * half + q] = square[0, 4 * half + q].astype(BF)
            piece = square[1, 4 * half + q]
            spare = piece if q == 0 else jnp.where(lane < 32 * q, spare, pltpu.roll(piece, 32 * q, 1))
        wire[base + 5 * half + 4] = spare.astype(BF)


def pack_body(attn, mlp, wire_attn, wire_mlp, square):
    pack_eight(attn, 0, wire_attn, 0, square)
    pack_eight(mlp, 0, wire_mlp, 0, square)
    pack_eight(mlp, 8, wire_mlp, 10, square)


def unpack_narrow(wire, narrow, groups):
    def body(g, carry):
        last = wire[5 * g + 4]
        for q in range(4):
            narrow[4 * g + q] = last[:, 32 * q : 32 * q + 32]
        return carry

    lax.fori_loop(0, groups, body, 0)


def unpack_sorted(wire, narrow, order, base, outs, rows, cols):
    def body(t, carry):
        row = t // cols
        col = t - row * cols
        stored = order[base + t]
        where_at = pl.multiple_of(row * SIDE, 32)
        outs[col, pl.ds(where_at, SIDE), 0:128] = wire[(stored // 4) * 5 + stored % 4]
        outs[col, pl.ds(where_at, SIDE), 128:160] = narrow[stored]
        return carry

    lax.fori_loop(0, rows * cols, body, 0)


def norm_parts(x):
    mean = jnp.mean(x, axis=-1, keepdims=True)
    centre = x - mean
    inverse = lax.rsqrt(jnp.mean(centre * centre, axis=-1, keepdims=True) + norm_eps)
    return centre * inverse, inverse


def norm_back(grad_in, unit, inverse, gain):
    w = grad_in * gain
    return inverse * (
        w - jnp.mean(w, axis=-1, keepdims=True) - unit * jnp.mean(w * unit, axis=-1, keepdims=True)
    )


def padded(ref, rows, kind=F32):
    value = ref[...].astype(kind)
    return jnp.concatenate([value, jnp.zeros((ROWS - rows, value.shape[1]), kind)], axis=0)


def attn_forward(mixed, rel_hi, rel_lo, pick, spread, probs, att, scale, tokens_here):
    lane = lane_at((ROWS, SIDE))
    key_ok = lane_at((ROWS, ROWS)) < tokens_here
    head = SIDE // 2
    for p in range(2):
        q, k, v = mixed[p], mixed[2 + p], mixed[4 + p]
        parts = []
        for h in range(2):
            mine = (lane >= head) if h else (lane < head)
            qm = jnp.where(mine, q, jnp.zeros_like(q))
            s = dot_nt(qm, k) * scale
            a_hi, a_lo = low_parts(dot_nt(qm, rel_hi[...]) + dot_nt(qm, rel_lo[...]))
            for c in range(7):
                mask = pick[:, 128 * c : 128 * c + 128]
                table = spread[128 * c : 128 * c + 128, :]
                s = s + dot(a_hi * mask, table) + dot(a_lo * mask, table)
            s = jnp.where(key_ok, s, -1e30)
            top = jnp.max(s, axis=-1, keepdims=True)
            e = jnp.exp(s - top)
            pr = e / jnp.sum(e, axis=-1, keepdims=True)
            probs[2 * p + h] = pr
            parts.append(dot(pr.astype(BF), v))
        att[p] = jnp.where(lane < head, parts[0], parts[1]).astype(BF)


def attn_backward(mixed, rel_hi, rel_lo, pick, spread, probs, gatt, gm, rel_out, scale):
    lane = lane_at((ROWS, SIDE))
    head = SIDE // 2
    for p in range(2):
        q, k, v = mixed[p], mixed[2 + p], mixed[4 + p]
        ga = gatt[p]
        dq, dk, dv, dr = [], [], [], []
        for h in range(2):
            mine = (lane >= head) if h else (lane < head)
            pr = probs[2 * p + h]
            gam = jnp.where(mine, ga, jnp.zeros_like(ga))
            gp = dot_nt(gam, v)
            dv.append(dot_tn(pr.astype(BF), ga))
            ds = (pr * (gp - jnp.sum(pr * gp, axis=-1, keepdims=True))).astype(BF)
            da = None
            for c in range(7):
                term = dot_nt(ds, spread[128 * c : 128 * c + 128, :]) * pick[:, 128 * c : 128 * c + 128].astype(F32)
                da = term if da is None else da + term
            da_hi, da_lo = low_parts(da)
            relq = dot(da_hi, rel_hi[...]) + dot(da_lo, rel_hi[...]) + dot(da_hi, rel_lo[...])
            dq.append(dot(ds, k) * scale + relq)
            dk.append(dot_tn(ds, q) * scale)
            dr.append(dot_tn(da_hi, q) + dot_tn(da_lo, q))
        gm[p] = jnp.where(lane < head, dq[0], dq[1]).astype(BF)
        gm[2 + p] = jnp.where(lane < head, dk[0], dk[1]).astype(BF)
        gm[4 + p] = jnp.where(lane < head, dv[0], dv[1]).astype(BF)
        rel = jnp.where(lane_at((128, SIDE)) < head, dr[0], dr[1])
        if p == 0:
            rel_out[...] = rel
        else:
            rel_out[...] += rel


def attn_fwd_body(order, tokens, live, gains, biases, qkv_bias, rel_hi, rel_lo, pick, spread, wire,
                  part, normed, mixed, probs, att, w_qkv, w_proj, narrow, block):
    t = tokens.shape[0]
    x = padded(tokens, t)
    unit, _ = norm_parts(x)
    normed[...] = ((unit * gains[0:1, :] + biases[0:1, :]) * live[...]).astype(BF)
    unpack_narrow(wire, narrow, wire.shape[0] // 5)
    unpack_sorted(wire, narrow, order, 0, w_qkv, 8, 6)
    unpack_sorted(wire, narrow, order, 48, w_proj, 2, 8)

    def mix(j, carry):
        mixed[j] = (dot(normed[...], w_qkv[j]) + qkv_bias[pl.ds(j, 1), :]).astype(BF)
        return carry

    lax.fori_loop(0, 6, mix, 0)
    attn_forward(mixed, rel_hi, rel_lo, pick, spread, probs, att, (SIDE // 2) ** -0.5, t)

    def project(n, carry):
        value = dot(att[0], w_proj[n, 0:SIDE, :]) + dot(att[1], w_proj[n, SIDE : 2 * SIDE, :])
        block[n] = value
        return carry

    lax.fori_loop(0, 8, project, 0)
    for n in range(8):
        part[:, SIDE * n : SIDE * n + SIDE] = block[n][0:t, :].astype(BF)


def mlp_body(order, tokens, live, cotangent, branch, gains, biases, out_biases, up_bias, wire,
             part_down, part_second, sec_blocks, act_blocks, gh, go, bias_sums, w_up, w_down, narrow, block, second):
    t = tokens.shape[0]
    x = padded(tokens, t)
    middle = x + padded(branch, t) + out_biases[0:1, :]
    unit, _ = norm_parts(middle)
    second[...] = (unit * gains[1:2, :] + biases[1:2, :]).astype(BF)
    grad_out = padded(cotangent, t) * live[...]
    for n in range(8):
        sec_blocks[n] = second[:, SIDE * n : SIDE * n + SIDE]
        go[n] = grad_out[:, SIDE * n : SIDE * n + SIDE].astype(BF)
    unpack_narrow(wire, narrow, wire.shape[0] // 5)
    unpack_sorted(wire, narrow, order, 0, w_up, 8, 8)
    unpack_sorted(wire, narrow, order, 64, w_down, 8, 8)

    def hidden_block(j, carry):
        row = pl.multiple_of(j * SIDE, 32)
        hid = dot(second[...], w_up[j]) + up_bias[pl.ds(j, 1), :]
        cdf = 0.5 * (1.0 + lax.erf(hid * 0.5**0.5))
        slope = cdf + hid * (jnp.exp(-0.5 * hid * hid) * (2.0 * math.pi) ** -0.5)
        act_blocks[j] = (hid * cdf).astype(BF)
        ga = dot_nt(go[0], w_down[0, pl.ds(row, SIDE), :])
        for n in range(1, 8):
            ga = ga + dot_nt(go[n], w_down[n, pl.ds(row, SIDE), :])
        low = (ga * slope).astype(BF)
        gh[j] = low
        bias_sums[pl.ds(j, 1), :] = jnp.sum(low.astype(F32), axis=0, keepdims=True)
        return carry

    lax.fori_loop(0, 8, hidden_block, 0)

    def second_back(i, carry):
        row = pl.multiple_of(i * SIDE, 32)
        value = dot_nt(gh[0], w_up[0, pl.ds(row, SIDE), :])
        for j in range(1, 8):
            value = value + dot_nt(gh[j], w_up[j, pl.ds(row, SIDE), :])
        block[i] = value
        return carry

    lax.fori_loop(0, 8, second_back, 0)
    for n in range(8):
        part_second[:, SIDE * n : SIDE * n + SIDE] = block[n][0:t, :].astype(BF)

    def down(n, carry):
        value = dot(act_blocks[0], w_down[n, 0:SIDE, :])
        for j in range(1, 8):
            value = value + dot(act_blocks[j], w_down[n, j * SIDE : (j + 1) * SIDE, :])
        block[n] = value
        return carry

    lax.fori_loop(0, 8, down, 0)
    for n in range(8):
        part_down[:, SIDE * n : SIDE * n + SIDE] = block[n][0:t, :].astype(BF)


def grad_tiles_body(left_at, right_at, count, read_left, read_right, wire):
    lane = lane_at((SIDE, 128))

    def body(g, carry):
        spare = None
        for q in range(4):
            s = 4 * g + q
            tile = dot_tn(read_left(left_at[s]), read_right(right_at[s]))
            wire[5 * g + q] = tile[:, 0:128].astype(BF)
            piece = jnp.concatenate([tile[:, 128:160], jnp.zeros((SIDE, 96), F32)], axis=1)
            spare = piece if q == 0 else jnp.where(lane < 32 * q, spare, pltpu.roll(piece, 32 * q, 1))
        wire[5 * g + 4] = spare.astype(BF)
        return carry

    lax.fori_loop(0, count // 4, body, 0)


def mid_back_body(order, tokens, live, cotangent, branch, down_sum, second_sum, gains, out_biases,
                  wire, mixed, probs, normed, att, rel_hi, rel_lo, pick, spread,
                  block_out, grad_middle_out, part_normed, rel_out, gm, gb, nb, sums, bias_sums,
                  w_qkv, w_proj, narrow, block, gatt):
    t = tokens.shape[0]
    x = padded(tokens, t)
    middle = x + padded(branch, t) + out_biases[0:1, :]
    result = (middle + padded(down_sum, t) + out_biases[1:2, :]) * live[...]
    block_out[...] = result[0:t, :].astype(BF)
    grad_out = padded(cotangent, t) * live[...]
    unit, inverse = norm_parts(middle)
    grad_second = padded(second_sum, t)
    sums[0:1, :] = jnp.sum(grad_second * unit, axis=0, keepdims=True)
    sums[1:2, :] = jnp.sum(grad_second, axis=0, keepdims=True)
    sums[2:3, :] = jnp.sum(grad_out, axis=0, keepdims=True)
    grad_middle = grad_out + norm_back(grad_second, unit, inverse, gains[1:2, :])
    sums[3:4, :] = jnp.sum(grad_middle, axis=0, keepdims=True)
    grad_middle_out[...] = grad_middle[0:t, :]
    for n in range(8):
        gb[n] = grad_middle[:, SIDE * n : SIDE * n + SIDE].astype(BF)
        nb[n] = normed[:, SIDE * n : SIDE * n + SIDE]
    unpack_narrow(wire, narrow, wire.shape[0] // 5)
    unpack_sorted(wire, narrow, order, 0, w_qkv, 8, 6)
    unpack_sorted(wire, narrow, order, 48, w_proj, 2, 8)
    for p in range(2):
        value = dot_nt(gb[0], w_proj[0, p * SIDE : (p + 1) * SIDE, :])
        for n in range(1, 8):
            value = value + dot_nt(gb[n], w_proj[n, p * SIDE : (p + 1) * SIDE, :])
        gatt[p] = value.astype(BF)
    attn_backward(mixed, rel_hi, rel_lo, pick, spread, probs, gatt, gm, rel_out, (SIDE // 2) ** -0.5)
    for j in range(6):
        bias_sums[j : j + 1, :] = jnp.sum(gm[j].astype(F32), axis=0, keepdims=True)

    def normed_back(i, carry):
        row = pl.multiple_of(i * SIDE, 32)
        value = dot_nt(gm[0], w_qkv[0, pl.ds(row, SIDE), :])
        for j in range(1, 6):
            value = value + dot_nt(gm[j], w_qkv[j, pl.ds(row, SIDE), :])
        block[i] = value
        return carry

    lax.fori_loop(0, 8, normed_back, 0)
    for n in range(8):
        part_normed[:, SIDE * n : SIDE * n + SIDE] = block[n][0:t, :].astype(BF)


def token_back_body(tokens, live, normed_sum, grad_middle, gains, tokens_grad, sums):
    x = tokens[...].astype(F32)
    unit, inverse = norm_parts(x)
    grad_normed = normed_sum[...].astype(F32) * live[...]
    sums[0:1, :] = jnp.sum(grad_normed * unit, axis=0, keepdims=True)
    sums[1:2, :] = jnp.sum(grad_normed, axis=0, keepdims=True)
    tokens_grad[...] = grad_middle[...] + norm_back(grad_normed, unit, inverse, gains[0:1, :])


def square_tile(square, t):
    return jnp.concatenate([square[0, t], square[1, t, :, 0:32]], axis=1)


def put_tile(square, t, value):
    square[0, t] = value[:, 0:128]
    square[1, t, :, 0:32] = value[:, 128:160]


def split_dot(kind, a, b):
    a_hi, a_lo = low_parts(a)
    b_hi, b_lo = low_parts(b)
    return kind(a_hi, b_hi) + (kind(a_hi, b_lo) + kind(a_lo, b_hi))


def soap_group(r0, grad_square, master, left, right, first, second,
               grad_out, new_out, copy_out, first_out, second_out, sq_left, sq_right, sq_work):
    rows = slice(r0, r0 + 8)

    def writer(ref):
        def write(at, value):
            ref[rows, pl.ds(at, 128)] = value
        return write

    flat_to_square(lambda at: left[rows, pl.ds(at, 128)], sq_left, 8)
    flat_to_square(lambda at: right[rows, pl.ds(at, 128)], sq_right, 8)
    square_to_flat(grad_square, writer(grad_out), 8)

    def rotate(t, carry):
        l, r = square_tile(sq_left, t), square_tile(sq_right, t)
        half = split_dot(dot_tn, l, square_tile(grad_square, t))
        put_tile(sq_work, t, split_dot(dot, half, r))
        return carry

    lax.fori_loop(0, 8, rotate, 0)

    def moments(at, rotated):
        cols = pl.ds(at, 128)
        f = beta_one * first[rows, cols] + (1.0 - beta_one) * rotated
        s = beta_two * second[rows, cols] + (1.0 - beta_two) * rotated * rotated
        first_out[rows, cols] = f
        second_out[rows, cols] = s
        new_out[rows, cols] = f / (jnp.sqrt(s) + adam_eps)

    square_to_flat(sq_work, moments, 8)
    flat_to_square(lambda at: new_out[rows, pl.ds(at, 128)], sq_work, 8)

    def turn_back(t, carry):
        l, r = square_tile(sq_left, t), square_tile(sq_right, t)
        half = split_dot(dot, l, square_tile(sq_work, t))
        put_tile(sq_work, t, split_dot(dot_nt, half, r))
        return carry

    lax.fori_loop(0, 8, turn_back, 0)

    def finish(at, update):
        cols = pl.ds(at, 128)
        value = master[rows, cols] - learn_rate * update
        new_out[rows, cols] = value
        copy_out[rows, cols] = value.astype(BF)

    square_to_flat(sq_work, finish, 8)


def soap_body(wire, master, left, right, first, second,
              grad_out, new_out, copy_out, first_out, second_out, sq_grad, sq_left, sq_right, sq_work):
    for r in range(master.shape[0] // 8):
        for half in range(2):
            last = wire[5 * (2 * r + half) + 4].astype(F32)
            for q in range(4):
                sq_grad[0, 4 * half + q] = wire[5 * (2 * r + half) + q].astype(F32)
                sq_grad[1, 4 * half + q] = last if q == 0 else pltpu.roll(last, 128 - 32 * q, 1)
        soap_group(8 * r, sq_grad, master, left, right, first, second,
                   grad_out, new_out, copy_out, first_out, second_out, sq_left, sq_right, sq_work)


def build(mesh):
    placed = (
        P("dp", None, None),
        P("dp", None),
        P("dp", None, None),
        P(),
        P(),
        P(),
        P("mp"),
        P("mp"),
        P(),
        P("mp", None),
        P("mp", None),
        P("mp", "dp", None),
        P("mp", "dp", None),
        P("mp", "dp", None),
        P("mp", "dp", None),
        P("mp", "dp", None),
        P("mp", "dp", None),
        P("mp", "dp", None),
        P("mp", "dp", None),
        P("mp", "dp", None),
        P("mp", "dp", None),
    )
    return jax.shard_map(
        fast_local if dict(mesh.shape) == {"dp": 8, "mp": 4} else local,
        mesh=mesh,
        in_specs=placed,
        out_specs=(
            P("dp", None, None),
            P("dp", None, None),
            P(),
            P(),
            P(),
            P("mp"),
            P("mp"),
            P(),
            P("mp", "dp", None),
            P("mp", "dp", None),
            P("mp", "dp", None),
            P("mp", "dp", None),
            P("mp", "dp", None),
            P("mp", "dp", None),
            P("mp", "dp", None),
            P("mp", "dp", None),
            P("mp", "dp", None),
            P("mp", "dp", None),
        ),
        check_vma=False,
    )


VM = pl.BlockSpec(memory_space=pltpu.VMEM)
SM = pl.BlockSpec(memory_space=pltpu.SMEM)
LIMIT = 60 * 1024 * 1024


def call(body, tables, args, outs, scratch, name):
    return pl.pallas_call(
        body,
        out_shape=[jax.ShapeDtypeStruct(shape, kind) for shape, kind in outs],
        in_specs=[SM] * len(tables) + [VM] * len(args),
        out_specs=[VM] * len(outs),
        scratch_shapes=[pltpu.VMEM(shape, kind) for shape, kind in scratch],
        compiler_params=pltpu.CompilerParams(vmem_limit_bytes=LIMIT),
        name=name,
    )(*tables, *args)


def rel_constants(side):
    rows = np.arange(ROWS)
    lanes = np.arange(896)
    within, along = lanes % 64, lanes // 64
    high = np.where(rows < side * side, rows // side, -1)[:, None]
    wide = np.where(rows < side * side, rows % side, -1)[:, None]
    pick = np.where(within[None] < 32, high == along[None], wide == along[None])
    keys = np.arange(ROWS)
    key_h, key_w = keys // side, keys % side
    offset = np.where(within[:, None] < 32, along[:, None] - key_h[None], along[:, None] - key_w[None]) + side - 1
    spread = (offset == (within % 32)[:, None]) & (keys < side * side)[None]
    return jnp.asarray(pick, BF), jnp.asarray(spread, BF)


def inverse_order(owner):
    count = owner.shape[0]
    at = jnp.arange(count, dtype=jnp.int32)
    return jnp.sum(jnp.where(owner[:, None] == at[None, :], at[:, None], 0), axis=0)


def fast_local(
    tokens, pad_mask, cotangent, norm_gains, norm_biases, out_biases, qkv_bias, up_bias, rel_pos,
    attn_owner, mlp_owner, attn_master, mlp_master, attn_left, attn_right, mlp_left, mlp_right,
    attn_first, attn_second, mlp_first, mlp_second,
):
    t, width = tokens.shape[1:]
    tok, cot = tokens[0], cotangent[0]
    live = jnp.pad(pad_mask[0].astype(F32), (0, ROWS - t))[:, None]
    qb, ub = qkv_bias.reshape(6, SIDE), up_bias.reshape(8, SIDE)
    rel = jnp.pad(rel_pos, ((0, 0), (0, 32 - rel_pos.shape[1]), (0, 0))).reshape(64, SIDE // 2)
    rel_hi, rel_lo = low_parts(jnp.tile(rel, (2, 2)))
    pick, spread = rel_constants((rel_pos.shape[1] + 1) // 2)
    own_a, own_m = attn_owner[0], mlp_owner[0]
    ord_a, ord_m = inverse_order(own_a), inverse_order(own_m)
    xa = jnp.where(own_a < 48, own_a // 6, 8 + (own_a - 48) // 8)
    ya = jnp.where(own_a < 48, own_a % 6, 6 + (own_a - 48) % 8)
    xm, ym = own_m // 8, (own_m // 64) * 8 + own_m % 8

    wire_a, wire_m = call(
        pack_body, (), (attn_master[0], mlp_master[0]),
        [((10, SIDE, 128), BF), ((20, SIDE, 128), BF)], [((2, 8, SIDE, 128), F32)], "pack")
    all_a = lax.all_gather(wire_a, "dp", axis=0, tiled=True)
    all_m = lax.all_gather(wire_m, "dp", axis=0, tiled=True)

    part, normed, mixed, probs, att = call(
        attn_fwd_body, (ord_a,),
        (tok, live, norm_gains, norm_biases, qb, rel_hi, rel_lo, pick, spread, all_a),
        [((t, width), BF), ((ROWS, width), BF), ((6, ROWS, SIDE), BF), ((4, ROWS, ROWS), F32), ((2, ROWS, SIDE), BF)],
        [((6, 8 * SIDE, SIDE), BF), ((8, 2 * SIDE, SIDE), BF), ((64, SIDE, 32), BF), ((8, ROWS, SIDE), F32)],
        "attn_fwd")
    branch = lax.psum(part, "mp")
    part_down, part_second, sec_blocks, act_blocks, gh, go, up_sums = call(
        mlp_body, (ord_m,),
        (tok, live, cot, branch, norm_gains, norm_biases, out_biases, ub, all_m),
        [((t, width), BF), ((t, width), BF)] + [((8, ROWS, SIDE), BF)] * 4 + [((8, SIDE), F32)],
        [((8, 8 * SIDE, SIDE), BF), ((8, 8 * SIDE, SIDE), BF), ((128, SIDE, 32), BF), ((8, ROWS, SIDE), F32), ((ROWS, width), BF)],
        "mlp")
    second_sum = lax.psum(part_second, "mp")
    down_sum = lax.psum(part_down, "mp")

    def mlp_tiles(left_at, right_at, sec, act, gh_ref, go_ref, wire, lefts, rights):
        lefts[0:8], lefts[8:16] = sec[...], act[...]
        rights[0:8], rights[8:16] = gh_ref[...], go_ref[...]
        grad_tiles_body(left_at, right_at, 128, lambda i: lefts[i], lambda i: rights[i], wire)

    stack_m, = call(
        mlp_tiles, (xm, ym), (sec_blocks, act_blocks, gh, go), [((160, SIDE, 128), BF)],
        [((16, ROWS, SIDE), BF)] * 2, "mlp_tiles")
    sum_m = lax.psum_scatter(stack_m, "dp", scatter_dimension=0, tiled=True)

    block_out, grad_middle, part_normed, rel_part, gm, gb, nb, sums_two, qkv_sums = call(
        mid_back_body, (ord_a,),
        (tok, live, cot, branch, down_sum, second_sum, norm_gains, out_biases, all_a, mixed, probs, normed, att,
         rel_hi, rel_lo, pick, spread),
        [((t, width), BF), ((t, width), F32), ((t, width), BF), ((128, SIDE), F32), ((6, ROWS, SIDE), BF),
         ((8, ROWS, SIDE), BF), ((8, ROWS, SIDE), BF), ((4, width), F32), ((6, SIDE), F32)],
        [((6, 8 * SIDE, SIDE), BF), ((8, 2 * SIDE, SIDE), BF), ((64, SIDE, 32), BF), ((8, ROWS, SIDE), F32),
         ((2, ROWS, SIDE), BF)],
        "mid_back")
    rel_half = SIDE // 2
    rel_fold = rel_part[:64] + rel_part[64:]
    rel_fold = (rel_fold[:, :rel_half] + rel_fold[:, rel_half:]).reshape(2, 32, rel_half)[:, : rel_pos.shape[1]]
    normed_sum = lax.psum(part_normed, "mp")
    rel_sum = lax.psum(rel_fold.astype(BF), "mp").astype(F32)

    def attn_tiles(left_at, right_at, nb_ref, att_ref, gm_ref, gb_ref, wire, lefts, rights):
        lefts[0:8], lefts[8:10] = nb_ref[...], att_ref[...]
        rights[0:6], rights[6:14] = gm_ref[...], gb_ref[...]
        grad_tiles_body(left_at, right_at, 64, lambda i: lefts[i], lambda i: rights[i], wire)

    stack_a, = call(
        attn_tiles, (xa, ya), (nb, att, gm, gb), [((80, SIDE, 128), BF)],
        [((10, ROWS, SIDE), BF), ((14, ROWS, SIDE), BF)], "attn_tiles")
    sum_a = lax.psum_scatter(stack_a, "dp", scatter_dimension=0, tiled=True)
    tokens_grad, sums_one = call(
        token_back_body, (), (tok, live[:t], normed_sum, grad_middle, norm_gains),
        [((t, width), F32), ((2, width), F32)], [], "token_back")
    gains_grad, biases_grad, outb_grad, rel_grad, qkv_grad, up_grad = lax.psum(
        (
            jnp.stack([sums_one[0], sums_two[0]]),
            jnp.stack([sums_one[1], sums_two[1]]),
            jnp.stack([sums_two[3], sums_two[2]]),
            rel_sum,
            qkv_sums.reshape(-1),
            up_sums.reshape(-1),
        ),
        "dp",
    )

    def soap(wire, master, left, right, first, second, name):
        shape = master.shape[1:]
        outs = call(
            soap_body, (), (wire, master[0], left[0], right[0], first[0], second[0]),
            [(shape, F32), (shape, F32), (shape, BF), (shape, F32), (shape, F32)],
            [((2, 8, SIDE, 128), F32)] * 4, name)
        return [value[None] for value in outs]

    mg, mn, mc, mf, ms = soap(sum_m, mlp_master, mlp_left, mlp_right, mlp_first, mlp_second, "soap_mlp")
    ag, an, ac, af, as_ = soap(sum_a, attn_master, attn_left, attn_right, attn_first, attn_second, "soap_attn")
    return (block_out[None], tokens_grad[None], gains_grad, biases_grad, outb_grad, qkv_grad, up_grad, rel_grad,
            ag, mg, an, mn, ac, mc, af, as_, mf, ms)


def solution(mesh):
    return build(mesh)
```

```python
import math

import jax
import jax.numpy as jnp
import numpy as np
from jax import lax
from jax.experimental import pallas as pl
from jax.experimental.pallas import tpu as pltpu
from jax.sharding import PartitionSpec as P

highest = lax.Precision.HIGHEST
norm_eps = 1e-06
beta_one = 0.9
beta_two = 0.95
adam_eps = 1e-08
learn_rate = 0.02


def untile(tile_rows, row_count, col_count, tile_side):
    shaped = tile_rows.reshape(row_count // tile_side, col_count // tile_side, tile_side, tile_side)
    return shaped.transpose(0, 2, 1, 3).reshape(row_count, col_count)


def retile(matrix, tile_side):
    row_count, col_count = matrix.shape
    shaped = matrix.reshape(row_count // tile_side, tile_side, col_count // tile_side, tile_side)
    return shaped.transpose(0, 2, 1, 3).reshape(-1, tile_side * tile_side)


def rel_onehot(win_side):
    positions = jnp.arange(win_side, dtype=jnp.int32)
    offset = positions[:, None] - positions[None, :] + (win_side - 1)
    entries = jnp.arange(2 * win_side - 1, dtype=jnp.int32)
    return (offset[:, :, None] == entries[None, None, :]).astype(jnp.float32)


def norm_forward(values, norm_gain, norm_shift):
    centre = values - jnp.mean(values, axis=-1, keepdims=True)
    inverse = lax.rsqrt(jnp.mean(centre * centre, axis=-1, keepdims=True) + norm_eps)
    unit_rows = centre * inverse
    return (unit_rows * norm_gain + norm_shift, unit_rows, inverse)


def norm_backward(grad_in, unit_rows, inverse, norm_gain):
    grad_unit = grad_in * norm_gain
    centred = grad_unit - jnp.mean(grad_unit, axis=-1, keepdims=True)
    return inverse * (centred - unit_rows * jnp.mean(grad_unit * unit_rows, axis=-1, keepdims=True))


def gelu_pair(values):
    normal_cdf = 0.5 * (1.0 + lax.erf(values * 0.5**0.5))
    density = jnp.exp(-0.5 * values * values) * (2.0 * math.pi) ** (-0.5)
    return (values * normal_cdf, normal_cdf + values * density)


def soap_step(grad_tiles, master, left_basis, right_basis, first_moment, second_moment):
    tile_side = math.isqrt(grad_tiles.shape[2])
    square = (grad_tiles.shape[0], grad_tiles.shape[1], tile_side, tile_side)
    left_square = left_basis.reshape(square)
    right_square = right_basis.reshape(square)
    half_turn = jnp.einsum(
        "mtji,mtjk->mtik", left_square, grad_tiles.reshape(square), precision=highest
    )
    rotated = jnp.einsum("mtik,mtkl->mtil", half_turn, right_square, precision=highest).reshape(
        grad_tiles.shape
    )
    first_new = beta_one * first_moment + (1.0 - beta_one) * rotated
    second_new = beta_two * second_moment + (1.0 - beta_two) * rotated * rotated
    direction = (first_new / (jnp.sqrt(second_new) + adam_eps)).reshape(square)
    back_half = jnp.einsum("mtij,mtjk->mtik", left_square, direction, precision=highest)
    update = jnp.einsum("mtik,mtlk->mtil", back_half, right_square, precision=highest).reshape(
        grad_tiles.shape
    )
    master_new = master - learn_rate * update
    return (master_new, master_new.astype(jnp.bfloat16), first_new, second_new)


def local(
    tokens,
    pad_mask,
    cotangent,
    norm_gains,
    norm_biases,
    out_biases,
    qkv_bias,
    up_bias,
    rel_pos,
    attn_owner,
    mlp_owner,
    attn_master,
    mlp_master,
    attn_left,
    attn_right,
    mlp_left,
    mlp_right,
    attn_first,
    attn_second,
    mlp_first,
    mlp_second,
):
    windows, win_tokens, model_width = tokens.shape
    row_count = windows * win_tokens
    qkv_cols = qkv_bias.shape[0]
    head_cols = qkv_cols // 3
    unit_cols = up_bias.shape[0]
    head_dim = rel_pos.shape[2]
    heads_here = head_cols // head_dim
    win_side = (rel_pos.shape[1] + 1) // 2
    tile_side = math.isqrt(attn_master.shape[2])
    qkv_count = model_width // tile_side * (qkv_cols // tile_side)
    up_count = model_width // tile_side * (unit_cols // tile_side)
    score_scale = head_dim ** (-0.5)
    attn_stored, mlp_stored = (
        lax.all_gather(attn_master.astype(jnp.bfloat16), "dp", axis=1, tiled=True),
        lax.all_gather(mlp_master.astype(jnp.bfloat16), "dp", axis=1, tiled=True),
    )
    attn_order = jnp.argsort(attn_owner[0])
    mlp_order = jnp.argsort(mlp_owner[0])
    attn_sorted = attn_stored[0][attn_order]
    mlp_sorted = mlp_stored[0][mlp_order]
    w_qkv = untile(attn_sorted[:qkv_count], model_width, qkv_cols, tile_side)
    w_proj = untile(attn_sorted[qkv_count:], head_cols, model_width, tile_side)
    w_up = untile(mlp_sorted[:up_count], model_width, unit_cols, tile_side)
    w_down = untile(mlp_sorted[up_count:], unit_cols, model_width, tile_side)
    onehot = rel_onehot(win_side)
    table_h = jnp.einsum("ijr,rc->ijc", onehot, rel_pos[0], precision=highest)
    table_w = jnp.einsum("ijr,rc->ijc", onehot, rel_pos[1], precision=highest)
    flat_rows = tokens.reshape(row_count, model_width).astype(jnp.float32)
    live_rows = pad_mask.reshape(row_count, 1).astype(jnp.float32)
    normed, unit_one, inverse_one = norm_forward(flat_rows, norm_gains[0], norm_biases[0])
    normed_low = (normed * live_rows).astype(jnp.bfloat16)
    mixed_rows = (jnp.dot(normed_low, w_qkv, preferred_element_type=jnp.float32) + qkv_bias).astype(
        jnp.bfloat16
    )
    head_parts = mixed_rows.reshape(windows, win_tokens, 3, heads_here, head_dim)
    queries = head_parts[:, :, 0]
    key_rows = head_parts[:, :, 1]
    value_rows = head_parts[:, :, 2]
    query_grid = queries.astype(jnp.float32).reshape(
        windows, win_side, win_side, heads_here, head_dim
    )

    def score_rows():
        direct = (
            jnp.einsum("wqhc,wkhc->whqk", queries, key_rows, preferred_element_type=jnp.float32)
            * score_scale
        )
        along_h = jnp.einsum("wabhc,akc->whabk", query_grid, table_h, precision=highest)
        along_w = jnp.einsum("wabhc,blc->whabl", query_grid, table_w, precision=highest)
        return direct + (along_h[..., :, None] + along_w[..., None, :]).reshape(
            windows, heads_here, win_tokens, win_tokens
        )

    scores = score_rows()
    row_top = jnp.max(scores, axis=-1, keepdims=True)
    exponent = jnp.exp(scores - row_top)
    row_total = jnp.sum(exponent, axis=-1, keepdims=True)
    log_total = row_top + jnp.log(row_total)
    probs_low = (exponent / row_total).astype(jnp.bfloat16)
    attended = jnp.einsum(
        "whqk,wkhc->wqhc", probs_low, value_rows, preferred_element_type=jnp.float32
    )
    attended_low = attended.reshape(row_count, head_cols).astype(jnp.bfloat16)
    branch = lax.psum(
        jnp.dot(attended_low, w_proj, preferred_element_type=jnp.float32).astype(jnp.bfloat16), "mp"
    ).astype(jnp.float32)
    middle = flat_rows + branch + out_biases[0]
    second, unit_two, inverse_two = norm_forward(middle, norm_gains[1], norm_biases[1])
    second_low = second.astype(jnp.bfloat16)
    hidden = jnp.dot(second_low, w_up, preferred_element_type=jnp.float32) + up_bias
    active, gelu_slope = gelu_pair(hidden)
    active_low = active.astype(jnp.bfloat16)
    down_sum = lax.psum(
        jnp.dot(active_low, w_down, preferred_element_type=jnp.float32).astype(jnp.bfloat16), "mp"
    ).astype(jnp.float32)
    block_output = (
        ((middle + down_sum + out_biases[1]) * live_rows)
        .astype(jnp.bfloat16)
        .reshape(windows, win_tokens, model_width)
    )
    grad_out = cotangent.reshape(row_count, model_width).astype(jnp.float32) * live_rows
    grad_out_low = grad_out.astype(jnp.bfloat16)
    down_bias_grad = jnp.sum(grad_out, axis=0)
    w_down_grad = jnp.einsum(
        "nf,nd->fd", active_low, grad_out_low, preferred_element_type=jnp.float32
    )
    grad_active = jnp.einsum("nd,fd->nf", grad_out_low, w_down, preferred_element_type=jnp.float32)
    grad_hidden = (grad_active * gelu_slope).astype(jnp.bfloat16)
    up_bias_grad = jnp.sum(grad_hidden.astype(jnp.float32), axis=0)
    w_up_grad = jnp.einsum("nd,nf->df", second_low, grad_hidden, preferred_element_type=jnp.float32)
    mlp_stack = jnp.concatenate(
        [retile(w_up_grad, tile_side), retile(w_down_grad, tile_side)], axis=0
    )[mlp_owner[0]][None]
    grad_second = lax.psum(
        jnp.einsum("nf,df->nd", grad_hidden, w_up, preferred_element_type=jnp.float32).astype(
            jnp.bfloat16
        ),
        "mp",
    ).astype(jnp.float32)
    gain_two_grad = jnp.sum(grad_second * unit_two, axis=0)
    shift_two_grad = jnp.sum(grad_second, axis=0)
    grad_middle = grad_out + norm_backward(grad_second, unit_two, inverse_two, norm_gains[1])
    proj_bias_grad = jnp.sum(grad_middle, axis=0)
    grad_branch = grad_middle.astype(jnp.bfloat16)
    w_proj_grad = jnp.einsum(
        "nc,nd->cd", attended_low, grad_branch, preferred_element_type=jnp.float32
    )
    grad_attended = jnp.einsum("nd,cd->nc", grad_branch, w_proj, preferred_element_type=jnp.float32)
    grad_attended = grad_attended.astype(jnp.bfloat16).reshape(
        windows, win_tokens, heads_here, head_dim
    )
    probs_full = jnp.exp(score_rows() - log_total)
    probs_again = probs_full.astype(jnp.bfloat16)
    grad_probs = jnp.einsum(
        "wqhc,wkhc->whqk", grad_attended, value_rows, preferred_element_type=jnp.float32
    )
    grad_values = jnp.einsum(
        "whqk,wqhc->wkhc", probs_again, grad_attended, preferred_element_type=jnp.float32
    )
    grad_scores = (
        probs_full * (grad_probs - jnp.sum(probs_full * grad_probs, axis=-1, keepdims=True))
    ).astype(jnp.bfloat16)
    grad_queries = (
        jnp.einsum("whqk,wkhc->wqhc", grad_scores, key_rows, preferred_element_type=jnp.float32)
        * score_scale
    )
    grad_keys = (
        jnp.einsum("whqk,wqhc->wkhc", grad_scores, queries, preferred_element_type=jnp.float32)
        * score_scale
    )
    grad_grid = grad_scores.astype(jnp.float32).reshape(
        windows, heads_here, win_side, win_side, win_side, win_side
    )
    grad_h = jnp.sum(grad_grid, axis=5)
    grad_w = jnp.sum(grad_grid, axis=4)
    grad_rel_q = jnp.einsum("whabk,akc->wabhc", grad_h, table_h, precision=highest) + jnp.einsum(
        "whabl,blc->wabhc", grad_w, table_w, precision=highest
    )
    grad_queries = grad_queries + grad_rel_q.reshape(windows, win_tokens, heads_here, head_dim)
    table_h_grad = jnp.einsum("whabk,wabhc->akc", grad_h, query_grid, precision=highest)
    table_w_grad = jnp.einsum("whabl,wabhc->blc", grad_w, query_grid, precision=highest)
    rel_part = jnp.stack(
        [
            jnp.einsum("ijr,ijc->rc", onehot, table_h_grad, precision=highest),
            jnp.einsum("ijr,ijc->rc", onehot, table_w_grad, precision=highest),
        ]
    )
    grad_mixed = (
        jnp.stack([grad_queries, grad_keys, grad_values], axis=2)
        .reshape(row_count, qkv_cols)
        .astype(jnp.bfloat16)
    )
    qkv_bias_grad = jnp.sum(grad_mixed.astype(jnp.float32), axis=0)
    w_qkv_grad = jnp.einsum("nd,nc->dc", normed_low, grad_mixed, preferred_element_type=jnp.float32)
    grad_normed, rel_sum = (
        lax.psum(
            jnp.einsum("nc,dc->nd", grad_mixed, w_qkv, preferred_element_type=jnp.float32).astype(
                jnp.bfloat16
            ),
            "mp",
        ).astype(jnp.float32),
        lax.psum(rel_part.astype(jnp.bfloat16), "mp").astype(jnp.float32),
    )
    grad_normed = grad_normed * live_rows
    gain_one_grad = jnp.sum(grad_normed * unit_one, axis=0)
    shift_one_grad = jnp.sum(grad_normed, axis=0)
    tokens_grad = (
        grad_middle + norm_backward(grad_normed, unit_one, inverse_one, norm_gains[0])
    ).reshape(windows, win_tokens, model_width)
    attn_stack = jnp.concatenate(
        [retile(w_qkv_grad, tile_side), retile(w_proj_grad, tile_side)], axis=0
    )[attn_owner[0]][None]
    attn_grad, mlp_grad = (
        lax.psum_scatter(attn_stack, "dp", scatter_dimension=1, tiled=True),
        lax.psum_scatter(mlp_stack, "dp", scatter_dimension=1, tiled=True),
    )
    gains_grad, biases_grad, out_biases_grad, rel_pos_grad, qkv_bias_total, up_bias_total = (
        lax.psum(
            (
                jnp.stack([gain_one_grad, gain_two_grad]),
                jnp.stack([shift_one_grad, shift_two_grad]),
                jnp.stack([proj_bias_grad, down_bias_grad]),
                rel_sum,
                qkv_bias_grad,
                up_bias_grad,
            ),
            "dp",
        )
    )
    attn_new, attn_copy, attn_first_new, attn_second_new = soap_step(
        attn_grad, attn_master, attn_left, attn_right, attn_first, attn_second
    )
    mlp_new, mlp_copy, mlp_first_new, mlp_second_new = soap_step(
        mlp_grad, mlp_master, mlp_left, mlp_right, mlp_first, mlp_second
    )
    return (
        block_output,
        tokens_grad,
        gains_grad,
        biases_grad,
        out_biases_grad,
        qkv_bias_total,
        up_bias_total,
        rel_pos_grad,
        attn_grad,
        mlp_grad,
        attn_new,
        mlp_new,
        attn_copy,
        mlp_copy,
        attn_first_new,
        attn_second_new,
        mlp_first_new,
        mlp_second_new,
    )


BF = jnp.bfloat16
F32 = jnp.float32
ROWS = 208
SIDE = 160


def dot(a, b):
    return jnp.dot(a, b, preferred_element_type=F32)


def dot_nt(a, b):
    return lax.dot_general(a, b, (((1,), (1,)), ((), ())), preferred_element_type=F32)


def dot_tn(a, b):
    return lax.dot_general(a, b, (((0,), (0,)), ((), ())), preferred_element_type=F32)


def lane_at(shape):
    return lax.broadcasted_iota(jnp.int32, shape, len(shape) - 1)


def low_parts(value):
    high = value.astype(BF)
    return high, (value - high.astype(F32)).astype(BF)


def flat_to_square(read, square, count=8):
    lane = lane_at((8, 128))

    def rows_of(base):
        x = [read(base + 128 * k) for k in range(5)]
        r1 = pltpu.roll(x[1], 96, 1)
        r2 = pltpu.roll(x[2], 96, 1)
        h2 = pltpu.roll(x[2], 64, 1)
        h3 = pltpu.roll(x[3], 64, 1)
        r3 = pltpu.roll(x[3], 32, 1)
        r4 = pltpu.roll(x[4], 32, 1)
        return (
            (x[0], x[1]),
            (jnp.where(lane < 96, r1, r2), r2),
            (jnp.where(lane < 64, h2, h3), h3),
            (jnp.where(lane < 32, r3, r4), r4),
        )

    def body(group, carry):
        base = pl.multiple_of(group * 1280, 128)
        rows = rows_of(base) + rows_of(base + 640)
        for part in range(2):
            stacked = jnp.stack([row[part] for row in rows], axis=0)
            square[part, :, pl.ds(pl.multiple_of(8 * group, 8), 8), :] = jnp.swapaxes(stacked, 0, 1)
        return carry

    lax.fori_loop(0, 20, body, 0)


def square_to_flat(square, write, count=8):
    lane = lane_at((8, 128))

    def body(group, carry):
        at = pl.ds(pl.multiple_of(8 * group, 8), 8)
        wide = jnp.swapaxes(square[0, :, at, :], 0, 1)
        narrow = jnp.swapaxes(square[1, :, at, :], 0, 1)
        for half in range(2):
            base = pl.multiple_of(group * 1280, 128) + 640 * half
            a = [wide[4 * half + m] for m in range(4)]
            b = [narrow[4 * half + m] for m in range(4)]
            a1 = pltpu.roll(a[1], 32, 1)
            b1 = pltpu.roll(b[1], 32, 1)
            a2 = pltpu.roll(a[2], 64, 1)
            b2 = pltpu.roll(b[2], 64, 1)
            a3 = pltpu.roll(a[3], 96, 1)
            b3 = pltpu.roll(b[3], 96, 1)
            write(base, a[0])
            write(base + 128, jnp.where(lane < 32, b[0], a1))
            write(base + 256, jnp.where(lane < 32, a1, jnp.where(lane < 64, b1, a2)))
            write(base + 384, jnp.where(lane < 64, a2, jnp.where(lane < 96, b2, a3)))
            write(base + 512, jnp.where(lane < 96, a3, b3))
        return carry

    lax.fori_loop(0, 20, body, 0)


def pack_eight(source, first, wire, base, square):
    lane = lane_at((SIDE, 128))
    flat_to_square(lambda at: source[first : first + 8, pl.ds(at, 128)], square)
    for half in range(2):
        spare = None
        for q in range(4):
            wire[base + 5 * half + q] = square[0, 4 * half + q].astype(BF)
            piece = square[1, 4 * half + q]
            spare = piece if q == 0 else jnp.where(lane < 32 * q, spare, pltpu.roll(piece, 32 * q, 1))
        wire[base + 5 * half + 4] = spare.astype(BF)


def pack_body(attn, mlp, wire_attn, wire_mlp, square):
    pack_eight(attn, 0, wire_attn, 0, square)
    pack_eight(mlp, 0, wire_mlp, 0, square)
    pack_eight(mlp, 8, wire_mlp, 10, square)


def unpack_narrow(wire, narrow, groups):
    def body(g, carry):
        last = wire[5 * g + 4]
        for q in range(4):
            narrow[4 * g + q] = last[:, 32 * q : 32 * q + 32]
        return carry

    lax.fori_loop(0, groups, body, 0)


def unpack_sorted(wire, narrow, order, base, outs, rows, cols):
    def body(t, carry):
        row = t // cols
        col = t - row * cols
        stored = order[base + t]
        where_at = pl.multiple_of(row * SIDE, 32)
        outs[col, pl.ds(where_at, SIDE), 0:128] = wire[(stored // 4) * 5 + stored % 4]
        outs[col, pl.ds(where_at, SIDE), 128:160] = narrow[stored]
        return carry

    lax.fori_loop(0, rows * cols, body, 0)


MESH_ID = pl.DeviceIdType.MESH
PIECE = 5


def gather_body(wire, out, send_sem, recv_sem, own_sem):
    count = wire.shape[0]
    pieces = count // PIECE
    me = lax.axis_index("dp")
    z, x = me // 2, me % 2
    side = me + 1 - 2 * x
    up, down = jnp.minimum(me + 2, 6 + x), jnp.maximum(me - 2, x)

    barrier = pltpu.get_barrier_semaphore()

    def greet(target):
        pl.semaphore_signal(barrier, inc=1, device_id={"dp": target}, device_id_type=MESH_ID)

    greet(side)
    pl.when(z < 3)(lambda: greet(up))
    pl.when(z > 0)(lambda: greet(down))
    inner = (z > 0) & (z < 3)
    pl.when(inner)(lambda: pl.semaphore_wait(barrier, 3))
    pl.when(jnp.logical_not(inner))(lambda: pl.semaphore_wait(barrier, 2))

    def copy(way, target, origin, k, own=False):
        place = out.at[pl.ds(origin * count + PIECE * k, PIECE)]
        return pltpu.make_async_remote_copy(
            src_ref=wire.at[pl.ds(PIECE * k, PIECE)] if own else place,
            dst_ref=place,
            send_sem=send_sem.at[way, origin // 2, k],
            recv_sem=recv_sem.at[origin, k],
            device_id={"dp": target},
            device_id_type=MESH_ID,
        )

    for k in range(pieces):
        copy(0, side, me, k, True).start()
        pl.when(z < 3)(lambda k=k: copy(1, up, me, k, True).start())
        pl.when(z > 0)(lambda k=k: copy(2, down, me, k, True).start())
    keep = pltpu.make_async_copy(wire, out.at[pl.ds(me * count, count)], own_sem)
    keep.start()

    for d in range(1, 4):
        for k in range(pieces):
            def from_below():
                origin = me - 2 * d
                copy(1, up, origin, k).wait_recv()
                copy(0, side, origin, k).start()
                pl.when(z < 3)(lambda: copy(1, up, origin, k).start())

            def from_above():
                origin = me + 2 * d
                copy(2, down, origin, k).wait_recv()
                copy(0, side, origin, k).start()
                pl.when(z > 0)(lambda: copy(2, down, origin, k).start())

            pl.when(z >= d)(from_below)
            pl.when(z + d <= 3)(from_above)

    keep.wait()
    for k in range(pieces):
        for line in range(4):
            origin = 2 * line + x
            copy(0, side, origin + 1 - 2 * x, k).wait_recv()
            copy(0, side, origin, k, False).wait_send()
            pl.when((line <= z) & (z < 3))(lambda: copy(1, up, origin, k).wait_send())
            pl.when((line >= z) & (z > 0))(lambda: copy(2, down, origin, k).wait_send())


def gather(wire, ident, name):
    count = wire.shape[0]
    return pl.pallas_call(
        gather_body,
        out_shape=jax.ShapeDtypeStruct((8 * count, SIDE, 128), BF),
        in_specs=[VM],
        out_specs=pl.BlockSpec(memory_space=pl.ANY),
        scratch_shapes=[
            pltpu.SemaphoreType.DMA((3, 4, count // PIECE)),
            pltpu.SemaphoreType.DMA((8, count // PIECE)),
            pltpu.SemaphoreType.DMA,
        ],
        compiler_params=pltpu.CompilerParams(
            collective_id=ident, has_side_effects=True, vmem_limit_bytes=LIMIT),
        cost_estimate=pl.CostEstimate(flops=0, bytes_accessed=count * 12_000_000, transcendentals=0),
        name=name,
    )(wire)


def norm_parts(x):
    mean = jnp.mean(x, axis=-1, keepdims=True)
    centre = x - mean
    inverse = lax.rsqrt(jnp.mean(centre * centre, axis=-1, keepdims=True) + norm_eps)
    return centre * inverse, inverse


def norm_back(grad_in, unit, inverse, gain):
    w = grad_in * gain
    return inverse * (
        w - jnp.mean(w, axis=-1, keepdims=True) - unit * jnp.mean(w * unit, axis=-1, keepdims=True)
    )


def padded(ref, rows, kind=F32):
    value = ref[...].astype(kind)
    return jnp.concatenate([value, jnp.zeros((ROWS - rows, value.shape[1]), kind)], axis=0)


def attn_forward(mixed, rel_hi, rel_lo, pick, spread, probs, att, scale, tokens_here):
    lane = lane_at((ROWS, SIDE))
    key_ok = lane_at((ROWS, ROWS)) < tokens_here
    head = SIDE // 2
    for p in range(2):
        q, k, v = mixed[p], mixed[2 + p], mixed[4 + p]
        parts = []
        for h in range(2):
            mine = (lane >= head) if h else (lane < head)
            qm = jnp.where(mine, q, jnp.zeros_like(q))
            s = dot_nt(qm, k) * scale
            a_hi, a_lo = low_parts(dot_nt(qm, rel_hi[...]) + dot_nt(qm, rel_lo[...]))
            for c in range(7):
                mask = pick[:, 128 * c : 128 * c + 128]
                table = spread[128 * c : 128 * c + 128, :]
                s = s + dot(a_hi * mask, table) + dot(a_lo * mask, table)
            s = jnp.where(key_ok, s, -1e30)
            top = jnp.max(s, axis=-1, keepdims=True)
            e = jnp.exp(s - top)
            pr = e / jnp.sum(e, axis=-1, keepdims=True)
            probs[2 * p + h] = pr
            parts.append(dot(pr.astype(BF), v))
        att[p] = jnp.where(lane < head, parts[0], parts[1]).astype(BF)


def attn_backward(mixed, rel_hi, rel_lo, pick, spread, probs, gatt, gm, rel_out, scale):
    lane = lane_at((ROWS, SIDE))
    head = SIDE // 2
    for p in range(2):
        q, k, v = mixed[p], mixed[2 + p], mixed[4 + p]
        ga = gatt[p]
        dq, dk, dv, dr = [], [], [], []
        for h in range(2):
            mine = (lane >= head) if h else (lane < head)
            pr = probs[2 * p + h]
            gam = jnp.where(mine, ga, jnp.zeros_like(ga))
            gp = dot_nt(gam, v)
            dv.append(dot_tn(pr.astype(BF), ga))
            ds = (pr * (gp - jnp.sum(pr * gp, axis=-1, keepdims=True))).astype(BF)
            da = None
            for c in range(7):
                term = dot_nt(ds, spread[128 * c : 128 * c + 128, :]) * pick[:, 128 * c : 128 * c + 128].astype(F32)
                da = term if da is None else da + term
            da_hi, da_lo = low_parts(da)
            relq = dot(da_hi, rel_hi[...]) + dot(da_lo, rel_hi[...]) + dot(da_hi, rel_lo[...])
            dq.append(dot(ds, k) * scale + relq)
            dk.append(dot_tn(ds, q) * scale)
            dr.append(dot_tn(da_hi, q) + dot_tn(da_lo, q))
        gm[p] = jnp.where(lane < head, dq[0], dq[1]).astype(BF)
        gm[2 + p] = jnp.where(lane < head, dk[0], dk[1]).astype(BF)
        gm[4 + p] = jnp.where(lane < head, dv[0], dv[1]).astype(BF)
        rel = jnp.where(lane_at((128, SIDE)) < head, dr[0], dr[1])
        if p == 0:
            rel_out[...] = rel
        else:
            rel_out[...] += rel


def attn_fwd_body(order, tokens, live, gains, biases, qkv_bias, rel_hi, rel_lo, pick, spread, wire,
                  part, normed, mixed, probs, att, w_qkv, w_proj, narrow, block):
    t = tokens.shape[0]
    x = padded(tokens, t)
    unit, _ = norm_parts(x)
    normed[...] = ((unit * gains[0:1, :] + biases[0:1, :]) * live[...]).astype(BF)
    unpack_narrow(wire, narrow, wire.shape[0] // 5)
    unpack_sorted(wire, narrow, order, 0, w_qkv, 8, 6)
    unpack_sorted(wire, narrow, order, 48, w_proj, 2, 8)

    def mix(j, carry):
        mixed[j] = (dot(normed[...], w_qkv[j]) + qkv_bias[pl.ds(j, 1), :]).astype(BF)
        return carry

    lax.fori_loop(0, 6, mix, 0)
    attn_forward(mixed, rel_hi, rel_lo, pick, spread, probs, att, (SIDE // 2) ** -0.5, t)

    def project(n, carry):
        value = dot(att[0], w_proj[n, 0:SIDE, :]) + dot(att[1], w_proj[n, SIDE : 2 * SIDE, :])
        block[n] = value
        return carry

    lax.fori_loop(0, 8, project, 0)
    for n in range(8):
        part[:, SIDE * n : SIDE * n + SIDE] = block[n][0:t, :].astype(BF)


def mlp_body(order, tokens, live, cotangent, branch, gains, biases, out_biases, up_bias, wire,
             part_down, part_second, sec_blocks, act_blocks, gh, go, bias_sums, w_up, w_down, narrow, block, second):
    t = tokens.shape[0]
    x = padded(tokens, t)
    middle = x + padded(branch, t) + out_biases[0:1, :]
    unit, _ = norm_parts(middle)
    second[...] = (unit * gains[1:2, :] + biases[1:2, :]).astype(BF)
    grad_out = padded(cotangent, t) * live[...]
    for n in range(8):
        sec_blocks[n] = second[:, SIDE * n : SIDE * n + SIDE]
        go[n] = grad_out[:, SIDE * n : SIDE * n + SIDE].astype(BF)
    unpack_narrow(wire, narrow, wire.shape[0] // 5)
    unpack_sorted(wire, narrow, order, 0, w_up, 8, 8)
    unpack_sorted(wire, narrow, order, 64, w_down, 8, 8)

    def hidden_block(j, carry):
        row = pl.multiple_of(j * SIDE, 32)
        hid = dot(second[...], w_up[j]) + up_bias[pl.ds(j, 1), :]
        cdf = 0.5 * (1.0 + lax.erf(hid * 0.5**0.5))
        slope = cdf + hid * (jnp.exp(-0.5 * hid * hid) * (2.0 * math.pi) ** -0.5)
        act_blocks[j] = (hid * cdf).astype(BF)
        ga = dot_nt(go[0], w_down[0, pl.ds(row, SIDE), :])
        for n in range(1, 8):
            ga = ga + dot_nt(go[n], w_down[n, pl.ds(row, SIDE), :])
        low = (ga * slope).astype(BF)
        gh[j] = low
        bias_sums[pl.ds(j, 1), :] = jnp.sum(low.astype(F32), axis=0, keepdims=True)
        return carry

    lax.fori_loop(0, 8, hidden_block, 0)

    def second_back(i, carry):
        row = pl.multiple_of(i * SIDE, 32)
        value = dot_nt(gh[0], w_up[0, pl.ds(row, SIDE), :])
        for j in range(1, 8):
            value = value + dot_nt(gh[j], w_up[j, pl.ds(row, SIDE), :])
        block[i] = value
        return carry

    lax.fori_loop(0, 8, second_back, 0)
    for n in range(8):
        part_second[:, SIDE * n : SIDE * n + SIDE] = block[n][0:t, :].astype(BF)

    def down(n, carry):
        value = dot(act_blocks[0], w_down[n, 0:SIDE, :])
        for j in range(1, 8):
            value = value + dot(act_blocks[j], w_down[n, j * SIDE : (j + 1) * SIDE, :])
        block[n] = value
        return carry

    lax.fori_loop(0, 8, down, 0)
    for n in range(8):
        part_down[:, SIDE * n : SIDE * n + SIDE] = block[n][0:t, :].astype(BF)


def grad_tiles_body(left_at, right_at, count, read_left, read_right, wire):
    lane = lane_at((SIDE, 128))

    def body(g, carry):
        spare = None
        for q in range(4):
            s = 4 * g + q
            tile = dot_tn(read_left(left_at[s]), read_right(right_at[s]))
            wire[5 * g + q] = tile[:, 0:128].astype(BF)
            piece = jnp.concatenate([tile[:, 128:160], jnp.zeros((SIDE, 96), F32)], axis=1)
            spare = piece if q == 0 else jnp.where(lane < 32 * q, spare, pltpu.roll(piece, 32 * q, 1))
        wire[5 * g + 4] = spare.astype(BF)
        return carry

    lax.fori_loop(0, count // 4, body, 0)


def mid_back_body(order, tokens, live, cotangent, branch, down_sum, second_sum, gains, out_biases,
                  wire, mixed, probs, normed, att, rel_hi, rel_lo, pick, spread,
                  block_out, grad_middle_out, part_normed, rel_out, gm, gb, nb, sums, bias_sums,
                  w_qkv, w_proj, narrow, block, gatt):
    t = tokens.shape[0]
    x = padded(tokens, t)
    middle = x + padded(branch, t) + out_biases[0:1, :]
    result = (middle + padded(down_sum, t) + out_biases[1:2, :]) * live[...]
    block_out[...] = result[0:t, :].astype(BF)
    grad_out = padded(cotangent, t) * live[...]
    unit, inverse = norm_parts(middle)
    grad_second = padded(second_sum, t)
    sums[0:1, :] = jnp.sum(grad_second * unit, axis=0, keepdims=True)
    sums[1:2, :] = jnp.sum(grad_second, axis=0, keepdims=True)
    sums[2:3, :] = jnp.sum(grad_out, axis=0, keepdims=True)
    grad_middle = grad_out + norm_back(grad_second, unit, inverse, gains[1:2, :])
    sums[3:4, :] = jnp.sum(grad_middle, axis=0, keepdims=True)
    grad_middle_out[...] = grad_middle[0:t, :]
    for n in range(8):
        gb[n] = grad_middle[:, SIDE * n : SIDE * n + SIDE].astype(BF)
        nb[n] = normed[:, SIDE * n : SIDE * n + SIDE]
    unpack_narrow(wire, narrow, wire.shape[0] // 5)
    unpack_sorted(wire, narrow, order, 0, w_qkv, 8, 6)
    unpack_sorted(wire, narrow, order, 48, w_proj, 2, 8)
    for p in range(2):
        value = dot_nt(gb[0], w_proj[0, p * SIDE : (p + 1) * SIDE, :])
        for n in range(1, 8):
            value = value + dot_nt(gb[n], w_proj[n, p * SIDE : (p + 1) * SIDE, :])
        gatt[p] = value.astype(BF)
    attn_backward(mixed, rel_hi, rel_lo, pick, spread, probs, gatt, gm, rel_out, (SIDE // 2) ** -0.5)
    for j in range(6):
        bias_sums[j : j + 1, :] = jnp.sum(gm[j].astype(F32), axis=0, keepdims=True)

    def normed_back(i, carry):
        row = pl.multiple_of(i * SIDE, 32)
        value = dot_nt(gm[0], w_qkv[0, pl.ds(row, SIDE), :])
        for j in range(1, 6):
            value = value + dot_nt(gm[j], w_qkv[j, pl.ds(row, SIDE), :])
        block[i] = value
        return carry

    lax.fori_loop(0, 8, normed_back, 0)
    for n in range(8):
        part_normed[:, SIDE * n : SIDE * n + SIDE] = block[n][0:t, :].astype(BF)


def token_back_body(tokens, live, normed_sum, grad_middle, gains, tokens_grad, sums):
    x = tokens[...].astype(F32)
    unit, inverse = norm_parts(x)
    grad_normed = normed_sum[...].astype(F32) * live[...]
    sums[0:1, :] = jnp.sum(grad_normed * unit, axis=0, keepdims=True)
    sums[1:2, :] = jnp.sum(grad_normed, axis=0, keepdims=True)
    tokens_grad[...] = grad_middle[...] + norm_back(grad_normed, unit, inverse, gains[0:1, :])


def square_tile(square, t):
    return jnp.concatenate([square[0, t], square[1, t, :, 0:32]], axis=1)


def put_tile(square, t, value):
    square[0, t] = value[:, 0:128]
    square[1, t, :, 0:32] = value[:, 128:160]


def split_dot(kind, a, b):
    a_hi, a_lo = low_parts(a)
    b_hi, b_lo = low_parts(b)
    return kind(a_hi, b_hi) + (kind(a_hi, b_lo) + kind(a_lo, b_hi))


def soap_group(r0, grad_square, master, left, right, first, second,
               grad_out, new_out, copy_out, first_out, second_out, sq_left, sq_right, sq_work):
    rows = slice(r0, r0 + 8)

    def writer(ref):
        def write(at, value):
            ref[rows, pl.ds(at, 128)] = value
        return write

    flat_to_square(lambda at: left[rows, pl.ds(at, 128)], sq_left, 8)
    flat_to_square(lambda at: right[rows, pl.ds(at, 128)], sq_right, 8)
    square_to_flat(grad_square, writer(grad_out), 8)

    def rotate(t, carry):
        l, r = square_tile(sq_left, t), square_tile(sq_right, t)
        half = split_dot(dot_tn, l, square_tile(grad_square, t))
        put_tile(sq_work, t, split_dot(dot, half, r))
        return carry

    lax.fori_loop(0, 8, rotate, 0)

    def moments(at, rotated):
        cols = pl.ds(at, 128)
        f = beta_one * first[rows, cols] + (1.0 - beta_one) * rotated
        s = beta_two * second[rows, cols] + (1.0 - beta_two) * rotated * rotated
        first_out[rows, cols] = f
        second_out[rows, cols] = s
        new_out[rows, cols] = f / (jnp.sqrt(s) + adam_eps)

    square_to_flat(sq_work, moments, 8)
    flat_to_square(lambda at: new_out[rows, pl.ds(at, 128)], sq_work, 8)

    def turn_back(t, carry):
        l, r = square_tile(sq_left, t), square_tile(sq_right, t)
        half = split_dot(dot, l, square_tile(sq_work, t))
        put_tile(sq_work, t, split_dot(dot_nt, half, r))
        return carry

    lax.fori_loop(0, 8, turn_back, 0)

    def finish(at, update):
        cols = pl.ds(at, 128)
        value = master[rows, cols] - learn_rate * update
        new_out[rows, cols] = value
        copy_out[rows, cols] = value.astype(BF)

    square_to_flat(sq_work, finish, 8)


def soap_body(wire, master, left, right, first, second,
              grad_out, new_out, copy_out, first_out, second_out, sq_grad, sq_left, sq_right, sq_work):
    for r in range(master.shape[0] // 8):
        for half in range(2):
            last = wire[5 * (2 * r + half) + 4].astype(F32)
            for q in range(4):
                sq_grad[0, 4 * half + q] = wire[5 * (2 * r + half) + q].astype(F32)
                sq_grad[1, 4 * half + q] = last if q == 0 else pltpu.roll(last, 128 - 32 * q, 1)
        soap_group(8 * r, sq_grad, master, left, right, first, second,
                   grad_out, new_out, copy_out, first_out, second_out, sq_left, sq_right, sq_work)


def build(mesh):
    placed = (
        P("dp", None, None),
        P("dp", None),
        P("dp", None, None),
        P(),
        P(),
        P(),
        P("mp"),
        P("mp"),
        P(),
        P("mp", None),
        P("mp", None),
        P("mp", "dp", None),
        P("mp", "dp", None),
        P("mp", "dp", None),
        P("mp", "dp", None),
        P("mp", "dp", None),
        P("mp", "dp", None),
        P("mp", "dp", None),
        P("mp", "dp", None),
        P("mp", "dp", None),
        P("mp", "dp", None),
    )
    return jax.shard_map(
        fast_local if dict(mesh.shape) == {"dp": 8, "mp": 4} else local,
        mesh=mesh,
        in_specs=placed,
        out_specs=(
            P("dp", None, None),
            P("dp", None, None),
            P(),
            P(),
            P(),
            P("mp"),
            P("mp"),
            P(),
            P("mp", "dp", None),
            P("mp", "dp", None),
            P("mp", "dp", None),
            P("mp", "dp", None),
            P("mp", "dp", None),
            P("mp", "dp", None),
            P("mp", "dp", None),
            P("mp", "dp", None),
            P("mp", "dp", None),
            P("mp", "dp", None),
        ),
        check_vma=False,
    )


VM = pl.BlockSpec(memory_space=pltpu.VMEM)
SM = pl.BlockSpec(memory_space=pltpu.SMEM)
LIMIT = 60 * 1024 * 1024


def call(body, tables, args, outs, scratch, name):
    return pl.pallas_call(
        body,
        out_shape=[jax.ShapeDtypeStruct(shape, kind) for shape, kind in outs],
        in_specs=[SM] * len(tables) + [VM] * len(args),
        out_specs=[VM] * len(outs),
        scratch_shapes=[pltpu.VMEM(shape, kind) for shape, kind in scratch],
        compiler_params=pltpu.CompilerParams(vmem_limit_bytes=LIMIT),
        name=name,
    )(*tables, *args)


def rel_constants(side):
    rows = np.arange(ROWS)
    lanes = np.arange(896)
    within, along = lanes % 64, lanes // 64
    high = np.where(rows < side * side, rows // side, -1)[:, None]
    wide = np.where(rows < side * side, rows % side, -1)[:, None]
    pick = np.where(within[None] < 32, high == along[None], wide == along[None])
    keys = np.arange(ROWS)
    key_h, key_w = keys // side, keys % side
    offset = np.where(within[:, None] < 32, along[:, None] - key_h[None], along[:, None] - key_w[None]) + side - 1
    spread = (offset == (within % 32)[:, None]) & (keys < side * side)[None]
    return jnp.asarray(pick, BF), jnp.asarray(spread, BF)


def inverse_order(owner):
    count = owner.shape[0]
    at = jnp.arange(count, dtype=jnp.int32)
    return jnp.sum(jnp.where(owner[:, None] == at[None, :], at[:, None], 0), axis=0)


def fast_local(
    tokens, pad_mask, cotangent, norm_gains, norm_biases, out_biases, qkv_bias, up_bias, rel_pos,
    attn_owner, mlp_owner, attn_master, mlp_master, attn_left, attn_right, mlp_left, mlp_right,
    attn_first, attn_second, mlp_first, mlp_second,
):
    t, width = tokens.shape[1:]
    tok, cot = tokens[0], cotangent[0]
    live = jnp.pad(pad_mask[0].astype(F32), (0, ROWS - t))[:, None]
    qb, ub = qkv_bias.reshape(6, SIDE), up_bias.reshape(8, SIDE)
    rel = jnp.pad(rel_pos, ((0, 0), (0, 32 - rel_pos.shape[1]), (0, 0))).reshape(64, SIDE // 2)
    rel_hi, rel_lo = low_parts(jnp.tile(rel, (2, 2)))
    pick, spread = rel_constants((rel_pos.shape[1] + 1) // 2)
    own_a, own_m = attn_owner[0], mlp_owner[0]
    ord_a, ord_m = inverse_order(own_a), inverse_order(own_m)
    xa = jnp.where(own_a < 48, own_a // 6, 8 + (own_a - 48) // 8)
    ya = jnp.where(own_a < 48, own_a % 6, 6 + (own_a - 48) % 8)
    xm, ym = own_m // 8, (own_m // 64) * 8 + own_m % 8

    wire_a, wire_m = call(
        pack_body, (), (attn_master[0], mlp_master[0]),
        [((10, SIDE, 128), BF), ((20, SIDE, 128), BF)], [((2, 8, SIDE, 128), F32)], "pack")
    all_a = gather(wire_a, 0, "gather_attn")

    part, normed, mixed, probs, att = call(
        attn_fwd_body, (ord_a,),
        (tok, live, norm_gains, norm_biases, qb, rel_hi, rel_lo, pick, spread, all_a),
        [((t, width), BF), ((ROWS, width), BF), ((6, ROWS, SIDE), BF), ((4, ROWS, ROWS), F32), ((2, ROWS, SIDE), BF)],
        [((6, 8 * SIDE, SIDE), BF), ((8, 2 * SIDE, SIDE), BF), ((64, SIDE, 32), BF), ((8, ROWS, SIDE), F32)],
        "attn_fwd")
    branch = lax.psum(part, "mp")
    wire_m, mixed = lax.optimization_barrier((wire_m, mixed))
    all_m = gather(wire_m, 1, "gather_mlp")
    part_down, part_second, sec_blocks, act_blocks, gh, go, up_sums = call(
        mlp_body, (ord_m,),
        (tok, live, cot, branch, norm_gains, norm_biases, out_biases, ub, all_m),
        [((t, width), BF), ((t, width), BF)] + [((8, ROWS, SIDE), BF)] * 4 + [((8, SIDE), F32)],
        [((8, 8 * SIDE, SIDE), BF), ((8, 8 * SIDE, SIDE), BF), ((128, SIDE, 32), BF), ((8, ROWS, SIDE), F32), ((ROWS, width), BF)],
        "mlp")
    second_sum = lax.psum(part_second, "mp")
    down_sum = lax.psum(part_down, "mp")

    def mlp_tiles(left_at, right_at, sec, act, gh_ref, go_ref, wire, lefts, rights):
        lefts[0:8], lefts[8:16] = sec[...], act[...]
        rights[0:8], rights[8:16] = gh_ref[...], go_ref[...]
        grad_tiles_body(left_at, right_at, 128, lambda i: lefts[i], lambda i: rights[i], wire)

    stack_m, = call(
        mlp_tiles, (xm, ym), (sec_blocks, act_blocks, gh, go), [((160, SIDE, 128), BF)],
        [((16, ROWS, SIDE), BF)] * 2, "mlp_tiles")
    sum_m = lax.psum_scatter(stack_m, "dp", scatter_dimension=0, tiled=True)
    second_sum, down_sum, stack_m = lax.optimization_barrier((second_sum, down_sum, stack_m))

    block_out, grad_middle, part_normed, rel_part, gm, gb, nb, sums_two, qkv_sums = call(
        mid_back_body, (ord_a,),
        (tok, live, cot, branch, down_sum, second_sum, norm_gains, out_biases, all_a, mixed, probs, normed, att,
         rel_hi, rel_lo, pick, spread),
        [((t, width), BF), ((t, width), F32), ((t, width), BF), ((128, SIDE), F32), ((6, ROWS, SIDE), BF),
         ((8, ROWS, SIDE), BF), ((8, ROWS, SIDE), BF), ((4, width), F32), ((6, SIDE), F32)],
        [((6, 8 * SIDE, SIDE), BF), ((8, 2 * SIDE, SIDE), BF), ((64, SIDE, 32), BF), ((8, ROWS, SIDE), F32),
         ((2, ROWS, SIDE), BF)],
        "mid_back")
    rel_half = SIDE // 2
    rel_fold = rel_part[:64] + rel_part[64:]
    rel_fold = (rel_fold[:, :rel_half] + rel_fold[:, rel_half:]).reshape(2, 32, rel_half)[:, : rel_pos.shape[1]]
    normed_sum = lax.psum(part_normed, "mp")
    rel_sum = lax.psum(rel_fold.astype(BF), "mp").astype(F32)

    def attn_tiles(left_at, right_at, nb_ref, att_ref, gm_ref, gb_ref, wire, lefts, rights):
        lefts[0:8], lefts[8:10] = nb_ref[...], att_ref[...]
        rights[0:6], rights[6:14] = gm_ref[...], gb_ref[...]
        grad_tiles_body(left_at, right_at, 64, lambda i: lefts[i], lambda i: rights[i], wire)

    stack_a, = call(
        attn_tiles, (xa, ya), (nb, att, gm, gb), [((80, SIDE, 128), BF)],
        [((10, ROWS, SIDE), BF), ((14, ROWS, SIDE), BF)], "attn_tiles")
    sum_a = lax.psum_scatter(stack_a, "dp", scatter_dimension=0, tiled=True)
    tokens_grad, sums_one = call(
        token_back_body, (), (tok, live[:t], normed_sum, grad_middle, norm_gains),
        [((t, width), F32), ((2, width), F32)], [], "token_back")
    gains_grad, biases_grad, outb_grad, rel_grad, qkv_grad, up_grad = lax.psum(
        (
            jnp.stack([sums_one[0], sums_two[0]]),
            jnp.stack([sums_one[1], sums_two[1]]),
            jnp.stack([sums_two[3], sums_two[2]]),
            rel_sum,
            qkv_sums.reshape(-1),
            up_sums.reshape(-1),
        ),
        "dp",
    )

    def soap(wire, master, left, right, first, second, name):
        shape = master.shape[1:]
        outs = call(
            soap_body, (), (wire, master[0], left[0], right[0], first[0], second[0]),
            [(shape, F32), (shape, F32), (shape, BF), (shape, F32), (shape, F32)],
            [((2, 8, SIDE, 128), F32)] * 4, name)
        return [value[None] for value in outs]

    mg, mn, mc, mf, ms = soap(sum_m, mlp_master, mlp_left, mlp_right, mlp_first, mlp_second, "soap_mlp")
    ag, an, ac, af, as_ = soap(sum_a, attn_master, attn_left, attn_right, attn_first, attn_second, "soap_attn")
    return (block_out[None], tokens_grad[None], gains_grad, biases_grad, outb_grad, qkv_grad, up_grad, rel_grad,
            ag, mg, an, mn, ac, mc, af, as_, mf, ms)


def solution(mesh):
    return build(mesh)
```

```python
import functools
import math

import jax
import jax.numpy as jnp
import numpy as np
from jax import lax
from jax.experimental import pallas as pl
from jax.experimental.pallas import tpu as pltpu
from jax.sharding import PartitionSpec as P

highest = lax.Precision.HIGHEST
norm_eps = 1e-06
beta_one = 0.9
beta_two = 0.95
adam_eps = 1e-08
learn_rate = 0.02


def untile(tile_rows, row_count, col_count, tile_side):
    shaped = tile_rows.reshape(row_count // tile_side, col_count // tile_side, tile_side, tile_side)
    return shaped.transpose(0, 2, 1, 3).reshape(row_count, col_count)


def retile(matrix, tile_side):
    row_count, col_count = matrix.shape
    shaped = matrix.reshape(row_count // tile_side, tile_side, col_count // tile_side, tile_side)
    return shaped.transpose(0, 2, 1, 3).reshape(-1, tile_side * tile_side)


def rel_onehot(win_side):
    positions = jnp.arange(win_side, dtype=jnp.int32)
    offset = positions[:, None] - positions[None, :] + (win_side - 1)
    entries = jnp.arange(2 * win_side - 1, dtype=jnp.int32)
    return (offset[:, :, None] == entries[None, None, :]).astype(jnp.float32)


def norm_forward(values, norm_gain, norm_shift):
    centre = values - jnp.mean(values, axis=-1, keepdims=True)
    inverse = lax.rsqrt(jnp.mean(centre * centre, axis=-1, keepdims=True) + norm_eps)
    unit_rows = centre * inverse
    return (unit_rows * norm_gain + norm_shift, unit_rows, inverse)


def norm_backward(grad_in, unit_rows, inverse, norm_gain):
    grad_unit = grad_in * norm_gain
    centred = grad_unit - jnp.mean(grad_unit, axis=-1, keepdims=True)
    return inverse * (centred - unit_rows * jnp.mean(grad_unit * unit_rows, axis=-1, keepdims=True))


def gelu_pair(values):
    normal_cdf = 0.5 * (1.0 + lax.erf(values * 0.5**0.5))
    density = jnp.exp(-0.5 * values * values) * (2.0 * math.pi) ** (-0.5)
    return (values * normal_cdf, normal_cdf + values * density)


def soap_step(grad_tiles, master, left_basis, right_basis, first_moment, second_moment):
    tile_side = math.isqrt(grad_tiles.shape[2])
    square = (grad_tiles.shape[0], grad_tiles.shape[1], tile_side, tile_side)
    left_square = left_basis.reshape(square)
    right_square = right_basis.reshape(square)
    half_turn = jnp.einsum(
        "mtji,mtjk->mtik", left_square, grad_tiles.reshape(square), precision=highest
    )
    rotated = jnp.einsum("mtik,mtkl->mtil", half_turn, right_square, precision=highest).reshape(
        grad_tiles.shape
    )
    first_new = beta_one * first_moment + (1.0 - beta_one) * rotated
    second_new = beta_two * second_moment + (1.0 - beta_two) * rotated * rotated
    direction = (first_new / (jnp.sqrt(second_new) + adam_eps)).reshape(square)
    back_half = jnp.einsum("mtij,mtjk->mtik", left_square, direction, precision=highest)
    update = jnp.einsum("mtik,mtlk->mtil", back_half, right_square, precision=highest).reshape(
        grad_tiles.shape
    )
    master_new = master - learn_rate * update
    return (master_new, master_new.astype(jnp.bfloat16), first_new, second_new)


def local(
    tokens,
    pad_mask,
    cotangent,
    norm_gains,
    norm_biases,
    out_biases,
    qkv_bias,
    up_bias,
    rel_pos,
    attn_owner,
    mlp_owner,
    attn_master,
    mlp_master,
    attn_left,
    attn_right,
    mlp_left,
    mlp_right,
    attn_first,
    attn_second,
    mlp_first,
    mlp_second,
):
    windows, win_tokens, model_width = tokens.shape
    row_count = windows * win_tokens
    qkv_cols = qkv_bias.shape[0]
    head_cols = qkv_cols // 3
    unit_cols = up_bias.shape[0]
    head_dim = rel_pos.shape[2]
    heads_here = head_cols // head_dim
    win_side = (rel_pos.shape[1] + 1) // 2
    tile_side = math.isqrt(attn_master.shape[2])
    qkv_count = model_width // tile_side * (qkv_cols // tile_side)
    up_count = model_width // tile_side * (unit_cols // tile_side)
    score_scale = head_dim ** (-0.5)
    attn_stored, mlp_stored = (
        lax.all_gather(attn_master.astype(jnp.bfloat16), "dp", axis=1, tiled=True),
        lax.all_gather(mlp_master.astype(jnp.bfloat16), "dp", axis=1, tiled=True),
    )
    attn_order = jnp.argsort(attn_owner[0])
    mlp_order = jnp.argsort(mlp_owner[0])
    attn_sorted = attn_stored[0][attn_order]
    mlp_sorted = mlp_stored[0][mlp_order]
    w_qkv = untile(attn_sorted[:qkv_count], model_width, qkv_cols, tile_side)
    w_proj = untile(attn_sorted[qkv_count:], head_cols, model_width, tile_side)
    w_up = untile(mlp_sorted[:up_count], model_width, unit_cols, tile_side)
    w_down = untile(mlp_sorted[up_count:], unit_cols, model_width, tile_side)
    onehot = rel_onehot(win_side)
    table_h = jnp.einsum("ijr,rc->ijc", onehot, rel_pos[0], precision=highest)
    table_w = jnp.einsum("ijr,rc->ijc", onehot, rel_pos[1], precision=highest)
    flat_rows = tokens.reshape(row_count, model_width).astype(jnp.float32)
    live_rows = pad_mask.reshape(row_count, 1).astype(jnp.float32)
    normed, unit_one, inverse_one = norm_forward(flat_rows, norm_gains[0], norm_biases[0])
    normed_low = (normed * live_rows).astype(jnp.bfloat16)
    mixed_rows = (jnp.dot(normed_low, w_qkv, preferred_element_type=jnp.float32) + qkv_bias).astype(
        jnp.bfloat16
    )
    head_parts = mixed_rows.reshape(windows, win_tokens, 3, heads_here, head_dim)
    queries = head_parts[:, :, 0]
    key_rows = head_parts[:, :, 1]
    value_rows = head_parts[:, :, 2]
    query_grid = queries.astype(jnp.float32).reshape(
        windows, win_side, win_side, heads_here, head_dim
    )

    def score_rows():
        direct = (
            jnp.einsum("wqhc,wkhc->whqk", queries, key_rows, preferred_element_type=jnp.float32)
            * score_scale
        )
        along_h = jnp.einsum("wabhc,akc->whabk", query_grid, table_h, precision=highest)
        along_w = jnp.einsum("wabhc,blc->whabl", query_grid, table_w, precision=highest)
        return direct + (along_h[..., :, None] + along_w[..., None, :]).reshape(
            windows, heads_here, win_tokens, win_tokens
        )

    scores = score_rows()
    row_top = jnp.max(scores, axis=-1, keepdims=True)
    exponent = jnp.exp(scores - row_top)
    row_total = jnp.sum(exponent, axis=-1, keepdims=True)
    log_total = row_top + jnp.log(row_total)
    probs_low = (exponent / row_total).astype(jnp.bfloat16)
    attended = jnp.einsum(
        "whqk,wkhc->wqhc", probs_low, value_rows, preferred_element_type=jnp.float32
    )
    attended_low = attended.reshape(row_count, head_cols).astype(jnp.bfloat16)
    branch = lax.psum(
        jnp.dot(attended_low, w_proj, preferred_element_type=jnp.float32).astype(jnp.bfloat16), "mp"
    ).astype(jnp.float32)
    middle = flat_rows + branch + out_biases[0]
    second, unit_two, inverse_two = norm_forward(middle, norm_gains[1], norm_biases[1])
    second_low = second.astype(jnp.bfloat16)
    hidden = jnp.dot(second_low, w_up, preferred_element_type=jnp.float32) + up_bias
    active, gelu_slope = gelu_pair(hidden)
    active_low = active.astype(jnp.bfloat16)
    down_sum = lax.psum(
        jnp.dot(active_low, w_down, preferred_element_type=jnp.float32).astype(jnp.bfloat16), "mp"
    ).astype(jnp.float32)
    block_output = (
        ((middle + down_sum + out_biases[1]) * live_rows)
        .astype(jnp.bfloat16)
        .reshape(windows, win_tokens, model_width)
    )
    grad_out = cotangent.reshape(row_count, model_width).astype(jnp.float32) * live_rows
    grad_out_low = grad_out.astype(jnp.bfloat16)
    down_bias_grad = jnp.sum(grad_out, axis=0)
    w_down_grad = jnp.einsum(
        "nf,nd->fd", active_low, grad_out_low, preferred_element_type=jnp.float32
    )
    grad_active = jnp.einsum("nd,fd->nf", grad_out_low, w_down, preferred_element_type=jnp.float32)
    grad_hidden = (grad_active * gelu_slope).astype(jnp.bfloat16)
    up_bias_grad = jnp.sum(grad_hidden.astype(jnp.float32), axis=0)
    w_up_grad = jnp.einsum("nd,nf->df", second_low, grad_hidden, preferred_element_type=jnp.float32)
    mlp_stack = jnp.concatenate(
        [retile(w_up_grad, tile_side), retile(w_down_grad, tile_side)], axis=0
    )[mlp_owner[0]][None]
    grad_second = lax.psum(
        jnp.einsum("nf,df->nd", grad_hidden, w_up, preferred_element_type=jnp.float32).astype(
            jnp.bfloat16
        ),
        "mp",
    ).astype(jnp.float32)
    gain_two_grad = jnp.sum(grad_second * unit_two, axis=0)
    shift_two_grad = jnp.sum(grad_second, axis=0)
    grad_middle = grad_out + norm_backward(grad_second, unit_two, inverse_two, norm_gains[1])
    proj_bias_grad = jnp.sum(grad_middle, axis=0)
    grad_branch = grad_middle.astype(jnp.bfloat16)
    w_proj_grad = jnp.einsum(
        "nc,nd->cd", attended_low, grad_branch, preferred_element_type=jnp.float32
    )
    grad_attended = jnp.einsum("nd,cd->nc", grad_branch, w_proj, preferred_element_type=jnp.float32)
    grad_attended = grad_attended.astype(jnp.bfloat16).reshape(
        windows, win_tokens, heads_here, head_dim
    )
    probs_full = jnp.exp(score_rows() - log_total)
    probs_again = probs_full.astype(jnp.bfloat16)
    grad_probs = jnp.einsum(
        "wqhc,wkhc->whqk", grad_attended, value_rows, preferred_element_type=jnp.float32
    )
    grad_values = jnp.einsum(
        "whqk,wqhc->wkhc", probs_again, grad_attended, preferred_element_type=jnp.float32
    )
    grad_scores = (
        probs_full * (grad_probs - jnp.sum(probs_full * grad_probs, axis=-1, keepdims=True))
    ).astype(jnp.bfloat16)
    grad_queries = (
        jnp.einsum("whqk,wkhc->wqhc", grad_scores, key_rows, preferred_element_type=jnp.float32)
        * score_scale
    )
    grad_keys = (
        jnp.einsum("whqk,wqhc->wkhc", grad_scores, queries, preferred_element_type=jnp.float32)
        * score_scale
    )
    grad_grid = grad_scores.astype(jnp.float32).reshape(
        windows, heads_here, win_side, win_side, win_side, win_side
    )
    grad_h = jnp.sum(grad_grid, axis=5)
    grad_w = jnp.sum(grad_grid, axis=4)
    grad_rel_q = jnp.einsum("whabk,akc->wabhc", grad_h, table_h, precision=highest) + jnp.einsum(
        "whabl,blc->wabhc", grad_w, table_w, precision=highest
    )
    grad_queries = grad_queries + grad_rel_q.reshape(windows, win_tokens, heads_here, head_dim)
    table_h_grad = jnp.einsum("whabk,wabhc->akc", grad_h, query_grid, precision=highest)
    table_w_grad = jnp.einsum("whabl,wabhc->blc", grad_w, query_grid, precision=highest)
    rel_part = jnp.stack(
        [
            jnp.einsum("ijr,ijc->rc", onehot, table_h_grad, precision=highest),
            jnp.einsum("ijr,ijc->rc", onehot, table_w_grad, precision=highest),
        ]
    )
    grad_mixed = (
        jnp.stack([grad_queries, grad_keys, grad_values], axis=2)
        .reshape(row_count, qkv_cols)
        .astype(jnp.bfloat16)
    )
    qkv_bias_grad = jnp.sum(grad_mixed.astype(jnp.float32), axis=0)
    w_qkv_grad = jnp.einsum("nd,nc->dc", normed_low, grad_mixed, preferred_element_type=jnp.float32)
    grad_normed, rel_sum = (
        lax.psum(
            jnp.einsum("nc,dc->nd", grad_mixed, w_qkv, preferred_element_type=jnp.float32).astype(
                jnp.bfloat16
            ),
            "mp",
        ).astype(jnp.float32),
        lax.psum(rel_part.astype(jnp.bfloat16), "mp").astype(jnp.float32),
    )
    grad_normed = grad_normed * live_rows
    gain_one_grad = jnp.sum(grad_normed * unit_one, axis=0)
    shift_one_grad = jnp.sum(grad_normed, axis=0)
    tokens_grad = (
        grad_middle + norm_backward(grad_normed, unit_one, inverse_one, norm_gains[0])
    ).reshape(windows, win_tokens, model_width)
    attn_stack = jnp.concatenate(
        [retile(w_qkv_grad, tile_side), retile(w_proj_grad, tile_side)], axis=0
    )[attn_owner[0]][None]
    attn_grad, mlp_grad = (
        lax.psum_scatter(attn_stack, "dp", scatter_dimension=1, tiled=True),
        lax.psum_scatter(mlp_stack, "dp", scatter_dimension=1, tiled=True),
    )
    gains_grad, biases_grad, out_biases_grad, rel_pos_grad, qkv_bias_total, up_bias_total = (
        lax.psum(
            (
                jnp.stack([gain_one_grad, gain_two_grad]),
                jnp.stack([shift_one_grad, shift_two_grad]),
                jnp.stack([proj_bias_grad, down_bias_grad]),
                rel_sum,
                qkv_bias_grad,
                up_bias_grad,
            ),
            "dp",
        )
    )
    attn_new, attn_copy, attn_first_new, attn_second_new = soap_step(
        attn_grad, attn_master, attn_left, attn_right, attn_first, attn_second
    )
    mlp_new, mlp_copy, mlp_first_new, mlp_second_new = soap_step(
        mlp_grad, mlp_master, mlp_left, mlp_right, mlp_first, mlp_second
    )
    return (
        block_output,
        tokens_grad,
        gains_grad,
        biases_grad,
        out_biases_grad,
        qkv_bias_total,
        up_bias_total,
        rel_pos_grad,
        attn_grad,
        mlp_grad,
        attn_new,
        mlp_new,
        attn_copy,
        mlp_copy,
        attn_first_new,
        attn_second_new,
        mlp_first_new,
        mlp_second_new,
    )


BF = jnp.bfloat16
F32 = jnp.float32
ROWS = 208
SIDE = 160


def dot(a, b):
    return jnp.dot(a, b, preferred_element_type=F32)


def dot_nt(a, b):
    return lax.dot_general(a, b, (((1,), (1,)), ((), ())), preferred_element_type=F32)


def dot_tn(a, b):
    return lax.dot_general(a, b, (((0,), (0,)), ((), ())), preferred_element_type=F32)


def lane_at(shape):
    return lax.broadcasted_iota(jnp.int32, shape, len(shape) - 1)


def low_parts(value):
    high = value.astype(BF)
    return high, (value - high.astype(F32)).astype(BF)


def flat_to_square(read, square, count=8):
    lane = lane_at((8, 128))

    def rows_of(base):
        x = [read(base + 128 * k) for k in range(5)]
        r1 = pltpu.roll(x[1], 96, 1)
        r2 = pltpu.roll(x[2], 96, 1)
        h2 = pltpu.roll(x[2], 64, 1)
        h3 = pltpu.roll(x[3], 64, 1)
        r3 = pltpu.roll(x[3], 32, 1)
        r4 = pltpu.roll(x[4], 32, 1)
        return (
            (x[0], x[1]),
            (jnp.where(lane < 96, r1, r2), r2),
            (jnp.where(lane < 64, h2, h3), h3),
            (jnp.where(lane < 32, r3, r4), r4),
        )

    def body(group, carry):
        base = pl.multiple_of(group * 1280, 128)
        rows = rows_of(base) + rows_of(base + 640)
        for part in range(2):
            stacked = jnp.stack([row[part] for row in rows], axis=0)
            square[part, :, pl.ds(pl.multiple_of(8 * group, 8), 8), :] = jnp.swapaxes(stacked, 0, 1)
        return carry

    lax.fori_loop(0, 20, body, 0)


def square_to_flat(square, write, count=8):
    lane = lane_at((8, 128))

    def body(group, carry):
        at = pl.ds(pl.multiple_of(8 * group, 8), 8)
        wide = jnp.swapaxes(square[0, :, at, :], 0, 1)
        narrow = jnp.swapaxes(square[1, :, at, :], 0, 1)
        for half in range(2):
            base = pl.multiple_of(group * 1280, 128) + 640 * half
            a = [wide[4 * half + m] for m in range(4)]
            b = [narrow[4 * half + m] for m in range(4)]
            a1 = pltpu.roll(a[1], 32, 1)
            b1 = pltpu.roll(b[1], 32, 1)
            a2 = pltpu.roll(a[2], 64, 1)
            b2 = pltpu.roll(b[2], 64, 1)
            a3 = pltpu.roll(a[3], 96, 1)
            b3 = pltpu.roll(b[3], 96, 1)
            write(base, a[0])
            write(base + 128, jnp.where(lane < 32, b[0], a1))
            write(base + 256, jnp.where(lane < 32, a1, jnp.where(lane < 64, b1, a2)))
            write(base + 384, jnp.where(lane < 64, a2, jnp.where(lane < 96, b2, a3)))
            write(base + 512, jnp.where(lane < 96, a3, b3))
        return carry

    lax.fori_loop(0, 20, body, 0)


def pack_eight(source, first, wire, base, square):
    lane = lane_at((SIDE, 128))
    flat_to_square(lambda at: source[first : first + 8, pl.ds(at, 128)], square)
    for half in range(2):
        spare = None
        for q in range(4):
            wire[base + 5 * half + q] = square[0, 4 * half + q].astype(BF)
            piece = square[1, 4 * half + q]
            spare = piece if q == 0 else jnp.where(lane < 32 * q, spare, pltpu.roll(piece, 32 * q, 1))
        wire[base + 5 * half + 4] = spare.astype(BF)


def pack_body(attn, mlp, wire_attn, wire_mlp, square):
    pack_eight(attn, 0, wire_attn, 0, square)
    pack_eight(mlp, 0, wire_mlp, 0, square)
    pack_eight(mlp, 8, wire_mlp, 10, square)


def unpack_narrow(wire, narrow, groups):
    def body(g, carry):
        last = wire[5 * g + 4]
        for q in range(4):
            narrow[4 * g + q] = last[:, 32 * q : 32 * q + 32]
        return carry

    lax.fori_loop(0, groups, body, 0)


def unpack_sorted(wire, narrow, order, base, outs, rows, cols):
    def body(t, carry):
        row = t // cols
        col = t - row * cols
        stored = order[base + t]
        where_at = pl.multiple_of(row * SIDE, 32)
        outs[col, pl.ds(where_at, SIDE), 0:128] = wire[(stored // 4) * 5 + stored % 4]
        outs[col, pl.ds(where_at, SIDE), 128:160] = narrow[stored]
        return carry

    lax.fori_loop(0, rows * cols, body, 0)


MESH_ID = pl.DeviceIdType.MESH


def gather_body(piece, wire, out, send_sem, recv_sem, own_sem):
    count = wire.shape[0]
    pieces = count // piece
    me = lax.axis_index("dp")
    z, x = me // 2, me % 2
    side = me + 1 - 2 * x
    up, down = jnp.minimum(me + 2, 6 + x), jnp.maximum(me - 2, x)

    barrier = pltpu.get_barrier_semaphore()

    def greet(target):
        pl.semaphore_signal(barrier, inc=1, device_id={"dp": target}, device_id_type=MESH_ID)

    greet(side)
    pl.when(z < 3)(lambda: greet(up))
    pl.when(z > 0)(lambda: greet(down))
    inner = (z > 0) & (z < 3)
    pl.when(inner)(lambda: pl.semaphore_wait(barrier, 3))
    pl.when(jnp.logical_not(inner))(lambda: pl.semaphore_wait(barrier, 2))

    def copy(way, target, origin, k, own=False):
        place = out.at[pl.ds(origin * count + piece * k, piece)]
        return pltpu.make_async_remote_copy(
            src_ref=wire.at[pl.ds(piece * k, piece)] if own else place,
            dst_ref=place,
            send_sem=send_sem.at[way, origin // 2, k],
            recv_sem=recv_sem.at[origin, k],
            device_id={"dp": target},
            device_id_type=MESH_ID,
        )

    for k in range(pieces):
        copy(0, side, me, k, True).start()
        pl.when(z < 3)(lambda k=k: copy(1, up, me, k, True).start())
        pl.when(z > 0)(lambda k=k: copy(2, down, me, k, True).start())
    keep = pltpu.make_async_copy(wire, out.at[pl.ds(me * count, count)], own_sem)
    keep.start()

    for d in range(1, 4):
        for k in range(pieces):
            def from_below():
                origin = me - 2 * d
                copy(1, up, origin, k).wait_recv()
                copy(0, side, origin, k).start()
                pl.when(z < 3)(lambda: copy(1, up, origin, k).start())

            def from_above():
                origin = me + 2 * d
                copy(2, down, origin, k).wait_recv()
                copy(0, side, origin, k).start()
                pl.when(z > 0)(lambda: copy(2, down, origin, k).start())

            pl.when(z >= d)(from_below)
            pl.when(z + d <= 3)(from_above)

    keep.wait()
    for k in range(pieces):
        for line in range(4):
            origin = 2 * line + x
            copy(0, side, origin + 1 - 2 * x, k).wait_recv()
            copy(0, side, origin, k, False).wait_send()
            pl.when((line <= z) & (z < 3))(lambda: copy(1, up, origin, k).wait_send())
            pl.when((line >= z) & (z > 0))(lambda: copy(2, down, origin, k).wait_send())


def gather(wire, ident, name, piece=5):
    count = wire.shape[0]
    return pl.pallas_call(
        functools.partial(gather_body, piece),
        out_shape=jax.ShapeDtypeStruct((8 * count,) + wire.shape[1:], wire.dtype),
        in_specs=[VM],
        out_specs=pl.BlockSpec(memory_space=pl.ANY),
        scratch_shapes=[
            pltpu.SemaphoreType.DMA((3, 4, count // piece)),
            pltpu.SemaphoreType.DMA((8, count // piece)),
            pltpu.SemaphoreType.DMA,
        ],
        compiler_params=pltpu.CompilerParams(
            collective_id=ident, has_side_effects=True, vmem_limit_bytes=LIMIT),
        cost_estimate=pl.CostEstimate(flops=0, bytes_accessed=count * 12_000_000, transcendentals=0),
        name=name,
    )(wire)


CHUNK = 5
AHEAD = 4


def scatter_body(stack_a, stack_m, out_a, out_m, inbox_a, inbox_m, half_a, half_m,
                 side_send_a, side_recv_a, line_send_a, line_recv_a,
                 side_send_m, side_recv_m, line_send_m, line_recv_m, own_a, own_m):
    me = lax.axis_index("dp")
    z, x = me // 2, me % 2
    side = me + 1 - 2 * x

    def line_at(j):
        return lax.rem(z + j, 4)

    barrier = pltpu.get_barrier_semaphore()
    for target in (side, 2 * line_at(1) + x, 2 * line_at(2) + x, 2 * line_at(3) + x):
        pl.semaphore_signal(barrier, inc=1, device_id={"dp": target}, device_id_type=MESH_ID)
    pl.semaphore_wait(barrier, 4)

    sets = (
        (stack_a, out_a, inbox_a, half_a, side_send_a, side_recv_a, line_send_a, line_recv_a, own_a),
        (stack_m, out_m, inbox_m, half_m, side_send_m, side_recv_m, line_send_m, line_recv_m, own_m),
    )
    steps = [(part, j, k) for part in range(2) for j in (1, 2, 3, 4) for k in range(sets[part][0].shape[0] // 8 // CHUNK)]

    def to_side(part, j, k):
        stack, _, inbox, _, send, recv, _, _, _ = sets[part]
        count = stack.shape[0] // 8
        line = line_at(j)
        return pltpu.make_async_remote_copy(
            src_ref=stack.at[pl.ds((2 * line + 1 - x) * count + CHUNK * k, CHUNK)],
            dst_ref=inbox.at[pl.ds(line * count + CHUNK * k, CHUNK)],
            send_sem=send.at[j - 1, k], recv_sem=recv.at[j - 1, k],
            device_id={"dp": side}, device_id_type=MESH_ID)

    def to_line(part, j, k):
        stack, out, _, half, _, _, send, recv, _ = sets[part]
        count = stack.shape[0] // 8
        line = line_at(j)
        return pltpu.make_async_remote_copy(
            src_ref=half.at[pl.ds(line * count + CHUNK * k, CHUNK)],
            dst_ref=out.at[pl.ds(z * count + CHUNK * k, CHUNK)],
            send_sem=send.at[j - 1, k], recv_sem=recv.at[j - 1, k],
            device_id={"dp": 2 * line + x}, device_id_type=MESH_ID)

    for step in steps[:AHEAD]:
        to_side(*step).start()
    keeps = []
    for at, (part, j, k) in enumerate(steps):
        stack, out, inbox, half, _, _, _, _, own = sets[part]
        count = stack.shape[0] // 8
        to_side(part, j, k).wait_recv()
        if at + AHEAD < len(steps):
            to_side(*steps[at + AHEAD]).start()
        line = line_at(j)

        def add(i, carry):
            to = line * count + CHUNK * k + i
            total = stack[(2 * line + x) * count + CHUNK * k + i].astype(F32) + inbox[to].astype(F32)
            half[to] = total.astype(BF)
            return carry

        lax.fori_loop(0, CHUNK, add, 0)
        if j < 4:
            to_line(part, j, k).start()
        else:
            place = pl.ds(line * count + CHUNK * k, CHUNK)
            keep = pltpu.make_async_copy(half.at[place], out.at[place], own.at[k])
            keep.start()
            keeps.append(keep)
    for part, j, k in steps:
        to_side(part, j, k).wait_send()
        if j < 4:
            to_line(part, j, k).wait_send()
            to_line(part, j, k).wait_recv()
    for keep in keeps:
        keep.wait()


def scatter(stack_a, stack_m, ident, name):
    shapes = [(4 * (stack.shape[0] // 8),) + stack.shape[1:] for stack in (stack_a, stack_m)]
    sems = []
    for stack in (stack_a, stack_m):
        sems += [pltpu.SemaphoreType.DMA((4, stack.shape[0] // 8 // CHUNK))] * 4
    sems += [pltpu.SemaphoreType.DMA((stack.shape[0] // 8 // CHUNK,)) for stack in (stack_a, stack_m)]
    return pl.pallas_call(
        scatter_body,
        out_shape=[jax.ShapeDtypeStruct(shape, BF) for shape in shapes],
        in_specs=[VM, VM],
        out_specs=[pl.BlockSpec(memory_space=pl.ANY)] * 2,
        scratch_shapes=[pltpu.VMEM(shape, BF) for shape in shapes + shapes] + sems,
        compiler_params=pltpu.CompilerParams(
            collective_id=ident, has_side_effects=True, vmem_limit_bytes=LIMIT),
        cost_estimate=pl.CostEstimate(flops=0, bytes_accessed=350_000_000, transcendentals=0),
        name=name,
    )(stack_a, stack_m)


def norm_parts(x):
    mean = jnp.mean(x, axis=-1, keepdims=True)
    centre = x - mean
    inverse = lax.rsqrt(jnp.mean(centre * centre, axis=-1, keepdims=True) + norm_eps)
    return centre * inverse, inverse


def norm_back(grad_in, unit, inverse, gain):
    w = grad_in * gain
    return inverse * (
        w - jnp.mean(w, axis=-1, keepdims=True) - unit * jnp.mean(w * unit, axis=-1, keepdims=True)
    )


def padded(ref, rows, kind=F32):
    value = ref[...].astype(kind)
    return jnp.concatenate([value, jnp.zeros((ROWS - rows, value.shape[1]), kind)], axis=0)


def attn_forward(mixed, rel_hi, rel_lo, pick, spread, probs, att, scale, tokens_here):
    lane = lane_at((ROWS, SIDE))
    key_ok = lane_at((ROWS, ROWS)) < tokens_here
    head = SIDE // 2
    for p in range(2):
        q, k, v = mixed[p], mixed[2 + p], mixed[4 + p]
        parts = []
        for h in range(2):
            mine = (lane >= head) if h else (lane < head)
            qm = jnp.where(mine, q, jnp.zeros_like(q))
            s = dot_nt(qm, k) * scale
            a_hi, a_lo = low_parts(dot_nt(qm, rel_hi[...]) + dot_nt(qm, rel_lo[...]))
            for c in range(7):
                mask = pick[:, 128 * c : 128 * c + 128]
                table = spread[128 * c : 128 * c + 128, :]
                s = s + dot(a_hi * mask, table) + dot(a_lo * mask, table)
            s = jnp.where(key_ok, s, -1e30)
            top = jnp.max(s, axis=-1, keepdims=True)
            e = jnp.exp(s - top)
            pr = e / jnp.sum(e, axis=-1, keepdims=True)
            probs[2 * p + h] = pr
            parts.append(dot(pr.astype(BF), v))
        att[p] = jnp.where(lane < head, parts[0], parts[1]).astype(BF)


def attn_backward(mixed, rel_hi, rel_lo, pick, spread, probs, gatt, gm, rel_out, scale):
    lane = lane_at((ROWS, SIDE))
    head = SIDE // 2
    for p in range(2):
        q, k, v = mixed[p], mixed[2 + p], mixed[4 + p]
        ga = gatt[p]
        dq, dk, dv, dr = [], [], [], []
        for h in range(2):
            mine = (lane >= head) if h else (lane < head)
            pr = probs[2 * p + h]
            gam = jnp.where(mine, ga, jnp.zeros_like(ga))
            gp = dot_nt(gam, v)
            dv.append(dot_tn(pr.astype(BF), ga))
            ds = (pr * (gp - jnp.sum(pr * gp, axis=-1, keepdims=True))).astype(BF)
            da = None
            for c in range(7):
                term = dot_nt(ds, spread[128 * c : 128 * c + 128, :]) * pick[:, 128 * c : 128 * c + 128].astype(F32)
                da = term if da is None else da + term
            da_hi, da_lo = low_parts(da)
            relq = dot(da_hi, rel_hi[...]) + dot(da_lo, rel_hi[...]) + dot(da_hi, rel_lo[...])
            dq.append(dot(ds, k) * scale + relq)
            dk.append(dot_tn(ds, q) * scale)
            dr.append(dot_tn(da_hi, q) + dot_tn(da_lo, q))
        gm[p] = jnp.where(lane < head, dq[0], dq[1]).astype(BF)
        gm[2 + p] = jnp.where(lane < head, dk[0], dk[1]).astype(BF)
        gm[4 + p] = jnp.where(lane < head, dv[0], dv[1]).astype(BF)
        rel = jnp.where(lane_at((128, SIDE)) < head, dr[0], dr[1])
        if p == 0:
            rel_out[...] = rel
        else:
            rel_out[...] += rel


def attn_fwd_body(order, tokens, live, gains, biases, qkv_bias, rel_hi, rel_lo, pick, spread, wire,
                  part, normed, mixed, probs, att, w_qkv, w_proj, narrow, block):
    t = tokens.shape[0]
    x = padded(tokens, t)
    unit, _ = norm_parts(x)
    normed[...] = ((unit * gains[0:1, :] + biases[0:1, :]) * live[...]).astype(BF)
    unpack_narrow(wire, narrow, wire.shape[0] // 5)
    unpack_sorted(wire, narrow, order, 0, w_qkv, 8, 6)
    unpack_sorted(wire, narrow, order, 48, w_proj, 2, 8)

    def mix(j, carry):
        mixed[j] = (dot(normed[...], w_qkv[j]) + qkv_bias[pl.ds(j, 1), :]).astype(BF)
        return carry

    lax.fori_loop(0, 6, mix, 0)
    attn_forward(mixed, rel_hi, rel_lo, pick, spread, probs, att, (SIDE // 2) ** -0.5, t)

    def project(n, carry):
        value = dot(att[0], w_proj[n, 0:SIDE, :]) + dot(att[1], w_proj[n, SIDE : 2 * SIDE, :])
        block[n] = value
        return carry

    lax.fori_loop(0, 8, project, 0)
    for n in range(8):
        part[:, SIDE * n : SIDE * n + SIDE] = block[n][0:t, :].astype(BF)


def mlp_body(order, tokens, live, cotangent, branch, gains, biases, out_biases, up_bias, wire,
             part_down, part_second, sec_blocks, act_blocks, gh, go, bias_sums, w_up, w_down, narrow, block, second):
    t = tokens.shape[0]
    x = padded(tokens, t)
    middle = x + padded(branch, t) + out_biases[0:1, :]
    unit, _ = norm_parts(middle)
    second[...] = (unit * gains[1:2, :] + biases[1:2, :]).astype(BF)
    grad_out = padded(cotangent, t) * live[...]
    for n in range(8):
        sec_blocks[n] = second[:, SIDE * n : SIDE * n + SIDE]
        go[n] = grad_out[:, SIDE * n : SIDE * n + SIDE].astype(BF)
    unpack_narrow(wire, narrow, wire.shape[0] // 5)
    unpack_sorted(wire, narrow, order, 0, w_up, 8, 8)
    unpack_sorted(wire, narrow, order, 64, w_down, 8, 8)

    def hidden_block(j, carry):
        row = pl.multiple_of(j * SIDE, 32)
        hid = dot(second[...], w_up[j]) + up_bias[pl.ds(j, 1), :]
        cdf = 0.5 * (1.0 + lax.erf(hid * 0.5**0.5))
        slope = cdf + hid * (jnp.exp(-0.5 * hid * hid) * (2.0 * math.pi) ** -0.5)
        act_blocks[j] = (hid * cdf).astype(BF)
        ga = dot_nt(go[0], w_down[0, pl.ds(row, SIDE), :])
        for n in range(1, 8):
            ga = ga + dot_nt(go[n], w_down[n, pl.ds(row, SIDE), :])
        low = (ga * slope).astype(BF)
        gh[j] = low
        bias_sums[pl.ds(j, 1), :] = jnp.sum(low.astype(F32), axis=0, keepdims=True)
        return carry

    lax.fori_loop(0, 8, hidden_block, 0)

    def second_back(i, carry):
        row = pl.multiple_of(i * SIDE, 32)
        value = dot_nt(gh[0], w_up[0, pl.ds(row, SIDE), :])
        for j in range(1, 8):
            value = value + dot_nt(gh[j], w_up[j, pl.ds(row, SIDE), :])
        block[i] = value
        return carry

    lax.fori_loop(0, 8, second_back, 0)
    for n in range(8):
        part_second[:, SIDE * n : SIDE * n + SIDE] = block[n][0:t, :].astype(BF)

    def down(n, carry):
        value = dot(act_blocks[0], w_down[n, 0:SIDE, :])
        for j in range(1, 8):
            value = value + dot(act_blocks[j], w_down[n, j * SIDE : (j + 1) * SIDE, :])
        block[n] = value
        return carry

    lax.fori_loop(0, 8, down, 0)
    for n in range(8):
        part_down[:, SIDE * n : SIDE * n + SIDE] = block[n][0:t, :].astype(BF)


def grad_tiles_body(left_at, right_at, count, read_left, read_right, wire):
    lane = lane_at((SIDE, 128))

    def body(g, carry):
        spare = None
        for q in range(4):
            s = 4 * g + q
            tile = dot_tn(read_left(left_at[s]), read_right(right_at[s]))
            wire[5 * g + q] = tile[:, 0:128].astype(BF)
            piece = jnp.concatenate([tile[:, 128:160], jnp.zeros((SIDE, 96), F32)], axis=1)
            spare = piece if q == 0 else jnp.where(lane < 32 * q, spare, pltpu.roll(piece, 32 * q, 1))
        wire[5 * g + 4] = spare.astype(BF)
        return carry

    lax.fori_loop(0, count // 4, body, 0)


def mid_back_body(order, tokens, live, cotangent, branch, down_sum, second_sum, gains, out_biases,
                  wire, mixed, probs, normed, att, rel_hi, rel_lo, pick, spread,
                  block_out, grad_middle_out, part_normed, rel_out, gm, gb, nb, sums, bias_sums,
                  w_qkv, w_proj, narrow, block, gatt):
    t = tokens.shape[0]
    x = padded(tokens, t)
    middle = x + padded(branch, t) + out_biases[0:1, :]
    result = (middle + padded(down_sum, t) + out_biases[1:2, :]) * live[...]
    block_out[...] = result[0:t, :].astype(BF)
    grad_out = padded(cotangent, t) * live[...]
    unit, inverse = norm_parts(middle)
    grad_second = padded(second_sum, t)
    sums[0:1, :] = jnp.sum(grad_second * unit, axis=0, keepdims=True)
    sums[1:2, :] = jnp.sum(grad_second, axis=0, keepdims=True)
    sums[2:3, :] = jnp.sum(grad_out, axis=0, keepdims=True)
    grad_middle = grad_out + norm_back(grad_second, unit, inverse, gains[1:2, :])
    sums[3:4, :] = jnp.sum(grad_middle, axis=0, keepdims=True)
    grad_middle_out[...] = grad_middle[0:t, :]
    for n in range(8):
        gb[n] = grad_middle[:, SIDE * n : SIDE * n + SIDE].astype(BF)
        nb[n] = normed[:, SIDE * n : SIDE * n + SIDE]
    unpack_narrow(wire, narrow, wire.shape[0] // 5)
    unpack_sorted(wire, narrow, order, 0, w_qkv, 8, 6)
    unpack_sorted(wire, narrow, order, 48, w_proj, 2, 8)
    for p in range(2):
        value = dot_nt(gb[0], w_proj[0, p * SIDE : (p + 1) * SIDE, :])
        for n in range(1, 8):
            value = value + dot_nt(gb[n], w_proj[n, p * SIDE : (p + 1) * SIDE, :])
        gatt[p] = value.astype(BF)
    attn_backward(mixed, rel_hi, rel_lo, pick, spread, probs, gatt, gm, rel_out, (SIDE // 2) ** -0.5)
    for j in range(6):
        bias_sums[j : j + 1, :] = jnp.sum(gm[j].astype(F32), axis=0, keepdims=True)

    def normed_back(i, carry):
        row = pl.multiple_of(i * SIDE, 32)
        value = dot_nt(gm[0], w_qkv[0, pl.ds(row, SIDE), :])
        for j in range(1, 6):
            value = value + dot_nt(gm[j], w_qkv[j, pl.ds(row, SIDE), :])
        block[i] = value
        return carry

    lax.fori_loop(0, 8, normed_back, 0)
    for n in range(8):
        part_normed[:, SIDE * n : SIDE * n + SIDE] = block[n][0:t, :].astype(BF)


def token_back_body(tokens, live, normed_sum, grad_middle, gains, tokens_grad, sums):
    x = tokens[...].astype(F32)
    unit, inverse = norm_parts(x)
    grad_normed = normed_sum[...].astype(F32) * live[...]
    sums[0:1, :] = jnp.sum(grad_normed * unit, axis=0, keepdims=True)
    sums[1:2, :] = jnp.sum(grad_normed, axis=0, keepdims=True)
    tokens_grad[...] = grad_middle[...] + norm_back(grad_normed, unit, inverse, gains[0:1, :])


def square_tile(square, t):
    return jnp.concatenate([square[0, t], square[1, t, :, 0:32]], axis=1)


def put_tile(square, t, value):
    square[0, t] = value[:, 0:128]
    square[1, t, :, 0:32] = value[:, 128:160]


def split_dot(kind, a, b):
    a_hi, a_lo = low_parts(a)
    b_hi, b_lo = low_parts(b)
    return kind(a_hi, b_hi) + (kind(a_hi, b_lo) + kind(a_lo, b_hi))


def soap_group(r0, grad_square, master, left, right, first, second,
               grad_out, new_out, copy_out, first_out, second_out, sq_left, sq_right, sq_work):
    rows = slice(r0, r0 + 8)

    def writer(ref):
        def write(at, value):
            ref[rows, pl.ds(at, 128)] = value
        return write

    flat_to_square(lambda at: left[rows, pl.ds(at, 128)], sq_left, 8)
    flat_to_square(lambda at: right[rows, pl.ds(at, 128)], sq_right, 8)
    square_to_flat(grad_square, writer(grad_out), 8)

    def rotate(t, carry):
        l, r = square_tile(sq_left, t), square_tile(sq_right, t)
        half = split_dot(dot_tn, l, square_tile(grad_square, t))
        put_tile(sq_work, t, split_dot(dot, half, r))
        return carry

    lax.fori_loop(0, 8, rotate, 0)

    def moments(at, rotated):
        cols = pl.ds(at, 128)
        f = beta_one * first[rows, cols] + (1.0 - beta_one) * rotated
        s = beta_two * second[rows, cols] + (1.0 - beta_two) * rotated * rotated
        first_out[rows, cols] = f
        second_out[rows, cols] = s
        new_out[rows, cols] = f / (jnp.sqrt(s) + adam_eps)

    square_to_flat(sq_work, moments, 8)
    flat_to_square(lambda at: new_out[rows, pl.ds(at, 128)], sq_work, 8)

    def turn_back(t, carry):
        l, r = square_tile(sq_left, t), square_tile(sq_right, t)
        half = split_dot(dot, l, square_tile(sq_work, t))
        put_tile(sq_work, t, split_dot(dot_nt, half, r))
        return carry

    lax.fori_loop(0, 8, turn_back, 0)

    def finish(at, update):
        cols = pl.ds(at, 128)
        value = master[rows, cols] - learn_rate * update
        new_out[rows, cols] = value
        copy_out[rows, cols] = value.astype(BF)

    square_to_flat(sq_work, finish, 8)


def soap_body(wire, master, left, right, first, second,
              grad_out, new_out, copy_out, first_out, second_out, sq_grad, sq_left, sq_right, sq_work):
    count = wire.shape[0] // 4
    for r in range(master.shape[0] // 8):
        for half in range(2):
            def total(i):
                w = [wire[p * count + i].astype(F32) for p in range(4)]
                return (w[0] + w[1]) + (w[2] + w[3])

            last = total(5 * (2 * r + half) + 4)
            for q in range(4):
                sq_grad[0, 4 * half + q] = total(5 * (2 * r + half) + q)
                sq_grad[1, 4 * half + q] = last if q == 0 else pltpu.roll(last, 128 - 32 * q, 1)
        soap_group(8 * r, sq_grad, master, left, right, first, second,
                   grad_out, new_out, copy_out, first_out, second_out, sq_left, sq_right, sq_work)


def build(mesh):
    placed = (
        P("dp", None, None),
        P("dp", None),
        P("dp", None, None),
        P(),
        P(),
        P(),
        P("mp"),
        P("mp"),
        P(),
        P("mp", None),
        P("mp", None),
        P("mp", "dp", None),
        P("mp", "dp", None),
        P("mp", "dp", None),
        P("mp", "dp", None),
        P("mp", "dp", None),
        P("mp", "dp", None),
        P("mp", "dp", None),
        P("mp", "dp", None),
        P("mp", "dp", None),
        P("mp", "dp", None),
    )
    return jax.shard_map(
        fast_local if dict(mesh.shape) == {"dp": 8, "mp": 4} else local,
        mesh=mesh,
        in_specs=placed,
        out_specs=(
            P("dp", None, None),
            P("dp", None, None),
            P(),
            P(),
            P(),
            P("mp"),
            P("mp"),
            P(),
            P("mp", "dp", None),
            P("mp", "dp", None),
            P("mp", "dp", None),
            P("mp", "dp", None),
            P("mp", "dp", None),
            P("mp", "dp", None),
            P("mp", "dp", None),
            P("mp", "dp", None),
            P("mp", "dp", None),
            P("mp", "dp", None),
        ),
        check_vma=False,
    )


VM = pl.BlockSpec(memory_space=pltpu.VMEM)
SM = pl.BlockSpec(memory_space=pltpu.SMEM)
LIMIT = 60 * 1024 * 1024


def call(body, tables, args, outs, scratch, name):
    return pl.pallas_call(
        body,
        out_shape=[jax.ShapeDtypeStruct(shape, kind) for shape, kind in outs],
        in_specs=[SM] * len(tables) + [VM] * len(args),
        out_specs=[VM] * len(outs),
        scratch_shapes=[pltpu.VMEM(shape, kind) for shape, kind in scratch],
        compiler_params=pltpu.CompilerParams(vmem_limit_bytes=LIMIT),
        name=name,
    )(*tables, *args)


def rel_constants(side):
    rows = np.arange(ROWS)
    lanes = np.arange(896)
    within, along = lanes % 64, lanes // 64
    high = np.where(rows < side * side, rows // side, -1)[:, None]
    wide = np.where(rows < side * side, rows % side, -1)[:, None]
    pick = np.where(within[None] < 32, high == along[None], wide == along[None])
    keys = np.arange(ROWS)
    key_h, key_w = keys // side, keys % side
    offset = np.where(within[:, None] < 32, along[:, None] - key_h[None], along[:, None] - key_w[None]) + side - 1
    spread = (offset == (within % 32)[:, None]) & (keys < side * side)[None]
    return jnp.asarray(pick, BF), jnp.asarray(spread, BF)


def inverse_order(owner):
    count = owner.shape[0]
    at = jnp.arange(count, dtype=jnp.int32)
    return jnp.sum(jnp.where(owner[:, None] == at[None, :], at[:, None], 0), axis=0)


def fast_local(
    tokens, pad_mask, cotangent, norm_gains, norm_biases, out_biases, qkv_bias, up_bias, rel_pos,
    attn_owner, mlp_owner, attn_master, mlp_master, attn_left, attn_right, mlp_left, mlp_right,
    attn_first, attn_second, mlp_first, mlp_second,
):
    t, width = tokens.shape[1:]
    tok, cot = tokens[0], cotangent[0]
    live = jnp.pad(pad_mask[0].astype(F32), (0, ROWS - t))[:, None]
    qb, ub = qkv_bias.reshape(6, SIDE), up_bias.reshape(8, SIDE)
    rel = jnp.pad(rel_pos, ((0, 0), (0, 32 - rel_pos.shape[1]), (0, 0))).reshape(64, SIDE // 2)
    rel_hi, rel_lo = low_parts(jnp.tile(rel, (2, 2)))
    pick, spread = rel_constants((rel_pos.shape[1] + 1) // 2)
    own_a, own_m = attn_owner[0], mlp_owner[0]
    ord_a, ord_m = inverse_order(own_a), inverse_order(own_m)
    xa = jnp.where(own_a < 48, own_a // 6, 8 + (own_a - 48) // 8)
    ya = jnp.where(own_a < 48, own_a % 6, 6 + (own_a - 48) % 8)
    xm, ym = own_m // 8, (own_m // 64) * 8 + own_m % 8

    wire_a, wire_m = call(
        pack_body, (), (attn_master[0], mlp_master[0]),
        [((10, SIDE, 128), BF), ((20, SIDE, 128), BF)], [((2, 8, SIDE, 128), F32)], "pack")
    all_a = gather(wire_a, 0, "gather_attn")

    part, normed, mixed, probs, att = call(
        attn_fwd_body, (ord_a,),
        (tok, live, norm_gains, norm_biases, qb, rel_hi, rel_lo, pick, spread, all_a),
        [((t, width), BF), ((ROWS, width), BF), ((6, ROWS, SIDE), BF), ((4, ROWS, ROWS), F32), ((2, ROWS, SIDE), BF)],
        [((6, 8 * SIDE, SIDE), BF), ((8, 2 * SIDE, SIDE), BF), ((64, SIDE, 32), BF), ((8, ROWS, SIDE), F32)],
        "attn_fwd")
    branch = lax.psum(part, "mp")
    wire_m, mixed = lax.optimization_barrier((wire_m, mixed))
    all_m = gather(wire_m, 1, "gather_mlp")
    part_down, part_second, sec_blocks, act_blocks, gh, go, up_sums = call(
        mlp_body, (ord_m,),
        (tok, live, cot, branch, norm_gains, norm_biases, out_biases, ub, all_m),
        [((t, width), BF), ((t, width), BF)] + [((8, ROWS, SIDE), BF)] * 4 + [((8, SIDE), F32)],
        [((8, 8 * SIDE, SIDE), BF), ((8, 8 * SIDE, SIDE), BF), ((128, SIDE, 32), BF), ((8, ROWS, SIDE), F32), ((ROWS, width), BF)],
        "mlp")
    second_sum = lax.psum(part_second, "mp")
    down_sum = lax.psum(part_down, "mp")

    def mlp_tiles(left_at, right_at, sec, act, gh_ref, go_ref, wire, lefts, rights):
        lefts[0:8], lefts[8:16] = sec[...], act[...]
        rights[0:8], rights[8:16] = gh_ref[...], go_ref[...]
        grad_tiles_body(left_at, right_at, 128, lambda i: lefts[i], lambda i: rights[i], wire)

    stack_m, = call(
        mlp_tiles, (xm, ym), (sec_blocks, act_blocks, gh, go), [((160, SIDE, 128), BF)],
        [((16, ROWS, SIDE), BF)] * 2, "mlp_tiles")
    second_sum, down_sum, stack_m = lax.optimization_barrier((second_sum, down_sum, stack_m))

    block_out, grad_middle, part_normed, rel_part, gm, gb, nb, sums_two, qkv_sums = call(
        mid_back_body, (ord_a,),
        (tok, live, cot, branch, down_sum, second_sum, norm_gains, out_biases, all_a, mixed, probs, normed, att,
         rel_hi, rel_lo, pick, spread),
        [((t, width), BF), ((t, width), F32), ((t, width), BF), ((128, SIDE), F32), ((6, ROWS, SIDE), BF),
         ((8, ROWS, SIDE), BF), ((8, ROWS, SIDE), BF), ((4, width), F32), ((6, SIDE), F32)],
        [((6, 8 * SIDE, SIDE), BF), ((8, 2 * SIDE, SIDE), BF), ((64, SIDE, 32), BF), ((8, ROWS, SIDE), F32),
         ((2, ROWS, SIDE), BF)],
        "mid_back")
    rel_half = SIDE // 2
    rel_fold = rel_part[:64] + rel_part[64:]
    rel_fold = (rel_fold[:, :rel_half] + rel_fold[:, rel_half:]).reshape(2, 32, rel_half)[:, : rel_pos.shape[1]]
    rel_size = rel_fold.size
    rel_rows = -(-rel_size // width)
    rel_flat = jnp.pad(rel_fold.reshape(-1).astype(BF), (0, rel_rows * width - rel_size)).reshape(rel_rows, width)
    both_sum = lax.psum(jnp.concatenate([part_normed, rel_flat], axis=0), "mp")

    def attn_tiles(left_at, right_at, nb_ref, att_ref, gm_ref, gb_ref, wire, lefts, rights):
        lefts[0:8], lefts[8:10] = nb_ref[...], att_ref[...]
        rights[0:6], rights[6:14] = gm_ref[...], gb_ref[...]
        grad_tiles_body(left_at, right_at, 64, lambda i: lefts[i], lambda i: rights[i], wire)

    stack_a, = call(
        attn_tiles, (xa, ya), (nb, att, gm, gb), [((80, SIDE, 128), BF)],
        [((10, ROWS, SIDE), BF), ((14, ROWS, SIDE), BF)], "attn_tiles")
    sum_a, sum_m = scatter(stack_a, stack_m, 2, "scatter")
    both_sum, sum_a = lax.optimization_barrier((both_sum, sum_a))
    normed_sum, rel_sum = both_sum[:t], both_sum[t:].reshape(-1)[:rel_size].astype(F32)
    tokens_grad, sums_one = call(
        token_back_body, (), (tok, live[:t], normed_sum, grad_middle, norm_gains),
        [((t, width), F32), ((2, width), F32)], [], "token_back")
    small = [sums_one.reshape(-1), sums_two.reshape(-1), qkv_sums.reshape(-1), up_sums.reshape(-1), rel_sum]
    edges = np.cumsum([0] + [v.shape[0] for v in small])
    lines = -(-int(edges[-1]) // 1024) * 8
    small = jnp.pad(jnp.concatenate(small), (0, lines * 128 - int(edges[-1]))).reshape(1, lines, 128)
    total = jnp.sum(gather(small, 3, "gather_sums", 1), axis=0).reshape(-1)
    one, two, qkv_grad, up_grad, rel_grad = [total[edges[i]:edges[i + 1]] for i in range(5)]
    one, two = one.reshape(2, width), two.reshape(4, width)
    gains_grad = jnp.stack([one[0], two[0]])
    biases_grad = jnp.stack([one[1], two[1]])
    outb_grad = jnp.stack([two[3], two[2]])
    rel_grad = rel_grad.reshape(rel_pos.shape)

    def soap(wire, master, left, right, first, second, name):
        shape = master.shape[1:]
        outs = call(
            soap_body, (), (wire, master[0], left[0], right[0], first[0], second[0]),
            [(shape, F32), (shape, F32), (shape, BF), (shape, F32), (shape, F32)],
            [((2, 8, SIDE, 128), F32)] * 4, name)
        return [value[None] for value in outs]

    mg, mn, mc, mf, ms = soap(sum_m, mlp_master, mlp_left, mlp_right, mlp_first, mlp_second, "soap_mlp")
    ag, an, ac, af, as_ = soap(sum_a, attn_master, attn_left, attn_right, attn_first, attn_second, "soap_attn")
    return (block_out[None], tokens_grad[None], gains_grad, biases_grad, outb_grad, qkv_grad, up_grad, rel_grad,
            ag, mg, an, mn, ac, mc, af, as_, mf, ms)


def solution(mesh):
    return build(mesh)
```

```python
import functools
import math

import jax
import jax.numpy as jnp
import numpy as np
from jax import lax
from jax.experimental import pallas as pl
from jax.experimental.pallas import tpu as pltpu
from jax.sharding import PartitionSpec as P

highest = lax.Precision.HIGHEST
norm_eps = 1e-06
beta_one = 0.9
beta_two = 0.95
adam_eps = 1e-08
learn_rate = 0.02


def untile(tile_rows, row_count, col_count, tile_side):
    shaped = tile_rows.reshape(row_count // tile_side, col_count // tile_side, tile_side, tile_side)
    return shaped.transpose(0, 2, 1, 3).reshape(row_count, col_count)


def retile(matrix, tile_side):
    row_count, col_count = matrix.shape
    shaped = matrix.reshape(row_count // tile_side, tile_side, col_count // tile_side, tile_side)
    return shaped.transpose(0, 2, 1, 3).reshape(-1, tile_side * tile_side)


def rel_onehot(win_side):
    positions = jnp.arange(win_side, dtype=jnp.int32)
    offset = positions[:, None] - positions[None, :] + (win_side - 1)
    entries = jnp.arange(2 * win_side - 1, dtype=jnp.int32)
    return (offset[:, :, None] == entries[None, None, :]).astype(jnp.float32)


def norm_forward(values, norm_gain, norm_shift):
    centre = values - jnp.mean(values, axis=-1, keepdims=True)
    inverse = lax.rsqrt(jnp.mean(centre * centre, axis=-1, keepdims=True) + norm_eps)
    unit_rows = centre * inverse
    return (unit_rows * norm_gain + norm_shift, unit_rows, inverse)


def norm_backward(grad_in, unit_rows, inverse, norm_gain):
    grad_unit = grad_in * norm_gain
    centred = grad_unit - jnp.mean(grad_unit, axis=-1, keepdims=True)
    return inverse * (centred - unit_rows * jnp.mean(grad_unit * unit_rows, axis=-1, keepdims=True))


def gelu_pair(values):
    normal_cdf = 0.5 * (1.0 + lax.erf(values * 0.5**0.5))
    density = jnp.exp(-0.5 * values * values) * (2.0 * math.pi) ** (-0.5)
    return (values * normal_cdf, normal_cdf + values * density)


def soap_step(grad_tiles, master, left_basis, right_basis, first_moment, second_moment):
    tile_side = math.isqrt(grad_tiles.shape[2])
    square = (grad_tiles.shape[0], grad_tiles.shape[1], tile_side, tile_side)
    left_square = left_basis.reshape(square)
    right_square = right_basis.reshape(square)
    half_turn = jnp.einsum(
        "mtji,mtjk->mtik", left_square, grad_tiles.reshape(square), precision=highest
    )
    rotated = jnp.einsum("mtik,mtkl->mtil", half_turn, right_square, precision=highest).reshape(
        grad_tiles.shape
    )
    first_new = beta_one * first_moment + (1.0 - beta_one) * rotated
    second_new = beta_two * second_moment + (1.0 - beta_two) * rotated * rotated
    direction = (first_new / (jnp.sqrt(second_new) + adam_eps)).reshape(square)
    back_half = jnp.einsum("mtij,mtjk->mtik", left_square, direction, precision=highest)
    update = jnp.einsum("mtik,mtlk->mtil", back_half, right_square, precision=highest).reshape(
        grad_tiles.shape
    )
    master_new = master - learn_rate * update
    return (master_new, master_new.astype(jnp.bfloat16), first_new, second_new)


def local(
    tokens,
    pad_mask,
    cotangent,
    norm_gains,
    norm_biases,
    out_biases,
    qkv_bias,
    up_bias,
    rel_pos,
    attn_owner,
    mlp_owner,
    attn_master,
    mlp_master,
    attn_left,
    attn_right,
    mlp_left,
    mlp_right,
    attn_first,
    attn_second,
    mlp_first,
    mlp_second,
):
    windows, win_tokens, model_width = tokens.shape
    row_count = windows * win_tokens
    qkv_cols = qkv_bias.shape[0]
    head_cols = qkv_cols // 3
    unit_cols = up_bias.shape[0]
    head_dim = rel_pos.shape[2]
    heads_here = head_cols // head_dim
    win_side = (rel_pos.shape[1] + 1) // 2
    tile_side = math.isqrt(attn_master.shape[2])
    qkv_count = model_width // tile_side * (qkv_cols // tile_side)
    up_count = model_width // tile_side * (unit_cols // tile_side)
    score_scale = head_dim ** (-0.5)
    attn_stored, mlp_stored = (
        lax.all_gather(attn_master.astype(jnp.bfloat16), "dp", axis=1, tiled=True),
        lax.all_gather(mlp_master.astype(jnp.bfloat16), "dp", axis=1, tiled=True),
    )
    attn_order = jnp.argsort(attn_owner[0])
    mlp_order = jnp.argsort(mlp_owner[0])
    attn_sorted = attn_stored[0][attn_order]
    mlp_sorted = mlp_stored[0][mlp_order]
    w_qkv = untile(attn_sorted[:qkv_count], model_width, qkv_cols, tile_side)
    w_proj = untile(attn_sorted[qkv_count:], head_cols, model_width, tile_side)
    w_up = untile(mlp_sorted[:up_count], model_width, unit_cols, tile_side)
    w_down = untile(mlp_sorted[up_count:], unit_cols, model_width, tile_side)
    onehot = rel_onehot(win_side)
    table_h = jnp.einsum("ijr,rc->ijc", onehot, rel_pos[0], precision=highest)
    table_w = jnp.einsum("ijr,rc->ijc", onehot, rel_pos[1], precision=highest)
    flat_rows = tokens.reshape(row_count, model_width).astype(jnp.float32)
    live_rows = pad_mask.reshape(row_count, 1).astype(jnp.float32)
    normed, unit_one, inverse_one = norm_forward(flat_rows, norm_gains[0], norm_biases[0])
    normed_low = (normed * live_rows).astype(jnp.bfloat16)
    mixed_rows = (jnp.dot(normed_low, w_qkv, preferred_element_type=jnp.float32) + qkv_bias).astype(
        jnp.bfloat16
    )
    head_parts = mixed_rows.reshape(windows, win_tokens, 3, heads_here, head_dim)
    queries = head_parts[:, :, 0]
    key_rows = head_parts[:, :, 1]
    value_rows = head_parts[:, :, 2]
    query_grid = queries.astype(jnp.float32).reshape(
        windows, win_side, win_side, heads_here, head_dim
    )

    def score_rows():
        direct = (
            jnp.einsum("wqhc,wkhc->whqk", queries, key_rows, preferred_element_type=jnp.float32)
            * score_scale
        )
        along_h = jnp.einsum("wabhc,akc->whabk", query_grid, table_h, precision=highest)
        along_w = jnp.einsum("wabhc,blc->whabl", query_grid, table_w, precision=highest)
        return direct + (along_h[..., :, None] + along_w[..., None, :]).reshape(
            windows, heads_here, win_tokens, win_tokens
        )

    scores = score_rows()
    row_top = jnp.max(scores, axis=-1, keepdims=True)
    exponent = jnp.exp(scores - row_top)
    row_total = jnp.sum(exponent, axis=-1, keepdims=True)
    log_total = row_top + jnp.log(row_total)
    probs_low = (exponent / row_total).astype(jnp.bfloat16)
    attended = jnp.einsum(
        "whqk,wkhc->wqhc", probs_low, value_rows, preferred_element_type=jnp.float32
    )
    attended_low = attended.reshape(row_count, head_cols).astype(jnp.bfloat16)
    branch = lax.psum(
        jnp.dot(attended_low, w_proj, preferred_element_type=jnp.float32).astype(jnp.bfloat16), "mp"
    ).astype(jnp.float32)
    middle = flat_rows + branch + out_biases[0]
    second, unit_two, inverse_two = norm_forward(middle, norm_gains[1], norm_biases[1])
    second_low = second.astype(jnp.bfloat16)
    hidden = jnp.dot(second_low, w_up, preferred_element_type=jnp.float32) + up_bias
    active, gelu_slope = gelu_pair(hidden)
    active_low = active.astype(jnp.bfloat16)
    down_sum = lax.psum(
        jnp.dot(active_low, w_down, preferred_element_type=jnp.float32).astype(jnp.bfloat16), "mp"
    ).astype(jnp.float32)
    block_output = (
        ((middle + down_sum + out_biases[1]) * live_rows)
        .astype(jnp.bfloat16)
        .reshape(windows, win_tokens, model_width)
    )
    grad_out = cotangent.reshape(row_count, model_width).astype(jnp.float32) * live_rows
    grad_out_low = grad_out.astype(jnp.bfloat16)
    down_bias_grad = jnp.sum(grad_out, axis=0)
    w_down_grad = jnp.einsum(
        "nf,nd->fd", active_low, grad_out_low, preferred_element_type=jnp.float32
    )
    grad_active = jnp.einsum("nd,fd->nf", grad_out_low, w_down, preferred_element_type=jnp.float32)
    grad_hidden = (grad_active * gelu_slope).astype(jnp.bfloat16)
    up_bias_grad = jnp.sum(grad_hidden.astype(jnp.float32), axis=0)
    w_up_grad = jnp.einsum("nd,nf->df", second_low, grad_hidden, preferred_element_type=jnp.float32)
    mlp_stack = jnp.concatenate(
        [retile(w_up_grad, tile_side), retile(w_down_grad, tile_side)], axis=0
    )[mlp_owner[0]][None]
    grad_second = lax.psum(
        jnp.einsum("nf,df->nd", grad_hidden, w_up, preferred_element_type=jnp.float32).astype(
            jnp.bfloat16
        ),
        "mp",
    ).astype(jnp.float32)
    gain_two_grad = jnp.sum(grad_second * unit_two, axis=0)
    shift_two_grad = jnp.sum(grad_second, axis=0)
    grad_middle = grad_out + norm_backward(grad_second, unit_two, inverse_two, norm_gains[1])
    proj_bias_grad = jnp.sum(grad_middle, axis=0)
    grad_branch = grad_middle.astype(jnp.bfloat16)
    w_proj_grad = jnp.einsum(
        "nc,nd->cd", attended_low, grad_branch, preferred_element_type=jnp.float32
    )
    grad_attended = jnp.einsum("nd,cd->nc", grad_branch, w_proj, preferred_element_type=jnp.float32)
    grad_attended = grad_attended.astype(jnp.bfloat16).reshape(
        windows, win_tokens, heads_here, head_dim
    )
    probs_full = jnp.exp(score_rows() - log_total)
    probs_again = probs_full.astype(jnp.bfloat16)
    grad_probs = jnp.einsum(
        "wqhc,wkhc->whqk", grad_attended, value_rows, preferred_element_type=jnp.float32
    )
    grad_values = jnp.einsum(
        "whqk,wqhc->wkhc", probs_again, grad_attended, preferred_element_type=jnp.float32
    )
    grad_scores = (
        probs_full * (grad_probs - jnp.sum(probs_full * grad_probs, axis=-1, keepdims=True))
    ).astype(jnp.bfloat16)
    grad_queries = (
        jnp.einsum("whqk,wkhc->wqhc", grad_scores, key_rows, preferred_element_type=jnp.float32)
        * score_scale
    )
    grad_keys = (
        jnp.einsum("whqk,wqhc->wkhc", grad_scores, queries, preferred_element_type=jnp.float32)
        * score_scale
    )
    grad_grid = grad_scores.astype(jnp.float32).reshape(
        windows, heads_here, win_side, win_side, win_side, win_side
    )
    grad_h = jnp.sum(grad_grid, axis=5)
    grad_w = jnp.sum(grad_grid, axis=4)
    grad_rel_q = jnp.einsum("whabk,akc->wabhc", grad_h, table_h, precision=highest) + jnp.einsum(
        "whabl,blc->wabhc", grad_w, table_w, precision=highest
    )
    grad_queries = grad_queries + grad_rel_q.reshape(windows, win_tokens, heads_here, head_dim)
    table_h_grad = jnp.einsum("whabk,wabhc->akc", grad_h, query_grid, precision=highest)
    table_w_grad = jnp.einsum("whabl,wabhc->blc", grad_w, query_grid, precision=highest)
    rel_part = jnp.stack(
        [
            jnp.einsum("ijr,ijc->rc", onehot, table_h_grad, precision=highest),
            jnp.einsum("ijr,ijc->rc", onehot, table_w_grad, precision=highest),
        ]
    )
    grad_mixed = (
        jnp.stack([grad_queries, grad_keys, grad_values], axis=2)
        .reshape(row_count, qkv_cols)
        .astype(jnp.bfloat16)
    )
    qkv_bias_grad = jnp.sum(grad_mixed.astype(jnp.float32), axis=0)
    w_qkv_grad = jnp.einsum("nd,nc->dc", normed_low, grad_mixed, preferred_element_type=jnp.float32)
    grad_normed, rel_sum = (
        lax.psum(
            jnp.einsum("nc,dc->nd", grad_mixed, w_qkv, preferred_element_type=jnp.float32).astype(
                jnp.bfloat16
            ),
            "mp",
        ).astype(jnp.float32),
        lax.psum(rel_part.astype(jnp.bfloat16), "mp").astype(jnp.float32),
    )
    grad_normed = grad_normed * live_rows
    gain_one_grad = jnp.sum(grad_normed * unit_one, axis=0)
    shift_one_grad = jnp.sum(grad_normed, axis=0)
    tokens_grad = (
        grad_middle + norm_backward(grad_normed, unit_one, inverse_one, norm_gains[0])
    ).reshape(windows, win_tokens, model_width)
    attn_stack = jnp.concatenate(
        [retile(w_qkv_grad, tile_side), retile(w_proj_grad, tile_side)], axis=0
    )[attn_owner[0]][None]
    attn_grad, mlp_grad = (
        lax.psum_scatter(attn_stack, "dp", scatter_dimension=1, tiled=True),
        lax.psum_scatter(mlp_stack, "dp", scatter_dimension=1, tiled=True),
    )
    gains_grad, biases_grad, out_biases_grad, rel_pos_grad, qkv_bias_total, up_bias_total = (
        lax.psum(
            (
                jnp.stack([gain_one_grad, gain_two_grad]),
                jnp.stack([shift_one_grad, shift_two_grad]),
                jnp.stack([proj_bias_grad, down_bias_grad]),
                rel_sum,
                qkv_bias_grad,
                up_bias_grad,
            ),
            "dp",
        )
    )
    attn_new, attn_copy, attn_first_new, attn_second_new = soap_step(
        attn_grad, attn_master, attn_left, attn_right, attn_first, attn_second
    )
    mlp_new, mlp_copy, mlp_first_new, mlp_second_new = soap_step(
        mlp_grad, mlp_master, mlp_left, mlp_right, mlp_first, mlp_second
    )
    return (
        block_output,
        tokens_grad,
        gains_grad,
        biases_grad,
        out_biases_grad,
        qkv_bias_total,
        up_bias_total,
        rel_pos_grad,
        attn_grad,
        mlp_grad,
        attn_new,
        mlp_new,
        attn_copy,
        mlp_copy,
        attn_first_new,
        attn_second_new,
        mlp_first_new,
        mlp_second_new,
    )


BF = jnp.bfloat16
F32 = jnp.float32
ROWS = 208
SIDE = 160


def dot(a, b):
    return jnp.dot(a, b, preferred_element_type=F32)


def dot_nt(a, b):
    return lax.dot_general(a, b, (((1,), (1,)), ((), ())), preferred_element_type=F32)


def dot_tn(a, b):
    return lax.dot_general(a, b, (((0,), (0,)), ((), ())), preferred_element_type=F32)


def lane_at(shape):
    return lax.broadcasted_iota(jnp.int32, shape, len(shape) - 1)


def low_parts(value):
    high = value.astype(BF)
    return high, (value - high.astype(F32)).astype(BF)


def flat_to_square(read, square, count=8):
    lane = lane_at((8, 128))

    def rows_of(base):
        x = [read(base + 128 * k) for k in range(5)]
        r1 = pltpu.roll(x[1], 96, 1)
        r2 = pltpu.roll(x[2], 96, 1)
        h2 = pltpu.roll(x[2], 64, 1)
        h3 = pltpu.roll(x[3], 64, 1)
        r3 = pltpu.roll(x[3], 32, 1)
        r4 = pltpu.roll(x[4], 32, 1)
        return (
            (x[0], x[1]),
            (jnp.where(lane < 96, r1, r2), r2),
            (jnp.where(lane < 64, h2, h3), h3),
            (jnp.where(lane < 32, r3, r4), r4),
        )

    def body(group, carry):
        base = pl.multiple_of(group * 1280, 128)
        rows = rows_of(base) + rows_of(base + 640)
        for part in range(2):
            stacked = jnp.stack([row[part] for row in rows], axis=0)
            square[part, :, pl.ds(pl.multiple_of(8 * group, 8), 8), :] = jnp.swapaxes(stacked, 0, 1)
        return carry

    lax.fori_loop(0, 20, body, 0)


def square_to_flat(square, write, count=8):
    lane = lane_at((8, 128))

    def body(group, carry):
        at = pl.ds(pl.multiple_of(8 * group, 8), 8)
        wide = jnp.swapaxes(square[0, :, at, :], 0, 1)
        narrow = jnp.swapaxes(square[1, :, at, :], 0, 1)
        for half in range(2):
            base = pl.multiple_of(group * 1280, 128) + 640 * half
            a = [wide[4 * half + m] for m in range(4)]
            b = [narrow[4 * half + m] for m in range(4)]
            a1 = pltpu.roll(a[1], 32, 1)
            b1 = pltpu.roll(b[1], 32, 1)
            a2 = pltpu.roll(a[2], 64, 1)
            b2 = pltpu.roll(b[2], 64, 1)
            a3 = pltpu.roll(a[3], 96, 1)
            b3 = pltpu.roll(b[3], 96, 1)
            write(base, a[0])
            write(base + 128, jnp.where(lane < 32, b[0], a1))
            write(base + 256, jnp.where(lane < 32, a1, jnp.where(lane < 64, b1, a2)))
            write(base + 384, jnp.where(lane < 64, a2, jnp.where(lane < 96, b2, a3)))
            write(base + 512, jnp.where(lane < 96, a3, b3))
        return carry

    lax.fori_loop(0, 20, body, 0)


def pack_eight(source, first, wire, base, square):
    lane = lane_at((SIDE, 128))
    flat_to_square(lambda at: source[first : first + 8, pl.ds(at, 128)], square)
    for half in range(2):
        spare = None
        for q in range(4):
            wire[base + 5 * half + q] = square[0, 4 * half + q].astype(BF)
            piece = square[1, 4 * half + q]
            spare = piece if q == 0 else jnp.where(lane < 32 * q, spare, pltpu.roll(piece, 32 * q, 1))
        wire[base + 5 * half + 4] = spare.astype(BF)


def pack_body(attn, mlp, wire_attn, wire_mlp, square):
    pack_eight(attn, 0, wire_attn, 0, square)
    pack_eight(mlp, 0, wire_mlp, 0, square)
    pack_eight(mlp, 8, wire_mlp, 10, square)


def unpack_narrow(wire, narrow, groups):
    def body(g, carry):
        last = wire[5 * g + 4]
        for q in range(4):
            narrow[4 * g + q] = last[:, 32 * q : 32 * q + 32]
        return carry

    lax.fori_loop(0, groups, body, 0)


def unpack_sorted(wire, narrow, order, base, outs, rows, cols):
    def body(t, carry):
        row = t // cols
        col = t - row * cols
        stored = order[base + t]
        where_at = pl.multiple_of(row * SIDE, 32)
        outs[col, pl.ds(where_at, SIDE), 0:128] = wire[(stored // 4) * 5 + stored % 4]
        outs[col, pl.ds(where_at, SIDE), 128:160] = narrow[stored]
        return carry

    lax.fori_loop(0, rows * cols, body, 0)


MESH_ID = pl.DeviceIdType.MESH


def gather_body(piece, wire, out, send_sem, recv_sem, own_sem):
    count = wire.shape[0]
    pieces = count // piece
    me = lax.axis_index("dp")
    z, x = me // 2, me % 2
    side = me + 1 - 2 * x
    up, down = jnp.minimum(me + 2, 6 + x), jnp.maximum(me - 2, x)

    barrier = pltpu.get_barrier_semaphore()

    def greet(target):
        pl.semaphore_signal(barrier, inc=1, device_id={"dp": target}, device_id_type=MESH_ID)

    greet(side)
    pl.when(z < 3)(lambda: greet(up))
    pl.when(z > 0)(lambda: greet(down))
    inner = (z > 0) & (z < 3)
    pl.when(inner)(lambda: pl.semaphore_wait(barrier, 3))
    pl.when(jnp.logical_not(inner))(lambda: pl.semaphore_wait(barrier, 2))

    def copy(way, target, origin, k, own=False):
        place = out.at[pl.ds(origin * count + piece * k, piece)]
        return pltpu.make_async_remote_copy(
            src_ref=wire.at[pl.ds(piece * k, piece)] if own else place,
            dst_ref=place,
            send_sem=send_sem.at[way, origin // 2, k],
            recv_sem=recv_sem.at[origin, k],
            device_id={"dp": target},
            device_id_type=MESH_ID,
        )

    for k in range(pieces):
        copy(0, side, me, k, True).start()
        pl.when(z < 3)(lambda k=k: copy(1, up, me, k, True).start())
        pl.when(z > 0)(lambda k=k: copy(2, down, me, k, True).start())
    keep = pltpu.make_async_copy(wire, out.at[pl.ds(me * count, count)], own_sem)
    keep.start()

    for d in range(1, 4):
        for k in range(pieces):
            def from_below():
                origin = me - 2 * d
                copy(1, up, origin, k).wait_recv()
                copy(0, side, origin, k).start()
                pl.when(z < 3)(lambda: copy(1, up, origin, k).start())

            def from_above():
                origin = me + 2 * d
                copy(2, down, origin, k).wait_recv()
                copy(0, side, origin, k).start()
                pl.when(z > 0)(lambda: copy(2, down, origin, k).start())

            pl.when(z >= d)(from_below)
            pl.when(z + d <= 3)(from_above)

    keep.wait()
    for k in range(pieces):
        for line in range(4):
            origin = 2 * line + x
            copy(0, side, origin + 1 - 2 * x, k).wait_recv()
            copy(0, side, origin, k, False).wait_send()
            pl.when((line <= z) & (z < 3))(lambda: copy(1, up, origin, k).wait_send())
            pl.when((line >= z) & (z > 0))(lambda: copy(2, down, origin, k).wait_send())


def gather(wire, ident, name, piece=5):
    count = wire.shape[0]
    return pl.pallas_call(
        functools.partial(gather_body, piece),
        out_shape=jax.ShapeDtypeStruct((8 * count,) + wire.shape[1:], wire.dtype),
        in_specs=[VM],
        out_specs=pl.BlockSpec(memory_space=pl.ANY),
        scratch_shapes=[
            pltpu.SemaphoreType.DMA((3, 4, count // piece)),
            pltpu.SemaphoreType.DMA((8, count // piece)),
            pltpu.SemaphoreType.DMA,
        ],
        compiler_params=pltpu.CompilerParams(
            collective_id=ident, has_side_effects=True, vmem_limit_bytes=LIMIT),
        cost_estimate=pl.CostEstimate(flops=0, bytes_accessed=count * 12_000_000, transcendentals=0),
        name=name,
    )(wire)


CHUNK = 5
AHEAD = 4


def scatter_steps(stack, out, inbox, half, side_send, side_recv, line_send, line_recv, own, units):
    me = lax.axis_index("dp")
    z, x = me // 2, me % 2
    side = me + 1 - 2 * x
    count = stack.shape[0] // 8

    def line_at(j):
        return lax.rem(z + j, 4)

    barrier = pltpu.get_barrier_semaphore()
    for target in (side, 2 * line_at(1) + x, 2 * line_at(2) + x, 2 * line_at(3) + x):
        pl.semaphore_signal(barrier, inc=1, device_id={"dp": target}, device_id_type=MESH_ID)
    pl.semaphore_wait(barrier, 4)
    steps = [(j, k) for j in (1, 2, 3, 4) for k in range(count // CHUNK)]

    def to_side(j, k):
        line = line_at(j)
        return pltpu.make_async_remote_copy(
            src_ref=stack.at[pl.ds((2 * line + 1 - x) * count + CHUNK * k, CHUNK)],
            dst_ref=inbox.at[pl.ds(line * count + CHUNK * k, CHUNK)],
            send_sem=side_send.at[j - 1, k], recv_sem=side_recv.at[j - 1, k],
            device_id={"dp": side}, device_id_type=MESH_ID)

    def to_line(j, k):
        line = line_at(j)
        return pltpu.make_async_remote_copy(
            src_ref=half.at[pl.ds(line * count + CHUNK * k, CHUNK)],
            dst_ref=out.at[pl.ds(z * count + CHUNK * k, CHUNK)],
            send_sem=line_send.at[j - 1, k], recv_sem=line_recv.at[j - 1, k],
            device_id={"dp": 2 * line + x}, device_id_type=MESH_ID)

    for step in steps[:AHEAD]:
        to_side(*step).start()
    keeps = []
    units = list(units)
    for at, (j, k) in enumerate(steps):
        if units:
            units.pop(0)()
        to_side(j, k).wait_recv()
        if at + AHEAD < len(steps):
            to_side(*steps[at + AHEAD]).start()
        line = line_at(j)

        def add(i, carry):
            to = line * count + CHUNK * k + i
            total = stack[(2 * line + x) * count + CHUNK * k + i].astype(F32) + inbox[to].astype(F32)
            half[to] = total.astype(BF)
            return carry

        lax.fori_loop(0, CHUNK, add, 0)
        if j < 4:
            to_line(j, k).start()
        else:
            place = pl.ds(line * count + CHUNK * k, CHUNK)
            keep = pltpu.make_async_copy(half.at[place], out.at[place], own.at[k])
            keep.start()
            keeps.append(keep)
    for unit in units:
        unit()
    for j, k in steps:
        to_side(j, k).wait_send()
        if j < 4:
            to_line(j, k).wait_send()
            to_line(j, k).wait_recv()
    for keep in keeps:
        keep.wait()


def scatter_call(body, stack, args, outs, scratch, ident, cost, name):
    count = stack.shape[0] // 8
    shape = (4 * count,) + stack.shape[1:]
    pieces = count // CHUNK
    return pl.pallas_call(
        body,
        out_shape=[jax.ShapeDtypeStruct(shape, BF)] + [jax.ShapeDtypeStruct(*out) for out in outs],
        in_specs=[VM] * (1 + len(args)),
        out_specs=[pl.BlockSpec(memory_space=pl.ANY)] + [VM] * len(outs),
        scratch_shapes=[pltpu.VMEM(shape, BF)] * 2 + [pltpu.SemaphoreType.DMA((4, pieces))] * 4
        + [pltpu.SemaphoreType.DMA((pieces,))] + [pltpu.VMEM(*item) for item in scratch],
        compiler_params=pltpu.CompilerParams(
            collective_id=ident, has_side_effects=True, vmem_limit_bytes=LIMIT),
        cost_estimate=pl.CostEstimate(flops=0, bytes_accessed=cost, transcendentals=0),
        name=name,
    )(stack, *args)


def scatter_mlp_body(stack, left_m, right_m, left_a, right_a, out, sq_left_m, sq_right_m, sq_left_a, sq_right_a, *wires):
    units = []
    for flat, square in ((left_m, sq_left_m), (right_m, sq_right_m), (left_a, sq_left_a), (right_a, sq_right_a)):
        for g in range(square.shape[0]):
            units.append(lambda f=flat, r=8 * g, sq=square, g=g: flat_to_square(
                lambda at: f[r : r + 8, pl.ds(at, 128)], sq.at[g]))
    scatter_steps(stack, out, *wires, units)


def scatter_attn_body(stack, wire, sq_left, sq_right, master, first, second,
                      out, grad_out, new_out, copy_out, first_out, second_out, *rest):
    wires, (sq_grad, sq_work) = rest[:-2], rest[-2:]
    units = []
    for g in range(2):
        units += soap_units(g, g, wire, sq_left, sq_right, master, first, second,
                            grad_out, new_out, copy_out, first_out, second_out, sq_grad, sq_work)
    scatter_steps(stack, out, *wires, units)


def norm_parts(x):
    mean = jnp.mean(x, axis=-1, keepdims=True)
    centre = x - mean
    inverse = lax.rsqrt(jnp.mean(centre * centre, axis=-1, keepdims=True) + norm_eps)
    return centre * inverse, inverse


def norm_back(grad_in, unit, inverse, gain):
    w = grad_in * gain
    return inverse * (
        w - jnp.mean(w, axis=-1, keepdims=True) - unit * jnp.mean(w * unit, axis=-1, keepdims=True)
    )


def padded(ref, rows, kind=F32):
    value = ref[...].astype(kind)
    return jnp.concatenate([value, jnp.zeros((ROWS - rows, value.shape[1]), kind)], axis=0)


def attn_forward(mixed, rel_hi, rel_lo, pick, spread, probs, att, scale, tokens_here):
    lane = lane_at((ROWS, SIDE))
    key_ok = lane_at((ROWS, ROWS)) < tokens_here
    head = SIDE // 2
    for p in range(2):
        q, k, v = mixed[p], mixed[2 + p], mixed[4 + p]
        parts = []
        for h in range(2):
            mine = (lane >= head) if h else (lane < head)
            qm = jnp.where(mine, q, jnp.zeros_like(q))
            s = dot_nt(qm, k) * scale
            a_hi, a_lo = low_parts(dot_nt(qm, rel_hi[...]) + dot_nt(qm, rel_lo[...]))
            for c in range(7):
                mask = pick[:, 128 * c : 128 * c + 128]
                table = spread[128 * c : 128 * c + 128, :]
                s = s + dot(a_hi * mask, table) + dot(a_lo * mask, table)
            s = jnp.where(key_ok, s, -1e30)
            top = jnp.max(s, axis=-1, keepdims=True)
            e = jnp.exp(s - top)
            pr = e / jnp.sum(e, axis=-1, keepdims=True)
            probs[2 * p + h] = pr
            parts.append(dot(pr.astype(BF), v))
        att[p] = jnp.where(lane < head, parts[0], parts[1]).astype(BF)


def attn_backward(mixed, rel_hi, rel_lo, pick, spread, probs, gatt, gm, rel_out, scale):
    lane = lane_at((ROWS, SIDE))
    head = SIDE // 2
    for p in range(2):
        q, k, v = mixed[p], mixed[2 + p], mixed[4 + p]
        ga = gatt[p]
        dq, dk, dv, dr = [], [], [], []
        for h in range(2):
            mine = (lane >= head) if h else (lane < head)
            pr = probs[2 * p + h]
            gam = jnp.where(mine, ga, jnp.zeros_like(ga))
            gp = dot_nt(gam, v)
            dv.append(dot_tn(pr.astype(BF), ga))
            ds = (pr * (gp - jnp.sum(pr * gp, axis=-1, keepdims=True))).astype(BF)
            da = None
            for c in range(7):
                term = dot_nt(ds, spread[128 * c : 128 * c + 128, :]) * pick[:, 128 * c : 128 * c + 128].astype(F32)
                da = term if da is None else da + term
            da_hi, da_lo = low_parts(da)
            relq = dot(da_hi, rel_hi[...]) + dot(da_lo, rel_hi[...]) + dot(da_hi, rel_lo[...])
            dq.append(dot(ds, k) * scale + relq)
            dk.append(dot_tn(ds, q) * scale)
            dr.append(dot_tn(da_hi, q) + dot_tn(da_lo, q))
        gm[p] = jnp.where(lane < head, dq[0], dq[1]).astype(BF)
        gm[2 + p] = jnp.where(lane < head, dk[0], dk[1]).astype(BF)
        gm[4 + p] = jnp.where(lane < head, dv[0], dv[1]).astype(BF)
        rel = jnp.where(lane_at((128, SIDE)) < head, dr[0], dr[1])
        if p == 0:
            rel_out[...] = rel
        else:
            rel_out[...] += rel


def attn_fwd_body(order, tokens, live, gains, biases, qkv_bias, rel_hi, rel_lo, pick, spread, wire,
                  part, normed, mixed, probs, att, w_qkv, w_proj, narrow, block):
    t = tokens.shape[0]
    x = padded(tokens, t)
    unit, _ = norm_parts(x)
    normed[...] = ((unit * gains[0:1, :] + biases[0:1, :]) * live[...]).astype(BF)
    unpack_narrow(wire, narrow, wire.shape[0] // 5)
    unpack_sorted(wire, narrow, order, 0, w_qkv, 8, 6)
    unpack_sorted(wire, narrow, order, 48, w_proj, 2, 8)

    def mix(j, carry):
        mixed[j] = (dot(normed[...], w_qkv[j]) + qkv_bias[pl.ds(j, 1), :]).astype(BF)
        return carry

    lax.fori_loop(0, 6, mix, 0)
    attn_forward(mixed, rel_hi, rel_lo, pick, spread, probs, att, (SIDE // 2) ** -0.5, t)

    def project(n, carry):
        value = dot(att[0], w_proj[n, 0:SIDE, :]) + dot(att[1], w_proj[n, SIDE : 2 * SIDE, :])
        block[n] = value
        return carry

    lax.fori_loop(0, 8, project, 0)
    for n in range(8):
        part[:, SIDE * n : SIDE * n + SIDE] = block[n][0:t, :].astype(BF)


def mlp_body(order, tokens, live, cotangent, branch, gains, biases, out_biases, up_bias, wire,
             part_down, part_second, sec_blocks, act_blocks, gh, go, bias_sums, w_up, w_down, narrow, block, second):
    t = tokens.shape[0]
    x = padded(tokens, t)
    middle = x + padded(branch, t) + out_biases[0:1, :]
    unit, _ = norm_parts(middle)
    second[...] = (unit * gains[1:2, :] + biases[1:2, :]).astype(BF)
    grad_out = padded(cotangent, t) * live[...]
    for n in range(8):
        sec_blocks[n] = second[:, SIDE * n : SIDE * n + SIDE]
        go[n] = grad_out[:, SIDE * n : SIDE * n + SIDE].astype(BF)
    unpack_narrow(wire, narrow, wire.shape[0] // 5)
    unpack_sorted(wire, narrow, order, 0, w_up, 8, 8)
    unpack_sorted(wire, narrow, order, 64, w_down, 8, 8)

    def hidden_block(j, carry):
        row = pl.multiple_of(j * SIDE, 32)
        hid = dot(second[...], w_up[j]) + up_bias[pl.ds(j, 1), :]
        cdf = 0.5 * (1.0 + lax.erf(hid * 0.5**0.5))
        slope = cdf + hid * (jnp.exp(-0.5 * hid * hid) * (2.0 * math.pi) ** -0.5)
        act_blocks[j] = (hid * cdf).astype(BF)
        ga = dot_nt(go[0], w_down[0, pl.ds(row, SIDE), :])
        for n in range(1, 8):
            ga = ga + dot_nt(go[n], w_down[n, pl.ds(row, SIDE), :])
        low = (ga * slope).astype(BF)
        gh[j] = low
        bias_sums[pl.ds(j, 1), :] = jnp.sum(low.astype(F32), axis=0, keepdims=True)
        return carry

    lax.fori_loop(0, 8, hidden_block, 0)

    def second_back(i, carry):
        row = pl.multiple_of(i * SIDE, 32)
        value = dot_nt(gh[0], w_up[0, pl.ds(row, SIDE), :])
        for j in range(1, 8):
            value = value + dot_nt(gh[j], w_up[j, pl.ds(row, SIDE), :])
        block[i] = value
        return carry

    lax.fori_loop(0, 8, second_back, 0)
    for n in range(8):
        part_second[:, SIDE * n : SIDE * n + SIDE] = block[n][0:t, :].astype(BF)

    def down(n, carry):
        value = dot(act_blocks[0], w_down[n, 0:SIDE, :])
        for j in range(1, 8):
            value = value + dot(act_blocks[j], w_down[n, j * SIDE : (j + 1) * SIDE, :])
        block[n] = value
        return carry

    lax.fori_loop(0, 8, down, 0)
    for n in range(8):
        part_down[:, SIDE * n : SIDE * n + SIDE] = block[n][0:t, :].astype(BF)


def grad_tiles_body(left_at, right_at, count, read_left, read_right, wire):
    lane = lane_at((SIDE, 128))

    def body(g, carry):
        spare = None
        for q in range(4):
            s = 4 * g + q
            tile = dot_tn(read_left(left_at[s]), read_right(right_at[s]))
            wire[5 * g + q] = tile[:, 0:128].astype(BF)
            piece = jnp.concatenate([tile[:, 128:160], jnp.zeros((SIDE, 96), F32)], axis=1)
            spare = piece if q == 0 else jnp.where(lane < 32 * q, spare, pltpu.roll(piece, 32 * q, 1))
        wire[5 * g + 4] = spare.astype(BF)
        return carry

    lax.fori_loop(0, count // 4, body, 0)


def mid_back_body(order, tokens, live, cotangent, branch, down_sum, second_sum, gains, out_biases,
                  wire, mixed, probs, normed, att, rel_hi, rel_lo, pick, spread,
                  block_out, grad_middle_out, part_normed, rel_out, gm, gb, nb, sums, bias_sums,
                  w_qkv, w_proj, narrow, block, gatt):
    t = tokens.shape[0]
    x = padded(tokens, t)
    middle = x + padded(branch, t) + out_biases[0:1, :]
    result = (middle + padded(down_sum, t) + out_biases[1:2, :]) * live[...]
    block_out[...] = result[0:t, :].astype(BF)
    grad_out = padded(cotangent, t) * live[...]
    unit, inverse = norm_parts(middle)
    grad_second = padded(second_sum, t)
    sums[0:1, :] = jnp.sum(grad_second * unit, axis=0, keepdims=True)
    sums[1:2, :] = jnp.sum(grad_second, axis=0, keepdims=True)
    sums[2:3, :] = jnp.sum(grad_out, axis=0, keepdims=True)
    grad_middle = grad_out + norm_back(grad_second, unit, inverse, gains[1:2, :])
    sums[3:4, :] = jnp.sum(grad_middle, axis=0, keepdims=True)
    grad_middle_out[...] = grad_middle[0:t, :]
    for n in range(8):
        gb[n] = grad_middle[:, SIDE * n : SIDE * n + SIDE].astype(BF)
        nb[n] = normed[:, SIDE * n : SIDE * n + SIDE]
    unpack_narrow(wire, narrow, wire.shape[0] // 5)
    unpack_sorted(wire, narrow, order, 0, w_qkv, 8, 6)
    unpack_sorted(wire, narrow, order, 48, w_proj, 2, 8)
    for p in range(2):
        value = dot_nt(gb[0], w_proj[0, p * SIDE : (p + 1) * SIDE, :])
        for n in range(1, 8):
            value = value + dot_nt(gb[n], w_proj[n, p * SIDE : (p + 1) * SIDE, :])
        gatt[p] = value.astype(BF)
    attn_backward(mixed, rel_hi, rel_lo, pick, spread, probs, gatt, gm, rel_out, (SIDE // 2) ** -0.5)
    for j in range(6):
        bias_sums[j : j + 1, :] = jnp.sum(gm[j].astype(F32), axis=0, keepdims=True)

    def normed_back(i, carry):
        row = pl.multiple_of(i * SIDE, 32)
        value = dot_nt(gm[0], w_qkv[0, pl.ds(row, SIDE), :])
        for j in range(1, 6):
            value = value + dot_nt(gm[j], w_qkv[j, pl.ds(row, SIDE), :])
        block[i] = value
        return carry

    lax.fori_loop(0, 8, normed_back, 0)
    for n in range(8):
        part_normed[:, SIDE * n : SIDE * n + SIDE] = block[n][0:t, :].astype(BF)


def token_back_body(tokens, live, normed_sum, grad_middle, gains, tokens_grad, sums):
    x = tokens[...].astype(F32)
    unit, inverse = norm_parts(x)
    grad_normed = normed_sum[...].astype(F32) * live[...]
    sums[0:1, :] = jnp.sum(grad_normed * unit, axis=0, keepdims=True)
    sums[1:2, :] = jnp.sum(grad_normed, axis=0, keepdims=True)
    tokens_grad[...] = grad_middle[...] + norm_back(grad_normed, unit, inverse, gains[0:1, :])


def square_tile(square, t):
    return jnp.concatenate([square[0, t], square[1, t, :, 0:32]], axis=1)


def put_tile(square, t, value):
    square[0, t] = value[:, 0:128]
    square[1, t, :, 0:32] = value[:, 128:160]


def split_dot(kind, a, b):
    a_hi, a_lo = low_parts(a)
    b_hi, b_lo = low_parts(b)
    return kind(a_hi, b_hi) + (kind(a_hi, b_lo) + kind(a_lo, b_hi))


def soap_units(r, g, wire, sq_left, sq_right, master, first, second,
               grad_out, new_out, copy_out, first_out, second_out, sq_grad, sq_work):
    rows = slice(8 * r, 8 * r + 8)
    count = wire.shape[0] // 4
    left, right = sq_left.at[g], sq_right.at[g]

    def total(i):
        w = [wire[p * count + i].astype(F32) for p in range(4)]
        return (w[0] + w[1]) + (w[2] + w[3])

    def load():
        for half in range(2):
            last = total(5 * (2 * r + half) + 4)
            for q in range(4):
                sq_grad[0, 4 * half + q] = total(5 * (2 * r + half) + q)
                sq_grad[1, 4 * half + q] = last if q == 0 else pltpu.roll(last, 128 - 32 * q, 1)

        def write(at, value):
            grad_out[rows, pl.ds(at, 128)] = value

        square_to_flat(sq_grad, write)

    def rotate(t, carry):
        half = split_dot(dot_tn, square_tile(left, t), square_tile(sq_grad, t))
        put_tile(sq_work, t, split_dot(dot, half, square_tile(right, t)))
        return carry

    def moments(at, rotated):
        cols = pl.ds(at, 128)
        f = beta_one * first[rows, cols] + (1.0 - beta_one) * rotated
        s = beta_two * second[rows, cols] + (1.0 - beta_two) * rotated * rotated
        first_out[rows, cols] = f
        second_out[rows, cols] = s
        new_out[rows, cols] = f / (jnp.sqrt(s) + adam_eps)

    def turn_back(t, carry):
        half = split_dot(dot, square_tile(left, t), square_tile(sq_work, t))
        put_tile(sq_work, t, split_dot(dot_nt, half, square_tile(right, t)))
        return carry

    def finish(at, update):
        cols = pl.ds(at, 128)
        value = master[rows, cols] - learn_rate * update
        new_out[rows, cols] = value
        copy_out[rows, cols] = value.astype(BF)

    def loop(body):
        lax.fori_loop(0, 8, body, 0)

    return [
        load,
        lambda: loop(rotate),
        lambda: square_to_flat(sq_work, moments),
        lambda: flat_to_square(lambda at: new_out[rows, pl.ds(at, 128)], sq_work),
        lambda: loop(turn_back),
        lambda: square_to_flat(sq_work, finish),
    ]


def soap_attn_body(wire, sq_left, sq_right, master, first, second,
                   grad_out, new_out, copy_out, first_out, second_out, sq_grad, sq_work):
    for unit in soap_units(0, 0, wire, sq_left, sq_right, master, first, second,
                           grad_out, new_out, copy_out, first_out, second_out, sq_grad, sq_work):
        unit()


def build(mesh):
    placed = (
        P("dp", None, None),
        P("dp", None),
        P("dp", None, None),
        P(),
        P(),
        P(),
        P("mp"),
        P("mp"),
        P(),
        P("mp", None),
        P("mp", None),
        P("mp", "dp", None),
        P("mp", "dp", None),
        P("mp", "dp", None),
        P("mp", "dp", None),
        P("mp", "dp", None),
        P("mp", "dp", None),
        P("mp", "dp", None),
        P("mp", "dp", None),
        P("mp", "dp", None),
        P("mp", "dp", None),
    )
    return jax.shard_map(
        fast_local if dict(mesh.shape) == {"dp": 8, "mp": 4} else local,
        mesh=mesh,
        in_specs=placed,
        out_specs=(
            P("dp", None, None),
            P("dp", None, None),
            P(),
            P(),
            P(),
            P("mp"),
            P("mp"),
            P(),
            P("mp", "dp", None),
            P("mp", "dp", None),
            P("mp", "dp", None),
            P("mp", "dp", None),
            P("mp", "dp", None),
            P("mp", "dp", None),
            P("mp", "dp", None),
            P("mp", "dp", None),
            P("mp", "dp", None),
            P("mp", "dp", None),
        ),
        check_vma=False,
    )


VM = pl.BlockSpec(memory_space=pltpu.VMEM)
SM = pl.BlockSpec(memory_space=pltpu.SMEM)
LIMIT = 60 * 1024 * 1024


def call(body, tables, args, outs, scratch, name):
    return pl.pallas_call(
        body,
        out_shape=[jax.ShapeDtypeStruct(shape, kind) for shape, kind in outs],
        in_specs=[SM] * len(tables) + [VM] * len(args),
        out_specs=[VM] * len(outs),
        scratch_shapes=[pltpu.VMEM(shape, kind) for shape, kind in scratch],
        compiler_params=pltpu.CompilerParams(vmem_limit_bytes=LIMIT),
        name=name,
    )(*tables, *args)


def rel_constants(side):
    rows = np.arange(ROWS)
    lanes = np.arange(896)
    within, along = lanes % 64, lanes // 64
    high = np.where(rows < side * side, rows // side, -1)[:, None]
    wide = np.where(rows < side * side, rows % side, -1)[:, None]
    pick = np.where(within[None] < 32, high == along[None], wide == along[None])
    keys = np.arange(ROWS)
    key_h, key_w = keys // side, keys % side
    offset = np.where(within[:, None] < 32, along[:, None] - key_h[None], along[:, None] - key_w[None]) + side - 1
    spread = (offset == (within % 32)[:, None]) & (keys < side * side)[None]
    return jnp.asarray(pick, BF), jnp.asarray(spread, BF)


def inverse_order(owner):
    count = owner.shape[0]
    at = jnp.arange(count, dtype=jnp.int32)
    return jnp.sum(jnp.where(owner[:, None] == at[None, :], at[:, None], 0), axis=0)


def fast_local(
    tokens, pad_mask, cotangent, norm_gains, norm_biases, out_biases, qkv_bias, up_bias, rel_pos,
    attn_owner, mlp_owner, attn_master, mlp_master, attn_left, attn_right, mlp_left, mlp_right,
    attn_first, attn_second, mlp_first, mlp_second,
):
    t, width = tokens.shape[1:]
    tok, cot = tokens[0], cotangent[0]
    live = jnp.pad(pad_mask[0].astype(F32), (0, ROWS - t))[:, None]
    qb, ub = qkv_bias.reshape(6, SIDE), up_bias.reshape(8, SIDE)
    rel = jnp.pad(rel_pos, ((0, 0), (0, 32 - rel_pos.shape[1]), (0, 0))).reshape(64, SIDE // 2)
    rel_hi, rel_lo = low_parts(jnp.tile(rel, (2, 2)))
    pick, spread = rel_constants((rel_pos.shape[1] + 1) // 2)
    own_a, own_m = attn_owner[0], mlp_owner[0]
    ord_a, ord_m = inverse_order(own_a), inverse_order(own_m)
    xa = jnp.where(own_a < 48, own_a // 6, 8 + (own_a - 48) // 8)
    ya = jnp.where(own_a < 48, own_a % 6, 6 + (own_a - 48) % 8)
    xm, ym = own_m // 8, (own_m // 64) * 8 + own_m % 8

    wire_a, wire_m = call(
        pack_body, (), (attn_master[0], mlp_master[0]),
        [((10, SIDE, 128), BF), ((20, SIDE, 128), BF)], [((2, 8, SIDE, 128), F32)], "pack")
    all_a = gather(wire_a, 0, "gather_attn")

    part, normed, mixed, probs, att = call(
        attn_fwd_body, (ord_a,),
        (tok, live, norm_gains, norm_biases, qb, rel_hi, rel_lo, pick, spread, all_a),
        [((t, width), BF), ((ROWS, width), BF), ((6, ROWS, SIDE), BF), ((4, ROWS, ROWS), F32), ((2, ROWS, SIDE), BF)],
        [((6, 8 * SIDE, SIDE), BF), ((8, 2 * SIDE, SIDE), BF), ((64, SIDE, 32), BF), ((8, ROWS, SIDE), F32)],
        "attn_fwd")
    branch = lax.psum(part, "mp")
    wire_m, mixed = lax.optimization_barrier((wire_m, mixed))
    all_m = gather(wire_m, 1, "gather_mlp")
    part_down, part_second, sec_blocks, act_blocks, gh, go, up_sums = call(
        mlp_body, (ord_m,),
        (tok, live, cot, branch, norm_gains, norm_biases, out_biases, ub, all_m),
        [((t, width), BF), ((t, width), BF)] + [((8, ROWS, SIDE), BF)] * 4 + [((8, SIDE), F32)],
        [((8, 8 * SIDE, SIDE), BF), ((8, 8 * SIDE, SIDE), BF), ((128, SIDE, 32), BF), ((8, ROWS, SIDE), F32), ((ROWS, width), BF)],
        "mlp")
    second_sum = lax.psum(part_second, "mp")
    down_sum = lax.psum(part_down, "mp")

    def mlp_tiles(left_at, right_at, sec, act, gh_ref, go_ref, wire, lefts, rights):
        lefts[0:8], lefts[8:16] = sec[...], act[...]
        rights[0:8], rights[8:16] = gh_ref[...], go_ref[...]
        grad_tiles_body(left_at, right_at, 128, lambda i: lefts[i], lambda i: rights[i], wire)

    stack_m, = call(
        mlp_tiles, (xm, ym), (sec_blocks, act_blocks, gh, go), [((160, SIDE, 128), BF)],
        [((16, ROWS, SIDE), BF)] * 2, "mlp_tiles")
    sum_m, sq_left_m, sq_right_m, sq_left_a, sq_right_a = scatter_call(
        scatter_mlp_body, stack_m, (mlp_left[0], mlp_right[0], attn_left[0], attn_right[0]),
        [((2, 2, 8, SIDE, 128), F32)] * 2 + [((1, 2, 8, SIDE, 128), F32)] * 2, [], 2, 250_000_000, "scatter_mlp")
    second_sum, down_sum, sum_m = lax.optimization_barrier((second_sum, down_sum, sum_m))

    block_out, grad_middle, part_normed, rel_part, gm, gb, nb, sums_two, qkv_sums = call(
        mid_back_body, (ord_a,),
        (tok, live, cot, branch, down_sum, second_sum, norm_gains, out_biases, all_a, mixed, probs, normed, att,
         rel_hi, rel_lo, pick, spread),
        [((t, width), BF), ((t, width), F32), ((t, width), BF), ((128, SIDE), F32), ((6, ROWS, SIDE), BF),
         ((8, ROWS, SIDE), BF), ((8, ROWS, SIDE), BF), ((4, width), F32), ((6, SIDE), F32)],
        [((6, 8 * SIDE, SIDE), BF), ((8, 2 * SIDE, SIDE), BF), ((64, SIDE, 32), BF), ((8, ROWS, SIDE), F32),
         ((2, ROWS, SIDE), BF)],
        "mid_back")
    rel_half = SIDE // 2
    rel_fold = rel_part[:64] + rel_part[64:]
    rel_fold = (rel_fold[:, :rel_half] + rel_fold[:, rel_half:]).reshape(2, 32, rel_half)[:, : rel_pos.shape[1]]
    rel_size = rel_fold.size
    rel_rows = -(-rel_size // width)
    rel_flat = jnp.pad(rel_fold.reshape(-1).astype(BF), (0, rel_rows * width - rel_size)).reshape(rel_rows, width)
    both_sum = lax.psum(jnp.concatenate([part_normed, rel_flat], axis=0), "mp")

    def attn_tiles(left_at, right_at, nb_ref, att_ref, gm_ref, gb_ref, wire, lefts, rights):
        lefts[0:8], lefts[8:10] = nb_ref[...], att_ref[...]
        rights[0:6], rights[6:14] = gm_ref[...], gb_ref[...]
        grad_tiles_body(left_at, right_at, 64, lambda i: lefts[i], lambda i: rights[i], wire)

    stack_a, = call(
        attn_tiles, (xa, ya), (nb, att, gm, gb), [((80, SIDE, 128), BF)],
        [((10, ROWS, SIDE), BF), ((14, ROWS, SIDE), BF)], "attn_tiles")
    def soap_outs(shape):
        return [(shape, F32), (shape, F32), (shape, BF), (shape, F32), (shape, F32)]

    sum_a, mg, mn, mc, mf, ms = scatter_call(
        scatter_attn_body, stack_a, (sum_m, sq_left_m, sq_right_m, mlp_master[0], mlp_first[0], mlp_second[0]),
        soap_outs(mlp_master.shape[1:]), [((2, 8, SIDE, 128), F32)] * 2, 4, 150_000_000, "scatter_attn")
    both_sum, sum_a = lax.optimization_barrier((both_sum, sum_a))
    normed_sum, rel_sum = both_sum[:t], both_sum[t:].reshape(-1)[:rel_size].astype(F32)
    tokens_grad, sums_one = call(
        token_back_body, (), (tok, live[:t], normed_sum, grad_middle, norm_gains),
        [((t, width), F32), ((2, width), F32)], [], "token_back")
    small = [sums_one.reshape(-1), sums_two.reshape(-1), qkv_sums.reshape(-1), up_sums.reshape(-1), rel_sum]
    edges = np.cumsum([0] + [v.shape[0] for v in small])
    lines = -(-int(edges[-1]) // 1024) * 8
    small = jnp.pad(jnp.concatenate(small), (0, lines * 128 - int(edges[-1]))).reshape(1, lines, 128)
    total = jnp.sum(gather(small, 3, "gather_sums", 1), axis=0).reshape(-1)
    one, two, qkv_grad, up_grad, rel_grad = [total[edges[i]:edges[i + 1]] for i in range(5)]
    one, two = one.reshape(2, width), two.reshape(4, width)
    gains_grad = jnp.stack([one[0], two[0]])
    biases_grad = jnp.stack([one[1], two[1]])
    outb_grad = jnp.stack([two[3], two[2]])
    rel_grad = rel_grad.reshape(rel_pos.shape)

    ag, an, ac, af, as_ = call(
        soap_attn_body, (), (sum_a, sq_left_a, sq_right_a, attn_master[0], attn_first[0], attn_second[0]),
        soap_outs(attn_master.shape[1:]), [((2, 8, SIDE, 128), F32)] * 2, "soap_attn")
    return (block_out[None], tokens_grad[None], gains_grad, biases_grad, outb_grad, qkv_grad, up_grad, rel_grad,
            *(value[None] for value in (ag, mg, an, mn, ac, mc, af, as_, mf, ms)))


def solution(mesh):
    return build(mesh)
```

```python
import functools
import math

import jax
import jax.numpy as jnp
import numpy as np
from jax import lax
from jax.experimental import pallas as pl
from jax.experimental.pallas import tpu as pltpu
from jax.sharding import PartitionSpec as P

highest = lax.Precision.HIGHEST
norm_eps = 1e-06
beta_one = 0.9
beta_two = 0.95
adam_eps = 1e-08
learn_rate = 0.02


def untile(tile_rows, row_count, col_count, tile_side):
    shaped = tile_rows.reshape(row_count // tile_side, col_count // tile_side, tile_side, tile_side)
    return shaped.transpose(0, 2, 1, 3).reshape(row_count, col_count)


def retile(matrix, tile_side):
    row_count, col_count = matrix.shape
    shaped = matrix.reshape(row_count // tile_side, tile_side, col_count // tile_side, tile_side)
    return shaped.transpose(0, 2, 1, 3).reshape(-1, tile_side * tile_side)


def rel_onehot(win_side):
    positions = jnp.arange(win_side, dtype=jnp.int32)
    offset = positions[:, None] - positions[None, :] + (win_side - 1)
    entries = jnp.arange(2 * win_side - 1, dtype=jnp.int32)
    return (offset[:, :, None] == entries[None, None, :]).astype(jnp.float32)


def norm_forward(values, norm_gain, norm_shift):
    centre = values - jnp.mean(values, axis=-1, keepdims=True)
    inverse = lax.rsqrt(jnp.mean(centre * centre, axis=-1, keepdims=True) + norm_eps)
    unit_rows = centre * inverse
    return (unit_rows * norm_gain + norm_shift, unit_rows, inverse)


def norm_backward(grad_in, unit_rows, inverse, norm_gain):
    grad_unit = grad_in * norm_gain
    centred = grad_unit - jnp.mean(grad_unit, axis=-1, keepdims=True)
    return inverse * (centred - unit_rows * jnp.mean(grad_unit * unit_rows, axis=-1, keepdims=True))


def gelu_pair(values):
    normal_cdf = 0.5 * (1.0 + lax.erf(values * 0.5**0.5))
    density = jnp.exp(-0.5 * values * values) * (2.0 * math.pi) ** (-0.5)
    return (values * normal_cdf, normal_cdf + values * density)


def soap_step(grad_tiles, master, left_basis, right_basis, first_moment, second_moment):
    tile_side = math.isqrt(grad_tiles.shape[2])
    square = (grad_tiles.shape[0], grad_tiles.shape[1], tile_side, tile_side)
    left_square = left_basis.reshape(square)
    right_square = right_basis.reshape(square)
    half_turn = jnp.einsum(
        "mtji,mtjk->mtik", left_square, grad_tiles.reshape(square), precision=highest
    )
    rotated = jnp.einsum("mtik,mtkl->mtil", half_turn, right_square, precision=highest).reshape(
        grad_tiles.shape
    )
    first_new = beta_one * first_moment + (1.0 - beta_one) * rotated
    second_new = beta_two * second_moment + (1.0 - beta_two) * rotated * rotated
    direction = (first_new / (jnp.sqrt(second_new) + adam_eps)).reshape(square)
    back_half = jnp.einsum("mtij,mtjk->mtik", left_square, direction, precision=highest)
    update = jnp.einsum("mtik,mtlk->mtil", back_half, right_square, precision=highest).reshape(
        grad_tiles.shape
    )
    master_new = master - learn_rate * update
    return (master_new, master_new.astype(jnp.bfloat16), first_new, second_new)


def local(
    tokens,
    pad_mask,
    cotangent,
    norm_gains,
    norm_biases,
    out_biases,
    qkv_bias,
    up_bias,
    rel_pos,
    attn_owner,
    mlp_owner,
    attn_master,
    mlp_master,
    attn_left,
    attn_right,
    mlp_left,
    mlp_right,
    attn_first,
    attn_second,
    mlp_first,
    mlp_second,
):
    windows, win_tokens, model_width = tokens.shape
    row_count = windows * win_tokens
    qkv_cols = qkv_bias.shape[0]
    head_cols = qkv_cols // 3
    unit_cols = up_bias.shape[0]
    head_dim = rel_pos.shape[2]
    heads_here = head_cols // head_dim
    win_side = (rel_pos.shape[1] + 1) // 2
    tile_side = math.isqrt(attn_master.shape[2])
    qkv_count = model_width // tile_side * (qkv_cols // tile_side)
    up_count = model_width // tile_side * (unit_cols // tile_side)
    score_scale = head_dim ** (-0.5)
    attn_stored, mlp_stored = (
        lax.all_gather(attn_master.astype(jnp.bfloat16), "dp", axis=1, tiled=True),
        lax.all_gather(mlp_master.astype(jnp.bfloat16), "dp", axis=1, tiled=True),
    )
    attn_order = jnp.argsort(attn_owner[0])
    mlp_order = jnp.argsort(mlp_owner[0])
    attn_sorted = attn_stored[0][attn_order]
    mlp_sorted = mlp_stored[0][mlp_order]
    w_qkv = untile(attn_sorted[:qkv_count], model_width, qkv_cols, tile_side)
    w_proj = untile(attn_sorted[qkv_count:], head_cols, model_width, tile_side)
    w_up = untile(mlp_sorted[:up_count], model_width, unit_cols, tile_side)
    w_down = untile(mlp_sorted[up_count:], unit_cols, model_width, tile_side)
    onehot = rel_onehot(win_side)
    table_h = jnp.einsum("ijr,rc->ijc", onehot, rel_pos[0], precision=highest)
    table_w = jnp.einsum("ijr,rc->ijc", onehot, rel_pos[1], precision=highest)
    flat_rows = tokens.reshape(row_count, model_width).astype(jnp.float32)
    live_rows = pad_mask.reshape(row_count, 1).astype(jnp.float32)
    normed, unit_one, inverse_one = norm_forward(flat_rows, norm_gains[0], norm_biases[0])
    normed_low = (normed * live_rows).astype(jnp.bfloat16)
    mixed_rows = (jnp.dot(normed_low, w_qkv, preferred_element_type=jnp.float32) + qkv_bias).astype(
        jnp.bfloat16
    )
    head_parts = mixed_rows.reshape(windows, win_tokens, 3, heads_here, head_dim)
    queries = head_parts[:, :, 0]
    key_rows = head_parts[:, :, 1]
    value_rows = head_parts[:, :, 2]
    query_grid = queries.astype(jnp.float32).reshape(
        windows, win_side, win_side, heads_here, head_dim
    )

    def score_rows():
        direct = (
            jnp.einsum("wqhc,wkhc->whqk", queries, key_rows, preferred_element_type=jnp.float32)
            * score_scale
        )
        along_h = jnp.einsum("wabhc,akc->whabk", query_grid, table_h, precision=highest)
        along_w = jnp.einsum("wabhc,blc->whabl", query_grid, table_w, precision=highest)
        return direct + (along_h[..., :, None] + along_w[..., None, :]).reshape(
            windows, heads_here, win_tokens, win_tokens
        )

    scores = score_rows()
    row_top = jnp.max(scores, axis=-1, keepdims=True)
    exponent = jnp.exp(scores - row_top)
    row_total = jnp.sum(exponent, axis=-1, keepdims=True)
    log_total = row_top + jnp.log(row_total)
    probs_low = (exponent / row_total).astype(jnp.bfloat16)
    attended = jnp.einsum(
        "whqk,wkhc->wqhc", probs_low, value_rows, preferred_element_type=jnp.float32
    )
    attended_low = attended.reshape(row_count, head_cols).astype(jnp.bfloat16)
    branch = lax.psum(
        jnp.dot(attended_low, w_proj, preferred_element_type=jnp.float32).astype(jnp.bfloat16), "mp"
    ).astype(jnp.float32)
    middle = flat_rows + branch + out_biases[0]
    second, unit_two, inverse_two = norm_forward(middle, norm_gains[1], norm_biases[1])
    second_low = second.astype(jnp.bfloat16)
    hidden = jnp.dot(second_low, w_up, preferred_element_type=jnp.float32) + up_bias
    active, gelu_slope = gelu_pair(hidden)
    active_low = active.astype(jnp.bfloat16)
    down_sum = lax.psum(
        jnp.dot(active_low, w_down, preferred_element_type=jnp.float32).astype(jnp.bfloat16), "mp"
    ).astype(jnp.float32)
    block_output = (
        ((middle + down_sum + out_biases[1]) * live_rows)
        .astype(jnp.bfloat16)
        .reshape(windows, win_tokens, model_width)
    )
    grad_out = cotangent.reshape(row_count, model_width).astype(jnp.float32) * live_rows
    grad_out_low = grad_out.astype(jnp.bfloat16)
    down_bias_grad = jnp.sum(grad_out, axis=0)
    w_down_grad = jnp.einsum(
        "nf,nd->fd", active_low, grad_out_low, preferred_element_type=jnp.float32
    )
    grad_active = jnp.einsum("nd,fd->nf", grad_out_low, w_down, preferred_element_type=jnp.float32)
    grad_hidden = (grad_active * gelu_slope).astype(jnp.bfloat16)
    up_bias_grad = jnp.sum(grad_hidden.astype(jnp.float32), axis=0)
    w_up_grad = jnp.einsum("nd,nf->df", second_low, grad_hidden, preferred_element_type=jnp.float32)
    mlp_stack = jnp.concatenate(
        [retile(w_up_grad, tile_side), retile(w_down_grad, tile_side)], axis=0
    )[mlp_owner[0]][None]
    grad_second = lax.psum(
        jnp.einsum("nf,df->nd", grad_hidden, w_up, preferred_element_type=jnp.float32).astype(
            jnp.bfloat16
        ),
        "mp",
    ).astype(jnp.float32)
    gain_two_grad = jnp.sum(grad_second * unit_two, axis=0)
    shift_two_grad = jnp.sum(grad_second, axis=0)
    grad_middle = grad_out + norm_backward(grad_second, unit_two, inverse_two, norm_gains[1])
    proj_bias_grad = jnp.sum(grad_middle, axis=0)
    grad_branch = grad_middle.astype(jnp.bfloat16)
    w_proj_grad = jnp.einsum(
        "nc,nd->cd", attended_low, grad_branch, preferred_element_type=jnp.float32
    )
    grad_attended = jnp.einsum("nd,cd->nc", grad_branch, w_proj, preferred_element_type=jnp.float32)
    grad_attended = grad_attended.astype(jnp.bfloat16).reshape(
        windows, win_tokens, heads_here, head_dim
    )
    probs_full = jnp.exp(score_rows() - log_total)
    probs_again = probs_full.astype(jnp.bfloat16)
    grad_probs = jnp.einsum(
        "wqhc,wkhc->whqk", grad_attended, value_rows, preferred_element_type=jnp.float32
    )
    grad_values = jnp.einsum(
        "whqk,wqhc->wkhc", probs_again, grad_attended, preferred_element_type=jnp.float32
    )
    grad_scores = (
        probs_full * (grad_probs - jnp.sum(probs_full * grad_probs, axis=-1, keepdims=True))
    ).astype(jnp.bfloat16)
    grad_queries = (
        jnp.einsum("whqk,wkhc->wqhc", grad_scores, key_rows, preferred_element_type=jnp.float32)
        * score_scale
    )
    grad_keys = (
        jnp.einsum("whqk,wqhc->wkhc", grad_scores, queries, preferred_element_type=jnp.float32)
        * score_scale
    )
    grad_grid = grad_scores.astype(jnp.float32).reshape(
        windows, heads_here, win_side, win_side, win_side, win_side
    )
    grad_h = jnp.sum(grad_grid, axis=5)
    grad_w = jnp.sum(grad_grid, axis=4)
    grad_rel_q = jnp.einsum("whabk,akc->wabhc", grad_h, table_h, precision=highest) + jnp.einsum(
        "whabl,blc->wabhc", grad_w, table_w, precision=highest
    )
    grad_queries = grad_queries + grad_rel_q.reshape(windows, win_tokens, heads_here, head_dim)
    table_h_grad = jnp.einsum("whabk,wabhc->akc", grad_h, query_grid, precision=highest)
    table_w_grad = jnp.einsum("whabl,wabhc->blc", grad_w, query_grid, precision=highest)
    rel_part = jnp.stack(
        [
            jnp.einsum("ijr,ijc->rc", onehot, table_h_grad, precision=highest),
            jnp.einsum("ijr,ijc->rc", onehot, table_w_grad, precision=highest),
        ]
    )
    grad_mixed = (
        jnp.stack([grad_queries, grad_keys, grad_values], axis=2)
        .reshape(row_count, qkv_cols)
        .astype(jnp.bfloat16)
    )
    qkv_bias_grad = jnp.sum(grad_mixed.astype(jnp.float32), axis=0)
    w_qkv_grad = jnp.einsum("nd,nc->dc", normed_low, grad_mixed, preferred_element_type=jnp.float32)
    grad_normed, rel_sum = (
        lax.psum(
            jnp.einsum("nc,dc->nd", grad_mixed, w_qkv, preferred_element_type=jnp.float32).astype(
                jnp.bfloat16
            ),
            "mp",
        ).astype(jnp.float32),
        lax.psum(rel_part.astype(jnp.bfloat16), "mp").astype(jnp.float32),
    )
    grad_normed = grad_normed * live_rows
    gain_one_grad = jnp.sum(grad_normed * unit_one, axis=0)
    shift_one_grad = jnp.sum(grad_normed, axis=0)
    tokens_grad = (
        grad_middle + norm_backward(grad_normed, unit_one, inverse_one, norm_gains[0])
    ).reshape(windows, win_tokens, model_width)
    attn_stack = jnp.concatenate(
        [retile(w_qkv_grad, tile_side), retile(w_proj_grad, tile_side)], axis=0
    )[attn_owner[0]][None]
    attn_grad, mlp_grad = (
        lax.psum_scatter(attn_stack, "dp", scatter_dimension=1, tiled=True),
        lax.psum_scatter(mlp_stack, "dp", scatter_dimension=1, tiled=True),
    )
    gains_grad, biases_grad, out_biases_grad, rel_pos_grad, qkv_bias_total, up_bias_total = (
        lax.psum(
            (
                jnp.stack([gain_one_grad, gain_two_grad]),
                jnp.stack([shift_one_grad, shift_two_grad]),
                jnp.stack([proj_bias_grad, down_bias_grad]),
                rel_sum,
                qkv_bias_grad,
                up_bias_grad,
            ),
            "dp",
        )
    )
    attn_new, attn_copy, attn_first_new, attn_second_new = soap_step(
        attn_grad, attn_master, attn_left, attn_right, attn_first, attn_second
    )
    mlp_new, mlp_copy, mlp_first_new, mlp_second_new = soap_step(
        mlp_grad, mlp_master, mlp_left, mlp_right, mlp_first, mlp_second
    )
    return (
        block_output,
        tokens_grad,
        gains_grad,
        biases_grad,
        out_biases_grad,
        qkv_bias_total,
        up_bias_total,
        rel_pos_grad,
        attn_grad,
        mlp_grad,
        attn_new,
        mlp_new,
        attn_copy,
        mlp_copy,
        attn_first_new,
        attn_second_new,
        mlp_first_new,
        mlp_second_new,
    )


BF = jnp.bfloat16
F32 = jnp.float32
ROWS = 208
SIDE = 160


def dot(a, b):
    return jnp.dot(a, b, preferred_element_type=F32)


def dot_nt(a, b):
    return lax.dot_general(a, b, (((1,), (1,)), ((), ())), preferred_element_type=F32)


def dot_tn(a, b):
    return lax.dot_general(a, b, (((0,), (0,)), ((), ())), preferred_element_type=F32)


def lane_at(shape):
    return lax.broadcasted_iota(jnp.int32, shape, len(shape) - 1)


def low_parts(value):
    high = value.astype(BF)
    return high, (value - high.astype(F32)).astype(BF)


def flat_to_square(read, square, count=8):
    lane = lane_at((8, 128))

    def rows_of(base):
        x = [read(base + 128 * k) for k in range(5)]
        r1 = pltpu.roll(x[1], 96, 1)
        r2 = pltpu.roll(x[2], 96, 1)
        h2 = pltpu.roll(x[2], 64, 1)
        h3 = pltpu.roll(x[3], 64, 1)
        r3 = pltpu.roll(x[3], 32, 1)
        r4 = pltpu.roll(x[4], 32, 1)
        return (
            (x[0], x[1]),
            (jnp.where(lane < 96, r1, r2), r2),
            (jnp.where(lane < 64, h2, h3), h3),
            (jnp.where(lane < 32, r3, r4), r4),
        )

    def body(group, carry):
        base = pl.multiple_of(group * 1280, 128)
        rows = rows_of(base) + rows_of(base + 640)
        for part in range(2):
            stacked = jnp.stack([row[part] for row in rows], axis=0)
            square[part, :, pl.ds(pl.multiple_of(8 * group, 8), 8), :] = jnp.swapaxes(stacked, 0, 1)
        return carry

    lax.fori_loop(0, 20, body, 0)


def square_to_flat(square, write, count=8):
    lane = lane_at((8, 128))

    def body(group, carry):
        at = pl.ds(pl.multiple_of(8 * group, 8), 8)
        wide = jnp.swapaxes(square[0, :, at, :], 0, 1)
        narrow = jnp.swapaxes(square[1, :, at, :], 0, 1)
        for half in range(2):
            base = pl.multiple_of(group * 1280, 128) + 640 * half
            a = [wide[4 * half + m] for m in range(4)]
            b = [narrow[4 * half + m] for m in range(4)]
            a1 = pltpu.roll(a[1], 32, 1)
            b1 = pltpu.roll(b[1], 32, 1)
            a2 = pltpu.roll(a[2], 64, 1)
            b2 = pltpu.roll(b[2], 64, 1)
            a3 = pltpu.roll(a[3], 96, 1)
            b3 = pltpu.roll(b[3], 96, 1)
            write(base, a[0])
            write(base + 128, jnp.where(lane < 32, b[0], a1))
            write(base + 256, jnp.where(lane < 32, a1, jnp.where(lane < 64, b1, a2)))
            write(base + 384, jnp.where(lane < 64, a2, jnp.where(lane < 96, b2, a3)))
            write(base + 512, jnp.where(lane < 96, a3, b3))
        return carry

    lax.fori_loop(0, 20, body, 0)


def pack_eight(source, first, wire, base, square):
    lane = lane_at((SIDE, 128))
    flat_to_square(lambda at: source[first : first + 8, pl.ds(at, 128)], square)
    for half in range(2):
        spare = None
        for q in range(4):
            wire[base + 5 * half + q] = square[0, 4 * half + q].astype(BF)
            piece = square[1, 4 * half + q]
            spare = piece if q == 0 else jnp.where(lane < 32 * q, spare, pltpu.roll(piece, 32 * q, 1))
        wire[base + 5 * half + 4] = spare.astype(BF)


def pack_body(attn, mlp, wire_attn, wire_mlp, square):
    pack_eight(attn, 0, wire_attn, 0, square)
    pack_eight(mlp, 0, wire_mlp, 0, square)
    pack_eight(mlp, 8, wire_mlp, 10, square)


def unpack_narrow(wire, narrow, groups):
    def body(g, carry):
        last = wire[5 * g + 4]
        for q in range(4):
            narrow[4 * g + q] = last[:, 32 * q : 32 * q + 32]
        return carry

    lax.fori_loop(0, groups, body, 0)


def unpack_sorted(wire, narrow, order, base, outs, rows, cols):
    def body(t, carry):
        row = t // cols
        col = t - row * cols
        stored = order[base + t]
        where_at = pl.multiple_of(row * SIDE, 32)
        outs[col, pl.ds(where_at, SIDE), 0:128] = wire[(stored // 4) * 5 + stored % 4]
        outs[col, pl.ds(where_at, SIDE), 128:160] = narrow[stored]
        return carry

    lax.fori_loop(0, rows * cols, body, 0)


MESH_ID = pl.DeviceIdType.MESH


def gather_body(piece, wire, out, send_sem, recv_sem, own_sem):
    count = wire.shape[0]
    pieces = count // piece
    me = lax.axis_index("dp")
    z, x = me // 2, me % 2
    side = me + 1 - 2 * x
    up, down = jnp.minimum(me + 2, 6 + x), jnp.maximum(me - 2, x)

    barrier = pltpu.get_barrier_semaphore()

    def greet(target):
        pl.semaphore_signal(barrier, inc=1, device_id={"dp": target}, device_id_type=MESH_ID)

    greet(side)
    pl.when(z < 3)(lambda: greet(up))
    pl.when(z > 0)(lambda: greet(down))
    inner = (z > 0) & (z < 3)
    pl.when(inner)(lambda: pl.semaphore_wait(barrier, 3))
    pl.when(jnp.logical_not(inner))(lambda: pl.semaphore_wait(barrier, 2))

    def copy(way, target, origin, k, own=False):
        place = out.at[pl.ds(origin * count + piece * k, piece)]
        return pltpu.make_async_remote_copy(
            src_ref=wire.at[pl.ds(piece * k, piece)] if own else place,
            dst_ref=place,
            send_sem=send_sem.at[way, origin // 2, k],
            recv_sem=recv_sem.at[origin, k],
            device_id={"dp": target},
            device_id_type=MESH_ID,
        )

    for k in range(pieces):
        copy(0, side, me, k, True).start()
        pl.when(z < 3)(lambda k=k: copy(1, up, me, k, True).start())
        pl.when(z > 0)(lambda k=k: copy(2, down, me, k, True).start())
    keep = pltpu.make_async_copy(wire, out.at[pl.ds(me * count, count)], own_sem)
    keep.start()

    for d in range(1, 4):
        for k in range(pieces):
            def from_below():
                origin = me - 2 * d
                copy(1, up, origin, k).wait_recv()
                copy(0, side, origin, k).start()
                pl.when(z < 3)(lambda: copy(1, up, origin, k).start())

            def from_above():
                origin = me + 2 * d
                copy(2, down, origin, k).wait_recv()
                copy(0, side, origin, k).start()
                pl.when(z > 0)(lambda: copy(2, down, origin, k).start())

            pl.when(z >= d)(from_below)
            pl.when(z + d <= 3)(from_above)

    keep.wait()
    for k in range(pieces):
        for line in range(4):
            origin = 2 * line + x
            copy(0, side, origin + 1 - 2 * x, k).wait_recv()
            copy(0, side, origin, k, False).wait_send()
            pl.when((line <= z) & (z < 3))(lambda: copy(1, up, origin, k).wait_send())
            pl.when((line >= z) & (z > 0))(lambda: copy(2, down, origin, k).wait_send())


def gather(wire, ident, name, piece=5):
    count = wire.shape[0]
    return pl.pallas_call(
        functools.partial(gather_body, piece),
        out_shape=jax.ShapeDtypeStruct((8 * count,) + wire.shape[1:], wire.dtype),
        in_specs=[VM],
        out_specs=pl.BlockSpec(memory_space=pl.ANY),
        scratch_shapes=[
            pltpu.SemaphoreType.DMA((3, 4, count // piece)),
            pltpu.SemaphoreType.DMA((8, count // piece)),
            pltpu.SemaphoreType.DMA,
        ],
        compiler_params=pltpu.CompilerParams(
            collective_id=ident, has_side_effects=True, vmem_limit_bytes=LIMIT),
        cost_estimate=pl.CostEstimate(flops=0, bytes_accessed=count * 12_000_000, transcendentals=0),
        name=name,
    )(wire)


CHUNK = 5
AHEAD = 4


def scatter_steps(count, prepare, source, own_part, out, inbox, half,
                  side_send, side_recv, line_send, line_recv, own, units, each=1):
    me = lax.axis_index("dp")
    z, x = me // 2, me % 2
    side = me + 1 - 2 * x
    pieces = count // CHUNK
    steps = 4 * pieces

    def line_at(j):
        return lax.rem(z + j, 4)

    barrier = pltpu.get_barrier_semaphore()
    for target in (side, 2 * line_at(1) + x, 2 * line_at(2) + x, 2 * line_at(3) + x):
        pl.semaphore_signal(barrier, inc=1, device_id={"dp": target}, device_id_type=MESH_ID)
    pl.semaphore_wait(barrier, 4)

    def place(at):
        j, k = lax.div(at, pieces), lax.rem(at, pieces)
        return j, k, line_at(j + 1)

    def to_side(at):
        j, k, line = place(at)
        return pltpu.make_async_remote_copy(
            src_ref=source(2 * line + 1 - x, line, k),
            dst_ref=inbox.at[pl.ds(line * count + CHUNK * k, CHUNK)],
            send_sem=side_send.at[j, k], recv_sem=side_recv.at[j, k],
            device_id={"dp": side}, device_id_type=MESH_ID)

    def to_line(at):
        j, k, line = place(at)
        return pltpu.make_async_remote_copy(
            src_ref=half.at[pl.ds(line * count + CHUNK * k, CHUNK)],
            dst_ref=out.at[pl.ds(z * count + CHUNK * k, CHUNK)],
            send_sem=line_send.at[j, k], recv_sem=line_recv.at[j, k],
            device_id={"dp": 2 * line + x}, device_id_type=MESH_ID)

    def keep(k):
        return pltpu.make_async_copy(
            half.at[pl.ds(z * count + CHUNK * k, CHUNK)], out.at[pl.ds(z * count + CHUNK * k, CHUNK)], own.at[k])

    def send(at):
        _, k, line = place(at)
        prepare(2 * line + 1 - x, line, k)
        to_side(at).start()

    def first(at, carry):
        send(at)
        return carry

    def step(at, carry):
        _, k, line = place(at)
        for i, unit in enumerate(units):
            turn = i // 2 if i < 2 * each else i - each
            pl.when(at == min(turn, steps - 1))(unit)
        to_side(at).wait_recv()
        pl.when(at + AHEAD < steps)(lambda: send(at + AHEAD))
        own_part(2 * line + x, line, k)
        pl.when(at < 3 * pieces)(lambda: to_line(at).start())
        pl.when(at >= 3 * pieces)(lambda: keep(k).start())
        return carry

    def last(at, carry):
        to_side(at).wait_send()

        def lines():
            to_line(at).wait_send()
            to_line(at).wait_recv()

        pl.when(at < 3 * pieces)(lines)
        pl.when(at >= 3 * pieces)(lambda: keep(place(at)[1]).wait())
        return carry

    lax.fori_loop(0, AHEAD, first, 0)
    lax.fori_loop(0, steps, step, 0)
    lax.fori_loop(0, steps, last, 0)


def scatter_call(body, count, tables, args, outs, scratch, ident, cost, name):
    shape = (4 * count, SIDE, 128)
    pieces = count // CHUNK
    return pl.pallas_call(
        body,
        out_shape=[jax.ShapeDtypeStruct(shape, BF)] + [jax.ShapeDtypeStruct(*out) for out in outs],
        in_specs=[SM] * len(tables) + [VM] * len(args),
        out_specs=[pl.BlockSpec(memory_space=pl.ANY)] + [VM] * len(outs),
        scratch_shapes=[pltpu.VMEM(shape, BF)] * 2 + [pltpu.SemaphoreType.DMA((4, pieces))] * 4
        + [pltpu.SemaphoreType.DMA((pieces,))] + [pltpu.VMEM(*item) for item in scratch],
        compiler_params=pltpu.CompilerParams(
            collective_id=ident, has_side_effects=True, vmem_limit_bytes=LIMIT),
        cost_estimate=pl.CostEstimate(flops=0, bytes_accessed=cost, transcendentals=0),
        name=name,
    )(*tables, *args)


def scatter_mlp_body(left_at, right_at, sec, act, gh, go, left_m, right_m, left_a, right_a,
                     out, sq_left_m, sq_right_m, sq_left_a, sq_right_a, inbox, half,
                     side_send, side_recv, line_send, line_recv, own, lefts, rights, sent):
    lefts[0:8], lefts[8:16] = sec[...], act[...]
    rights[0:8], rights[8:16] = gh[...], go[...]
    lane = lane_at((SIDE, 128))

    def tiles(chunk, k, emit):
        spare = None
        for q in range(4):
            s = 16 * chunk + 4 * k + q
            tile = dot_tn(lefts[left_at[s]], rights[right_at[s]])
            emit(q, tile[:, 0:128])
            piece = jnp.concatenate([tile[:, 128:160], jnp.zeros((SIDE, 96), F32)], axis=1)
            spare = piece if q == 0 else jnp.where(lane < 32 * q, spare, pltpu.roll(piece, 32 * q, 1))
        emit(4, spare)

    def prepare(chunk, line, k):
        def emit(q, value):
            sent[20 * line + CHUNK * k + q] = value.astype(BF)
        tiles(chunk, k, emit)

    def own_part(chunk, line, k):
        def emit(q, value):
            half[20 * line + CHUNK * k + q] = (value + inbox[20 * line + CHUNK * k + q].astype(F32)).astype(BF)
        tiles(chunk, k, emit)

    units = []
    for flat, square in ((left_m, sq_left_m), (right_m, sq_right_m), (left_a, sq_left_a), (right_a, sq_right_a)):
        for g in range(square.shape[0]):
            units.append(lambda f=flat, r=8 * g, sq=square, g=g: flat_to_square(
                lambda at: f[r : r + 8, pl.ds(at, 128)], sq.at[g]))
    scatter_steps(20, prepare, lambda chunk, line, k: sent.at[pl.ds(20 * line + CHUNK * k, CHUNK)], own_part,
                  out, inbox, half, side_send, side_recv, line_send, line_recv, own, units)


def scatter_attn_body(stack, wire, sq_left, sq_right, master, first, second,
                      out, grad_out, new_out, copy_out, first_out, second_out, inbox, half,
                      side_send, side_recv, line_send, line_recv, own, sq_grad, sq_work):
    units = []
    for g in range(2):
        units += soap_units(g, g, wire, sq_left, sq_right, master, first, second,
                            grad_out, new_out, copy_out, first_out, second_out, sq_grad, sq_work)

    def own_part(chunk, line, k):
        def add(i, carry):
            to = 10 * line + CHUNK * k + i
            half[to] = (stack[10 * chunk + CHUNK * k + i].astype(F32) + inbox[to].astype(F32)).astype(BF)
            return carry

        lax.fori_loop(0, CHUNK, add, 0)

    scatter_steps(10, lambda chunk, line, k: None,
                  lambda chunk, line, k: stack.at[pl.ds(10 * chunk + CHUNK * k, CHUNK)], own_part,
                  out, inbox, half, side_send, side_recv, line_send, line_recv, own, units, 4)


def norm_parts(x):
    mean = jnp.mean(x, axis=-1, keepdims=True)
    centre = x - mean
    inverse = lax.rsqrt(jnp.mean(centre * centre, axis=-1, keepdims=True) + norm_eps)
    return centre * inverse, inverse


def norm_back(grad_in, unit, inverse, gain):
    w = grad_in * gain
    return inverse * (
        w - jnp.mean(w, axis=-1, keepdims=True) - unit * jnp.mean(w * unit, axis=-1, keepdims=True)
    )


def padded(ref, rows, kind=F32):
    value = ref[...].astype(kind)
    return jnp.concatenate([value, jnp.zeros((ROWS - rows, value.shape[1]), kind)], axis=0)


def attn_forward(mixed, rel_hi, rel_lo, pick, spread, probs, att, scale, tokens_here):
    lane = lane_at((ROWS, SIDE))
    key_ok = lane_at((ROWS, ROWS)) < tokens_here
    head = SIDE // 2
    for p in range(2):
        q, k, v = mixed[p], mixed[2 + p], mixed[4 + p]
        parts = []
        for h in range(2):
            mine = (lane >= head) if h else (lane < head)
            qm = jnp.where(mine, q, jnp.zeros_like(q))
            s = dot_nt(qm, k) * scale
            a_hi, a_lo = low_parts(dot_nt(qm, rel_hi[...]) + dot_nt(qm, rel_lo[...]))
            for c in range(7):
                mask = pick[:, 128 * c : 128 * c + 128]
                table = spread[128 * c : 128 * c + 128, :]
                s = s + dot(a_hi * mask, table) + dot(a_lo * mask, table)
            s = jnp.where(key_ok, s, -1e30)
            top = jnp.max(s, axis=-1, keepdims=True)
            e = jnp.exp(s - top)
            pr = e / jnp.sum(e, axis=-1, keepdims=True)
            probs[2 * p + h] = pr
            parts.append(dot(pr.astype(BF), v))
        att[p] = jnp.where(lane < head, parts[0], parts[1]).astype(BF)


def attn_backward(mixed, rel_hi, rel_lo, pick, spread, probs, gatt, gm, rel_out, scale):
    lane = lane_at((ROWS, SIDE))
    head = SIDE // 2
    for p in range(2):
        q, k, v = mixed[p], mixed[2 + p], mixed[4 + p]
        ga = gatt[p]
        dq, dk, dv, dr = [], [], [], []
        for h in range(2):
            mine = (lane >= head) if h else (lane < head)
            pr = probs[2 * p + h]
            gam = jnp.where(mine, ga, jnp.zeros_like(ga))
            gp = dot_nt(gam, v)
            dv.append(dot_tn(pr.astype(BF), ga))
            ds = (pr * (gp - jnp.sum(pr * gp, axis=-1, keepdims=True))).astype(BF)
            da = None
            for c in range(7):
                term = dot_nt(ds, spread[128 * c : 128 * c + 128, :]) * pick[:, 128 * c : 128 * c + 128].astype(F32)
                da = term if da is None else da + term
            da_hi, da_lo = low_parts(da)
            relq = dot(da_hi, rel_hi[...]) + dot(da_lo, rel_hi[...]) + dot(da_hi, rel_lo[...])
            dq.append(dot(ds, k) * scale + relq)
            dk.append(dot_tn(ds, q) * scale)
            dr.append(dot_tn(da_hi, q) + dot_tn(da_lo, q))
        gm[p] = jnp.where(lane < head, dq[0], dq[1]).astype(BF)
        gm[2 + p] = jnp.where(lane < head, dk[0], dk[1]).astype(BF)
        gm[4 + p] = jnp.where(lane < head, dv[0], dv[1]).astype(BF)
        rel = jnp.where(lane_at((128, SIDE)) < head, dr[0], dr[1])
        if p == 0:
            rel_out[...] = rel
        else:
            rel_out[...] += rel


def attn_fwd_body(order, tokens, live, gains, biases, qkv_bias, rel_hi, rel_lo, pick, spread, wire,
                  part, normed, mixed, probs, att, w_qkv, w_proj, narrow, block):
    t = tokens.shape[0]
    x = padded(tokens, t)
    unit, _ = norm_parts(x)
    normed[...] = ((unit * gains[0:1, :] + biases[0:1, :]) * live[...]).astype(BF)
    unpack_narrow(wire, narrow, wire.shape[0] // 5)
    unpack_sorted(wire, narrow, order, 0, w_qkv, 8, 6)
    unpack_sorted(wire, narrow, order, 48, w_proj, 2, 8)

    def mix(j, carry):
        mixed[j] = (dot(normed[...], w_qkv[j]) + qkv_bias[pl.ds(j, 1), :]).astype(BF)
        return carry

    lax.fori_loop(0, 6, mix, 0)
    attn_forward(mixed, rel_hi, rel_lo, pick, spread, probs, att, (SIDE // 2) ** -0.5, t)

    def project(n, carry):
        value = dot(att[0], w_proj[n, 0:SIDE, :]) + dot(att[1], w_proj[n, SIDE : 2 * SIDE, :])
        block[n] = value
        return carry

    lax.fori_loop(0, 8, project, 0)
    for n in range(8):
        part[:, SIDE * n : SIDE * n + SIDE] = block[n][0:t, :].astype(BF)


def mlp_body(order, tokens, live, cotangent, branch, gains, biases, out_biases, up_bias, wire,
             part_down, part_second, sec_blocks, act_blocks, gh, go, bias_sums, w_up, w_down, narrow, block, second):
    t = tokens.shape[0]
    x = padded(tokens, t)
    middle = x + padded(branch, t) + out_biases[0:1, :]
    unit, _ = norm_parts(middle)
    second[...] = (unit * gains[1:2, :] + biases[1:2, :]).astype(BF)
    grad_out = padded(cotangent, t) * live[...]
    for n in range(8):
        sec_blocks[n] = second[:, SIDE * n : SIDE * n + SIDE]
        go[n] = grad_out[:, SIDE * n : SIDE * n + SIDE].astype(BF)
    unpack_narrow(wire, narrow, wire.shape[0] // 5)
    unpack_sorted(wire, narrow, order, 0, w_up, 8, 8)
    unpack_sorted(wire, narrow, order, 64, w_down, 8, 8)

    def hidden_block(j, carry):
        row = pl.multiple_of(j * SIDE, 32)
        hid = dot(second[...], w_up[j]) + up_bias[pl.ds(j, 1), :]
        cdf = 0.5 * (1.0 + lax.erf(hid * 0.5**0.5))
        slope = cdf + hid * (jnp.exp(-0.5 * hid * hid) * (2.0 * math.pi) ** -0.5)
        act_blocks[j] = (hid * cdf).astype(BF)
        ga = dot_nt(go[0], w_down[0, pl.ds(row, SIDE), :])
        for n in range(1, 8):
            ga = ga + dot_nt(go[n], w_down[n, pl.ds(row, SIDE), :])
        low = (ga * slope).astype(BF)
        gh[j] = low
        bias_sums[pl.ds(j, 1), :] = jnp.sum(low.astype(F32), axis=0, keepdims=True)
        return carry

    lax.fori_loop(0, 8, hidden_block, 0)

    def second_back(i, carry):
        row = pl.multiple_of(i * SIDE, 32)
        value = dot_nt(gh[0], w_up[0, pl.ds(row, SIDE), :])
        for j in range(1, 8):
            value = value + dot_nt(gh[j], w_up[j, pl.ds(row, SIDE), :])
        block[i] = value
        return carry

    lax.fori_loop(0, 8, second_back, 0)
    for n in range(8):
        part_second[:, SIDE * n : SIDE * n + SIDE] = block[n][0:t, :].astype(BF)

    def down(n, carry):
        value = dot(act_blocks[0], w_down[n, 0:SIDE, :])
        for j in range(1, 8):
            value = value + dot(act_blocks[j], w_down[n, j * SIDE : (j + 1) * SIDE, :])
        block[n] = value
        return carry

    lax.fori_loop(0, 8, down, 0)
    for n in range(8):
        part_down[:, SIDE * n : SIDE * n + SIDE] = block[n][0:t, :].astype(BF)


def grad_tiles_body(left_at, right_at, count, read_left, read_right, wire):
    lane = lane_at((SIDE, 128))

    def body(g, carry):
        spare = None
        for q in range(4):
            s = 4 * g + q
            tile = dot_tn(read_left(left_at[s]), read_right(right_at[s]))
            wire[5 * g + q] = tile[:, 0:128].astype(BF)
            piece = jnp.concatenate([tile[:, 128:160], jnp.zeros((SIDE, 96), F32)], axis=1)
            spare = piece if q == 0 else jnp.where(lane < 32 * q, spare, pltpu.roll(piece, 32 * q, 1))
        wire[5 * g + 4] = spare.astype(BF)
        return carry

    lax.fori_loop(0, count // 4, body, 0)


def mid_back_body(order, tokens, live, cotangent, branch, down_sum, second_sum, gains, out_biases,
                  wire, mixed, probs, normed, att, rel_hi, rel_lo, pick, spread,
                  block_out, grad_middle_out, part_normed, rel_out, gm, gb, nb, sums, bias_sums,
                  w_qkv, w_proj, narrow, block, gatt):
    t = tokens.shape[0]
    x = padded(tokens, t)
    middle = x + padded(branch, t) + out_biases[0:1, :]
    result = (middle + padded(down_sum, t) + out_biases[1:2, :]) * live[...]
    block_out[...] = result[0:t, :].astype(BF)
    grad_out = padded(cotangent, t) * live[...]
    unit, inverse = norm_parts(middle)
    grad_second = padded(second_sum, t)
    sums[0:1, :] = jnp.sum(grad_second * unit, axis=0, keepdims=True)
    sums[1:2, :] = jnp.sum(grad_second, axis=0, keepdims=True)
    sums[2:3, :] = jnp.sum(grad_out, axis=0, keepdims=True)
    grad_middle = grad_out + norm_back(grad_second, unit, inverse, gains[1:2, :])
    sums[3:4, :] = jnp.sum(grad_middle, axis=0, keepdims=True)
    grad_middle_out[...] = grad_middle[0:t, :]
    for n in range(8):
        gb[n] = grad_middle[:, SIDE * n : SIDE * n + SIDE].astype(BF)
        nb[n] = normed[:, SIDE * n : SIDE * n + SIDE]
    unpack_narrow(wire, narrow, wire.shape[0] // 5)
    unpack_sorted(wire, narrow, order, 0, w_qkv, 8, 6)
    unpack_sorted(wire, narrow, order, 48, w_proj, 2, 8)
    for p in range(2):
        value = dot_nt(gb[0], w_proj[0, p * SIDE : (p + 1) * SIDE, :])
        for n in range(1, 8):
            value = value + dot_nt(gb[n], w_proj[n, p * SIDE : (p + 1) * SIDE, :])
        gatt[p] = value.astype(BF)
    attn_backward(mixed, rel_hi, rel_lo, pick, spread, probs, gatt, gm, rel_out, (SIDE // 2) ** -0.5)
    for j in range(6):
        bias_sums[j : j + 1, :] = jnp.sum(gm[j].astype(F32), axis=0, keepdims=True)

    def normed_back(i, carry):
        row = pl.multiple_of(i * SIDE, 32)
        value = dot_nt(gm[0], w_qkv[0, pl.ds(row, SIDE), :])
        for j in range(1, 6):
            value = value + dot_nt(gm[j], w_qkv[j, pl.ds(row, SIDE), :])
        block[i] = value
        return carry

    lax.fori_loop(0, 8, normed_back, 0)
    for n in range(8):
        part_normed[:, SIDE * n : SIDE * n + SIDE] = block[n][0:t, :].astype(BF)


def token_back_body(tokens, live, normed_sum, grad_middle, gains, tokens_grad, sums):
    x = tokens[...].astype(F32)
    unit, inverse = norm_parts(x)
    grad_normed = normed_sum[...].astype(F32) * live[...]
    sums[0:1, :] = jnp.sum(grad_normed * unit, axis=0, keepdims=True)
    sums[1:2, :] = jnp.sum(grad_normed, axis=0, keepdims=True)
    tokens_grad[...] = grad_middle[...] + norm_back(grad_normed, unit, inverse, gains[0:1, :])


def square_tile(square, t):
    return jnp.concatenate([square[0, t], square[1, t, :, 0:32]], axis=1)


def put_tile(square, t, value):
    square[0, t] = value[:, 0:128]
    square[1, t, :, 0:32] = value[:, 128:160]


def split_dot(kind, a, b):
    a_hi, a_lo = low_parts(a)
    b_hi, b_lo = low_parts(b)
    return kind(a_hi, b_hi) + (kind(a_hi, b_lo) + kind(a_lo, b_hi))


def soap_units(r, g, wire, sq_left, sq_right, master, first, second,
               grad_out, new_out, copy_out, first_out, second_out, sq_grad, sq_work):
    rows = slice(8 * r, 8 * r + 8)
    count = wire.shape[0] // 4
    left, right = sq_left.at[g], sq_right.at[g]

    def total(i):
        w = [wire[p * count + i].astype(F32) for p in range(4)]
        return (w[0] + w[1]) + (w[2] + w[3])

    def load():
        for half in range(2):
            last = total(5 * (2 * r + half) + 4)
            for q in range(4):
                sq_grad[0, 4 * half + q] = total(5 * (2 * r + half) + q)
                sq_grad[1, 4 * half + q] = last if q == 0 else pltpu.roll(last, 128 - 32 * q, 1)

        def write(at, value):
            grad_out[rows, pl.ds(at, 128)] = value

        square_to_flat(sq_grad, write)

    def rotate(t, carry):
        half = split_dot(dot_tn, square_tile(left, t), square_tile(sq_grad, t))
        put_tile(sq_work, t, split_dot(dot, half, square_tile(right, t)))
        return carry

    def moments(at, rotated):
        cols = pl.ds(at, 128)
        f = beta_one * first[rows, cols] + (1.0 - beta_one) * rotated
        s = beta_two * second[rows, cols] + (1.0 - beta_two) * rotated * rotated
        first_out[rows, cols] = f
        second_out[rows, cols] = s
        new_out[rows, cols] = f / (jnp.sqrt(s) + adam_eps)

    def turn_back(t, carry):
        half = split_dot(dot, square_tile(left, t), square_tile(sq_work, t))
        put_tile(sq_work, t, split_dot(dot_nt, half, square_tile(right, t)))
        return carry

    def finish(at, update):
        cols = pl.ds(at, 128)
        value = master[rows, cols] - learn_rate * update
        new_out[rows, cols] = value
        copy_out[rows, cols] = value.astype(BF)

    def loop(body):
        lax.fori_loop(0, 8, body, 0)

    return [
        load,
        lambda: loop(rotate),
        lambda: square_to_flat(sq_work, moments),
        lambda: flat_to_square(lambda at: new_out[rows, pl.ds(at, 128)], sq_work),
        lambda: loop(turn_back),
        lambda: square_to_flat(sq_work, finish),
    ]


def soap_attn_body(wire, sq_left, sq_right, master, first, second,
                   grad_out, new_out, copy_out, first_out, second_out, sq_grad, sq_work):
    for unit in soap_units(0, 0, wire, sq_left, sq_right, master, first, second,
                           grad_out, new_out, copy_out, first_out, second_out, sq_grad, sq_work):
        unit()


def build(mesh):
    placed = (
        P("dp", None, None),
        P("dp", None),
        P("dp", None, None),
        P(),
        P(),
        P(),
        P("mp"),
        P("mp"),
        P(),
        P("mp", None),
        P("mp", None),
        P("mp", "dp", None),
        P("mp", "dp", None),
        P("mp", "dp", None),
        P("mp", "dp", None),
        P("mp", "dp", None),
        P("mp", "dp", None),
        P("mp", "dp", None),
        P("mp", "dp", None),
        P("mp", "dp", None),
        P("mp", "dp", None),
    )
    return jax.shard_map(
        fast_local if dict(mesh.shape) == {"dp": 8, "mp": 4} else local,
        mesh=mesh,
        in_specs=placed,
        out_specs=(
            P("dp", None, None),
            P("dp", None, None),
            P(),
            P(),
            P(),
            P("mp"),
            P("mp"),
            P(),
            P("mp", "dp", None),
            P("mp", "dp", None),
            P("mp", "dp", None),
            P("mp", "dp", None),
            P("mp", "dp", None),
            P("mp", "dp", None),
            P("mp", "dp", None),
            P("mp", "dp", None),
            P("mp", "dp", None),
            P("mp", "dp", None),
        ),
        check_vma=False,
    )


VM = pl.BlockSpec(memory_space=pltpu.VMEM)
SM = pl.BlockSpec(memory_space=pltpu.SMEM)
LIMIT = 60 * 1024 * 1024


def call(body, tables, args, outs, scratch, name):
    return pl.pallas_call(
        body,
        out_shape=[jax.ShapeDtypeStruct(shape, kind) for shape, kind in outs],
        in_specs=[SM] * len(tables) + [VM] * len(args),
        out_specs=[VM] * len(outs),
        scratch_shapes=[pltpu.VMEM(shape, kind) for shape, kind in scratch],
        compiler_params=pltpu.CompilerParams(vmem_limit_bytes=LIMIT),
        name=name,
    )(*tables, *args)


def rel_constants(side):
    rows = np.arange(ROWS)
    lanes = np.arange(896)
    within, along = lanes % 64, lanes // 64
    high = np.where(rows < side * side, rows // side, -1)[:, None]
    wide = np.where(rows < side * side, rows % side, -1)[:, None]
    pick = np.where(within[None] < 32, high == along[None], wide == along[None])
    keys = np.arange(ROWS)
    key_h, key_w = keys // side, keys % side
    offset = np.where(within[:, None] < 32, along[:, None] - key_h[None], along[:, None] - key_w[None]) + side - 1
    spread = (offset == (within % 32)[:, None]) & (keys < side * side)[None]
    return jnp.asarray(pick, BF), jnp.asarray(spread, BF)


def inverse_order(owner):
    count = owner.shape[0]
    at = jnp.arange(count, dtype=jnp.int32)
    return jnp.sum(jnp.where(owner[:, None] == at[None, :], at[:, None], 0), axis=0)


def fast_local(
    tokens, pad_mask, cotangent, norm_gains, norm_biases, out_biases, qkv_bias, up_bias, rel_pos,
    attn_owner, mlp_owner, attn_master, mlp_master, attn_left, attn_right, mlp_left, mlp_right,
    attn_first, attn_second, mlp_first, mlp_second,
):
    t, width = tokens.shape[1:]
    tok, cot = tokens[0], cotangent[0]
    live = jnp.pad(pad_mask[0].astype(F32), (0, ROWS - t))[:, None]
    qb, ub = qkv_bias.reshape(6, SIDE), up_bias.reshape(8, SIDE)
    rel = jnp.pad(rel_pos, ((0, 0), (0, 32 - rel_pos.shape[1]), (0, 0))).reshape(64, SIDE // 2)
    rel_hi, rel_lo = low_parts(jnp.tile(rel, (2, 2)))
    pick, spread = rel_constants((rel_pos.shape[1] + 1) // 2)
    own_a, own_m = attn_owner[0], mlp_owner[0]
    ord_a, ord_m = inverse_order(own_a), inverse_order(own_m)
    xa = jnp.where(own_a < 48, own_a // 6, 8 + (own_a - 48) // 8)
    ya = jnp.where(own_a < 48, own_a % 6, 6 + (own_a - 48) % 8)
    xm, ym = own_m // 8, (own_m // 64) * 8 + own_m % 8

    wire_a, wire_m = call(
        pack_body, (), (attn_master[0], mlp_master[0]),
        [((10, SIDE, 128), BF), ((20, SIDE, 128), BF)], [((2, 8, SIDE, 128), F32)], "pack")
    all_a = gather(wire_a, 0, "gather_attn")

    part, normed, mixed, probs, att = call(
        attn_fwd_body, (ord_a,),
        (tok, live, norm_gains, norm_biases, qb, rel_hi, rel_lo, pick, spread, all_a),
        [((t, width), BF), ((ROWS, width), BF), ((6, ROWS, SIDE), BF), ((4, ROWS, ROWS), F32), ((2, ROWS, SIDE), BF)],
        [((6, 8 * SIDE, SIDE), BF), ((8, 2 * SIDE, SIDE), BF), ((64, SIDE, 32), BF), ((8, ROWS, SIDE), F32)],
        "attn_fwd")
    branch = lax.psum(part, "mp")
    wire_m, mixed = lax.optimization_barrier((wire_m, mixed))
    all_m = gather(wire_m, 1, "gather_mlp")
    part_down, part_second, sec_blocks, act_blocks, gh, go, up_sums = call(
        mlp_body, (ord_m,),
        (tok, live, cot, branch, norm_gains, norm_biases, out_biases, ub, all_m),
        [((t, width), BF), ((t, width), BF)] + [((8, ROWS, SIDE), BF)] * 4 + [((8, SIDE), F32)],
        [((8, 8 * SIDE, SIDE), BF), ((8, 8 * SIDE, SIDE), BF), ((128, SIDE, 32), BF), ((8, ROWS, SIDE), F32), ((ROWS, width), BF)],
        "mlp")
    second_sum = lax.psum(part_second, "mp")
    down_sum = lax.psum(part_down, "mp")

    sum_m, sq_left_m, sq_right_m, sq_left_a, sq_right_a = scatter_call(
        scatter_mlp_body, 20, (xm, ym),
        (sec_blocks, act_blocks, gh, go, mlp_left[0], mlp_right[0], attn_left[0], attn_right[0]),
        [((2, 2, 8, SIDE, 128), F32)] * 2 + [((1, 2, 8, SIDE, 128), F32)] * 2,
        [((16, ROWS, SIDE), BF)] * 2 + [((80, SIDE, 128), BF)], 2, 250_000_000, "scatter_mlp")
    second_sum, down_sum, sum_m = lax.optimization_barrier((second_sum, down_sum, sum_m))

    block_out, grad_middle, part_normed, rel_part, gm, gb, nb, sums_two, qkv_sums = call(
        mid_back_body, (ord_a,),
        (tok, live, cot, branch, down_sum, second_sum, norm_gains, out_biases, all_a, mixed, probs, normed, att,
         rel_hi, rel_lo, pick, spread),
        [((t, width), BF), ((t, width), F32), ((t, width), BF), ((128, SIDE), F32), ((6, ROWS, SIDE), BF),
         ((8, ROWS, SIDE), BF), ((8, ROWS, SIDE), BF), ((4, width), F32), ((6, SIDE), F32)],
        [((6, 8 * SIDE, SIDE), BF), ((8, 2 * SIDE, SIDE), BF), ((64, SIDE, 32), BF), ((8, ROWS, SIDE), F32),
         ((2, ROWS, SIDE), BF)],
        "mid_back")
    rel_half = SIDE // 2
    rel_fold = rel_part[:64] + rel_part[64:]
    rel_fold = (rel_fold[:, :rel_half] + rel_fold[:, rel_half:]).reshape(2, 32, rel_half)[:, : rel_pos.shape[1]]
    rel_size = rel_fold.size
    rel_rows = -(-rel_size // width)
    rel_flat = jnp.pad(rel_fold.reshape(-1).astype(BF), (0, rel_rows * width - rel_size)).reshape(rel_rows, width)
    both_sum = lax.psum(jnp.concatenate([part_normed, rel_flat], axis=0), "mp")

    def attn_tiles(left_at, right_at, nb_ref, att_ref, gm_ref, gb_ref, wire, lefts, rights):
        lefts[0:8], lefts[8:10] = nb_ref[...], att_ref[...]
        rights[0:6], rights[6:14] = gm_ref[...], gb_ref[...]
        grad_tiles_body(left_at, right_at, 64, lambda i: lefts[i], lambda i: rights[i], wire)

    stack_a, = call(
        attn_tiles, (xa, ya), (nb, att, gm, gb), [((80, SIDE, 128), BF)],
        [((10, ROWS, SIDE), BF), ((14, ROWS, SIDE), BF)], "attn_tiles")
    def soap_outs(shape):
        return [(shape, F32), (shape, F32), (shape, BF), (shape, F32), (shape, F32)]

    sum_a, mg, mn, mc, mf, ms = scatter_call(
        scatter_attn_body, 10, (), (stack_a, sum_m, sq_left_m, sq_right_m, mlp_master[0], mlp_first[0], mlp_second[0]),
        soap_outs(mlp_master.shape[1:]), [((2, 8, SIDE, 128), F32)] * 2, 4, 150_000_000, "scatter_attn")
    both_sum, sum_a = lax.optimization_barrier((both_sum, sum_a))
    normed_sum, rel_sum = both_sum[:t], both_sum[t:].reshape(-1)[:rel_size].astype(F32)
    tokens_grad, sums_one = call(
        token_back_body, (), (tok, live[:t], normed_sum, grad_middle, norm_gains),
        [((t, width), F32), ((2, width), F32)], [], "token_back")
    small = [sums_one.reshape(-1), sums_two.reshape(-1), qkv_sums.reshape(-1), up_sums.reshape(-1), rel_sum]
    edges = np.cumsum([0] + [v.shape[0] for v in small])
    lines = -(-int(edges[-1]) // 1024) * 8
    small = jnp.pad(jnp.concatenate(small), (0, lines * 128 - int(edges[-1]))).reshape(1, lines, 128)
    total = jnp.sum(gather(small, 3, "gather_sums", 1), axis=0).reshape(-1)
    one, two, qkv_grad, up_grad, rel_grad = [total[edges[i]:edges[i + 1]] for i in range(5)]
    one, two = one.reshape(2, width), two.reshape(4, width)
    gains_grad = jnp.stack([one[0], two[0]])
    biases_grad = jnp.stack([one[1], two[1]])
    outb_grad = jnp.stack([two[3], two[2]])
    rel_grad = rel_grad.reshape(rel_pos.shape)

    ag, an, ac, af, as_ = call(
        soap_attn_body, (), (sum_a, sq_left_a, sq_right_a, attn_master[0], attn_first[0], attn_second[0]),
        soap_outs(attn_master.shape[1:]), [((2, 8, SIDE, 128), F32)] * 2, "soap_attn")
    return (block_out[None], tokens_grad[None], gains_grad, biases_grad, outb_grad, qkv_grad, up_grad, rel_grad,
            *(value[None] for value in (ag, mg, an, mn, ac, mc, af, as_, mf, ms)))


def solution(mesh):
    return build(mesh)
```

```python
import functools
import math

import jax
import jax.numpy as jnp
import numpy as np
from jax import lax
from jax.experimental import pallas as pl
from jax.experimental.pallas import tpu as pltpu
from jax.sharding import PartitionSpec as P

highest = lax.Precision.HIGHEST
norm_eps = 1e-06
beta_one = 0.9
beta_two = 0.95
adam_eps = 1e-08
learn_rate = 0.02


def untile(tile_rows, row_count, col_count, tile_side):
    shaped = tile_rows.reshape(row_count // tile_side, col_count // tile_side, tile_side, tile_side)
    return shaped.transpose(0, 2, 1, 3).reshape(row_count, col_count)


def retile(matrix, tile_side):
    row_count, col_count = matrix.shape
    shaped = matrix.reshape(row_count // tile_side, tile_side, col_count // tile_side, tile_side)
    return shaped.transpose(0, 2, 1, 3).reshape(-1, tile_side * tile_side)


def rel_onehot(win_side):
    positions = jnp.arange(win_side, dtype=jnp.int32)
    offset = positions[:, None] - positions[None, :] + (win_side - 1)
    entries = jnp.arange(2 * win_side - 1, dtype=jnp.int32)
    return (offset[:, :, None] == entries[None, None, :]).astype(jnp.float32)


def norm_forward(values, norm_gain, norm_shift):
    centre = values - jnp.mean(values, axis=-1, keepdims=True)
    inverse = lax.rsqrt(jnp.mean(centre * centre, axis=-1, keepdims=True) + norm_eps)
    unit_rows = centre * inverse
    return (unit_rows * norm_gain + norm_shift, unit_rows, inverse)


def norm_backward(grad_in, unit_rows, inverse, norm_gain):
    grad_unit = grad_in * norm_gain
    centred = grad_unit - jnp.mean(grad_unit, axis=-1, keepdims=True)
    return inverse * (centred - unit_rows * jnp.mean(grad_unit * unit_rows, axis=-1, keepdims=True))


def gelu_pair(values):
    normal_cdf = 0.5 * (1.0 + lax.erf(values * 0.5**0.5))
    density = jnp.exp(-0.5 * values * values) * (2.0 * math.pi) ** (-0.5)
    return (values * normal_cdf, normal_cdf + values * density)


def soap_step(grad_tiles, master, left_basis, right_basis, first_moment, second_moment):
    tile_side = math.isqrt(grad_tiles.shape[2])
    square = (grad_tiles.shape[0], grad_tiles.shape[1], tile_side, tile_side)
    left_square = left_basis.reshape(square)
    right_square = right_basis.reshape(square)
    half_turn = jnp.einsum(
        "mtji,mtjk->mtik", left_square, grad_tiles.reshape(square), precision=highest
    )
    rotated = jnp.einsum("mtik,mtkl->mtil", half_turn, right_square, precision=highest).reshape(
        grad_tiles.shape
    )
    first_new = beta_one * first_moment + (1.0 - beta_one) * rotated
    second_new = beta_two * second_moment + (1.0 - beta_two) * rotated * rotated
    direction = (first_new / (jnp.sqrt(second_new) + adam_eps)).reshape(square)
    back_half = jnp.einsum("mtij,mtjk->mtik", left_square, direction, precision=highest)
    update = jnp.einsum("mtik,mtlk->mtil", back_half, right_square, precision=highest).reshape(
        grad_tiles.shape
    )
    master_new = master - learn_rate * update
    return (master_new, master_new.astype(jnp.bfloat16), first_new, second_new)


def local(
    tokens,
    pad_mask,
    cotangent,
    norm_gains,
    norm_biases,
    out_biases,
    qkv_bias,
    up_bias,
    rel_pos,
    attn_owner,
    mlp_owner,
    attn_master,
    mlp_master,
    attn_left,
    attn_right,
    mlp_left,
    mlp_right,
    attn_first,
    attn_second,
    mlp_first,
    mlp_second,
):
    windows, win_tokens, model_width = tokens.shape
    row_count = windows * win_tokens
    qkv_cols = qkv_bias.shape[0]
    head_cols = qkv_cols // 3
    unit_cols = up_bias.shape[0]
    head_dim = rel_pos.shape[2]
    heads_here = head_cols // head_dim
    win_side = (rel_pos.shape[1] + 1) // 2
    tile_side = math.isqrt(attn_master.shape[2])
    qkv_count = model_width // tile_side * (qkv_cols // tile_side)
    up_count = model_width // tile_side * (unit_cols // tile_side)
    score_scale = head_dim ** (-0.5)
    attn_stored, mlp_stored = (
        lax.all_gather(attn_master.astype(jnp.bfloat16), "dp", axis=1, tiled=True),
        lax.all_gather(mlp_master.astype(jnp.bfloat16), "dp", axis=1, tiled=True),
    )
    attn_order = jnp.argsort(attn_owner[0])
    mlp_order = jnp.argsort(mlp_owner[0])
    attn_sorted = attn_stored[0][attn_order]
    mlp_sorted = mlp_stored[0][mlp_order]
    w_qkv = untile(attn_sorted[:qkv_count], model_width, qkv_cols, tile_side)
    w_proj = untile(attn_sorted[qkv_count:], head_cols, model_width, tile_side)
    w_up = untile(mlp_sorted[:up_count], model_width, unit_cols, tile_side)
    w_down = untile(mlp_sorted[up_count:], unit_cols, model_width, tile_side)
    onehot = rel_onehot(win_side)
    table_h = jnp.einsum("ijr,rc->ijc", onehot, rel_pos[0], precision=highest)
    table_w = jnp.einsum("ijr,rc->ijc", onehot, rel_pos[1], precision=highest)
    flat_rows = tokens.reshape(row_count, model_width).astype(jnp.float32)
    live_rows = pad_mask.reshape(row_count, 1).astype(jnp.float32)
    normed, unit_one, inverse_one = norm_forward(flat_rows, norm_gains[0], norm_biases[0])
    normed_low = (normed * live_rows).astype(jnp.bfloat16)
    mixed_rows = (jnp.dot(normed_low, w_qkv, preferred_element_type=jnp.float32) + qkv_bias).astype(
        jnp.bfloat16
    )
    head_parts = mixed_rows.reshape(windows, win_tokens, 3, heads_here, head_dim)
    queries = head_parts[:, :, 0]
    key_rows = head_parts[:, :, 1]
    value_rows = head_parts[:, :, 2]
    query_grid = queries.astype(jnp.float32).reshape(
        windows, win_side, win_side, heads_here, head_dim
    )

    def score_rows():
        direct = (
            jnp.einsum("wqhc,wkhc->whqk", queries, key_rows, preferred_element_type=jnp.float32)
            * score_scale
        )
        along_h = jnp.einsum("wabhc,akc->whabk", query_grid, table_h, precision=highest)
        along_w = jnp.einsum("wabhc,blc->whabl", query_grid, table_w, precision=highest)
        return direct + (along_h[..., :, None] + along_w[..., None, :]).reshape(
            windows, heads_here, win_tokens, win_tokens
        )

    scores = score_rows()
    row_top = jnp.max(scores, axis=-1, keepdims=True)
    exponent = jnp.exp(scores - row_top)
    row_total = jnp.sum(exponent, axis=-1, keepdims=True)
    log_total = row_top + jnp.log(row_total)
    probs_low = (exponent / row_total).astype(jnp.bfloat16)
    attended = jnp.einsum(
        "whqk,wkhc->wqhc", probs_low, value_rows, preferred_element_type=jnp.float32
    )
    attended_low = attended.reshape(row_count, head_cols).astype(jnp.bfloat16)
    branch = lax.psum(
        jnp.dot(attended_low, w_proj, preferred_element_type=jnp.float32).astype(jnp.bfloat16), "mp"
    ).astype(jnp.float32)
    middle = flat_rows + branch + out_biases[0]
    second, unit_two, inverse_two = norm_forward(middle, norm_gains[1], norm_biases[1])
    second_low = second.astype(jnp.bfloat16)
    hidden = jnp.dot(second_low, w_up, preferred_element_type=jnp.float32) + up_bias
    active, gelu_slope = gelu_pair(hidden)
    active_low = active.astype(jnp.bfloat16)
    down_sum = lax.psum(
        jnp.dot(active_low, w_down, preferred_element_type=jnp.float32).astype(jnp.bfloat16), "mp"
    ).astype(jnp.float32)
    block_output = (
        ((middle + down_sum + out_biases[1]) * live_rows)
        .astype(jnp.bfloat16)
        .reshape(windows, win_tokens, model_width)
    )
    grad_out = cotangent.reshape(row_count, model_width).astype(jnp.float32) * live_rows
    grad_out_low = grad_out.astype(jnp.bfloat16)
    down_bias_grad = jnp.sum(grad_out, axis=0)
    w_down_grad = jnp.einsum(
        "nf,nd->fd", active_low, grad_out_low, preferred_element_type=jnp.float32
    )
    grad_active = jnp.einsum("nd,fd->nf", grad_out_low, w_down, preferred_element_type=jnp.float32)
    grad_hidden = (grad_active * gelu_slope).astype(jnp.bfloat16)
    up_bias_grad = jnp.sum(grad_hidden.astype(jnp.float32), axis=0)
    w_up_grad = jnp.einsum("nd,nf->df", second_low, grad_hidden, preferred_element_type=jnp.float32)
    mlp_stack = jnp.concatenate(
        [retile(w_up_grad, tile_side), retile(w_down_grad, tile_side)], axis=0
    )[mlp_owner[0]][None]
    grad_second = lax.psum(
        jnp.einsum("nf,df->nd", grad_hidden, w_up, preferred_element_type=jnp.float32).astype(
            jnp.bfloat16
        ),
        "mp",
    ).astype(jnp.float32)
    gain_two_grad = jnp.sum(grad_second * unit_two, axis=0)
    shift_two_grad = jnp.sum(grad_second, axis=0)
    grad_middle = grad_out + norm_backward(grad_second, unit_two, inverse_two, norm_gains[1])
    proj_bias_grad = jnp.sum(grad_middle, axis=0)
    grad_branch = grad_middle.astype(jnp.bfloat16)
    w_proj_grad = jnp.einsum(
        "nc,nd->cd", attended_low, grad_branch, preferred_element_type=jnp.float32
    )
    grad_attended = jnp.einsum("nd,cd->nc", grad_branch, w_proj, preferred_element_type=jnp.float32)
    grad_attended = grad_attended.astype(jnp.bfloat16).reshape(
        windows, win_tokens, heads_here, head_dim
    )
    probs_full = jnp.exp(score_rows() - log_total)
    probs_again = probs_full.astype(jnp.bfloat16)
    grad_probs = jnp.einsum(
        "wqhc,wkhc->whqk", grad_attended, value_rows, preferred_element_type=jnp.float32
    )
    grad_values = jnp.einsum(
        "whqk,wqhc->wkhc", probs_again, grad_attended, preferred_element_type=jnp.float32
    )
    grad_scores = (
        probs_full * (grad_probs - jnp.sum(probs_full * grad_probs, axis=-1, keepdims=True))
    ).astype(jnp.bfloat16)
    grad_queries = (
        jnp.einsum("whqk,wkhc->wqhc", grad_scores, key_rows, preferred_element_type=jnp.float32)
        * score_scale
    )
    grad_keys = (
        jnp.einsum("whqk,wqhc->wkhc", grad_scores, queries, preferred_element_type=jnp.float32)
        * score_scale
    )
    grad_grid = grad_scores.astype(jnp.float32).reshape(
        windows, heads_here, win_side, win_side, win_side, win_side
    )
    grad_h = jnp.sum(grad_grid, axis=5)
    grad_w = jnp.sum(grad_grid, axis=4)
    grad_rel_q = jnp.einsum("whabk,akc->wabhc", grad_h, table_h, precision=highest) + jnp.einsum(
        "whabl,blc->wabhc", grad_w, table_w, precision=highest
    )
    grad_queries = grad_queries + grad_rel_q.reshape(windows, win_tokens, heads_here, head_dim)
    table_h_grad = jnp.einsum("whabk,wabhc->akc", grad_h, query_grid, precision=highest)
    table_w_grad = jnp.einsum("whabl,wabhc->blc", grad_w, query_grid, precision=highest)
    rel_part = jnp.stack(
        [
            jnp.einsum("ijr,ijc->rc", onehot, table_h_grad, precision=highest),
            jnp.einsum("ijr,ijc->rc", onehot, table_w_grad, precision=highest),
        ]
    )
    grad_mixed = (
        jnp.stack([grad_queries, grad_keys, grad_values], axis=2)
        .reshape(row_count, qkv_cols)
        .astype(jnp.bfloat16)
    )
    qkv_bias_grad = jnp.sum(grad_mixed.astype(jnp.float32), axis=0)
    w_qkv_grad = jnp.einsum("nd,nc->dc", normed_low, grad_mixed, preferred_element_type=jnp.float32)
    grad_normed, rel_sum = (
        lax.psum(
            jnp.einsum("nc,dc->nd", grad_mixed, w_qkv, preferred_element_type=jnp.float32).astype(
                jnp.bfloat16
            ),
            "mp",
        ).astype(jnp.float32),
        lax.psum(rel_part.astype(jnp.bfloat16), "mp").astype(jnp.float32),
    )
    grad_normed = grad_normed * live_rows
    gain_one_grad = jnp.sum(grad_normed * unit_one, axis=0)
    shift_one_grad = jnp.sum(grad_normed, axis=0)
    tokens_grad = (
        grad_middle + norm_backward(grad_normed, unit_one, inverse_one, norm_gains[0])
    ).reshape(windows, win_tokens, model_width)
    attn_stack = jnp.concatenate(
        [retile(w_qkv_grad, tile_side), retile(w_proj_grad, tile_side)], axis=0
    )[attn_owner[0]][None]
    attn_grad, mlp_grad = (
        lax.psum_scatter(attn_stack, "dp", scatter_dimension=1, tiled=True),
        lax.psum_scatter(mlp_stack, "dp", scatter_dimension=1, tiled=True),
    )
    gains_grad, biases_grad, out_biases_grad, rel_pos_grad, qkv_bias_total, up_bias_total = (
        lax.psum(
            (
                jnp.stack([gain_one_grad, gain_two_grad]),
                jnp.stack([shift_one_grad, shift_two_grad]),
                jnp.stack([proj_bias_grad, down_bias_grad]),
                rel_sum,
                qkv_bias_grad,
                up_bias_grad,
            ),
            "dp",
        )
    )
    attn_new, attn_copy, attn_first_new, attn_second_new = soap_step(
        attn_grad, attn_master, attn_left, attn_right, attn_first, attn_second
    )
    mlp_new, mlp_copy, mlp_first_new, mlp_second_new = soap_step(
        mlp_grad, mlp_master, mlp_left, mlp_right, mlp_first, mlp_second
    )
    return (
        block_output,
        tokens_grad,
        gains_grad,
        biases_grad,
        out_biases_grad,
        qkv_bias_total,
        up_bias_total,
        rel_pos_grad,
        attn_grad,
        mlp_grad,
        attn_new,
        mlp_new,
        attn_copy,
        mlp_copy,
        attn_first_new,
        attn_second_new,
        mlp_first_new,
        mlp_second_new,
    )


BF = jnp.bfloat16
F32 = jnp.float32
ROWS = 208
SIDE = 160


def dot(a, b):
    return jnp.dot(a, b, preferred_element_type=F32)


def dot_nt(a, b):
    return lax.dot_general(a, b, (((1,), (1,)), ((), ())), preferred_element_type=F32)


def dot_tn(a, b):
    return lax.dot_general(a, b, (((0,), (0,)), ((), ())), preferred_element_type=F32)


def lane_at(shape):
    return lax.broadcasted_iota(jnp.int32, shape, len(shape) - 1)


def low_parts(value):
    high = value.astype(BF)
    return high, (value - high.astype(F32)).astype(BF)


def flat_to_square(read, square, count=8):
    lane = lane_at((8, 128))

    def rows_of(base):
        x = [read(base + 128 * k) for k in range(5)]
        r1 = pltpu.roll(x[1], 96, 1)
        r2 = pltpu.roll(x[2], 96, 1)
        h2 = pltpu.roll(x[2], 64, 1)
        h3 = pltpu.roll(x[3], 64, 1)
        r3 = pltpu.roll(x[3], 32, 1)
        r4 = pltpu.roll(x[4], 32, 1)
        return (
            (x[0], x[1]),
            (jnp.where(lane < 96, r1, r2), r2),
            (jnp.where(lane < 64, h2, h3), h3),
            (jnp.where(lane < 32, r3, r4), r4),
        )

    def body(group, carry):
        base = pl.multiple_of(group * 1280, 128)
        rows = rows_of(base) + rows_of(base + 640)
        for part in range(2):
            stacked = jnp.stack([row[part] for row in rows], axis=0)
            square[part, :, pl.ds(pl.multiple_of(8 * group, 8), 8), :] = jnp.swapaxes(stacked, 0, 1)
        return carry

    lax.fori_loop(0, 20, body, 0)


def square_to_flat(square, write, count=8):
    lane = lane_at((8, 128))

    def body(group, carry):
        at = pl.ds(pl.multiple_of(8 * group, 8), 8)
        wide = jnp.swapaxes(square[0, :, at, :], 0, 1)
        narrow = jnp.swapaxes(square[1, :, at, :], 0, 1)
        for half in range(2):
            base = pl.multiple_of(group * 1280, 128) + 640 * half
            a = [wide[4 * half + m] for m in range(4)]
            b = [narrow[4 * half + m] for m in range(4)]
            a1 = pltpu.roll(a[1], 32, 1)
            b1 = pltpu.roll(b[1], 32, 1)
            a2 = pltpu.roll(a[2], 64, 1)
            b2 = pltpu.roll(b[2], 64, 1)
            a3 = pltpu.roll(a[3], 96, 1)
            b3 = pltpu.roll(b[3], 96, 1)
            write(base, a[0])
            write(base + 128, jnp.where(lane < 32, b[0], a1))
            write(base + 256, jnp.where(lane < 32, a1, jnp.where(lane < 64, b1, a2)))
            write(base + 384, jnp.where(lane < 64, a2, jnp.where(lane < 96, b2, a3)))
            write(base + 512, jnp.where(lane < 96, a3, b3))
        return carry

    lax.fori_loop(0, 20, body, 0)


def pack_eight(source, first, wire, base, square):
    lane = lane_at((SIDE, 128))
    flat_to_square(lambda at: source[first : first + 8, pl.ds(at, 128)], square)
    for half in range(2):
        spare = None
        for q in range(4):
            wire[base + 5 * half + q] = square[0, 4 * half + q].astype(BF)
            piece = square[1, 4 * half + q]
            spare = piece if q == 0 else jnp.where(lane < 32 * q, spare, pltpu.roll(piece, 32 * q, 1))
        wire[base + 5 * half + 4] = spare.astype(BF)


def pack_attn_body(attn, wire, square):
    pack_eight(attn, 0, wire, 0, square)


def pack_mlp_units(mlp, wire, square):
    return [
        lambda: pack_eight(mlp, 0, wire, 0, square),
        lambda: pack_eight(mlp, 8, wire, 10, square),
    ]


def unpack_narrow(wire, narrow, groups):
    def body(g, carry):
        last = wire[5 * g + 4]
        for q in range(4):
            narrow[4 * g + q] = last[:, 32 * q : 32 * q + 32]
        return carry

    lax.fori_loop(0, groups, body, 0)


def unpack_sorted(wire, narrow, order, base, outs, rows, cols):
    def body(t, carry):
        row = t // cols
        col = t - row * cols
        stored = order[base + t]
        where_at = pl.multiple_of(row * SIDE, 32)
        outs[col, pl.ds(where_at, SIDE), 0:128] = wire[(stored // 4) * 5 + stored % 4]
        outs[col, pl.ds(where_at, SIDE), 128:160] = narrow[stored]
        return carry

    lax.fori_loop(0, rows * cols, body, 0)


MESH_ID = pl.DeviceIdType.MESH


def gather_body(piece, inputs, outputs, make_units, wire, *refs):
    args, refs = refs[:inputs], refs[inputs:]
    out, outs, refs = refs[0], refs[1 : 1 + outputs], refs[1 + outputs :]
    send_sem, recv_sem, own_sem = refs[:3]
    units = make_units(*args, *outs, *refs[3:]) if make_units else []
    count = wire.shape[0]
    pieces = count // piece
    me = lax.axis_index("dp")
    z, x = me // 2, me % 2
    side = me + 1 - 2 * x
    up, down = jnp.minimum(me + 2, 6 + x), jnp.maximum(me - 2, x)

    barrier = pltpu.get_barrier_semaphore()

    def greet(target):
        pl.semaphore_signal(barrier, inc=1, device_id={"dp": target}, device_id_type=MESH_ID)

    greet(side)
    pl.when(z < 3)(lambda: greet(up))
    pl.when(z > 0)(lambda: greet(down))
    inner = (z > 0) & (z < 3)
    pl.when(inner)(lambda: pl.semaphore_wait(barrier, 3))
    pl.when(jnp.logical_not(inner))(lambda: pl.semaphore_wait(barrier, 2))

    def copy(way, target, origin, k, own=False):
        place = out.at[pl.ds(origin * count + piece * k, piece)]
        return pltpu.make_async_remote_copy(
            src_ref=wire.at[pl.ds(piece * k, piece)] if own else place,
            dst_ref=place,
            send_sem=send_sem.at[way, origin // 2, k],
            recv_sem=recv_sem.at[origin, k],
            device_id={"dp": target},
            device_id_type=MESH_ID,
        )

    for k in range(pieces):
        copy(0, side, me, k, True).start()
        pl.when(z < 3)(lambda k=k: copy(1, up, me, k, True).start())
        pl.when(z > 0)(lambda k=k: copy(2, down, me, k, True).start())
    keep = pltpu.make_async_copy(wire, out.at[pl.ds(me * count, count)], own_sem)
    keep.start()
    slots = 1 + 3 * pieces

    def work(slot):
        for i, unit in enumerate(units):
            if i * slots // len(units) == slot:
                unit()

    work(0)
    for d in range(1, 4):
        for k in range(pieces):
            def from_below():
                origin = me - 2 * d
                copy(1, up, origin, k).wait_recv()
                copy(0, side, origin, k).start()
                pl.when(z < 3)(lambda: copy(1, up, origin, k).start())

            def from_above():
                origin = me + 2 * d
                copy(2, down, origin, k).wait_recv()
                copy(0, side, origin, k).start()
                pl.when(z > 0)(lambda: copy(2, down, origin, k).start())

            pl.when(z >= d)(from_below)
            pl.when(z + d <= 3)(from_above)
            work(1 + (d - 1) * pieces + k)

    keep.wait()
    for k in range(pieces):
        for line in range(4):
            origin = 2 * line + x
            copy(0, side, origin + 1 - 2 * x, k).wait_recv()
            copy(0, side, origin, k, False).wait_send()
            pl.when((line <= z) & (z < 3))(lambda: copy(1, up, origin, k).wait_send())
            pl.when((line >= z) & (z > 0))(lambda: copy(2, down, origin, k).wait_send())


def gather(wire, ident, name, piece=5, make_units=None, args=(), outs=(), scratch=()):
    count = wire.shape[0]
    results = pl.pallas_call(
        functools.partial(gather_body, piece, len(args), len(outs), make_units),
        out_shape=[jax.ShapeDtypeStruct((8 * count,) + wire.shape[1:], wire.dtype)]
        + [jax.ShapeDtypeStruct(*out) for out in outs],
        in_specs=[VM] * (1 + len(args)),
        out_specs=[pl.BlockSpec(memory_space=pl.ANY)] + [VM] * len(outs),
        scratch_shapes=[
            pltpu.SemaphoreType.DMA((3, 4, count // piece)),
            pltpu.SemaphoreType.DMA((8, count // piece)),
            pltpu.SemaphoreType.DMA,
        ] + [pltpu.VMEM(*item) for item in scratch],
        compiler_params=pltpu.CompilerParams(
            collective_id=ident, has_side_effects=True, vmem_limit_bytes=LIMIT),
        cost_estimate=pl.CostEstimate(flops=0, bytes_accessed=count * 12_000_000, transcendentals=0),
        name=name,
    )(wire, *args)
    return results if outs else results[0]


CHUNK = 5
AHEAD = 4


def scatter_steps(count, prepare, source, own_part, out, inbox, half,
                  side_send, side_recv, line_send, line_recv, own, units, each=1):
    me = lax.axis_index("dp")
    z, x = me // 2, me % 2
    side = me + 1 - 2 * x
    pieces = count // CHUNK
    steps = 4 * pieces

    def line_at(j):
        return lax.rem(z + j, 4)

    barrier = pltpu.get_barrier_semaphore()
    for target in (side, 2 * line_at(1) + x, 2 * line_at(2) + x, 2 * line_at(3) + x):
        pl.semaphore_signal(barrier, inc=1, device_id={"dp": target}, device_id_type=MESH_ID)
    pl.semaphore_wait(barrier, 4)

    def place(at):
        j, k = lax.div(at, pieces), lax.rem(at, pieces)
        return j, k, line_at(j + 1)

    def to_side(at):
        j, k, line = place(at)
        return pltpu.make_async_remote_copy(
            src_ref=source(2 * line + 1 - x, line, k),
            dst_ref=inbox.at[pl.ds(line * count + CHUNK * k, CHUNK)],
            send_sem=side_send.at[j, k], recv_sem=side_recv.at[j, k],
            device_id={"dp": side}, device_id_type=MESH_ID)

    def to_line(at):
        j, k, line = place(at)
        return pltpu.make_async_remote_copy(
            src_ref=half.at[pl.ds(line * count + CHUNK * k, CHUNK)],
            dst_ref=out.at[pl.ds(z * count + CHUNK * k, CHUNK)],
            send_sem=line_send.at[j, k], recv_sem=line_recv.at[j, k],
            device_id={"dp": 2 * line + x}, device_id_type=MESH_ID)

    def keep(k):
        return pltpu.make_async_copy(
            half.at[pl.ds(z * count + CHUNK * k, CHUNK)], out.at[pl.ds(z * count + CHUNK * k, CHUNK)], own.at[k])

    def send(at):
        _, k, line = place(at)
        prepare(2 * line + 1 - x, line, k)
        to_side(at).start()

    def first(at, carry):
        send(at)
        return carry

    def step(at, carry):
        _, k, line = place(at)
        for i, unit in enumerate(units):
            turn = i // 2 if i < 2 * each else i - each
            pl.when(at == min(turn, steps - 1))(unit)
        to_side(at).wait_recv()
        pl.when(at + AHEAD < steps)(lambda: send(at + AHEAD))
        own_part(2 * line + x, line, k)
        pl.when(at < 3 * pieces)(lambda: to_line(at).start())
        pl.when(at >= 3 * pieces)(lambda: keep(k).start())
        return carry

    def last(at, carry):
        to_side(at).wait_send()

        def lines():
            to_line(at).wait_send()
            to_line(at).wait_recv()

        pl.when(at < 3 * pieces)(lines)
        pl.when(at >= 3 * pieces)(lambda: keep(place(at)[1]).wait())
        return carry

    lax.fori_loop(0, AHEAD, first, 0)
    lax.fori_loop(0, steps, step, 0)
    lax.fori_loop(0, steps, last, 0)


def scatter_call(body, count, tables, args, outs, scratch, ident, cost, name):
    shape = (4 * count, SIDE, 128)
    pieces = count // CHUNK
    return pl.pallas_call(
        body,
        out_shape=[jax.ShapeDtypeStruct(shape, BF)] + [jax.ShapeDtypeStruct(*out) for out in outs],
        in_specs=[SM] * len(tables) + [VM] * len(args),
        out_specs=[pl.BlockSpec(memory_space=pl.ANY)] + [VM] * len(outs),
        scratch_shapes=[pltpu.VMEM(shape, BF)] * 2 + [pltpu.SemaphoreType.DMA((4, pieces))] * 4
        + [pltpu.SemaphoreType.DMA((pieces,))] + [pltpu.VMEM(*item) for item in scratch],
        compiler_params=pltpu.CompilerParams(
            collective_id=ident, has_side_effects=True, vmem_limit_bytes=LIMIT),
        cost_estimate=pl.CostEstimate(flops=0, bytes_accessed=cost, transcendentals=0),
        name=name,
    )(*tables, *args)


def tile_steps(count, left_at, right_at, lefts, rights, inbox, half, sent):
    lane = lane_at((SIDE, 128))

    def tiles(chunk, k, emit):
        spare = None
        for q in range(4):
            s = count // 5 * 4 * chunk + 4 * k + q
            tile = dot_tn(lefts[left_at[s]], rights[right_at[s]])
            emit(q, tile[:, 0:128])
            piece = jnp.concatenate([tile[:, 128:160], jnp.zeros((SIDE, 96), F32)], axis=1)
            spare = piece if q == 0 else jnp.where(lane < 32 * q, spare, pltpu.roll(piece, 32 * q, 1))
        emit(4, spare)

    def prepare(chunk, line, k):
        def emit(q, value):
            sent[count * line + CHUNK * k + q] = value.astype(BF)
        tiles(chunk, k, emit)

    def source(chunk, line, k):
        return sent.at[pl.ds(count * line + CHUNK * k, CHUNK)]

    def own_part(chunk, line, k):
        def emit(q, value):
            at = count * line + CHUNK * k + q
            half[at] = (value + inbox[at].astype(F32)).astype(BF)
        tiles(chunk, k, emit)

    return prepare, source, own_part


def scatter_mlp_body(left_at, right_at, sec, act, gh, go, left_m, right_m, left_a, right_a,
                     out, sq_left_m, sq_right_m, sq_left_a, sq_right_a, inbox, half,
                     side_send, side_recv, line_send, line_recv, own, lefts, rights, sent):
    lefts[0:8], lefts[8:16] = sec[...], act[...]
    rights[0:8], rights[8:16] = gh[...], go[...]
    units = []
    for flat, square in ((left_m, sq_left_m), (right_m, sq_right_m), (left_a, sq_left_a), (right_a, sq_right_a)):
        for g in range(square.shape[0]):
            units.append(lambda f=flat, r=8 * g, sq=square, g=g: flat_to_square(
                lambda at: f[r : r + 8, pl.ds(at, 128)], sq.at[g]))
    scatter_steps(20, *tile_steps(20, left_at, right_at, lefts, rights, inbox, half, sent),
                  out, inbox, half, side_send, side_recv, line_send, line_recv, own, units)


def scatter_attn_body(left_at, right_at, nb, att, gm, gb, wire, sq_left, sq_right, master, first, second,
                      out, grad_out, new_out, copy_out, first_out, second_out, inbox, half,
                      side_send, side_recv, line_send, line_recv, own, lefts, rights, sent, sq_grad, sq_work):
    lefts[0:8], lefts[8:10] = nb[...], att[...]
    rights[0:6], rights[6:14] = gm[...], gb[...]
    units = []
    for g in range(2):
        units += soap_units(g, g, wire, sq_left, sq_right, master, first, second,
                            grad_out, new_out, copy_out, first_out, second_out, sq_grad, sq_work)
    scatter_steps(10, *tile_steps(10, left_at, right_at, lefts, rights, inbox, half, sent),
                  out, inbox, half, side_send, side_recv, line_send, line_recv, own, units, 4)


def norm_parts(x):
    mean = jnp.mean(x, axis=-1, keepdims=True)
    centre = x - mean
    inverse = lax.rsqrt(jnp.mean(centre * centre, axis=-1, keepdims=True) + norm_eps)
    return centre * inverse, inverse


def norm_back(grad_in, unit, inverse, gain):
    w = grad_in * gain
    return inverse * (
        w - jnp.mean(w, axis=-1, keepdims=True) - unit * jnp.mean(w * unit, axis=-1, keepdims=True)
    )


def padded(ref, rows, kind=F32):
    value = ref[...].astype(kind)
    return jnp.concatenate([value, jnp.zeros((ROWS - rows, value.shape[1]), kind)], axis=0)


def attn_forward(mixed, rel_hi, rel_lo, pick, spread, probs, att, scale, tokens_here):
    lane = lane_at((ROWS, SIDE))
    key_ok = lane_at((ROWS, ROWS)) < tokens_here
    head = SIDE // 2
    for p in range(2):
        q, k, v = mixed[p], mixed[2 + p], mixed[4 + p]
        parts = []
        for h in range(2):
            mine = (lane >= head) if h else (lane < head)
            qm = jnp.where(mine, q, jnp.zeros_like(q))
            s = dot_nt(qm, k) * scale
            a_hi, a_lo = low_parts(dot_nt(qm, rel_hi[...]) + dot_nt(qm, rel_lo[...]))
            for c in range(7):
                mask = pick[:, 128 * c : 128 * c + 128]
                table = spread[128 * c : 128 * c + 128, :]
                s = s + dot(a_hi * mask, table) + dot(a_lo * mask, table)
            s = jnp.where(key_ok, s, -1e30)
            top = jnp.max(s, axis=-1, keepdims=True)
            e = jnp.exp(s - top)
            pr = e / jnp.sum(e, axis=-1, keepdims=True)
            probs[2 * p + h] = pr
            parts.append(dot(pr.astype(BF), v))
        att[p] = jnp.where(lane < head, parts[0], parts[1]).astype(BF)


def attn_backward(mixed, rel_hi, rel_lo, pick, spread, probs, gatt, gm, rel_out, scale):
    lane = lane_at((ROWS, SIDE))
    head = SIDE // 2
    for p in range(2):
        q, k, v = mixed[p], mixed[2 + p], mixed[4 + p]
        ga = gatt[p]
        dq, dk, dv, dr = [], [], [], []
        for h in range(2):
            mine = (lane >= head) if h else (lane < head)
            pr = probs[2 * p + h]
            gam = jnp.where(mine, ga, jnp.zeros_like(ga))
            gp = dot_nt(gam, v)
            dv.append(dot_tn(pr.astype(BF), ga))
            ds = (pr * (gp - jnp.sum(pr * gp, axis=-1, keepdims=True))).astype(BF)
            da = None
            for c in range(7):
                term = dot_nt(ds, spread[128 * c : 128 * c + 128, :]) * pick[:, 128 * c : 128 * c + 128].astype(F32)
                da = term if da is None else da + term
            da_hi, da_lo = low_parts(da)
            relq = dot(da_hi, rel_hi[...]) + dot(da_lo, rel_hi[...]) + dot(da_hi, rel_lo[...])
            dq.append(dot(ds, k) * scale + relq)
            dk.append(dot_tn(ds, q) * scale)
            dr.append(dot_tn(da_hi, q) + dot_tn(da_lo, q))
        gm[p] = jnp.where(lane < head, dq[0], dq[1]).astype(BF)
        gm[2 + p] = jnp.where(lane < head, dk[0], dk[1]).astype(BF)
        gm[4 + p] = jnp.where(lane < head, dv[0], dv[1]).astype(BF)
        rel = jnp.where(lane_at((128, SIDE)) < head, dr[0], dr[1])
        if p == 0:
            rel_out[...] = rel
        else:
            rel_out[...] += rel


def attn_fwd_body(order, tokens, live, gains, biases, qkv_bias, rel_hi, rel_lo, pick, spread, wire,
                  part, normed, mixed, probs, att, w_qkv, w_proj, narrow, block):
    t = tokens.shape[0]
    x = padded(tokens, t)
    unit, _ = norm_parts(x)
    normed[...] = ((unit * gains[0:1, :] + biases[0:1, :]) * live[...]).astype(BF)
    unpack_narrow(wire, narrow, wire.shape[0] // 5)
    unpack_sorted(wire, narrow, order, 0, w_qkv, 8, 6)
    unpack_sorted(wire, narrow, order, 48, w_proj, 2, 8)

    def mix(j, carry):
        mixed[j] = (dot(normed[...], w_qkv[j]) + qkv_bias[pl.ds(j, 1), :]).astype(BF)
        return carry

    lax.fori_loop(0, 6, mix, 0)
    attn_forward(mixed, rel_hi, rel_lo, pick, spread, probs, att, (SIDE // 2) ** -0.5, t)

    def project(n, carry):
        value = dot(att[0], w_proj[n, 0:SIDE, :]) + dot(att[1], w_proj[n, SIDE : 2 * SIDE, :])
        block[n] = value
        return carry

    lax.fori_loop(0, 8, project, 0)
    for n in range(8):
        part[:, SIDE * n : SIDE * n + SIDE] = block[n][0:t, :].astype(BF)


def mlp_body(order, tokens, live, cotangent, branch, gains, biases, out_biases, up_bias, wire,
             part_down, part_second, sec_blocks, act_blocks, gh, go, bias_sums, w_up, w_down, narrow, block, second):
    t = tokens.shape[0]
    x = padded(tokens, t)
    middle = x + padded(branch, t) + out_biases[0:1, :]
    unit, _ = norm_parts(middle)
    second[...] = (unit * gains[1:2, :] + biases[1:2, :]).astype(BF)
    grad_out = padded(cotangent, t) * live[...]
    for n in range(8):
        sec_blocks[n] = second[:, SIDE * n : SIDE * n + SIDE]
        go[n] = grad_out[:, SIDE * n : SIDE * n + SIDE].astype(BF)
    unpack_narrow(wire, narrow, wire.shape[0] // 5)
    unpack_sorted(wire, narrow, order, 0, w_up, 8, 8)
    unpack_sorted(wire, narrow, order, 64, w_down, 8, 8)

    def hidden_block(j, carry):
        row = pl.multiple_of(j * SIDE, 32)
        hid = dot(second[...], w_up[j]) + up_bias[pl.ds(j, 1), :]
        cdf = 0.5 * (1.0 + lax.erf(hid * 0.5**0.5))
        slope = cdf + hid * (jnp.exp(-0.5 * hid * hid) * (2.0 * math.pi) ** -0.5)
        act_blocks[j] = (hid * cdf).astype(BF)
        ga = dot_nt(go[0], w_down[0, pl.ds(row, SIDE), :])
        for n in range(1, 8):
            ga = ga + dot_nt(go[n], w_down[n, pl.ds(row, SIDE), :])
        low = (ga * slope).astype(BF)
        gh[j] = low
        bias_sums[pl.ds(j, 1), :] = jnp.sum(low.astype(F32), axis=0, keepdims=True)
        return carry

    lax.fori_loop(0, 8, hidden_block, 0)

    def second_back(i, carry):
        row = pl.multiple_of(i * SIDE, 32)
        value = dot_nt(gh[0], w_up[0, pl.ds(row, SIDE), :])
        for j in range(1, 8):
            value = value + dot_nt(gh[j], w_up[j, pl.ds(row, SIDE), :])
        block[i] = value
        return carry

    lax.fori_loop(0, 8, second_back, 0)
    for n in range(8):
        part_second[:, SIDE * n : SIDE * n + SIDE] = block[n][0:t, :].astype(BF)

    def down(n, carry):
        value = dot(act_blocks[0], w_down[n, 0:SIDE, :])
        for j in range(1, 8):
            value = value + dot(act_blocks[j], w_down[n, j * SIDE : (j + 1) * SIDE, :])
        block[n] = value
        return carry

    lax.fori_loop(0, 8, down, 0)
    for n in range(8):
        part_down[:, SIDE * n : SIDE * n + SIDE] = block[n][0:t, :].astype(BF)


def mid_back_body(order, tokens, live, cotangent, branch, down_sum, second_sum, gains, out_biases,
                  wire, mixed, probs, normed, att, rel_hi, rel_lo, pick, spread,
                  block_out, grad_middle_out, part_normed, rel_out, gm, gb, nb, sums, bias_sums,
                  w_qkv, w_proj, narrow, block, gatt):
    t = tokens.shape[0]
    x = padded(tokens, t)
    middle = x + padded(branch, t) + out_biases[0:1, :]
    result = (middle + padded(down_sum, t) + out_biases[1:2, :]) * live[...]
    block_out[...] = result[0:t, :].astype(BF)
    grad_out = padded(cotangent, t) * live[...]
    unit, inverse = norm_parts(middle)
    grad_second = padded(second_sum, t)
    sums[0:1, :] = jnp.sum(grad_second * unit, axis=0, keepdims=True)
    sums[1:2, :] = jnp.sum(grad_second, axis=0, keepdims=True)
    sums[2:3, :] = jnp.sum(grad_out, axis=0, keepdims=True)
    grad_middle = grad_out + norm_back(grad_second, unit, inverse, gains[1:2, :])
    sums[3:4, :] = jnp.sum(grad_middle, axis=0, keepdims=True)
    grad_middle_out[...] = grad_middle[0:t, :]
    for n in range(8):
        gb[n] = grad_middle[:, SIDE * n : SIDE * n + SIDE].astype(BF)
        nb[n] = normed[:, SIDE * n : SIDE * n + SIDE]
    unpack_narrow(wire, narrow, wire.shape[0] // 5)
    unpack_sorted(wire, narrow, order, 0, w_qkv, 8, 6)
    unpack_sorted(wire, narrow, order, 48, w_proj, 2, 8)
    for p in range(2):
        value = dot_nt(gb[0], w_proj[0, p * SIDE : (p + 1) * SIDE, :])
        for n in range(1, 8):
            value = value + dot_nt(gb[n], w_proj[n, p * SIDE : (p + 1) * SIDE, :])
        gatt[p] = value.astype(BF)
    attn_backward(mixed, rel_hi, rel_lo, pick, spread, probs, gatt, gm, rel_out, (SIDE // 2) ** -0.5)
    for j in range(6):
        bias_sums[j : j + 1, :] = jnp.sum(gm[j].astype(F32), axis=0, keepdims=True)

    def normed_back(i, carry):
        row = pl.multiple_of(i * SIDE, 32)
        value = dot_nt(gm[0], w_qkv[0, pl.ds(row, SIDE), :])
        for j in range(1, 6):
            value = value + dot_nt(gm[j], w_qkv[j, pl.ds(row, SIDE), :])
        block[i] = value
        return carry

    lax.fori_loop(0, 8, normed_back, 0)
    for n in range(8):
        part_normed[:, SIDE * n : SIDE * n + SIDE] = block[n][0:t, :].astype(BF)


def token_back_body(tokens, live, normed_sum, grad_middle, gains, tokens_grad, sums):
    x = tokens[...].astype(F32)
    unit, inverse = norm_parts(x)
    grad_normed = normed_sum[...].astype(F32) * live[...]
    sums[0:1, :] = jnp.sum(grad_normed * unit, axis=0, keepdims=True)
    sums[1:2, :] = jnp.sum(grad_normed, axis=0, keepdims=True)
    tokens_grad[...] = grad_middle[...] + norm_back(grad_normed, unit, inverse, gains[0:1, :])


def square_tile(square, t):
    return jnp.concatenate([square[0, t], square[1, t, :, 0:32]], axis=1)


def put_tile(square, t, value):
    square[0, t] = value[:, 0:128]
    square[1, t, :, 0:32] = value[:, 128:160]


def split_dot(kind, a, b):
    a_hi, a_lo = low_parts(a)
    b_hi, b_lo = low_parts(b)
    return kind(a_hi, b_hi) + (kind(a_hi, b_lo) + kind(a_lo, b_hi))


def soap_units(r, g, wire, sq_left, sq_right, master, first, second,
               grad_out, new_out, copy_out, first_out, second_out, sq_grad, sq_work):
    rows = slice(8 * r, 8 * r + 8)
    count = wire.shape[0] // 4
    left, right = sq_left.at[g], sq_right.at[g]

    def total(i):
        w = [wire[p * count + i].astype(F32) for p in range(4)]
        return (w[0] + w[1]) + (w[2] + w[3])

    def load():
        for half in range(2):
            last = total(5 * (2 * r + half) + 4)
            for q in range(4):
                sq_grad[0, 4 * half + q] = total(5 * (2 * r + half) + q)
                sq_grad[1, 4 * half + q] = last if q == 0 else pltpu.roll(last, 128 - 32 * q, 1)

        def write(at, value):
            grad_out[rows, pl.ds(at, 128)] = value

        square_to_flat(sq_grad, write)

    def rotate(t, carry):
        half = split_dot(dot_tn, square_tile(left, t), square_tile(sq_grad, t))
        put_tile(sq_work, t, split_dot(dot, half, square_tile(right, t)))
        return carry

    def moments(at, rotated):
        cols = pl.ds(at, 128)
        f = beta_one * first[rows, cols] + (1.0 - beta_one) * rotated
        s = beta_two * second[rows, cols] + (1.0 - beta_two) * rotated * rotated
        first_out[rows, cols] = f
        second_out[rows, cols] = s
        new_out[rows, cols] = f / (jnp.sqrt(s) + adam_eps)

    def turn_back(t, carry):
        half = split_dot(dot, square_tile(left, t), square_tile(sq_work, t))
        put_tile(sq_work, t, split_dot(dot_nt, half, square_tile(right, t)))
        return carry

    def finish(at, update):
        cols = pl.ds(at, 128)
        value = master[rows, cols] - learn_rate * update
        new_out[rows, cols] = value
        copy_out[rows, cols] = value.astype(BF)

    def loop(body):
        lax.fori_loop(0, 8, body, 0)

    return [
        load,
        lambda: loop(rotate),
        lambda: square_to_flat(sq_work, moments),
        lambda: flat_to_square(lambda at: new_out[rows, pl.ds(at, 128)], sq_work),
        lambda: loop(turn_back),
        lambda: square_to_flat(sq_work, finish),
    ]


def build(mesh):
    placed = (
        P("dp", None, None),
        P("dp", None),
        P("dp", None, None),
        P(),
        P(),
        P(),
        P("mp"),
        P("mp"),
        P(),
        P("mp", None),
        P("mp", None),
        P("mp", "dp", None),
        P("mp", "dp", None),
        P("mp", "dp", None),
        P("mp", "dp", None),
        P("mp", "dp", None),
        P("mp", "dp", None),
        P("mp", "dp", None),
        P("mp", "dp", None),
        P("mp", "dp", None),
        P("mp", "dp", None),
    )
    return jax.shard_map(
        fast_local if dict(mesh.shape) == {"dp": 8, "mp": 4} else local,
        mesh=mesh,
        in_specs=placed,
        out_specs=(
            P("dp", None, None),
            P("dp", None, None),
            P(),
            P(),
            P(),
            P("mp"),
            P("mp"),
            P(),
            P("mp", "dp", None),
            P("mp", "dp", None),
            P("mp", "dp", None),
            P("mp", "dp", None),
            P("mp", "dp", None),
            P("mp", "dp", None),
            P("mp", "dp", None),
            P("mp", "dp", None),
            P("mp", "dp", None),
            P("mp", "dp", None),
        ),
        check_vma=False,
    )


VM = pl.BlockSpec(memory_space=pltpu.VMEM)
SM = pl.BlockSpec(memory_space=pltpu.SMEM)
LIMIT = 60 * 1024 * 1024


def call(body, tables, args, outs, scratch, name):
    return pl.pallas_call(
        body,
        out_shape=[jax.ShapeDtypeStruct(shape, kind) for shape, kind in outs],
        in_specs=[SM] * len(tables) + [VM] * len(args),
        out_specs=[VM] * len(outs),
        scratch_shapes=[pltpu.VMEM(shape, kind) for shape, kind in scratch],
        compiler_params=pltpu.CompilerParams(vmem_limit_bytes=LIMIT),
        name=name,
    )(*tables, *args)


def rel_constants(side):
    rows = np.arange(ROWS)
    lanes = np.arange(896)
    within, along = lanes % 64, lanes // 64
    high = np.where(rows < side * side, rows // side, -1)[:, None]
    wide = np.where(rows < side * side, rows % side, -1)[:, None]
    pick = np.where(within[None] < 32, high == along[None], wide == along[None])
    keys = np.arange(ROWS)
    key_h, key_w = keys // side, keys % side
    offset = np.where(within[:, None] < 32, along[:, None] - key_h[None], along[:, None] - key_w[None]) + side - 1
    spread = (offset == (within % 32)[:, None]) & (keys < side * side)[None]
    return jnp.asarray(pick, BF), jnp.asarray(spread, BF)


def inverse_order(owner):
    count = owner.shape[0]
    at = jnp.arange(count, dtype=jnp.int32)
    return jnp.sum(jnp.where(owner[:, None] == at[None, :], at[:, None], 0), axis=0)


def fast_local(
    tokens, pad_mask, cotangent, norm_gains, norm_biases, out_biases, qkv_bias, up_bias, rel_pos,
    attn_owner, mlp_owner, attn_master, mlp_master, attn_left, attn_right, mlp_left, mlp_right,
    attn_first, attn_second, mlp_first, mlp_second,
):
    t, width = tokens.shape[1:]
    tok, cot = tokens[0], cotangent[0]
    live = jnp.pad(pad_mask[0].astype(F32), (0, ROWS - t))[:, None]
    qb, ub = qkv_bias.reshape(6, SIDE), up_bias.reshape(8, SIDE)
    rel = jnp.pad(rel_pos, ((0, 0), (0, 32 - rel_pos.shape[1]), (0, 0))).reshape(64, SIDE // 2)
    rel_hi, rel_lo = low_parts(jnp.tile(rel, (2, 2)))
    pick, spread = rel_constants((rel_pos.shape[1] + 1) // 2)
    own_a, own_m = attn_owner[0], mlp_owner[0]
    ord_a, ord_m = inverse_order(own_a), inverse_order(own_m)
    xa = jnp.where(own_a < 48, own_a // 6, 8 + (own_a - 48) // 8)
    ya = jnp.where(own_a < 48, own_a % 6, 6 + (own_a - 48) % 8)
    xm, ym = own_m // 8, (own_m // 64) * 8 + own_m % 8

    wire_a, = call(
        pack_attn_body, (), (attn_master[0],), [((10, SIDE, 128), BF)], [((2, 8, SIDE, 128), F32)], "pack")
    all_a, wire_m = gather(
        wire_a, 0, "gather_attn", 5, pack_mlp_units, (mlp_master[0],), [((20, SIDE, 128), BF)],
        [((2, 8, SIDE, 128), F32)])

    part, normed, mixed, probs, att = call(
        attn_fwd_body, (ord_a,),
        (tok, live, norm_gains, norm_biases, qb, rel_hi, rel_lo, pick, spread, all_a),
        [((t, width), BF), ((ROWS, width), BF), ((6, ROWS, SIDE), BF), ((4, ROWS, ROWS), F32), ((2, ROWS, SIDE), BF)],
        [((6, 8 * SIDE, SIDE), BF), ((8, 2 * SIDE, SIDE), BF), ((64, SIDE, 32), BF), ((8, ROWS, SIDE), F32)],
        "attn_fwd")
    branch = lax.psum(part, "mp")
    wire_m, mixed = lax.optimization_barrier((wire_m, mixed))
    all_m = gather(wire_m, 1, "gather_mlp")
    part_down, part_second, sec_blocks, act_blocks, gh, go, up_sums = call(
        mlp_body, (ord_m,),
        (tok, live, cot, branch, norm_gains, norm_biases, out_biases, ub, all_m),
        [((t, width), BF), ((t, width), BF)] + [((8, ROWS, SIDE), BF)] * 4 + [((8, SIDE), F32)],
        [((8, 8 * SIDE, SIDE), BF), ((8, 8 * SIDE, SIDE), BF), ((128, SIDE, 32), BF), ((8, ROWS, SIDE), F32), ((ROWS, width), BF)],
        "mlp")
    second_sum = lax.psum(part_second, "mp")
    down_sum = lax.psum(part_down, "mp")

    sum_m, sq_left_m, sq_right_m, sq_left_a, sq_right_a = scatter_call(
        scatter_mlp_body, 20, (xm, ym),
        (sec_blocks, act_blocks, gh, go, mlp_left[0], mlp_right[0], attn_left[0], attn_right[0]),
        [((2, 2, 8, SIDE, 128), F32)] * 2 + [((1, 2, 8, SIDE, 128), F32)] * 2,
        [((16, ROWS, SIDE), BF)] * 2 + [((80, SIDE, 128), BF)], 2, 250_000_000, "scatter_mlp")
    second_sum, down_sum, sum_m = lax.optimization_barrier((second_sum, down_sum, sum_m))

    block_out, grad_middle, part_normed, rel_part, gm, gb, nb, sums_two, qkv_sums = call(
        mid_back_body, (ord_a,),
        (tok, live, cot, branch, down_sum, second_sum, norm_gains, out_biases, all_a, mixed, probs, normed, att,
         rel_hi, rel_lo, pick, spread),
        [((t, width), BF), ((t, width), F32), ((t, width), BF), ((128, SIDE), F32), ((6, ROWS, SIDE), BF),
         ((8, ROWS, SIDE), BF), ((8, ROWS, SIDE), BF), ((4, width), F32), ((6, SIDE), F32)],
        [((6, 8 * SIDE, SIDE), BF), ((8, 2 * SIDE, SIDE), BF), ((64, SIDE, 32), BF), ((8, ROWS, SIDE), F32),
         ((2, ROWS, SIDE), BF)],
        "mid_back")
    rel_half = SIDE // 2
    rel_fold = rel_part[:64] + rel_part[64:]
    rel_fold = (rel_fold[:, :rel_half] + rel_fold[:, rel_half:]).reshape(2, 32, rel_half)[:, : rel_pos.shape[1]]
    rel_size = rel_fold.size
    rel_rows = -(-rel_size // width)
    rel_flat = jnp.pad(rel_fold.reshape(-1).astype(BF), (0, rel_rows * width - rel_size)).reshape(rel_rows, width)
    both_sum = lax.psum(jnp.concatenate([part_normed, rel_flat], axis=0), "mp")

    def soap_outs(shape):
        return [(shape, F32), (shape, F32), (shape, BF), (shape, F32), (shape, F32)]

    sum_a, mg, mn, mc, mf, ms = scatter_call(
        scatter_attn_body, 10, (xa, ya), (nb, att, gm, gb, sum_m, sq_left_m, sq_right_m, mlp_master[0], mlp_first[0], mlp_second[0]),
        soap_outs(mlp_master.shape[1:]),
        [((10, ROWS, SIDE), BF), ((14, ROWS, SIDE), BF), ((40, SIDE, 128), BF)] + [((2, 8, SIDE, 128), F32)] * 2, 4, 150_000_000, "scatter_attn")
    both_sum, sum_a = lax.optimization_barrier((both_sum, sum_a))
    normed_sum, rel_sum = both_sum[:t], both_sum[t:].reshape(-1)[:rel_size].astype(F32)
    tokens_grad, sums_one = call(
        token_back_body, (), (tok, live[:t], normed_sum, grad_middle, norm_gains),
        [((t, width), F32), ((2, width), F32)], [], "token_back")
    small = [sums_one.reshape(-1), sums_two.reshape(-1), qkv_sums.reshape(-1), up_sums.reshape(-1), rel_sum]
    edges = np.cumsum([0] + [v.shape[0] for v in small])
    lines = -(-int(edges[-1]) // 1024) * 8
    small = jnp.pad(jnp.concatenate(small), (0, lines * 128 - int(edges[-1]))).reshape(1, lines, 128)
    gathered, ag, an, ac, af, as_ = gather(
        small, 3, "gather_sums", 1, functools.partial(soap_units, 0, 0),
        (sum_a, sq_left_a, sq_right_a, attn_master[0], attn_first[0], attn_second[0]),
        soap_outs(attn_master.shape[1:]), [((2, 8, SIDE, 128), F32)] * 2)
    total = jnp.sum(gathered, axis=0).reshape(-1)
    one, two, qkv_grad, up_grad, rel_grad = [total[edges[i]:edges[i + 1]] for i in range(5)]
    one, two = one.reshape(2, width), two.reshape(4, width)
    gains_grad = jnp.stack([one[0], two[0]])
    biases_grad = jnp.stack([one[1], two[1]])
    outb_grad = jnp.stack([two[3], two[2]])
    rel_grad = rel_grad.reshape(rel_pos.shape)

    return (block_out[None], tokens_grad[None], gains_grad, biases_grad, outb_grad, qkv_grad, up_grad, rel_grad,
            *(value[None] for value in (ag, mg, an, mn, ac, mc, af, as_, mf, ms)))


def solution(mesh):
    return build(mesh)
```

```python
import functools
import math

import jax
import jax.numpy as jnp
import numpy as np
from jax import lax
from jax.experimental import pallas as pl
from jax.experimental.pallas import tpu as pltpu
from jax.sharding import PartitionSpec as P

highest = lax.Precision.HIGHEST
norm_eps = 1e-06
beta_one = 0.9
beta_two = 0.95
adam_eps = 1e-08
learn_rate = 0.02


def untile(tile_rows, row_count, col_count, tile_side):
    shaped = tile_rows.reshape(row_count // tile_side, col_count // tile_side, tile_side, tile_side)
    return shaped.transpose(0, 2, 1, 3).reshape(row_count, col_count)


def retile(matrix, tile_side):
    row_count, col_count = matrix.shape
    shaped = matrix.reshape(row_count // tile_side, tile_side, col_count // tile_side, tile_side)
    return shaped.transpose(0, 2, 1, 3).reshape(-1, tile_side * tile_side)


def rel_onehot(win_side):
    positions = jnp.arange(win_side, dtype=jnp.int32)
    offset = positions[:, None] - positions[None, :] + (win_side - 1)
    entries = jnp.arange(2 * win_side - 1, dtype=jnp.int32)
    return (offset[:, :, None] == entries[None, None, :]).astype(jnp.float32)


def norm_forward(values, norm_gain, norm_shift):
    centre = values - jnp.mean(values, axis=-1, keepdims=True)
    inverse = lax.rsqrt(jnp.mean(centre * centre, axis=-1, keepdims=True) + norm_eps)
    unit_rows = centre * inverse
    return (unit_rows * norm_gain + norm_shift, unit_rows, inverse)


def norm_backward(grad_in, unit_rows, inverse, norm_gain):
    grad_unit = grad_in * norm_gain
    centred = grad_unit - jnp.mean(grad_unit, axis=-1, keepdims=True)
    return inverse * (centred - unit_rows * jnp.mean(grad_unit * unit_rows, axis=-1, keepdims=True))


def gelu_pair(values):
    normal_cdf = 0.5 * (1.0 + lax.erf(values * 0.5**0.5))
    density = jnp.exp(-0.5 * values * values) * (2.0 * math.pi) ** (-0.5)
    return (values * normal_cdf, normal_cdf + values * density)


def soap_step(grad_tiles, master, left_basis, right_basis, first_moment, second_moment):
    tile_side = math.isqrt(grad_tiles.shape[2])
    square = (grad_tiles.shape[0], grad_tiles.shape[1], tile_side, tile_side)
    left_square = left_basis.reshape(square)
    right_square = right_basis.reshape(square)
    half_turn = jnp.einsum(
        "mtji,mtjk->mtik", left_square, grad_tiles.reshape(square), precision=highest
    )
    rotated = jnp.einsum("mtik,mtkl->mtil", half_turn, right_square, precision=highest).reshape(
        grad_tiles.shape
    )
    first_new = beta_one * first_moment + (1.0 - beta_one) * rotated
    second_new = beta_two * second_moment + (1.0 - beta_two) * rotated * rotated
    direction = (first_new / (jnp.sqrt(second_new) + adam_eps)).reshape(square)
    back_half = jnp.einsum("mtij,mtjk->mtik", left_square, direction, precision=highest)
    update = jnp.einsum("mtik,mtlk->mtil", back_half, right_square, precision=highest).reshape(
        grad_tiles.shape
    )
    master_new = master - learn_rate * update
    return (master_new, master_new.astype(jnp.bfloat16), first_new, second_new)


def local(
    tokens,
    pad_mask,
    cotangent,
    norm_gains,
    norm_biases,
    out_biases,
    qkv_bias,
    up_bias,
    rel_pos,
    attn_owner,
    mlp_owner,
    attn_master,
    mlp_master,
    attn_left,
    attn_right,
    mlp_left,
    mlp_right,
    attn_first,
    attn_second,
    mlp_first,
    mlp_second,
):
    windows, win_tokens, model_width = tokens.shape
    row_count = windows * win_tokens
    qkv_cols = qkv_bias.shape[0]
    head_cols = qkv_cols // 3
    unit_cols = up_bias.shape[0]
    head_dim = rel_pos.shape[2]
    heads_here = head_cols // head_dim
    win_side = (rel_pos.shape[1] + 1) // 2
    tile_side = math.isqrt(attn_master.shape[2])
    qkv_count = model_width // tile_side * (qkv_cols // tile_side)
    up_count = model_width // tile_side * (unit_cols // tile_side)
    score_scale = head_dim ** (-0.5)
    attn_stored, mlp_stored = (
        lax.all_gather(attn_master.astype(jnp.bfloat16), "dp", axis=1, tiled=True),
        lax.all_gather(mlp_master.astype(jnp.bfloat16), "dp", axis=1, tiled=True),
    )
    attn_order = jnp.argsort(attn_owner[0])
    mlp_order = jnp.argsort(mlp_owner[0])
    attn_sorted = attn_stored[0][attn_order]
    mlp_sorted = mlp_stored[0][mlp_order]
    w_qkv = untile(attn_sorted[:qkv_count], model_width, qkv_cols, tile_side)
    w_proj = untile(attn_sorted[qkv_count:], head_cols, model_width, tile_side)
    w_up = untile(mlp_sorted[:up_count], model_width, unit_cols, tile_side)
    w_down = untile(mlp_sorted[up_count:], unit_cols, model_width, tile_side)
    onehot = rel_onehot(win_side)
    table_h = jnp.einsum("ijr,rc->ijc", onehot, rel_pos[0], precision=highest)
    table_w = jnp.einsum("ijr,rc->ijc", onehot, rel_pos[1], precision=highest)
    flat_rows = tokens.reshape(row_count, model_width).astype(jnp.float32)
    live_rows = pad_mask.reshape(row_count, 1).astype(jnp.float32)
    normed, unit_one, inverse_one = norm_forward(flat_rows, norm_gains[0], norm_biases[0])
    normed_low = (normed * live_rows).astype(jnp.bfloat16)
    mixed_rows = (jnp.dot(normed_low, w_qkv, preferred_element_type=jnp.float32) + qkv_bias).astype(
        jnp.bfloat16
    )
    head_parts = mixed_rows.reshape(windows, win_tokens, 3, heads_here, head_dim)
    queries = head_parts[:, :, 0]
    key_rows = head_parts[:, :, 1]
    value_rows = head_parts[:, :, 2]
    query_grid = queries.astype(jnp.float32).reshape(
        windows, win_side, win_side, heads_here, head_dim
    )

    def score_rows():
        direct = (
            jnp.einsum("wqhc,wkhc->whqk", queries, key_rows, preferred_element_type=jnp.float32)
            * score_scale
        )
        along_h = jnp.einsum("wabhc,akc->whabk", query_grid, table_h, precision=highest)
        along_w = jnp.einsum("wabhc,blc->whabl", query_grid, table_w, precision=highest)
        return direct + (along_h[..., :, None] + along_w[..., None, :]).reshape(
            windows, heads_here, win_tokens, win_tokens
        )

    scores = score_rows()
    row_top = jnp.max(scores, axis=-1, keepdims=True)
    exponent = jnp.exp(scores - row_top)
    row_total = jnp.sum(exponent, axis=-1, keepdims=True)
    log_total = row_top + jnp.log(row_total)
    probs_low = (exponent / row_total).astype(jnp.bfloat16)
    attended = jnp.einsum(
        "whqk,wkhc->wqhc", probs_low, value_rows, preferred_element_type=jnp.float32
    )
    attended_low = attended.reshape(row_count, head_cols).astype(jnp.bfloat16)
    branch = lax.psum(
        jnp.dot(attended_low, w_proj, preferred_element_type=jnp.float32).astype(jnp.bfloat16), "mp"
    ).astype(jnp.float32)
    middle = flat_rows + branch + out_biases[0]
    second, unit_two, inverse_two = norm_forward(middle, norm_gains[1], norm_biases[1])
    second_low = second.astype(jnp.bfloat16)
    hidden = jnp.dot(second_low, w_up, preferred_element_type=jnp.float32) + up_bias
    active, gelu_slope = gelu_pair(hidden)
    active_low = active.astype(jnp.bfloat16)
    down_sum = lax.psum(
        jnp.dot(active_low, w_down, preferred_element_type=jnp.float32).astype(jnp.bfloat16), "mp"
    ).astype(jnp.float32)
    block_output = (
        ((middle + down_sum + out_biases[1]) * live_rows)
        .astype(jnp.bfloat16)
        .reshape(windows, win_tokens, model_width)
    )
    grad_out = cotangent.reshape(row_count, model_width).astype(jnp.float32) * live_rows
    grad_out_low = grad_out.astype(jnp.bfloat16)
    down_bias_grad = jnp.sum(grad_out, axis=0)
    w_down_grad = jnp.einsum(
        "nf,nd->fd", active_low, grad_out_low, preferred_element_type=jnp.float32
    )
    grad_active = jnp.einsum("nd,fd->nf", grad_out_low, w_down, preferred_element_type=jnp.float32)
    grad_hidden = (grad_active * gelu_slope).astype(jnp.bfloat16)
    up_bias_grad = jnp.sum(grad_hidden.astype(jnp.float32), axis=0)
    w_up_grad = jnp.einsum("nd,nf->df", second_low, grad_hidden, preferred_element_type=jnp.float32)
    mlp_stack = jnp.concatenate(
        [retile(w_up_grad, tile_side), retile(w_down_grad, tile_side)], axis=0
    )[mlp_owner[0]][None]
    grad_second = lax.psum(
        jnp.einsum("nf,df->nd", grad_hidden, w_up, preferred_element_type=jnp.float32).astype(
            jnp.bfloat16
        ),
        "mp",
    ).astype(jnp.float32)
    gain_two_grad = jnp.sum(grad_second * unit_two, axis=0)
    shift_two_grad = jnp.sum(grad_second, axis=0)
    grad_middle = grad_out + norm_backward(grad_second, unit_two, inverse_two, norm_gains[1])
    proj_bias_grad = jnp.sum(grad_middle, axis=0)
    grad_branch = grad_middle.astype(jnp.bfloat16)
    w_proj_grad = jnp.einsum(
        "nc,nd->cd", attended_low, grad_branch, preferred_element_type=jnp.float32
    )
    grad_attended = jnp.einsum("nd,cd->nc", grad_branch, w_proj, preferred_element_type=jnp.float32)
    grad_attended = grad_attended.astype(jnp.bfloat16).reshape(
        windows, win_tokens, heads_here, head_dim
    )
    probs_full = jnp.exp(score_rows() - log_total)
    probs_again = probs_full.astype(jnp.bfloat16)
    grad_probs = jnp.einsum(
        "wqhc,wkhc->whqk", grad_attended, value_rows, preferred_element_type=jnp.float32
    )
    grad_values = jnp.einsum(
        "whqk,wqhc->wkhc", probs_again, grad_attended, preferred_element_type=jnp.float32
    )
    grad_scores = (
        probs_full * (grad_probs - jnp.sum(probs_full * grad_probs, axis=-1, keepdims=True))
    ).astype(jnp.bfloat16)
    grad_queries = (
        jnp.einsum("whqk,wkhc->wqhc", grad_scores, key_rows, preferred_element_type=jnp.float32)
        * score_scale
    )
    grad_keys = (
        jnp.einsum("whqk,wqhc->wkhc", grad_scores, queries, preferred_element_type=jnp.float32)
        * score_scale
    )
    grad_grid = grad_scores.astype(jnp.float32).reshape(
        windows, heads_here, win_side, win_side, win_side, win_side
    )
    grad_h = jnp.sum(grad_grid, axis=5)
    grad_w = jnp.sum(grad_grid, axis=4)
    grad_rel_q = jnp.einsum("whabk,akc->wabhc", grad_h, table_h, precision=highest) + jnp.einsum(
        "whabl,blc->wabhc", grad_w, table_w, precision=highest
    )
    grad_queries = grad_queries + grad_rel_q.reshape(windows, win_tokens, heads_here, head_dim)
    table_h_grad = jnp.einsum("whabk,wabhc->akc", grad_h, query_grid, precision=highest)
    table_w_grad = jnp.einsum("whabl,wabhc->blc", grad_w, query_grid, precision=highest)
    rel_part = jnp.stack(
        [
            jnp.einsum("ijr,ijc->rc", onehot, table_h_grad, precision=highest),
            jnp.einsum("ijr,ijc->rc", onehot, table_w_grad, precision=highest),
        ]
    )
    grad_mixed = (
        jnp.stack([grad_queries, grad_keys, grad_values], axis=2)
        .reshape(row_count, qkv_cols)
        .astype(jnp.bfloat16)
    )
    qkv_bias_grad = jnp.sum(grad_mixed.astype(jnp.float32), axis=0)
    w_qkv_grad = jnp.einsum("nd,nc->dc", normed_low, grad_mixed, preferred_element_type=jnp.float32)
    grad_normed, rel_sum = (
        lax.psum(
            jnp.einsum("nc,dc->nd", grad_mixed, w_qkv, preferred_element_type=jnp.float32).astype(
                jnp.bfloat16
            ),
            "mp",
        ).astype(jnp.float32),
        lax.psum(rel_part.astype(jnp.bfloat16), "mp").astype(jnp.float32),
    )
    grad_normed = grad_normed * live_rows
    gain_one_grad = jnp.sum(grad_normed * unit_one, axis=0)
    shift_one_grad = jnp.sum(grad_normed, axis=0)
    tokens_grad = (
        grad_middle + norm_backward(grad_normed, unit_one, inverse_one, norm_gains[0])
    ).reshape(windows, win_tokens, model_width)
    attn_stack = jnp.concatenate(
        [retile(w_qkv_grad, tile_side), retile(w_proj_grad, tile_side)], axis=0
    )[attn_owner[0]][None]
    attn_grad, mlp_grad = (
        lax.psum_scatter(attn_stack, "dp", scatter_dimension=1, tiled=True),
        lax.psum_scatter(mlp_stack, "dp", scatter_dimension=1, tiled=True),
    )
    gains_grad, biases_grad, out_biases_grad, rel_pos_grad, qkv_bias_total, up_bias_total = (
        lax.psum(
            (
                jnp.stack([gain_one_grad, gain_two_grad]),
                jnp.stack([shift_one_grad, shift_two_grad]),
                jnp.stack([proj_bias_grad, down_bias_grad]),
                rel_sum,
                qkv_bias_grad,
                up_bias_grad,
            ),
            "dp",
        )
    )
    attn_new, attn_copy, attn_first_new, attn_second_new = soap_step(
        attn_grad, attn_master, attn_left, attn_right, attn_first, attn_second
    )
    mlp_new, mlp_copy, mlp_first_new, mlp_second_new = soap_step(
        mlp_grad, mlp_master, mlp_left, mlp_right, mlp_first, mlp_second
    )
    return (
        block_output,
        tokens_grad,
        gains_grad,
        biases_grad,
        out_biases_grad,
        qkv_bias_total,
        up_bias_total,
        rel_pos_grad,
        attn_grad,
        mlp_grad,
        attn_new,
        mlp_new,
        attn_copy,
        mlp_copy,
        attn_first_new,
        attn_second_new,
        mlp_first_new,
        mlp_second_new,
    )


BF = jnp.bfloat16
F32 = jnp.float32
ROWS = 208
SIDE = 160


def dot(a, b):
    return jnp.dot(a, b, preferred_element_type=F32)


def dot_nt(a, b):
    return lax.dot_general(a, b, (((1,), (1,)), ((), ())), preferred_element_type=F32)


def dot_tn(a, b):
    return lax.dot_general(a, b, (((0,), (0,)), ((), ())), preferred_element_type=F32)


def lane_at(shape):
    return lax.broadcasted_iota(jnp.int32, shape, len(shape) - 1)


def low_parts(value):
    high = value.astype(BF)
    return high, (value - high.astype(F32)).astype(BF)


def flat_to_square(read, square, count=8):
    lane = lane_at((8, 128))

    def rows_of(base):
        x = [read(base + 128 * k) for k in range(5)]
        r1 = pltpu.roll(x[1], 96, 1)
        r2 = pltpu.roll(x[2], 96, 1)
        h2 = pltpu.roll(x[2], 64, 1)
        h3 = pltpu.roll(x[3], 64, 1)
        r3 = pltpu.roll(x[3], 32, 1)
        r4 = pltpu.roll(x[4], 32, 1)
        return (
            (x[0], x[1]),
            (jnp.where(lane < 96, r1, r2), r2),
            (jnp.where(lane < 64, h2, h3), h3),
            (jnp.where(lane < 32, r3, r4), r4),
        )

    def body(group, carry):
        base = pl.multiple_of(group * 1280, 128)
        rows = rows_of(base) + rows_of(base + 640)
        for part in range(2):
            stacked = jnp.stack([row[part] for row in rows], axis=0)
            square[part, :, pl.ds(pl.multiple_of(8 * group, 8), 8), :] = jnp.swapaxes(stacked, 0, 1)
        return carry

    lax.fori_loop(0, 20, body, 0)


def square_to_flat(square, write, count=8):
    lane = lane_at((8, 128))

    def body(group, carry):
        at = pl.ds(pl.multiple_of(8 * group, 8), 8)
        wide = jnp.swapaxes(square[0, :, at, :], 0, 1)
        narrow = jnp.swapaxes(square[1, :, at, :], 0, 1)
        for half in range(2):
            base = pl.multiple_of(group * 1280, 128) + 640 * half
            a = [wide[4 * half + m] for m in range(4)]
            b = [narrow[4 * half + m] for m in range(4)]
            a1 = pltpu.roll(a[1], 32, 1)
            b1 = pltpu.roll(b[1], 32, 1)
            a2 = pltpu.roll(a[2], 64, 1)
            b2 = pltpu.roll(b[2], 64, 1)
            a3 = pltpu.roll(a[3], 96, 1)
            b3 = pltpu.roll(b[3], 96, 1)
            write(base, a[0])
            write(base + 128, jnp.where(lane < 32, b[0], a1))
            write(base + 256, jnp.where(lane < 32, a1, jnp.where(lane < 64, b1, a2)))
            write(base + 384, jnp.where(lane < 64, a2, jnp.where(lane < 96, b2, a3)))
            write(base + 512, jnp.where(lane < 96, a3, b3))
        return carry

    lax.fori_loop(0, 20, body, 0)


def pack_eight(source, first, wire, base, square):
    lane = lane_at((SIDE, 128))
    flat_to_square(lambda at: source[first : first + 8, pl.ds(at, 128)], square)
    for half in range(2):
        spare = None
        for q in range(4):
            wire[base + 5 * half + q] = square[0, 4 * half + q].astype(BF)
            piece = square[1, 4 * half + q]
            spare = piece if q == 0 else jnp.where(lane < 32 * q, spare, pltpu.roll(piece, 32 * q, 1))
        wire[base + 5 * half + 4] = spare.astype(BF)


def pack_attn_body(attn, wire, square):
    pack_eight(attn, 0, wire, 0, square)


def pack_mlp_units(mlp, wire, square):
    return [
        lambda: pack_eight(mlp, 0, wire, 0, square),
        lambda: pack_eight(mlp, 8, wire, 10, square),
    ]


def unpack_narrow(wire, narrow, groups):
    def body(g, carry):
        last = wire[5 * g + 4]
        for q in range(4):
            narrow[4 * g + q] = last[:, 32 * q : 32 * q + 32]
        return carry

    lax.fori_loop(0, groups, body, 0)


def unpack_sorted(wire, narrow, order, base, outs, rows, cols):
    def body(t, carry):
        row = t // cols
        col = t - row * cols
        stored = order[base + t]
        where_at = pl.multiple_of(row * SIDE, 32)
        outs[col, pl.ds(where_at, SIDE), 0:128] = wire[(stored // 4) * 5 + stored % 4]
        outs[col, pl.ds(where_at, SIDE), 128:160] = narrow[stored]
        return carry

    lax.fori_loop(0, rows * cols, body, 0)


MESH_ID = pl.DeviceIdType.MESH


def gather_body(piece, inputs, outputs, make_units, wire, *refs):
    args, refs = refs[:inputs], refs[inputs:]
    out, outs, refs = refs[0], refs[1 : 1 + outputs], refs[1 + outputs :]
    send_sem, recv_sem, own_sem = refs[:3]
    units = make_units(*args, *outs, *refs[3:]) if make_units else []
    count = wire.shape[0]
    pieces = count // piece
    me = lax.axis_index("dp")
    z, x = me // 2, me % 2
    side = me + 1 - 2 * x
    up, down = jnp.minimum(me + 2, 6 + x), jnp.maximum(me - 2, x)

    barrier = pltpu.get_barrier_semaphore()

    def greet(target):
        pl.semaphore_signal(barrier, inc=1, device_id={"dp": target}, device_id_type=MESH_ID)

    greet(side)
    pl.when(z < 3)(lambda: greet(up))
    pl.when(z > 0)(lambda: greet(down))
    inner = (z > 0) & (z < 3)
    pl.when(inner)(lambda: pl.semaphore_wait(barrier, 3))
    pl.when(jnp.logical_not(inner))(lambda: pl.semaphore_wait(barrier, 2))

    def copy(way, target, origin, k, own=False):
        place = out.at[pl.ds(origin * count + piece * k, piece)]
        return pltpu.make_async_remote_copy(
            src_ref=wire.at[pl.ds(piece * k, piece)] if own else place,
            dst_ref=place,
            send_sem=send_sem.at[way, origin, k],
            recv_sem=recv_sem.at[origin, k],
            device_id={"dp": target},
            device_id_type=MESH_ID,
        )

    for k in range(pieces):
        copy(0, side, me, k, True).start()
        pl.when(z < 3)(lambda k=k: copy(1, up, me, k, True).start())
        pl.when(z > 0)(lambda k=k: copy(2, down, me, k, True).start())
    keep = pltpu.make_async_copy(wire, out.at[pl.ds(me * count, count)], own_sem)
    keep.start()
    slots = 1 + 3 * pieces
    split = (pieces + 1) // 2
    lone, high = 1 - x, 7 - x

    def work(slot):
        for i, unit in enumerate(units):
            if i * slots // len(units) == slot:
                unit()

    work(0)
    for d in range(1, 5):
        for k in range(pieces):
            def from_below():
                origin = me - 2 * d
                copy(1, up, origin, k).wait_recv()
                pl.when((z > d) | (k < split))(lambda: copy(0, side, origin, k).start())
                pl.when(z < 3)(lambda: copy(1, up, origin, k).start())

            def from_above():
                origin = me + 2 * d
                copy(2, down, origin, k).wait_recv()
                pl.when((z + d < 3) | (k < split))(lambda: copy(0, side, origin, k).start())
                pl.when(z > 0)(lambda: copy(2, down, origin, k).start())

            def other_low():
                copy(1, up, lone, k).wait_recv()
                pl.when(z < 3)(lambda: copy(1, up, lone, k).start())

            def other_high():
                copy(2, down, high, k).wait_recv()
                pl.when(z > 0)(lambda: copy(2, down, high, k).start())

            if d < 4:
                pl.when(z >= d)(from_below)
                pl.when(z + d <= 3)(from_above)
                work(1 + (d - 1) * pieces + k)
            if k >= split:
                pl.when(z == d - 1)(other_low)
                pl.when(z == 4 - d)(other_high)

    keep.wait()
    for k in range(pieces):
        for line in range(4):
            origin = 2 * line + x
            far = line in (0, 3) and k >= split
            if far:
                pl.when(z == line)(lambda: copy(0, side, origin, k).wait_send())
            else:
                copy(0, side, origin + 1 - 2 * x, k).wait_recv()
                copy(0, side, origin, k).wait_send()
            pl.when((line <= z) & (z < 3))(lambda: copy(1, up, origin, k).wait_send())
            pl.when((line >= z) & (z > 0))(lambda: copy(2, down, origin, k).wait_send())
        if k >= split:
            pl.when(z < 3)(lambda: copy(1, up, lone, k).wait_send())
            pl.when(z > 0)(lambda: copy(2, down, high, k).wait_send())


def gather(wire, ident, name, piece=5, make_units=None, args=(), outs=(), scratch=()):
    count = wire.shape[0]
    results = pl.pallas_call(
        functools.partial(gather_body, piece, len(args), len(outs), make_units),
        out_shape=[jax.ShapeDtypeStruct((8 * count,) + wire.shape[1:], wire.dtype)]
        + [jax.ShapeDtypeStruct(*out) for out in outs],
        in_specs=[VM] * (1 + len(args)),
        out_specs=[pl.BlockSpec(memory_space=pl.ANY)] + [VM] * len(outs),
        scratch_shapes=[
            pltpu.SemaphoreType.DMA((3, 8, count // piece)),
            pltpu.SemaphoreType.DMA((8, count // piece)),
            pltpu.SemaphoreType.DMA,
        ] + [pltpu.VMEM(*item) for item in scratch],
        compiler_params=pltpu.CompilerParams(
            collective_id=ident, has_side_effects=True, vmem_limit_bytes=LIMIT),
        cost_estimate=pl.CostEstimate(flops=0, bytes_accessed=count * 12_000_000, transcendentals=0),
        name=name,
    )(wire, *args)
    return results if outs else results[0]


CHUNK = 5
AHEAD = 4


def scatter_steps(count, prepare, source, own_part, out, inbox, half,
                  side_send, side_recv, line_send, line_recv, own, units, early=0, early_at=0):
    me = lax.axis_index("dp")
    z, x = me // 2, me % 2
    side = me + 1 - 2 * x
    pieces = count // CHUNK
    steps = 4 * pieces

    def line_at(j):
        return lax.rem(z + j, 4)

    barrier = pltpu.get_barrier_semaphore()
    for target in (side, 2 * line_at(1) + x, 2 * line_at(2) + x, 2 * line_at(3) + x):
        pl.semaphore_signal(barrier, inc=1, device_id={"dp": target}, device_id_type=MESH_ID)
    pl.semaphore_wait(barrier, 4)

    def place(at):
        j, k = lax.rem(at, 4), lax.div(at, 4)
        return j, k, line_at(j + 1)

    def to_side(at):
        j, k, line = place(at)
        return pltpu.make_async_remote_copy(
            src_ref=source(2 * line + 1 - x, line, k),
            dst_ref=inbox.at[pl.ds(line * count + CHUNK * k, CHUNK)],
            send_sem=side_send.at[j, k], recv_sem=side_recv.at[j, k],
            device_id={"dp": side}, device_id_type=MESH_ID)

    def to_line(at):
        j, k, line = place(at)
        return pltpu.make_async_remote_copy(
            src_ref=half.at[pl.ds(line * count + CHUNK * k, CHUNK)],
            dst_ref=out.at[pl.ds(z * count + CHUNK * k, CHUNK)],
            send_sem=line_send.at[j, k], recv_sem=line_recv.at[j, k],
            device_id={"dp": 2 * line + x}, device_id_type=MESH_ID)

    def keep(k):
        return pltpu.make_async_copy(
            half.at[pl.ds(z * count + CHUNK * k, CHUNK)], out.at[pl.ds(z * count + CHUNK * k, CHUNK)], own.at[k])

    def send(at):
        _, k, line = place(at)
        prepare(2 * line + 1 - x, line, k)
        to_side(at).start()

    def first(at, carry):
        send(at)
        return carry

    def arrived(at, carry):
        pl.when(lax.rem(at, 4) < 3)(lambda: to_line(at).wait_recv())
        pl.when(lax.rem(at, 4) == 3)(lambda: keep(lax.div(at, 4)).wait())
        return carry

    def early_wait():
        lax.fori_loop(0, 4 * early, arrived, 0)

    def step(at, carry):
        j, k, line = place(at)
        if early:
            pl.when(at == early_at)(early_wait)
        for turn, unit in units:
            pl.when(at == turn)(unit)
        to_side(at).wait_recv()
        pl.when(at + AHEAD < steps)(lambda: send(at + AHEAD))
        own_part(2 * line + x, line, k)
        pl.when(j < 3)(lambda: to_line(at).start())
        pl.when(j == 3)(lambda: keep(k).start())
        return carry

    def last(at, carry):
        to_side(at).wait_send()
        pl.when(lax.rem(at, 4) < 3)(lambda: to_line(at).wait_send())
        return carry

    lax.fori_loop(0, AHEAD, first, 0)
    lax.fori_loop(0, steps, step, 0)
    lax.fori_loop(0, steps, last, 0)
    lax.fori_loop(4 * early, steps, arrived, 0)


def scatter_call(body, count, tables, args, outs, scratch, ident, cost, name, given=0):
    shape = (4 * count, SIDE, 128)
    result = (given or 4 * count, SIDE, 128)
    pieces = count // CHUNK
    return pl.pallas_call(
        body,
        out_shape=[jax.ShapeDtypeStruct(result, BF)] + [jax.ShapeDtypeStruct(*out) for out in outs],
        in_specs=[SM] * len(tables) + [VM] * len(args),
        out_specs=[pl.BlockSpec(memory_space=pl.ANY)] + [VM] * len(outs),
        scratch_shapes=[pltpu.VMEM(shape, BF)] * 2 + [pltpu.SemaphoreType.DMA((4, pieces))] * 4
        + [pltpu.SemaphoreType.DMA((pieces,))]
        + [pltpu.VMEM(*item) if item else pltpu.SemaphoreType.DMA((4,)) for item in scratch],
        compiler_params=pltpu.CompilerParams(
            collective_id=ident, has_side_effects=True, vmem_limit_bytes=LIMIT),
        cost_estimate=pl.CostEstimate(flops=0, bytes_accessed=cost, transcendentals=0),
        name=name,
    )(*tables, *args)


def tile_steps(count, left_at, right_at, lefts, rights, inbox, half, sent):
    lane = lane_at((SIDE, 128))

    def tiles(chunk, k, emit):
        spare = None
        for q in range(4):
            s = count // 5 * 4 * chunk + 4 * k + q
            tile = dot_tn(lefts[left_at[s]], rights[right_at[s]])
            emit(q, tile[:, 0:128])
            piece = jnp.concatenate([tile[:, 128:160], jnp.zeros((SIDE, 96), F32)], axis=1)
            spare = piece if q == 0 else jnp.where(lane < 32 * q, spare, pltpu.roll(piece, 32 * q, 1))
        emit(4, spare)

    def prepare(chunk, line, k):
        def emit(q, value):
            sent[count * line + CHUNK * k + q] = value.astype(BF)
        tiles(chunk, k, emit)

    def source(chunk, line, k):
        return sent.at[pl.ds(count * line + CHUNK * k, CHUNK)]

    def own_part(chunk, line, k):
        def emit(q, value):
            at = count * line + CHUNK * k + q
            half[at] = (value + inbox[at].astype(F32)).astype(BF)
        tiles(chunk, k, emit)

    return prepare, source, own_part


def scatter_mlp_body(left_at, right_at, sec, act, gh, go, left_m, right_m, left_a, right_a, master, first, second,
                     out, sq_left_m, sq_right_m, sq_left_a, sq_right_a,
                     grad_out, new_out, copy_out, first_out, second_out, inbox, half,
                     side_send, side_recv, line_send, line_recv, own, lefts, rights, sent, landed, moved,
                     sq_left, sq_right, sq_grad, sq_work):
    lefts[0:8], lefts[8:16] = sec[...], act[...]
    rights[0:8], rights[8:16] = gh[...], go[...]
    units = []
    for turn, (flat, r, square) in enumerate((
            (left_m, 0, sq_left), (right_m, 0, sq_right), (left_m, 8, sq_left_m), (right_m, 8, sq_right_m),
            (left_a, 0, sq_left_a), (right_a, 0, sq_right_a))):
        units.append((turn, lambda f=flat, r=r, sq=square: flat_to_square(
            lambda at: f[r : r + 8, pl.ds(at, 128)], sq.at[0])))
    stages = soap_units(0, 0, landed, sq_left, sq_right, master, first, second,
                        grad_out, new_out, copy_out, first_out, second_out, sq_grad, sq_work)
    units += [(10 + i, stage) for i, stage in enumerate(stages)]
    scatter_steps(20, *tile_steps(20, left_at, right_at, lefts, rights, inbox, half, sent),
                  landed, inbox, half, side_send, side_recv, line_send, line_recv, own, units, 2, 10)
    moves = [pltpu.make_async_copy(landed.at[pl.ds(20 * p + 10, 10)], out.at[pl.ds(10 * p, 10)], moved.at[p])
             for p in range(4)]
    for move in moves:
        move.start()
    for move in moves:
        move.wait()


def scatter_attn_body(left_at, right_at, nb, att, gm, gb, wire, sq_left, sq_right, master, first, second,
                      out, grad_out, new_out, copy_out, first_out, second_out, inbox, half,
                      side_send, side_recv, line_send, line_recv, own, lefts, rights, sent, sq_grad, sq_work):
    lefts[0:8], lefts[8:10] = nb[...], att[...]
    rights[0:6], rights[6:14] = gm[...], gb[...]
    stages = soap_units(1, 0, wire, sq_left, sq_right, master, first, second,
                        grad_out, new_out, copy_out, first_out, second_out, sq_grad, sq_work)
    scatter_steps(10, *tile_steps(10, left_at, right_at, lefts, rights, inbox, half, sent),
                  out, inbox, half, side_send, side_recv, line_send, line_recv, own, list(enumerate(stages)))


def norm_parts(x):
    mean = jnp.mean(x, axis=-1, keepdims=True)
    centre = x - mean
    inverse = lax.rsqrt(jnp.mean(centre * centre, axis=-1, keepdims=True) + norm_eps)
    return centre * inverse, inverse


def norm_back(grad_in, unit, inverse, gain):
    w = grad_in * gain
    return inverse * (
        w - jnp.mean(w, axis=-1, keepdims=True) - unit * jnp.mean(w * unit, axis=-1, keepdims=True)
    )


def padded(ref, rows, kind=F32):
    value = ref[...].astype(kind)
    return jnp.concatenate([value, jnp.zeros((ROWS - rows, value.shape[1]), kind)], axis=0)


def attn_forward(mixed, rel_hi, rel_lo, pick, spread, probs, att, scale, tokens_here):
    lane = lane_at((ROWS, SIDE))
    key_ok = lane_at((ROWS, ROWS)) < tokens_here
    head = SIDE // 2
    for p in range(2):
        q, k, v = mixed[p], mixed[2 + p], mixed[4 + p]
        parts = []
        for h in range(2):
            mine = (lane >= head) if h else (lane < head)
            qm = jnp.where(mine, q, jnp.zeros_like(q))
            s = dot_nt(qm, k) * scale
            a_hi, a_lo = low_parts(dot_nt(qm, rel_hi[...]) + dot_nt(qm, rel_lo[...]))
            for c in range(7):
                mask = pick[:, 128 * c : 128 * c + 128]
                table = spread[128 * c : 128 * c + 128, :]
                s = s + dot(a_hi * mask, table) + dot(a_lo * mask, table)
            s = jnp.where(key_ok, s, -1e30)
            top = jnp.max(s, axis=-1, keepdims=True)
            e = jnp.exp(s - top)
            pr = e / jnp.sum(e, axis=-1, keepdims=True)
            probs[2 * p + h] = pr
            parts.append(dot(pr.astype(BF), v))
        att[p] = jnp.where(lane < head, parts[0], parts[1]).astype(BF)


def attn_backward(mixed, rel_hi, rel_lo, pick, spread, probs, gatt, gm, rel_out, scale):
    lane = lane_at((ROWS, SIDE))
    head = SIDE // 2
    for p in range(2):
        q, k, v = mixed[p], mixed[2 + p], mixed[4 + p]
        ga = gatt[p]
        dq, dk, dv, dr = [], [], [], []
        for h in range(2):
            mine = (lane >= head) if h else (lane < head)
            pr = probs[2 * p + h]
            gam = jnp.where(mine, ga, jnp.zeros_like(ga))
            gp = dot_nt(gam, v)
            dv.append(dot_tn(pr.astype(BF), ga))
            ds = (pr * (gp - jnp.sum(pr * gp, axis=-1, keepdims=True))).astype(BF)
            da = None
            for c in range(7):
                term = dot_nt(ds, spread[128 * c : 128 * c + 128, :]) * pick[:, 128 * c : 128 * c + 128].astype(F32)
                da = term if da is None else da + term
            da_hi, da_lo = low_parts(da)
            relq = dot(da_hi, rel_hi[...]) + dot(da_lo, rel_hi[...]) + dot(da_hi, rel_lo[...])
            dq.append(dot(ds, k) * scale + relq)
            dk.append(dot_tn(ds, q) * scale)
            dr.append(dot_tn(da_hi, q) + dot_tn(da_lo, q))
        gm[p] = jnp.where(lane < head, dq[0], dq[1]).astype(BF)
        gm[2 + p] = jnp.where(lane < head, dk[0], dk[1]).astype(BF)
        gm[4 + p] = jnp.where(lane < head, dv[0], dv[1]).astype(BF)
        rel = jnp.where(lane_at((128, SIDE)) < head, dr[0], dr[1])
        if p == 0:
            rel_out[...] = rel
        else:
            rel_out[...] += rel


def attn_fwd_body(order, tokens, live, gains, biases, qkv_bias, rel_hi, rel_lo, pick, spread, wire,
                  part, normed, mixed, probs, att, w_qkv, w_proj, narrow, block):
    t = tokens.shape[0]
    x = padded(tokens, t)
    unit, _ = norm_parts(x)
    normed[...] = ((unit * gains[0:1, :] + biases[0:1, :]) * live[...]).astype(BF)
    unpack_narrow(wire, narrow, wire.shape[0] // 5)
    unpack_sorted(wire, narrow, order, 0, w_qkv, 8, 6)
    unpack_sorted(wire, narrow, order, 48, w_proj, 2, 8)

    def mix(j, carry):
        mixed[j] = (dot(normed[...], w_qkv[j]) + qkv_bias[pl.ds(j, 1), :]).astype(BF)
        return carry

    lax.fori_loop(0, 6, mix, 0)
    attn_forward(mixed, rel_hi, rel_lo, pick, spread, probs, att, (SIDE // 2) ** -0.5, t)

    def project(n, carry):
        value = dot(att[0], w_proj[n, 0:SIDE, :]) + dot(att[1], w_proj[n, SIDE : 2 * SIDE, :])
        block[n] = value
        return carry

    lax.fori_loop(0, 8, project, 0)
    for n in range(8):
        part[:, SIDE * n : SIDE * n + SIDE] = block[n][0:t, :].astype(BF)


def mlp_body(order, tokens, live, cotangent, branch, gains, biases, out_biases, up_bias, wire,
             part_down, part_second, sec_blocks, act_blocks, gh, go, bias_sums, w_up, w_down, narrow, block, second):
    t = tokens.shape[0]
    x = padded(tokens, t)
    middle = x + padded(branch, t) + out_biases[0:1, :]
    unit, _ = norm_parts(middle)
    second[...] = (unit * gains[1:2, :] + biases[1:2, :]).astype(BF)
    grad_out = padded(cotangent, t) * live[...]
    for n in range(8):
        sec_blocks[n] = second[:, SIDE * n : SIDE * n + SIDE]
        go[n] = grad_out[:, SIDE * n : SIDE * n + SIDE].astype(BF)
    unpack_narrow(wire, narrow, wire.shape[0] // 5)
    unpack_sorted(wire, narrow, order, 0, w_up, 8, 8)
    unpack_sorted(wire, narrow, order, 64, w_down, 8, 8)

    def hidden_block(j, carry):
        row = pl.multiple_of(j * SIDE, 32)
        hid = dot(second[...], w_up[j]) + up_bias[pl.ds(j, 1), :]
        cdf = 0.5 * (1.0 + lax.erf(hid * 0.5**0.5))
        slope = cdf + hid * (jnp.exp(-0.5 * hid * hid) * (2.0 * math.pi) ** -0.5)
        act_blocks[j] = (hid * cdf).astype(BF)
        ga = dot_nt(go[0], w_down[0, pl.ds(row, SIDE), :])
        for n in range(1, 8):
            ga = ga + dot_nt(go[n], w_down[n, pl.ds(row, SIDE), :])
        low = (ga * slope).astype(BF)
        gh[j] = low
        bias_sums[pl.ds(j, 1), :] = jnp.sum(low.astype(F32), axis=0, keepdims=True)
        return carry

    lax.fori_loop(0, 8, hidden_block, 0)

    def second_back(i, carry):
        row = pl.multiple_of(i * SIDE, 32)
        value = dot_nt(gh[0], w_up[0, pl.ds(row, SIDE), :])
        for j in range(1, 8):
            value = value + dot_nt(gh[j], w_up[j, pl.ds(row, SIDE), :])
        block[i] = value
        return carry

    lax.fori_loop(0, 8, second_back, 0)
    for n in range(8):
        part_second[:, SIDE * n : SIDE * n + SIDE] = block[n][0:t, :].astype(BF)

    def down(n, carry):
        value = dot(act_blocks[0], w_down[n, 0:SIDE, :])
        for j in range(1, 8):
            value = value + dot(act_blocks[j], w_down[n, j * SIDE : (j + 1) * SIDE, :])
        block[n] = value
        return carry

    lax.fori_loop(0, 8, down, 0)
    for n in range(8):
        part_down[:, SIDE * n : SIDE * n + SIDE] = block[n][0:t, :].astype(BF)


def mid_back_body(order, tokens, live, cotangent, branch, down_sum, second_sum, gains, out_biases,
                  wire, mixed, probs, normed, att, rel_hi, rel_lo, pick, spread,
                  block_out, grad_middle_out, part_normed, rel_out, gm, gb, nb, sums, bias_sums,
                  w_qkv, w_proj, narrow, block, gatt):
    t = tokens.shape[0]
    x = padded(tokens, t)
    middle = x + padded(branch, t) + out_biases[0:1, :]
    result = (middle + padded(down_sum, t) + out_biases[1:2, :]) * live[...]
    block_out[...] = result[0:t, :].astype(BF)
    grad_out = padded(cotangent, t) * live[...]
    unit, inverse = norm_parts(middle)
    grad_second = padded(second_sum, t)
    sums[0:1, :] = jnp.sum(grad_second * unit, axis=0, keepdims=True)
    sums[1:2, :] = jnp.sum(grad_second, axis=0, keepdims=True)
    sums[2:3, :] = jnp.sum(grad_out, axis=0, keepdims=True)
    grad_middle = grad_out + norm_back(grad_second, unit, inverse, gains[1:2, :])
    sums[3:4, :] = jnp.sum(grad_middle, axis=0, keepdims=True)
    grad_middle_out[...] = grad_middle[0:t, :]
    for n in range(8):
        gb[n] = grad_middle[:, SIDE * n : SIDE * n + SIDE].astype(BF)
        nb[n] = normed[:, SIDE * n : SIDE * n + SIDE]
    unpack_narrow(wire, narrow, wire.shape[0] // 5)
    unpack_sorted(wire, narrow, order, 0, w_qkv, 8, 6)
    unpack_sorted(wire, narrow, order, 48, w_proj, 2, 8)
    for p in range(2):
        value = dot_nt(gb[0], w_proj[0, p * SIDE : (p + 1) * SIDE, :])
        for n in range(1, 8):
            value = value + dot_nt(gb[n], w_proj[n, p * SIDE : (p + 1) * SIDE, :])
        gatt[p] = value.astype(BF)
    attn_backward(mixed, rel_hi, rel_lo, pick, spread, probs, gatt, gm, rel_out, (SIDE // 2) ** -0.5)
    for j in range(6):
        bias_sums[j : j + 1, :] = jnp.sum(gm[j].astype(F32), axis=0, keepdims=True)

    def normed_back(i, carry):
        row = pl.multiple_of(i * SIDE, 32)
        value = dot_nt(gm[0], w_qkv[0, pl.ds(row, SIDE), :])
        for j in range(1, 6):
            value = value + dot_nt(gm[j], w_qkv[j, pl.ds(row, SIDE), :])
        block[i] = value
        return carry

    lax.fori_loop(0, 8, normed_back, 0)
    for n in range(8):
        part_normed[:, SIDE * n : SIDE * n + SIDE] = block[n][0:t, :].astype(BF)


def token_back_body(tokens, live, normed_sum, grad_middle, gains, tokens_grad, sums):
    x = tokens[...].astype(F32)
    unit, inverse = norm_parts(x)
    grad_normed = normed_sum[...].astype(F32) * live[...]
    sums[0:1, :] = jnp.sum(grad_normed * unit, axis=0, keepdims=True)
    sums[1:2, :] = jnp.sum(grad_normed, axis=0, keepdims=True)
    tokens_grad[...] = grad_middle[...] + norm_back(grad_normed, unit, inverse, gains[0:1, :])


def square_tile(square, t):
    return jnp.concatenate([square[0, t], square[1, t, :, 0:32]], axis=1)


def put_tile(square, t, value):
    square[0, t] = value[:, 0:128]
    square[1, t, :, 0:32] = value[:, 128:160]


def split_dot(kind, a, b):
    a_hi, a_lo = low_parts(a)
    b_hi, b_lo = low_parts(b)
    return kind(a_hi, b_hi) + (kind(a_hi, b_lo) + kind(a_lo, b_hi))


def soap_units(r, g, wire, sq_left, sq_right, master, first, second,
               grad_out, new_out, copy_out, first_out, second_out, sq_grad, sq_work):
    rows, to = slice(8 * r, 8 * r + 8), slice(0, 8)
    count = wire.shape[0] // 4
    left, right = sq_left.at[g], sq_right.at[g]

    def total(i):
        w = [wire[p * count + i].astype(F32) for p in range(4)]
        return (w[0] + w[1]) + (w[2] + w[3])

    def load():
        for half in range(2):
            last = total(5 * half + 4)
            for q in range(4):
                sq_grad[0, 4 * half + q] = total(5 * half + q)
                sq_grad[1, 4 * half + q] = last if q == 0 else pltpu.roll(last, 128 - 32 * q, 1)

        def write(at, value):
            grad_out[to, pl.ds(at, 128)] = value

        square_to_flat(sq_grad, write)

    def rotate(t, carry):
        half = split_dot(dot_tn, square_tile(left, t), square_tile(sq_grad, t))
        put_tile(sq_work, t, split_dot(dot, half, square_tile(right, t)))
        return carry

    def moments(at, rotated):
        cols = pl.ds(at, 128)
        f = beta_one * first[rows, cols] + (1.0 - beta_one) * rotated
        s = beta_two * second[rows, cols] + (1.0 - beta_two) * rotated * rotated
        first_out[to, cols] = f
        second_out[to, cols] = s
        new_out[to, cols] = f / (jnp.sqrt(s) + adam_eps)

    def turn_back(t, carry):
        half = split_dot(dot, square_tile(left, t), square_tile(sq_work, t))
        put_tile(sq_work, t, split_dot(dot_nt, half, square_tile(right, t)))
        return carry

    def finish(at, update):
        cols = pl.ds(at, 128)
        value = master[rows, cols] - learn_rate * update
        new_out[to, cols] = value
        copy_out[to, cols] = value.astype(BF)

    def loop(body):
        lax.fori_loop(0, 8, body, 0)

    return [
        load,
        lambda: loop(rotate),
        lambda: square_to_flat(sq_work, moments),
        lambda: flat_to_square(lambda at: new_out[to, pl.ds(at, 128)], sq_work),
        lambda: loop(turn_back),
        lambda: square_to_flat(sq_work, finish),
    ]


def build(mesh):
    placed = (
        P("dp", None, None),
        P("dp", None),
        P("dp", None, None),
        P(),
        P(),
        P(),
        P("mp"),
        P("mp"),
        P(),
        P("mp", None),
        P("mp", None),
        P("mp", "dp", None),
        P("mp", "dp", None),
        P("mp", "dp", None),
        P("mp", "dp", None),
        P("mp", "dp", None),
        P("mp", "dp", None),
        P("mp", "dp", None),
        P("mp", "dp", None),
        P("mp", "dp", None),
        P("mp", "dp", None),
    )
    return jax.shard_map(
        fast_local if dict(mesh.shape) == {"dp": 8, "mp": 4} else local,
        mesh=mesh,
        in_specs=placed,
        out_specs=(
            P("dp", None, None),
            P("dp", None, None),
            P(),
            P(),
            P(),
            P("mp"),
            P("mp"),
            P(),
            P("mp", "dp", None),
            P("mp", "dp", None),
            P("mp", "dp", None),
            P("mp", "dp", None),
            P("mp", "dp", None),
            P("mp", "dp", None),
            P("mp", "dp", None),
            P("mp", "dp", None),
            P("mp", "dp", None),
            P("mp", "dp", None),
        ),
        check_vma=False,
    )


VM = pl.BlockSpec(memory_space=pltpu.VMEM)
SM = pl.BlockSpec(memory_space=pltpu.SMEM)
LIMIT = 60 * 1024 * 1024


def call(body, tables, args, outs, scratch, name):
    return pl.pallas_call(
        body,
        out_shape=[jax.ShapeDtypeStruct(shape, kind) for shape, kind in outs],
        in_specs=[SM] * len(tables) + [VM] * len(args),
        out_specs=[VM] * len(outs),
        scratch_shapes=[pltpu.VMEM(shape, kind) for shape, kind in scratch],
        compiler_params=pltpu.CompilerParams(vmem_limit_bytes=LIMIT),
        name=name,
    )(*tables, *args)


def rel_constants(side):
    rows = np.arange(ROWS)
    lanes = np.arange(896)
    within, along = lanes % 64, lanes // 64
    high = np.where(rows < side * side, rows // side, -1)[:, None]
    wide = np.where(rows < side * side, rows % side, -1)[:, None]
    pick = np.where(within[None] < 32, high == along[None], wide == along[None])
    keys = np.arange(ROWS)
    key_h, key_w = keys // side, keys % side
    offset = np.where(within[:, None] < 32, along[:, None] - key_h[None], along[:, None] - key_w[None]) + side - 1
    spread = (offset == (within % 32)[:, None]) & (keys < side * side)[None]
    return jnp.asarray(pick, BF), jnp.asarray(spread, BF)


def inverse_order(owner):
    count = owner.shape[0]
    at = jnp.arange(count, dtype=jnp.int32)
    return jnp.sum(jnp.where(owner[:, None] == at[None, :], at[:, None], 0), axis=0)


def fast_local(
    tokens, pad_mask, cotangent, norm_gains, norm_biases, out_biases, qkv_bias, up_bias, rel_pos,
    attn_owner, mlp_owner, attn_master, mlp_master, attn_left, attn_right, mlp_left, mlp_right,
    attn_first, attn_second, mlp_first, mlp_second,
):
    t, width = tokens.shape[1:]
    tok, cot = tokens[0], cotangent[0]
    live = jnp.pad(pad_mask[0].astype(F32), (0, ROWS - t))[:, None]
    qb, ub = qkv_bias.reshape(6, SIDE), up_bias.reshape(8, SIDE)
    rel = jnp.pad(rel_pos, ((0, 0), (0, 32 - rel_pos.shape[1]), (0, 0))).reshape(64, SIDE // 2)
    rel_hi, rel_lo = low_parts(jnp.tile(rel, (2, 2)))
    pick, spread = rel_constants((rel_pos.shape[1] + 1) // 2)
    own_a, own_m = attn_owner[0], mlp_owner[0]
    ord_a, ord_m = inverse_order(own_a), inverse_order(own_m)
    xa = jnp.where(own_a < 48, own_a // 6, 8 + (own_a - 48) // 8)
    ya = jnp.where(own_a < 48, own_a % 6, 6 + (own_a - 48) % 8)
    xm, ym = own_m // 8, (own_m // 64) * 8 + own_m % 8

    wire_a, = call(
        pack_attn_body, (), (attn_master[0],), [((10, SIDE, 128), BF)], [((2, 8, SIDE, 128), F32)], "pack")
    all_a, wire_m = gather(
        wire_a, 0, "gather_attn", 5, pack_mlp_units, (mlp_master[0],), [((20, SIDE, 128), BF)],
        [((2, 8, SIDE, 128), F32)])

    part, normed, mixed, probs, att = call(
        attn_fwd_body, (ord_a,),
        (tok, live, norm_gains, norm_biases, qb, rel_hi, rel_lo, pick, spread, all_a),
        [((t, width), BF), ((ROWS, width), BF), ((6, ROWS, SIDE), BF), ((4, ROWS, ROWS), F32), ((2, ROWS, SIDE), BF)],
        [((6, 8 * SIDE, SIDE), BF), ((8, 2 * SIDE, SIDE), BF), ((64, SIDE, 32), BF), ((8, ROWS, SIDE), F32)],
        "attn_fwd")
    branch = lax.psum(part, "mp")
    wire_m, mixed = lax.optimization_barrier((wire_m, mixed))
    all_m = gather(wire_m, 1, "gather_mlp")
    part_down, part_second, sec_blocks, act_blocks, gh, go, up_sums = call(
        mlp_body, (ord_m,),
        (tok, live, cot, branch, norm_gains, norm_biases, out_biases, ub, all_m),
        [((t, width), BF), ((t, width), BF)] + [((8, ROWS, SIDE), BF)] * 4 + [((8, SIDE), F32)],
        [((8, 8 * SIDE, SIDE), BF), ((8, 8 * SIDE, SIDE), BF), ((128, SIDE, 32), BF), ((8, ROWS, SIDE), F32), ((ROWS, width), BF)],
        "mlp")
    second_sum = lax.psum(part_second, "mp")
    down_sum = lax.psum(part_down, "mp")

    def soap_outs():
        shape = (8, SIDE * SIDE)
        return [(shape, F32), (shape, F32), (shape, BF), (shape, F32), (shape, F32)]

    square = ((1, 2, 8, SIDE, 128), F32)
    sum_m, sq_left_m, sq_right_m, sq_left_a, sq_right_a, *upper = scatter_call(
        scatter_mlp_body, 20, (xm, ym),
        (sec_blocks, act_blocks, gh, go, mlp_left[0], mlp_right[0], attn_left[0], attn_right[0],
         mlp_master[0], mlp_first[0], mlp_second[0]),
        [square] * 4 + soap_outs(),
        [((16, ROWS, SIDE), BF)] * 2 + [((80, SIDE, 128), BF)] * 2 + [None] + [square] * 2 + [(square[0][1:], F32)] * 2,
        2, 250_000_000, "scatter_mlp", 40)
    second_sum, down_sum, sum_m = lax.optimization_barrier((second_sum, down_sum, sum_m))

    block_out, grad_middle, part_normed, rel_part, gm, gb, nb, sums_two, qkv_sums = call(
        mid_back_body, (ord_a,),
        (tok, live, cot, branch, down_sum, second_sum, norm_gains, out_biases, all_a, mixed, probs, normed, att,
         rel_hi, rel_lo, pick, spread),
        [((t, width), BF), ((t, width), F32), ((t, width), BF), ((128, SIDE), F32), ((6, ROWS, SIDE), BF),
         ((8, ROWS, SIDE), BF), ((8, ROWS, SIDE), BF), ((4, width), F32), ((6, SIDE), F32)],
        [((6, 8 * SIDE, SIDE), BF), ((8, 2 * SIDE, SIDE), BF), ((64, SIDE, 32), BF), ((8, ROWS, SIDE), F32),
         ((2, ROWS, SIDE), BF)],
        "mid_back")
    rel_half = SIDE // 2
    rel_fold = rel_part[:64] + rel_part[64:]
    rel_fold = (rel_fold[:, :rel_half] + rel_fold[:, rel_half:]).reshape(2, 32, rel_half)[:, : rel_pos.shape[1]]
    rel_size = rel_fold.size
    rel_rows = -(-rel_size // width)
    rel_flat = jnp.pad(rel_fold.reshape(-1).astype(BF), (0, rel_rows * width - rel_size)).reshape(rel_rows, width)
    both_sum = lax.psum(jnp.concatenate([part_normed, rel_flat], axis=0), "mp")

    sum_a, *lower = scatter_call(
        scatter_attn_body, 10, (xa, ya), (nb, att, gm, gb, sum_m, sq_left_m, sq_right_m, mlp_master[0], mlp_first[0], mlp_second[0]),
        soap_outs(),
        [((10, ROWS, SIDE), BF), ((14, ROWS, SIDE), BF), ((40, SIDE, 128), BF)] + [((2, 8, SIDE, 128), F32)] * 2, 4, 150_000_000, "scatter_attn")
    both_sum, sum_a = lax.optimization_barrier((both_sum, sum_a))
    normed_sum, rel_sum = both_sum[:t], both_sum[t:].reshape(-1)[:rel_size].astype(F32)
    tokens_grad, sums_one = call(
        token_back_body, (), (tok, live[:t], normed_sum, grad_middle, norm_gains),
        [((t, width), F32), ((2, width), F32)], [], "token_back")
    small = [sums_one.reshape(-1), sums_two.reshape(-1), qkv_sums.reshape(-1), up_sums.reshape(-1), rel_sum]
    edges = np.cumsum([0] + [v.shape[0] for v in small])
    lines = -(-int(edges[-1]) // 1024) * 8
    small = jnp.pad(jnp.concatenate(small), (0, lines * 128 - int(edges[-1]))).reshape(1, lines, 128)
    mg, mn, mc, mf, ms = [jnp.concatenate(pair, axis=0) for pair in zip(upper, lower)]
    gathered, ag, an, ac, af, as_ = gather(
        small, 3, "gather_sums", 1, functools.partial(soap_units, 0, 0),
        (sum_a, sq_left_a, sq_right_a, attn_master[0], attn_first[0], attn_second[0]),
        soap_outs(), [((2, 8, SIDE, 128), F32)] * 2)
    total = jnp.sum(gathered, axis=0).reshape(-1)
    one, two, qkv_grad, up_grad, rel_grad = [total[edges[i]:edges[i + 1]] for i in range(5)]
    one, two = one.reshape(2, width), two.reshape(4, width)
    gains_grad = jnp.stack([one[0], two[0]])
    biases_grad = jnp.stack([one[1], two[1]])
    outb_grad = jnp.stack([two[3], two[2]])
    rel_grad = rel_grad.reshape(rel_pos.shape)

    return (block_out[None], tokens_grad[None], gains_grad, biases_grad, outb_grad, qkv_grad, up_grad, rel_grad,
            *(value[None] for value in (ag, mg, an, mn, ac, mc, af, as_, mf, ms)))


def solution(mesh):
    return build(mesh)
```

```python
import functools
import math

import jax
import jax.numpy as jnp
import numpy as np
from jax import lax
from jax.experimental import pallas as pl
from jax.experimental.pallas import tpu as pltpu
from jax.sharding import PartitionSpec as P

highest = lax.Precision.HIGHEST
norm_eps = 1e-06
beta_one = 0.9
beta_two = 0.95
adam_eps = 1e-08
learn_rate = 0.02


def untile(tile_rows, row_count, col_count, tile_side):
    shaped = tile_rows.reshape(row_count // tile_side, col_count // tile_side, tile_side, tile_side)
    return shaped.transpose(0, 2, 1, 3).reshape(row_count, col_count)


def retile(matrix, tile_side):
    row_count, col_count = matrix.shape
    shaped = matrix.reshape(row_count // tile_side, tile_side, col_count // tile_side, tile_side)
    return shaped.transpose(0, 2, 1, 3).reshape(-1, tile_side * tile_side)


def rel_onehot(win_side):
    positions = jnp.arange(win_side, dtype=jnp.int32)
    offset = positions[:, None] - positions[None, :] + (win_side - 1)
    entries = jnp.arange(2 * win_side - 1, dtype=jnp.int32)
    return (offset[:, :, None] == entries[None, None, :]).astype(jnp.float32)


def norm_forward(values, norm_gain, norm_shift):
    centre = values - jnp.mean(values, axis=-1, keepdims=True)
    inverse = lax.rsqrt(jnp.mean(centre * centre, axis=-1, keepdims=True) + norm_eps)
    unit_rows = centre * inverse
    return (unit_rows * norm_gain + norm_shift, unit_rows, inverse)


def norm_backward(grad_in, unit_rows, inverse, norm_gain):
    grad_unit = grad_in * norm_gain
    centred = grad_unit - jnp.mean(grad_unit, axis=-1, keepdims=True)
    return inverse * (centred - unit_rows * jnp.mean(grad_unit * unit_rows, axis=-1, keepdims=True))


def gelu_pair(values):
    normal_cdf = 0.5 * (1.0 + lax.erf(values * 0.5**0.5))
    density = jnp.exp(-0.5 * values * values) * (2.0 * math.pi) ** (-0.5)
    return (values * normal_cdf, normal_cdf + values * density)


def soap_step(grad_tiles, master, left_basis, right_basis, first_moment, second_moment):
    tile_side = math.isqrt(grad_tiles.shape[2])
    square = (grad_tiles.shape[0], grad_tiles.shape[1], tile_side, tile_side)
    left_square = left_basis.reshape(square)
    right_square = right_basis.reshape(square)
    half_turn = jnp.einsum(
        "mtji,mtjk->mtik", left_square, grad_tiles.reshape(square), precision=highest
    )
    rotated = jnp.einsum("mtik,mtkl->mtil", half_turn, right_square, precision=highest).reshape(
        grad_tiles.shape
    )
    first_new = beta_one * first_moment + (1.0 - beta_one) * rotated
    second_new = beta_two * second_moment + (1.0 - beta_two) * rotated * rotated
    direction = (first_new / (jnp.sqrt(second_new) + adam_eps)).reshape(square)
    back_half = jnp.einsum("mtij,mtjk->mtik", left_square, direction, precision=highest)
    update = jnp.einsum("mtik,mtlk->mtil", back_half, right_square, precision=highest).reshape(
        grad_tiles.shape
    )
    master_new = master - learn_rate * update
    return (master_new, master_new.astype(jnp.bfloat16), first_new, second_new)


def local(
    tokens,
    pad_mask,
    cotangent,
    norm_gains,
    norm_biases,
    out_biases,
    qkv_bias,
    up_bias,
    rel_pos,
    attn_owner,
    mlp_owner,
    attn_master,
    mlp_master,
    attn_left,
    attn_right,
    mlp_left,
    mlp_right,
    attn_first,
    attn_second,
    mlp_first,
    mlp_second,
):
    windows, win_tokens, model_width = tokens.shape
    row_count = windows * win_tokens
    qkv_cols = qkv_bias.shape[0]
    head_cols = qkv_cols // 3
    unit_cols = up_bias.shape[0]
    head_dim = rel_pos.shape[2]
    heads_here = head_cols // head_dim
    win_side = (rel_pos.shape[1] + 1) // 2
    tile_side = math.isqrt(attn_master.shape[2])
    qkv_count = model_width // tile_side * (qkv_cols // tile_side)
    up_count = model_width // tile_side * (unit_cols // tile_side)
    score_scale = head_dim ** (-0.5)
    attn_stored, mlp_stored = (
        lax.all_gather(attn_master.astype(jnp.bfloat16), "dp", axis=1, tiled=True),
        lax.all_gather(mlp_master.astype(jnp.bfloat16), "dp", axis=1, tiled=True),
    )
    attn_order = jnp.argsort(attn_owner[0])
    mlp_order = jnp.argsort(mlp_owner[0])
    attn_sorted = attn_stored[0][attn_order]
    mlp_sorted = mlp_stored[0][mlp_order]
    w_qkv = untile(attn_sorted[:qkv_count], model_width, qkv_cols, tile_side)
    w_proj = untile(attn_sorted[qkv_count:], head_cols, model_width, tile_side)
    w_up = untile(mlp_sorted[:up_count], model_width, unit_cols, tile_side)
    w_down = untile(mlp_sorted[up_count:], unit_cols, model_width, tile_side)
    onehot = rel_onehot(win_side)
    table_h = jnp.einsum("ijr,rc->ijc", onehot, rel_pos[0], precision=highest)
    table_w = jnp.einsum("ijr,rc->ijc", onehot, rel_pos[1], precision=highest)
    flat_rows = tokens.reshape(row_count, model_width).astype(jnp.float32)
    live_rows = pad_mask.reshape(row_count, 1).astype(jnp.float32)
    normed, unit_one, inverse_one = norm_forward(flat_rows, norm_gains[0], norm_biases[0])
    normed_low = (normed * live_rows).astype(jnp.bfloat16)
    mixed_rows = (jnp.dot(normed_low, w_qkv, preferred_element_type=jnp.float32) + qkv_bias).astype(
        jnp.bfloat16
    )
    head_parts = mixed_rows.reshape(windows, win_tokens, 3, heads_here, head_dim)
    queries = head_parts[:, :, 0]
    key_rows = head_parts[:, :, 1]
    value_rows = head_parts[:, :, 2]
    query_grid = queries.astype(jnp.float32).reshape(
        windows, win_side, win_side, heads_here, head_dim
    )

    def score_rows():
        direct = (
            jnp.einsum("wqhc,wkhc->whqk", queries, key_rows, preferred_element_type=jnp.float32)
            * score_scale
        )
        along_h = jnp.einsum("wabhc,akc->whabk", query_grid, table_h, precision=highest)
        along_w = jnp.einsum("wabhc,blc->whabl", query_grid, table_w, precision=highest)
        return direct + (along_h[..., :, None] + along_w[..., None, :]).reshape(
            windows, heads_here, win_tokens, win_tokens
        )

    scores = score_rows()
    row_top = jnp.max(scores, axis=-1, keepdims=True)
    exponent = jnp.exp(scores - row_top)
    row_total = jnp.sum(exponent, axis=-1, keepdims=True)
    log_total = row_top + jnp.log(row_total)
    probs_low = (exponent / row_total).astype(jnp.bfloat16)
    attended = jnp.einsum(
        "whqk,wkhc->wqhc", probs_low, value_rows, preferred_element_type=jnp.float32
    )
    attended_low = attended.reshape(row_count, head_cols).astype(jnp.bfloat16)
    branch = lax.psum(
        jnp.dot(attended_low, w_proj, preferred_element_type=jnp.float32).astype(jnp.bfloat16), "mp"
    ).astype(jnp.float32)
    middle = flat_rows + branch + out_biases[0]
    second, unit_two, inverse_two = norm_forward(middle, norm_gains[1], norm_biases[1])
    second_low = second.astype(jnp.bfloat16)
    hidden = jnp.dot(second_low, w_up, preferred_element_type=jnp.float32) + up_bias
    active, gelu_slope = gelu_pair(hidden)
    active_low = active.astype(jnp.bfloat16)
    down_sum = lax.psum(
        jnp.dot(active_low, w_down, preferred_element_type=jnp.float32).astype(jnp.bfloat16), "mp"
    ).astype(jnp.float32)
    block_output = (
        ((middle + down_sum + out_biases[1]) * live_rows)
        .astype(jnp.bfloat16)
        .reshape(windows, win_tokens, model_width)
    )
    grad_out = cotangent.reshape(row_count, model_width).astype(jnp.float32) * live_rows
    grad_out_low = grad_out.astype(jnp.bfloat16)
    down_bias_grad = jnp.sum(grad_out, axis=0)
    w_down_grad = jnp.einsum(
        "nf,nd->fd", active_low, grad_out_low, preferred_element_type=jnp.float32
    )
    grad_active = jnp.einsum("nd,fd->nf", grad_out_low, w_down, preferred_element_type=jnp.float32)
    grad_hidden = (grad_active * gelu_slope).astype(jnp.bfloat16)
    up_bias_grad = jnp.sum(grad_hidden.astype(jnp.float32), axis=0)
    w_up_grad = jnp.einsum("nd,nf->df", second_low, grad_hidden, preferred_element_type=jnp.float32)
    mlp_stack = jnp.concatenate(
        [retile(w_up_grad, tile_side), retile(w_down_grad, tile_side)], axis=0
    )[mlp_owner[0]][None]
    grad_second = lax.psum(
        jnp.einsum("nf,df->nd", grad_hidden, w_up, preferred_element_type=jnp.float32).astype(
            jnp.bfloat16
        ),
        "mp",
    ).astype(jnp.float32)
    gain_two_grad = jnp.sum(grad_second * unit_two, axis=0)
    shift_two_grad = jnp.sum(grad_second, axis=0)
    grad_middle = grad_out + norm_backward(grad_second, unit_two, inverse_two, norm_gains[1])
    proj_bias_grad = jnp.sum(grad_middle, axis=0)
    grad_branch = grad_middle.astype(jnp.bfloat16)
    w_proj_grad = jnp.einsum(
        "nc,nd->cd", attended_low, grad_branch, preferred_element_type=jnp.float32
    )
    grad_attended = jnp.einsum("nd,cd->nc", grad_branch, w_proj, preferred_element_type=jnp.float32)
    grad_attended = grad_attended.astype(jnp.bfloat16).reshape(
        windows, win_tokens, heads_here, head_dim
    )
    probs_full = jnp.exp(score_rows() - log_total)
    probs_again = probs_full.astype(jnp.bfloat16)
    grad_probs = jnp.einsum(
        "wqhc,wkhc->whqk", grad_attended, value_rows, preferred_element_type=jnp.float32
    )
    grad_values = jnp.einsum(
        "whqk,wqhc->wkhc", probs_again, grad_attended, preferred_element_type=jnp.float32
    )
    grad_scores = (
        probs_full * (grad_probs - jnp.sum(probs_full * grad_probs, axis=-1, keepdims=True))
    ).astype(jnp.bfloat16)
    grad_queries = (
        jnp.einsum("whqk,wkhc->wqhc", grad_scores, key_rows, preferred_element_type=jnp.float32)
        * score_scale
    )
    grad_keys = (
        jnp.einsum("whqk,wqhc->wkhc", grad_scores, queries, preferred_element_type=jnp.float32)
        * score_scale
    )
    grad_grid = grad_scores.astype(jnp.float32).reshape(
        windows, heads_here, win_side, win_side, win_side, win_side
    )
    grad_h = jnp.sum(grad_grid, axis=5)
    grad_w = jnp.sum(grad_grid, axis=4)
    grad_rel_q = jnp.einsum("whabk,akc->wabhc", grad_h, table_h, precision=highest) + jnp.einsum(
        "whabl,blc->wabhc", grad_w, table_w, precision=highest
    )
    grad_queries = grad_queries + grad_rel_q.reshape(windows, win_tokens, heads_here, head_dim)
    table_h_grad = jnp.einsum("whabk,wabhc->akc", grad_h, query_grid, precision=highest)
    table_w_grad = jnp.einsum("whabl,wabhc->blc", grad_w, query_grid, precision=highest)
    rel_part = jnp.stack(
        [
            jnp.einsum("ijr,ijc->rc", onehot, table_h_grad, precision=highest),
            jnp.einsum("ijr,ijc->rc", onehot, table_w_grad, precision=highest),
        ]
    )
    grad_mixed = (
        jnp.stack([grad_queries, grad_keys, grad_values], axis=2)
        .reshape(row_count, qkv_cols)
        .astype(jnp.bfloat16)
    )
    qkv_bias_grad = jnp.sum(grad_mixed.astype(jnp.float32), axis=0)
    w_qkv_grad = jnp.einsum("nd,nc->dc", normed_low, grad_mixed, preferred_element_type=jnp.float32)
    grad_normed, rel_sum = (
        lax.psum(
            jnp.einsum("nc,dc->nd", grad_mixed, w_qkv, preferred_element_type=jnp.float32).astype(
                jnp.bfloat16
            ),
            "mp",
        ).astype(jnp.float32),
        lax.psum(rel_part.astype(jnp.bfloat16), "mp").astype(jnp.float32),
    )
    grad_normed = grad_normed * live_rows
    gain_one_grad = jnp.sum(grad_normed * unit_one, axis=0)
    shift_one_grad = jnp.sum(grad_normed, axis=0)
    tokens_grad = (
        grad_middle + norm_backward(grad_normed, unit_one, inverse_one, norm_gains[0])
    ).reshape(windows, win_tokens, model_width)
    attn_stack = jnp.concatenate(
        [retile(w_qkv_grad, tile_side), retile(w_proj_grad, tile_side)], axis=0
    )[attn_owner[0]][None]
    attn_grad, mlp_grad = (
        lax.psum_scatter(attn_stack, "dp", scatter_dimension=1, tiled=True),
        lax.psum_scatter(mlp_stack, "dp", scatter_dimension=1, tiled=True),
    )
    gains_grad, biases_grad, out_biases_grad, rel_pos_grad, qkv_bias_total, up_bias_total = (
        lax.psum(
            (
                jnp.stack([gain_one_grad, gain_two_grad]),
                jnp.stack([shift_one_grad, shift_two_grad]),
                jnp.stack([proj_bias_grad, down_bias_grad]),
                rel_sum,
                qkv_bias_grad,
                up_bias_grad,
            ),
            "dp",
        )
    )
    attn_new, attn_copy, attn_first_new, attn_second_new = soap_step(
        attn_grad, attn_master, attn_left, attn_right, attn_first, attn_second
    )
    mlp_new, mlp_copy, mlp_first_new, mlp_second_new = soap_step(
        mlp_grad, mlp_master, mlp_left, mlp_right, mlp_first, mlp_second
    )
    return (
        block_output,
        tokens_grad,
        gains_grad,
        biases_grad,
        out_biases_grad,
        qkv_bias_total,
        up_bias_total,
        rel_pos_grad,
        attn_grad,
        mlp_grad,
        attn_new,
        mlp_new,
        attn_copy,
        mlp_copy,
        attn_first_new,
        attn_second_new,
        mlp_first_new,
        mlp_second_new,
    )


BF = jnp.bfloat16
F32 = jnp.float32
ROWS = 208
SIDE = 160


def dot(a, b):
    return jnp.dot(a, b, preferred_element_type=F32)


def dot_nt(a, b):
    return lax.dot_general(a, b, (((1,), (1,)), ((), ())), preferred_element_type=F32)


def dot_tn(a, b):
    return lax.dot_general(a, b, (((0,), (0,)), ((), ())), preferred_element_type=F32)


def lane_at(shape):
    return lax.broadcasted_iota(jnp.int32, shape, len(shape) - 1)


def low_parts(value):
    high = value.astype(BF)
    return high, (value - high.astype(F32)).astype(BF)


def flat_to_square(read, square, count=8):
    lane = lane_at((8, 128))

    def rows_of(base):
        x = [read(base + 128 * k) for k in range(5)]
        r1 = pltpu.roll(x[1], 96, 1)
        r2 = pltpu.roll(x[2], 96, 1)
        h2 = pltpu.roll(x[2], 64, 1)
        h3 = pltpu.roll(x[3], 64, 1)
        r3 = pltpu.roll(x[3], 32, 1)
        r4 = pltpu.roll(x[4], 32, 1)
        return (
            (x[0], x[1]),
            (jnp.where(lane < 96, r1, r2), r2),
            (jnp.where(lane < 64, h2, h3), h3),
            (jnp.where(lane < 32, r3, r4), r4),
        )

    def body(group, carry):
        base = pl.multiple_of(group * 1280, 128)
        rows = rows_of(base) + rows_of(base + 640)
        for part in range(2):
            stacked = jnp.stack([row[part] for row in rows], axis=0)
            square[part, :, pl.ds(pl.multiple_of(8 * group, 8), 8), :] = jnp.swapaxes(stacked, 0, 1)
        return carry

    lax.fori_loop(0, 20, body, 0)


def square_to_flat(square, write, count=8):
    lane = lane_at((8, 128))

    def body(group, carry):
        at = pl.ds(pl.multiple_of(8 * group, 8), 8)
        wide = jnp.swapaxes(square[0, :, at, :], 0, 1)
        narrow = jnp.swapaxes(square[1, :, at, :], 0, 1)
        for half in range(2):
            base = pl.multiple_of(group * 1280, 128) + 640 * half
            a = [wide[4 * half + m] for m in range(4)]
            b = [narrow[4 * half + m] for m in range(4)]
            a1 = pltpu.roll(a[1], 32, 1)
            b1 = pltpu.roll(b[1], 32, 1)
            a2 = pltpu.roll(a[2], 64, 1)
            b2 = pltpu.roll(b[2], 64, 1)
            a3 = pltpu.roll(a[3], 96, 1)
            b3 = pltpu.roll(b[3], 96, 1)
            write(base, a[0])
            write(base + 128, jnp.where(lane < 32, b[0], a1))
            write(base + 256, jnp.where(lane < 32, a1, jnp.where(lane < 64, b1, a2)))
            write(base + 384, jnp.where(lane < 64, a2, jnp.where(lane < 96, b2, a3)))
            write(base + 512, jnp.where(lane < 96, a3, b3))
        return carry

    lax.fori_loop(0, 20, body, 0)


def pack_eight(source, first, wire, base, square):
    lane = lane_at((SIDE, 128))
    flat_to_square(lambda at: source[first : first + 8, pl.ds(at, 128)], square)
    for half in range(2):
        spare = None
        for q in range(4):
            wire[base + 5 * half + q] = square[0, 4 * half + q].astype(BF)
            piece = square[1, 4 * half + q]
            spare = piece if q == 0 else jnp.where(lane < 32 * q, spare, pltpu.roll(piece, 32 * q, 1))
        wire[base + 5 * half + 4] = spare.astype(BF)


def pack_attn_body(attn, wire, square):
    pack_eight(attn, 0, wire, 0, square)


def pack_mlp_units(mlp, wire, square):
    return [
        lambda: pack_eight(mlp, 0, wire, 0, square),
        lambda: pack_eight(mlp, 8, wire, 10, square),
    ]


def unpack_narrow(wire, narrow, groups):
    def body(g, carry):
        last = wire[5 * g + 4]
        for q in range(4):
            narrow[4 * g + q] = last[:, 32 * q : 32 * q + 32]
        return carry

    lax.fori_loop(0, groups, body, 0)


def unpack_sorted(wire, narrow, order, base, outs, rows, cols):
    def body(t, carry):
        row = t // cols
        col = t - row * cols
        stored = order[base + t]
        where_at = pl.multiple_of(row * SIDE, 32)
        outs[col, pl.ds(where_at, SIDE), 0:128] = wire[(stored // 4) * 5 + stored % 4]
        outs[col, pl.ds(where_at, SIDE), 128:160] = narrow[stored]
        return carry

    lax.fori_loop(0, rows * cols, body, 0)


MESH_ID = pl.DeviceIdType.MESH


def gather_body(piece, inputs, outputs, make_units, wire, *refs):
    args, refs = refs[:inputs], refs[inputs:]
    out, outs, refs = refs[0], refs[1 : 1 + outputs], refs[1 + outputs :]
    send_sem, recv_sem, own_sem = refs[:3]
    units = make_units(*args, *outs, *refs[3:]) if make_units else []
    count = wire.shape[0]
    pieces = count // piece
    me = lax.axis_index("dp")
    z, x = me // 2, me % 2
    side = me + 1 - 2 * x
    up, down = jnp.minimum(me + 2, 6 + x), jnp.maximum(me - 2, x)

    barrier = pltpu.get_barrier_semaphore()

    def greet(target):
        pl.semaphore_signal(barrier, inc=1, device_id={"dp": target}, device_id_type=MESH_ID)

    greet(side)
    pl.when(z < 3)(lambda: greet(up))
    pl.when(z > 0)(lambda: greet(down))
    inner = (z > 0) & (z < 3)
    pl.when(inner)(lambda: pl.semaphore_wait(barrier, 3))
    pl.when(jnp.logical_not(inner))(lambda: pl.semaphore_wait(barrier, 2))

    def copy(way, target, origin, k, own=False):
        place = out.at[pl.ds(origin * count + piece * k, piece)]
        return pltpu.make_async_remote_copy(
            src_ref=wire.at[pl.ds(piece * k, piece)] if own else place,
            dst_ref=place,
            send_sem=send_sem.at[way, origin, k],
            recv_sem=recv_sem.at[origin, k],
            device_id={"dp": target},
            device_id_type=MESH_ID,
        )

    for k in range(pieces):
        copy(0, side, me, k, True).start()
        pl.when(z < 3)(lambda k=k: copy(1, up, me, k, True).start())
        pl.when(z > 0)(lambda k=k: copy(2, down, me, k, True).start())
    keep = pltpu.make_async_copy(wire, out.at[pl.ds(me * count, count)], own_sem)
    keep.start()
    slots = 1 + 3 * pieces
    split = (pieces + 1) // 2
    lone, high = 1 - x, 7 - x

    def work(slot):
        for i, unit in enumerate(units):
            if i * slots // len(units) == slot:
                unit()

    work(0)
    for d in range(1, 5):
        for k in range(pieces):
            def from_below():
                origin = me - 2 * d
                copy(1, up, origin, k).wait_recv()
                pl.when((z > d) | (k < split))(lambda: copy(0, side, origin, k).start())
                pl.when(z < 3)(lambda: copy(1, up, origin, k).start())

            def from_above():
                origin = me + 2 * d
                copy(2, down, origin, k).wait_recv()
                pl.when((z + d < 3) | (k < split))(lambda: copy(0, side, origin, k).start())
                pl.when(z > 0)(lambda: copy(2, down, origin, k).start())

            def other_low():
                copy(1, up, lone, k).wait_recv()
                pl.when(z < 3)(lambda: copy(1, up, lone, k).start())

            def other_high():
                copy(2, down, high, k).wait_recv()
                pl.when(z > 0)(lambda: copy(2, down, high, k).start())

            if d < 4:
                pl.when(z >= d)(from_below)
                pl.when(z + d <= 3)(from_above)
                work(1 + (d - 1) * pieces + k)
            if k >= split:
                pl.when(z == d - 1)(other_low)
                pl.when(z == 4 - d)(other_high)

    keep.wait()
    for k in range(pieces):
        for line in range(4):
            origin = 2 * line + x
            far = line in (0, 3) and k >= split
            if far:
                pl.when(z == line)(lambda: copy(0, side, origin, k).wait_send())
            else:
                copy(0, side, origin + 1 - 2 * x, k).wait_recv()
                copy(0, side, origin, k).wait_send()
            pl.when((line <= z) & (z < 3))(lambda: copy(1, up, origin, k).wait_send())
            pl.when((line >= z) & (z > 0))(lambda: copy(2, down, origin, k).wait_send())
        if k >= split:
            pl.when(z < 3)(lambda: copy(1, up, lone, k).wait_send())
            pl.when(z > 0)(lambda: copy(2, down, high, k).wait_send())


def gather(wire, ident, name, piece=5, make_units=None, args=(), outs=(), scratch=()):
    count = wire.shape[0]
    results = pl.pallas_call(
        functools.partial(gather_body, piece, len(args), len(outs), make_units),
        out_shape=[jax.ShapeDtypeStruct((8 * count,) + wire.shape[1:], wire.dtype)]
        + [jax.ShapeDtypeStruct(*out) for out in outs],
        in_specs=[VM] * (1 + len(args)),
        out_specs=[pl.BlockSpec(memory_space=pl.ANY)] + [VM] * len(outs),
        scratch_shapes=[
            pltpu.SemaphoreType.DMA((3, 8, count // piece)),
            pltpu.SemaphoreType.DMA((8, count // piece)),
            pltpu.SemaphoreType.DMA,
        ] + [pltpu.VMEM(*item) for item in scratch],
        compiler_params=pltpu.CompilerParams(
            collective_id=ident, has_side_effects=True, vmem_limit_bytes=LIMIT),
        cost_estimate=pl.CostEstimate(flops=0, bytes_accessed=count * 12_000_000, transcendentals=0),
        name=name,
    )(wire, *args)
    return results if outs else results[0]


CHUNK = 5
AHEAD = 4


def scatter_steps(count, prepare, source, own_part, out, inbox, half,
                  side_send, side_recv, line_send, line_recv, own, units, early=0, early_at=0):
    me = lax.axis_index("dp")
    z, x = me // 2, me % 2
    side = me + 1 - 2 * x
    pieces = count // CHUNK
    steps = 4 * pieces

    def line_at(j):
        return lax.rem(z + j, 4)

    barrier = pltpu.get_barrier_semaphore()
    for target in (side, 2 * line_at(1) + x, 2 * line_at(2) + x, 2 * line_at(3) + x):
        pl.semaphore_signal(barrier, inc=1, device_id={"dp": target}, device_id_type=MESH_ID)

    def place(at):
        j, k = lax.rem(at, 4), lax.div(at, 4)
        return j, k, line_at(j + 1)

    def to_side(at):
        j, k, line = place(at)
        return pltpu.make_async_remote_copy(
            src_ref=source(2 * line + 1 - x, line, k),
            dst_ref=inbox.at[pl.ds(line * count + CHUNK * k, CHUNK)],
            send_sem=side_send.at[j, k], recv_sem=side_recv.at[j, k],
            device_id={"dp": side}, device_id_type=MESH_ID)

    def to_line(at):
        j, k, line = place(at)
        return pltpu.make_async_remote_copy(
            src_ref=half.at[pl.ds(line * count + CHUNK * k, CHUNK)],
            dst_ref=out.at[pl.ds(z * count + CHUNK * k, CHUNK)],
            send_sem=line_send.at[j, k], recv_sem=line_recv.at[j, k],
            device_id={"dp": 2 * line + x}, device_id_type=MESH_ID)

    def keep(k):
        return pltpu.make_async_copy(
            half.at[pl.ds(z * count + CHUNK * k, CHUNK)], out.at[pl.ds(z * count + CHUNK * k, CHUNK)], own.at[k])

    def send(at):
        _, k, line = place(at)
        prepare(2 * line + 1 - x, line, k)
        to_side(at).start()

    def ready(at, carry):
        _, k, line = place(at)
        prepare(2 * line + 1 - x, line, k)
        return carry

    def first(at, carry):
        to_side(at).start()
        return carry

    def arrived(at, carry):
        pl.when(lax.rem(at, 4) < 3)(lambda: to_line(at).wait_recv())
        pl.when(lax.rem(at, 4) == 3)(lambda: keep(lax.div(at, 4)).wait())
        return carry

    def early_wait():
        lax.fori_loop(0, 4 * early, arrived, 0)

    def step(at, carry):
        j, k, line = place(at)
        if early:
            pl.when(at == early_at)(early_wait)
        for turn, unit in units:
            pl.when(at == turn)(unit)
        to_side(at).wait_recv()
        pl.when(at + AHEAD < steps)(lambda: send(at + AHEAD))
        own_part(2 * line + x, line, k)
        pl.when(j < 3)(lambda: to_line(at).start())
        pl.when(j == 3)(lambda: keep(k).start())
        return carry

    def last(at, carry):
        to_side(at).wait_send()
        pl.when(lax.rem(at, 4) < 3)(lambda: to_line(at).wait_send())
        return carry

    lax.fori_loop(0, AHEAD, ready, 0)
    pl.semaphore_wait(barrier, 4)
    lax.fori_loop(0, AHEAD, first, 0)
    lax.fori_loop(0, steps, step, 0)
    lax.fori_loop(0, steps, last, 0)
    lax.fori_loop(4 * early, steps, arrived, 0)


def scatter_call(body, count, tables, args, outs, scratch, ident, cost, name, given=0):
    shape = (4 * count, SIDE, 128)
    result = (given or 4 * count, SIDE, 128)
    pieces = count // CHUNK
    return pl.pallas_call(
        body,
        out_shape=[jax.ShapeDtypeStruct(result, BF)] + [jax.ShapeDtypeStruct(*out) for out in outs],
        in_specs=[SM] * len(tables) + [VM] * len(args),
        out_specs=[pl.BlockSpec(memory_space=pl.ANY)] + [VM] * len(outs),
        scratch_shapes=[pltpu.VMEM(shape, BF)] * 2 + [pltpu.SemaphoreType.DMA((4, pieces))] * 4
        + [pltpu.SemaphoreType.DMA((pieces,))]
        + [pltpu.VMEM(*item) if item else pltpu.SemaphoreType.DMA((4,)) for item in scratch],
        compiler_params=pltpu.CompilerParams(
            collective_id=ident, has_side_effects=True, vmem_limit_bytes=LIMIT),
        cost_estimate=pl.CostEstimate(flops=0, bytes_accessed=cost, transcendentals=0),
        name=name,
    )(*tables, *args)


def tile_steps(count, left_at, right_at, lefts, rights, inbox, half, sent):
    lane = lane_at((SIDE, 128))

    def tiles(chunk, k, emit):
        spare = None
        for q in range(4):
            s = count // 5 * 4 * chunk + 4 * k + q
            tile = dot_tn(lefts[left_at[s]], rights[right_at[s]])
            emit(q, tile[:, 0:128])
            piece = jnp.concatenate([tile[:, 128:160], jnp.zeros((SIDE, 96), F32)], axis=1)
            spare = piece if q == 0 else jnp.where(lane < 32 * q, spare, pltpu.roll(piece, 32 * q, 1))
        emit(4, spare)

    def prepare(chunk, line, k):
        def emit(q, value):
            sent[count * line + CHUNK * k + q] = value.astype(BF)
        tiles(chunk, k, emit)

    def source(chunk, line, k):
        return sent.at[pl.ds(count * line + CHUNK * k, CHUNK)]

    def own_part(chunk, line, k):
        def emit(q, value):
            at = count * line + CHUNK * k + q
            half[at] = (value + inbox[at].astype(F32)).astype(BF)
        tiles(chunk, k, emit)

    return prepare, source, own_part


def scatter_mlp_body(left_at, right_at, sec, act, gh, go, left_m, right_m, left_a, right_a, master, first, second,
                     out, sq_left_m, sq_right_m, sq_left_a, sq_right_a,
                     grad_out, new_out, copy_out, first_out, second_out, inbox, half,
                     side_send, side_recv, line_send, line_recv, own, lefts, rights, sent, landed, moved,
                     sq_left, sq_right, sq_grad, sq_work):
    lefts[0:8], lefts[8:16] = sec[...], act[...]
    rights[0:8], rights[8:16] = gh[...], go[...]
    units = []
    for turn, (flat, r, square) in enumerate((
            (left_m, 0, sq_left), (right_m, 0, sq_right), (left_m, 8, sq_left_m), (right_m, 8, sq_right_m),
            (left_a, 0, sq_left_a), (right_a, 0, sq_right_a))):
        units.append((turn, lambda f=flat, r=r, sq=square: flat_to_square(
            lambda at: f[r : r + 8, pl.ds(at, 128)], sq.at[0])))
    stages = soap_units(0, 0, landed, sq_left, sq_right, master, first, second,
                        grad_out, new_out, copy_out, first_out, second_out, sq_grad, sq_work)
    units += [(10 + i, stage) for i, stage in enumerate(stages)]
    scatter_steps(20, *tile_steps(20, left_at, right_at, lefts, rights, inbox, half, sent),
                  landed, inbox, half, side_send, side_recv, line_send, line_recv, own, units, 2, 10)
    moves = [pltpu.make_async_copy(landed.at[pl.ds(20 * p + 10, 10)], out.at[pl.ds(10 * p, 10)], moved.at[p])
             for p in range(4)]
    for move in moves:
        move.start()
    for move in moves:
        move.wait()


def scatter_attn_body(left_at, right_at, nb, att, gm, gb, wire, sq_left, sq_right, master, first, second,
                      out, grad_out, new_out, copy_out, first_out, second_out, inbox, half,
                      side_send, side_recv, line_send, line_recv, own, lefts, rights, sent, sq_grad, sq_work):
    lefts[0:8], lefts[8:10] = nb[...], att[...]
    rights[0:6], rights[6:14] = gm[...], gb[...]
    stages = soap_units(1, 0, wire, sq_left, sq_right, master, first, second,
                        grad_out, new_out, copy_out, first_out, second_out, sq_grad, sq_work)
    scatter_steps(10, *tile_steps(10, left_at, right_at, lefts, rights, inbox, half, sent),
                  out, inbox, half, side_send, side_recv, line_send, line_recv, own, list(enumerate(stages)))


def norm_parts(x):
    mean = jnp.mean(x, axis=-1, keepdims=True)
    centre = x - mean
    inverse = lax.rsqrt(jnp.mean(centre * centre, axis=-1, keepdims=True) + norm_eps)
    return centre * inverse, inverse


def norm_back(grad_in, unit, inverse, gain):
    w = grad_in * gain
    return inverse * (
        w - jnp.mean(w, axis=-1, keepdims=True) - unit * jnp.mean(w * unit, axis=-1, keepdims=True)
    )


def padded(ref, rows, kind=F32):
    value = ref[...].astype(kind)
    return jnp.concatenate([value, jnp.zeros((ROWS - rows, value.shape[1]), kind)], axis=0)


def attn_forward(mixed, rel_hi, rel_lo, pick, spread, probs, att, scale, tokens_here):
    lane = lane_at((ROWS, SIDE))
    key_ok = lane_at((ROWS, ROWS)) < tokens_here
    head = SIDE // 2
    for p in range(2):
        q, k, v = mixed[p], mixed[2 + p], mixed[4 + p]
        parts = []
        for h in range(2):
            mine = (lane >= head) if h else (lane < head)
            qm = jnp.where(mine, q, jnp.zeros_like(q))
            s = dot_nt(qm, k) * scale
            a_hi, a_lo = low_parts(dot_nt(qm, rel_hi[...]) + dot_nt(qm, rel_lo[...]))
            for c in range(7):
                mask = pick[:, 128 * c : 128 * c + 128]
                table = spread[128 * c : 128 * c + 128, :]
                s = s + dot(a_hi * mask, table) + dot(a_lo * mask, table)
            s = jnp.where(key_ok, s, -1e30)
            top = jnp.max(s, axis=-1, keepdims=True)
            e = jnp.exp(s - top)
            pr = e / jnp.sum(e, axis=-1, keepdims=True)
            probs[2 * p + h] = pr
            parts.append(dot(pr.astype(BF), v))
        att[p] = jnp.where(lane < head, parts[0], parts[1]).astype(BF)


def attn_backward(mixed, rel_hi, rel_lo, pick, spread, probs, gatt, gm, rel_out, scale):
    lane = lane_at((ROWS, SIDE))
    head = SIDE // 2
    for p in range(2):
        q, k, v = mixed[p], mixed[2 + p], mixed[4 + p]
        ga = gatt[p]
        dq, dk, dv, dr = [], [], [], []
        for h in range(2):
            mine = (lane >= head) if h else (lane < head)
            pr = probs[2 * p + h]
            gam = jnp.where(mine, ga, jnp.zeros_like(ga))
            gp = dot_nt(gam, v)
            dv.append(dot_tn(pr.astype(BF), ga))
            ds = (pr * (gp - jnp.sum(pr * gp, axis=-1, keepdims=True))).astype(BF)
            da = None
            for c in range(7):
                term = dot_nt(ds, spread[128 * c : 128 * c + 128, :]) * pick[:, 128 * c : 128 * c + 128].astype(F32)
                da = term if da is None else da + term
            da_hi, da_lo = low_parts(da)
            relq = dot(da_hi, rel_hi[...]) + dot(da_lo, rel_hi[...]) + dot(da_hi, rel_lo[...])
            dq.append(dot(ds, k) * scale + relq)
            dk.append(dot_tn(ds, q) * scale)
            dr.append(dot_tn(da_hi, q) + dot_tn(da_lo, q))
        gm[p] = jnp.where(lane < head, dq[0], dq[1]).astype(BF)
        gm[2 + p] = jnp.where(lane < head, dk[0], dk[1]).astype(BF)
        gm[4 + p] = jnp.where(lane < head, dv[0], dv[1]).astype(BF)
        rel = jnp.where(lane_at((128, SIDE)) < head, dr[0], dr[1])
        if p == 0:
            rel_out[...] = rel
        else:
            rel_out[...] += rel


def attn_fwd_body(order, tokens, live, gains, biases, qkv_bias, rel_hi, rel_lo, pick, spread, wire,
                  part, normed, mixed, probs, att, w_qkv, w_proj, narrow, block):
    t = tokens.shape[0]
    x = padded(tokens, t)
    unit, _ = norm_parts(x)
    normed[...] = ((unit * gains[0:1, :] + biases[0:1, :]) * live[...]).astype(BF)
    unpack_narrow(wire, narrow, wire.shape[0] // 5)
    unpack_sorted(wire, narrow, order, 0, w_qkv, 8, 6)
    unpack_sorted(wire, narrow, order, 48, w_proj, 2, 8)

    def mix(j, carry):
        mixed[j] = (dot(normed[...], w_qkv[j]) + qkv_bias[pl.ds(j, 1), :]).astype(BF)
        return carry

    lax.fori_loop(0, 6, mix, 0)
    attn_forward(mixed, rel_hi, rel_lo, pick, spread, probs, att, (SIDE // 2) ** -0.5, t)

    def project(n, carry):
        value = dot(att[0], w_proj[n, 0:SIDE, :]) + dot(att[1], w_proj[n, SIDE : 2 * SIDE, :])
        block[n] = value
        return carry

    lax.fori_loop(0, 8, project, 0)
    for n in range(8):
        part[:, SIDE * n : SIDE * n + SIDE] = block[n][0:t, :].astype(BF)


def mlp_body(order, tokens, live, cotangent, branch, gains, biases, out_biases, up_bias, wire,
             part_down, part_second, sec_blocks, act_blocks, gh, go, bias_sums, w_up, w_down, narrow, block, second):
    t = tokens.shape[0]
    x = padded(tokens, t)
    middle = x + padded(branch, t) + out_biases[0:1, :]
    unit, _ = norm_parts(middle)
    second[...] = (unit * gains[1:2, :] + biases[1:2, :]).astype(BF)
    grad_out = padded(cotangent, t) * live[...]
    for n in range(8):
        sec_blocks[n] = second[:, SIDE * n : SIDE * n + SIDE]
        go[n] = grad_out[:, SIDE * n : SIDE * n + SIDE].astype(BF)
    unpack_narrow(wire, narrow, wire.shape[0] // 5)
    unpack_sorted(wire, narrow, order, 0, w_up, 8, 8)
    unpack_sorted(wire, narrow, order, 64, w_down, 8, 8)

    def hidden_block(j, carry):
        row = pl.multiple_of(j * SIDE, 32)
        hid = dot(second[...], w_up[j]) + up_bias[pl.ds(j, 1), :]
        cdf = 0.5 * (1.0 + lax.erf(hid * 0.5**0.5))
        slope = cdf + hid * (jnp.exp(-0.5 * hid * hid) * (2.0 * math.pi) ** -0.5)
        act_blocks[j] = (hid * cdf).astype(BF)
        ga = dot_nt(go[0], w_down[0, pl.ds(row, SIDE), :])
        for n in range(1, 8):
            ga = ga + dot_nt(go[n], w_down[n, pl.ds(row, SIDE), :])
        low = (ga * slope).astype(BF)
        gh[j] = low
        bias_sums[pl.ds(j, 1), :] = jnp.sum(low.astype(F32), axis=0, keepdims=True)
        return carry

    lax.fori_loop(0, 8, hidden_block, 0)

    def second_back(i, carry):
        row = pl.multiple_of(i * SIDE, 32)
        value = dot_nt(gh[0], w_up[0, pl.ds(row, SIDE), :])
        for j in range(1, 8):
            value = value + dot_nt(gh[j], w_up[j, pl.ds(row, SIDE), :])
        block[i] = value
        return carry

    lax.fori_loop(0, 8, second_back, 0)
    for n in range(8):
        part_second[:, SIDE * n : SIDE * n + SIDE] = block[n][0:t, :].astype(BF)

    def down(n, carry):
        value = dot(act_blocks[0], w_down[n, 0:SIDE, :])
        for j in range(1, 8):
            value = value + dot(act_blocks[j], w_down[n, j * SIDE : (j + 1) * SIDE, :])
        block[n] = value
        return carry

    lax.fori_loop(0, 8, down, 0)
    for n in range(8):
        part_down[:, SIDE * n : SIDE * n + SIDE] = block[n][0:t, :].astype(BF)


def mid_back_body(order, tokens, live, cotangent, branch, down_sum, second_sum, gains, out_biases,
                  wire, mixed, probs, normed, att, rel_hi, rel_lo, pick, spread,
                  block_out, grad_middle_out, part_normed, rel_out, gm, gb, nb, sums, bias_sums,
                  w_qkv, w_proj, narrow, block, gatt):
    t = tokens.shape[0]
    x = padded(tokens, t)
    middle = x + padded(branch, t) + out_biases[0:1, :]
    result = (middle + padded(down_sum, t) + out_biases[1:2, :]) * live[...]
    block_out[...] = result[0:t, :].astype(BF)
    grad_out = padded(cotangent, t) * live[...]
    unit, inverse = norm_parts(middle)
    grad_second = padded(second_sum, t)
    sums[0:1, :] = jnp.sum(grad_second * unit, axis=0, keepdims=True)
    sums[1:2, :] = jnp.sum(grad_second, axis=0, keepdims=True)
    sums[2:3, :] = jnp.sum(grad_out, axis=0, keepdims=True)
    grad_middle = grad_out + norm_back(grad_second, unit, inverse, gains[1:2, :])
    sums[3:4, :] = jnp.sum(grad_middle, axis=0, keepdims=True)
    grad_middle_out[...] = grad_middle[0:t, :]
    for n in range(8):
        gb[n] = grad_middle[:, SIDE * n : SIDE * n + SIDE].astype(BF)
        nb[n] = normed[:, SIDE * n : SIDE * n + SIDE]
    unpack_narrow(wire, narrow, wire.shape[0] // 5)
    unpack_sorted(wire, narrow, order, 0, w_qkv, 8, 6)
    unpack_sorted(wire, narrow, order, 48, w_proj, 2, 8)
    for p in range(2):
        value = dot_nt(gb[0], w_proj[0, p * SIDE : (p + 1) * SIDE, :])
        for n in range(1, 8):
            value = value + dot_nt(gb[n], w_proj[n, p * SIDE : (p + 1) * SIDE, :])
        gatt[p] = value.astype(BF)
    attn_backward(mixed, rel_hi, rel_lo, pick, spread, probs, gatt, gm, rel_out, (SIDE // 2) ** -0.5)
    for j in range(6):
        bias_sums[j : j + 1, :] = jnp.sum(gm[j].astype(F32), axis=0, keepdims=True)

    def normed_back(i, carry):
        row = pl.multiple_of(i * SIDE, 32)
        value = dot_nt(gm[0], w_qkv[0, pl.ds(row, SIDE), :])
        for j in range(1, 6):
            value = value + dot_nt(gm[j], w_qkv[j, pl.ds(row, SIDE), :])
        block[i] = value
        return carry

    lax.fori_loop(0, 8, normed_back, 0)
    for n in range(8):
        part_normed[:, SIDE * n : SIDE * n + SIDE] = block[n][0:t, :].astype(BF)


def token_back_body(tokens, live, normed_sum, grad_middle, gains, tokens_grad, sums):
    x = tokens[...].astype(F32)
    unit, inverse = norm_parts(x)
    grad_normed = normed_sum[...].astype(F32) * live[...]
    sums[0:1, :] = jnp.sum(grad_normed * unit, axis=0, keepdims=True)
    sums[1:2, :] = jnp.sum(grad_normed, axis=0, keepdims=True)
    tokens_grad[...] = grad_middle[...] + norm_back(grad_normed, unit, inverse, gains[0:1, :])


def square_tile(square, t):
    return jnp.concatenate([square[0, t], square[1, t, :, 0:32]], axis=1)


def put_tile(square, t, value):
    square[0, t] = value[:, 0:128]
    square[1, t, :, 0:32] = value[:, 128:160]


def split_dot(kind, a, b):
    a_hi, a_lo = low_parts(a)
    b_hi, b_lo = low_parts(b)
    return kind(a_hi, b_hi) + (kind(a_hi, b_lo) + kind(a_lo, b_hi))


def soap_units(r, g, wire, sq_left, sq_right, master, first, second,
               grad_out, new_out, copy_out, first_out, second_out, sq_grad, sq_work):
    rows, to = slice(8 * r, 8 * r + 8), slice(0, 8)
    count = wire.shape[0] // 4
    left, right = sq_left.at[g], sq_right.at[g]

    def total(i):
        w = [wire[p * count + i].astype(F32) for p in range(4)]
        return (w[0] + w[1]) + (w[2] + w[3])

    def load():
        for half in range(2):
            last = total(5 * half + 4)
            for q in range(4):
                sq_grad[0, 4 * half + q] = total(5 * half + q)
                sq_grad[1, 4 * half + q] = last if q == 0 else pltpu.roll(last, 128 - 32 * q, 1)

        def write(at, value):
            grad_out[to, pl.ds(at, 128)] = value

        square_to_flat(sq_grad, write)

    def rotate(t, carry):
        half = split_dot(dot_tn, square_tile(left, t), square_tile(sq_grad, t))
        put_tile(sq_work, t, split_dot(dot, half, square_tile(right, t)))
        return carry

    def moments(at, rotated):
        cols = pl.ds(at, 128)
        f = beta_one * first[rows, cols] + (1.0 - beta_one) * rotated
        s = beta_two * second[rows, cols] + (1.0 - beta_two) * rotated * rotated
        first_out[to, cols] = f
        second_out[to, cols] = s
        new_out[to, cols] = f / (jnp.sqrt(s) + adam_eps)

    def turn_back(t, carry):
        half = split_dot(dot, square_tile(left, t), square_tile(sq_work, t))
        put_tile(sq_work, t, split_dot(dot_nt, half, square_tile(right, t)))
        return carry

    def finish(at, update):
        cols = pl.ds(at, 128)
        value = master[rows, cols] - learn_rate * update
        new_out[to, cols] = value
        copy_out[to, cols] = value.astype(BF)

    def loop(body):
        lax.fori_loop(0, 8, body, 0)

    return [
        load,
        lambda: loop(rotate),
        lambda: square_to_flat(sq_work, moments),
        lambda: flat_to_square(lambda at: new_out[to, pl.ds(at, 128)], sq_work),
        lambda: loop(turn_back),
        lambda: square_to_flat(sq_work, finish),
    ]


def build(mesh):
    placed = (
        P("dp", None, None),
        P("dp", None),
        P("dp", None, None),
        P(),
        P(),
        P(),
        P("mp"),
        P("mp"),
        P(),
        P("mp", None),
        P("mp", None),
        P("mp", "dp", None),
        P("mp", "dp", None),
        P("mp", "dp", None),
        P("mp", "dp", None),
        P("mp", "dp", None),
        P("mp", "dp", None),
        P("mp", "dp", None),
        P("mp", "dp", None),
        P("mp", "dp", None),
        P("mp", "dp", None),
    )
    return jax.shard_map(
        fast_local if dict(mesh.shape) == {"dp": 8, "mp": 4} else local,
        mesh=mesh,
        in_specs=placed,
        out_specs=(
            P("dp", None, None),
            P("dp", None, None),
            P(),
            P(),
            P(),
            P("mp"),
            P("mp"),
            P(),
            P("mp", "dp", None),
            P("mp", "dp", None),
            P("mp", "dp", None),
            P("mp", "dp", None),
            P("mp", "dp", None),
            P("mp", "dp", None),
            P("mp", "dp", None),
            P("mp", "dp", None),
            P("mp", "dp", None),
            P("mp", "dp", None),
        ),
        check_vma=False,
    )


VM = pl.BlockSpec(memory_space=pltpu.VMEM)
SM = pl.BlockSpec(memory_space=pltpu.SMEM)
LIMIT = 60 * 1024 * 1024


def call(body, tables, args, outs, scratch, name):
    return pl.pallas_call(
        body,
        out_shape=[jax.ShapeDtypeStruct(shape, kind) for shape, kind in outs],
        in_specs=[SM] * len(tables) + [VM] * len(args),
        out_specs=[VM] * len(outs),
        scratch_shapes=[pltpu.VMEM(shape, kind) for shape, kind in scratch],
        compiler_params=pltpu.CompilerParams(vmem_limit_bytes=LIMIT),
        name=name,
    )(*tables, *args)


def rel_constants(side):
    rows = np.arange(ROWS)
    lanes = np.arange(896)
    within, along = lanes % 64, lanes // 64
    high = np.where(rows < side * side, rows // side, -1)[:, None]
    wide = np.where(rows < side * side, rows % side, -1)[:, None]
    pick = np.where(within[None] < 32, high == along[None], wide == along[None])
    keys = np.arange(ROWS)
    key_h, key_w = keys // side, keys % side
    offset = np.where(within[:, None] < 32, along[:, None] - key_h[None], along[:, None] - key_w[None]) + side - 1
    spread = (offset == (within % 32)[:, None]) & (keys < side * side)[None]
    return jnp.asarray(pick, BF), jnp.asarray(spread, BF)


def inverse_order(owner):
    count = owner.shape[0]
    at = jnp.arange(count, dtype=jnp.int32)
    return jnp.sum(jnp.where(owner[:, None] == at[None, :], at[:, None], 0), axis=0)


def fast_local(
    tokens, pad_mask, cotangent, norm_gains, norm_biases, out_biases, qkv_bias, up_bias, rel_pos,
    attn_owner, mlp_owner, attn_master, mlp_master, attn_left, attn_right, mlp_left, mlp_right,
    attn_first, attn_second, mlp_first, mlp_second,
):
    t, width = tokens.shape[1:]
    tok, cot = tokens[0], cotangent[0]
    live = jnp.pad(pad_mask[0].astype(F32), (0, ROWS - t))[:, None]
    qb, ub = qkv_bias.reshape(6, SIDE), up_bias.reshape(8, SIDE)
    rel = jnp.pad(rel_pos, ((0, 0), (0, 32 - rel_pos.shape[1]), (0, 0))).reshape(64, SIDE // 2)
    rel_hi, rel_lo = low_parts(jnp.tile(rel, (2, 2)))
    pick, spread = rel_constants((rel_pos.shape[1] + 1) // 2)
    own_a, own_m = attn_owner[0], mlp_owner[0]
    ord_a, ord_m = inverse_order(own_a), inverse_order(own_m)
    xa = jnp.where(own_a < 48, own_a // 6, 8 + (own_a - 48) // 8)
    ya = jnp.where(own_a < 48, own_a % 6, 6 + (own_a - 48) % 8)
    xm, ym = own_m // 8, (own_m // 64) * 8 + own_m % 8

    wire_a, = call(
        pack_attn_body, (), (attn_master[0],), [((10, SIDE, 128), BF)], [((2, 8, SIDE, 128), F32)], "pack")
    all_a, wire_m = gather(
        wire_a, 0, "gather_attn", 5, pack_mlp_units, (mlp_master[0],), [((20, SIDE, 128), BF)],
        [((2, 8, SIDE, 128), F32)])

    part, normed, mixed, probs, att = call(
        attn_fwd_body, (ord_a,),
        (tok, live, norm_gains, norm_biases, qb, rel_hi, rel_lo, pick, spread, all_a),
        [((t, width), BF), ((ROWS, width), BF), ((6, ROWS, SIDE), BF), ((4, ROWS, ROWS), F32), ((2, ROWS, SIDE), BF)],
        [((6, 8 * SIDE, SIDE), BF), ((8, 2 * SIDE, SIDE), BF), ((64, SIDE, 32), BF), ((8, ROWS, SIDE), F32)],
        "attn_fwd")
    branch = lax.psum(part, "mp")
    wire_m, mixed = lax.optimization_barrier((wire_m, mixed))
    all_m = gather(wire_m, 1, "gather_mlp")
    part_down, part_second, sec_blocks, act_blocks, gh, go, up_sums = call(
        mlp_body, (ord_m,),
        (tok, live, cot, branch, norm_gains, norm_biases, out_biases, ub, all_m),
        [((t, width), BF), ((t, width), BF)] + [((8, ROWS, SIDE), BF)] * 4 + [((8, SIDE), F32)],
        [((8, 8 * SIDE, SIDE), BF), ((8, 8 * SIDE, SIDE), BF), ((128, SIDE, 32), BF), ((8, ROWS, SIDE), F32), ((ROWS, width), BF)],
        "mlp")
    second_sum = lax.psum(part_second, "mp")
    down_sum = lax.psum(part_down, "mp")

    def soap_outs():
        shape = (8, SIDE * SIDE)
        return [(shape, F32), (shape, F32), (shape, BF), (shape, F32), (shape, F32)]

    square = ((1, 2, 8, SIDE, 128), F32)
    sum_m, sq_left_m, sq_right_m, sq_left_a, sq_right_a, *upper = scatter_call(
        scatter_mlp_body, 20, (xm, ym),
        (sec_blocks, act_blocks, gh, go, mlp_left[0], mlp_right[0], attn_left[0], attn_right[0],
         mlp_master[0], mlp_first[0], mlp_second[0]),
        [square] * 4 + soap_outs(),
        [((16, ROWS, SIDE), BF)] * 2 + [((80, SIDE, 128), BF)] * 2 + [None] + [square] * 2 + [(square[0][1:], F32)] * 2,
        2, 250_000_000, "scatter_mlp", 40)
    second_sum, down_sum, sum_m = lax.optimization_barrier((second_sum, down_sum, sum_m))

    block_out, grad_middle, part_normed, rel_part, gm, gb, nb, sums_two, qkv_sums = call(
        mid_back_body, (ord_a,),
        (tok, live, cot, branch, down_sum, second_sum, norm_gains, out_biases, all_a, mixed, probs, normed, att,
         rel_hi, rel_lo, pick, spread),
        [((t, width), BF), ((t, width), F32), ((t, width), BF), ((128, SIDE), F32), ((6, ROWS, SIDE), BF),
         ((8, ROWS, SIDE), BF), ((8, ROWS, SIDE), BF), ((4, width), F32), ((6, SIDE), F32)],
        [((6, 8 * SIDE, SIDE), BF), ((8, 2 * SIDE, SIDE), BF), ((64, SIDE, 32), BF), ((8, ROWS, SIDE), F32),
         ((2, ROWS, SIDE), BF)],
        "mid_back")
    rel_half = SIDE // 2
    rel_fold = rel_part[:64] + rel_part[64:]
    rel_fold = (rel_fold[:, :rel_half] + rel_fold[:, rel_half:]).reshape(2, 32, rel_half)[:, : rel_pos.shape[1]]
    rel_size = rel_fold.size
    rel_rows = -(-rel_size // width)
    rel_flat = jnp.pad(rel_fold.reshape(-1).astype(BF), (0, rel_rows * width - rel_size)).reshape(rel_rows, width)
    both_sum = lax.psum(jnp.concatenate([part_normed, rel_flat], axis=0), "mp")

    sum_a, *lower = scatter_call(
        scatter_attn_body, 10, (xa, ya), (nb, att, gm, gb, sum_m, sq_left_m, sq_right_m, mlp_master[0], mlp_first[0], mlp_second[0]),
        soap_outs(),
        [((10, ROWS, SIDE), BF), ((14, ROWS, SIDE), BF), ((40, SIDE, 128), BF)] + [((2, 8, SIDE, 128), F32)] * 2, 4, 150_000_000, "scatter_attn")
    both_sum, sum_a = lax.optimization_barrier((both_sum, sum_a))
    normed_sum, rel_sum = both_sum[:t], both_sum[t:].reshape(-1)[:rel_size].astype(F32)
    tokens_grad, sums_one = call(
        token_back_body, (), (tok, live[:t], normed_sum, grad_middle, norm_gains),
        [((t, width), F32), ((2, width), F32)], [], "token_back")
    small = [sums_one.reshape(-1), sums_two.reshape(-1), qkv_sums.reshape(-1), up_sums.reshape(-1), rel_sum]
    edges = np.cumsum([0] + [v.shape[0] for v in small])
    lines = -(-int(edges[-1]) // 1024) * 8
    small = jnp.pad(jnp.concatenate(small), (0, lines * 128 - int(edges[-1]))).reshape(1, lines, 128)
    mg, mn, mc, mf, ms = [jnp.concatenate(pair, axis=0) for pair in zip(upper, lower)]
    gathered, ag, an, ac, af, as_ = gather(
        small, 3, "gather_sums", 1, functools.partial(soap_units, 0, 0),
        (sum_a, sq_left_a, sq_right_a, attn_master[0], attn_first[0], attn_second[0]),
        soap_outs(), [((2, 8, SIDE, 128), F32)] * 2)
    total = jnp.sum(gathered, axis=0).reshape(-1)
    one, two, qkv_grad, up_grad, rel_grad = [total[edges[i]:edges[i + 1]] for i in range(5)]
    one, two = one.reshape(2, width), two.reshape(4, width)
    gains_grad = jnp.stack([one[0], two[0]])
    biases_grad = jnp.stack([one[1], two[1]])
    outb_grad = jnp.stack([two[3], two[2]])
    rel_grad = rel_grad.reshape(rel_pos.shape)

    return (block_out[None], tokens_grad[None], gains_grad, biases_grad, outb_grad, qkv_grad, up_grad, rel_grad,
            *(value[None] for value in (ag, mg, an, mn, ac, mc, af, as_, mf, ms)))


def solution(mesh):
    return build(mesh)
```
